32 devices in a mesh: ctx: 8 (over y, x, core), fsdp: 4 (over z).
Axes of the slice: x: 2, y: 2, z: 4, core: 2. Of those that a mesh axis runs over, the one named last changes fastest.
Arguments:
- tokens: bfloat16 [4, 2048, 1024], P('fsdp', 'ctx'), may hold values from -6 to 6
- cotangent: bfloat16 [4, 2048, 1024], P('fsdp', 'ctx'), may hold values from -6 to 6
- block_map: int32 [4, 16], P('fsdp'), may hold values from 0 to 15, as said below
- attn_gain: bfloat16 [1024], P(('ctx', 'fsdp')), may hold values from 0.5 to 1.5
- query_weight: bfloat16 [1024, 2048], P(('ctx', 'fsdp')), may hold values from -0.1875 to 0.1875
- key_weight: bfloat16 [1024, 1024], P(('ctx', 'fsdp')), may hold values from -0.1875 to 0.1875
- value_weight: bfloat16 [1024, 1024], P(('ctx', 'fsdp')), may hold values from -0.1875 to 0.1875
- query_gain: bfloat16 [128], P(('ctx', 'fsdp')), may hold values from 0.5 to 1.5
- key_gain: bfloat16 [128], P(('ctx', 'fsdp')), may hold values from 0.5 to 1.5
- output_weight: bfloat16 [2048, 1024], P(('ctx', 'fsdp')), may hold values from -4 to 4
- mlp_gain: bfloat16 [1024], P(('ctx', 'fsdp')), may hold values from 0.5 to 1.5
- gate_weight: bfloat16 [1024, 3072], P(('ctx', 'fsdp')), may hold values from -0.1875 to 0.1875
- up_weight: bfloat16 [1024, 3072], P(('ctx', 'fsdp')), may hold values from -0.1875 to 0.1875
- down_weight: bfloat16 [3072, 1024], P(('ctx', 'fsdp')), may hold values from -0.109375 to 0.109375
Outputs:
- output: bfloat16 [4, 2048, 1024], P('fsdp', 'ctx')
- grad_tokens: bfloat16 [4, 2048, 1024], P('fsdp', 'ctx')
- grad_attn_gain: float32 [1024], P(('ctx', 'fsdp'))
- grad_query_weight: float32 [1024, 2048], P(('ctx', 'fsdp'))
- grad_key_weight: float32 [1024, 1024], P(('ctx', 'fsdp'))
- grad_value_weight: float32 [1024, 1024], P(('ctx', 'fsdp'))
- grad_query_gain: float32 [128], P(('ctx', 'fsdp'))
- grad_key_gain: float32 [128], P(('ctx', 'fsdp'))
- grad_output_weight: float32 [2048, 1024], P(('ctx', 'fsdp'))
- grad_mlp_gain: float32 [1024], P(('ctx', 'fsdp'))
- grad_gate_weight: float32 [1024, 3072], P(('ctx', 'fsdp'))
- up_projection_gradient: float32 [1024, 3072], P(('ctx', 'fsdp'))
- grad_down_weight: float32 [3072, 1024], P(('ctx', 'fsdp'))
The draws below stay inside these ranges and needn't reach their ends.
Inputs may be any that keep to these rules, and one draw needn't show every extreme that they name: Each row of block_map holds every block number of its sequence once, and the two slots 2c and 2c + 1 of one index c of ctx hold blocks b and 15 - b.
All inputs are finite; a program needn't handle non-finite values.
Results may differ from the reference program's by a relative error of at most 0.018.
Values may be sent and summed in bfloat16 or wider, within the bound.
A program may use at most 256 MiB of HBM per device.

```python
import math
import jax
import jax.numpy as jnp
from jax import lax

D = 1024
H = 16
KVH = 8
HD = 128
FF = 3072
BLK = 128
NBLK = 16
LEN = 2048
SEQS = 4


def draw_block_map(key, part):
    half = NBLK // 2
    seq_keys = jax.random.split(jax.random.fold_in(key, 11), SEQS)
    orders = jax.vmap(lambda single: jax.random.permutation(single, half))(seq_keys)
    flips = jax.random.randint(jax.random.fold_in(key, 23), (SEQS, half), 0, 2)
    first = jnp.where(flips == 1, NBLK - 1 - orders, orders)
    second = NBLK - 1 - first
    return jnp.stack([first, second], axis=-1).reshape(SEQS, NBLK).astype(jnp.int32)


def level_of(stream_key, shape, shards, low, largest):
    def one(position, shards_of):
        steps = jax.random.uniform(jax.random.fold_in(jax.random.fold_in(stream_key, 6), position), (shards_of,), jnp.float32, low / len(shards), largest / len(shards))
        return jnp.repeat(jnp.exp(steps), shape[position] // shards_of).reshape((-1,) + (1,) * (len(shape) - position - 1))

    loudness = one(*shards[0])
    for cut in shards[1:]:
        loudness = loudness * one(*cut)
    return loudness


def scatter_about(key, extent, spread, limit, pieces=(), held_as=jnp.bfloat16):
    level = level_of(key, extent, pieces, -0.22, 0.18) if pieces else 1.0
    values = jax.random.normal(key, extent, jnp.float32) * spread * level
    return jnp.minimum(jnp.maximum(values, -limit), limit).astype(held_as)


def setup_inputs(seed: int = 0) -> dict:
    arg_keys = jax.random.split(jax.random.key(seed), 15)
    tokens = scatter_about(arg_keys[0], (SEQS, LEN, D), 1.0, 6.0, ((0, 4), (1, 8)))
    cotangent = scatter_about(arg_keys[1], (SEQS, LEN, D), 1.0, 6.0, ((0, 4), (1, 8)))
    block_map = draw_block_map(jax.random.fold_in(arg_keys[14], 71), 0)
    attn_gain = jnp.clip(1.0 + 0.1 * jax.random.normal(arg_keys[3], (D,), jnp.float32), 0.5, 1.5).astype(jnp.bfloat16)
    query_weight = scatter_about(arg_keys[4], (D, H * HD), D ** -0.5, 0.1875, ((0, 32),))
    key_weight = scatter_about(arg_keys[5], (D, KVH * HD), D ** -0.5, 0.1875, ((0, 32),))
    value_weight = scatter_about(arg_keys[6], (D, KVH * HD), D ** -0.5, 0.1875, ((0, 32),))
    query_gain = jnp.clip(1.0 + 0.1 * jax.random.normal(arg_keys[7], (HD,), jnp.float32), 0.5, 1.5).astype(jnp.bfloat16)
    key_gain = jnp.clip(1.0 + 0.1 * jax.random.normal(arg_keys[8], (HD,), jnp.float32), 0.5, 1.5).astype(jnp.bfloat16)
    output_weight = scatter_about(arg_keys[9], (H * HD, D), (max(1, 2 * H * HD // LEN)) ** -0.5, 4.0, ((0, 32),))
    mlp_gain = jnp.clip(1.0 + 0.1 * jax.random.normal(arg_keys[10], (D,), jnp.float32), 0.5, 1.5).astype(jnp.bfloat16)
    gate_weight = scatter_about(arg_keys[11], (D, FF), D ** -0.5, 0.1875, ((0, 32),))
    up_weight = scatter_about(arg_keys[12], (D, FF), D ** -0.5, 0.1875, ((0, 32),))
    down_weight = scatter_about(arg_keys[13], (FF, D), FF ** -0.5, 0.109375, ((0, 32),))
    return dict(tokens=tokens, cotangent=cotangent, block_map=block_map, attn_gain=attn_gain, query_weight=query_weight, key_weight=key_weight, value_weight=value_weight, query_gain=query_gain, key_gain=key_gain, output_weight=output_weight, mlp_gain=mlp_gain, gate_weight=gate_weight, up_weight=up_weight, down_weight=down_weight)


EPSILON = 1e-06
ROPE_BASE = 1000000.0
HIGHEST = lax.Precision.HIGHEST

@jax.custom_vjp
def low(v):
    return lax.optimization_barrier(v.astype(jnp.bfloat16)).astype(jnp.float32)

@jax.custom_vjp
def low_back(v):
    return v

def low_keep(v):
    return (low(v), None)

def low_pass(kept, grad):
    return (grad,)

def back_keep(v):
    return (v, None)

def back_low(kept, grad):
    return (low(grad),)
low.defvjp(low_keep, low_pass)
low_back.defvjp(back_keep, back_low)

def matmul(left, right):
    return jnp.dot(left, right, precision=HIGHEST)

def rms_scale(value_vectors):
    return value_vectors * lax.rsqrt(lax.optimization_barrier(jnp.mean(value_vectors * value_vectors, axis=-1, keepdims=True)) + EPSILON)

def rope_tables(positions):
    half = HD // 2
    freqs = jnp.exp(jnp.arange(half, dtype=jnp.float32) * (-2.0 * math.log(ROPE_BASE) / HD))
    angles = positions.astype(jnp.float32)[..., None] * freqs
    cosine = jnp.cos(angles)
    sine = jnp.sin(angles)
    return (jnp.concatenate([cosine, cosine], axis=-1), jnp.concatenate([sine, sine], axis=-1))

def rotate(value_vectors):
    half = value_vectors.shape[-1] // 2
    return jnp.concatenate([-value_vectors[..., half:], value_vectors[..., :half]], axis=-1)

def attention(queries, keys, value_vectors, positions):
    rows = min(512, LEN)
    count = LEN // rows
    grouped = queries.reshape(count, rows, KVH, H // KVH, HD)
    spots = positions.reshape(count, rows)

    def one_block(pair):
        block_queries, block_positions = pair
        scores = jnp.einsum('qkrd,tkd->krqt', block_queries, keys, precision=HIGHEST) * HD ** (-0.5)
        scores = low_back(scores)
        allowed = positions[None, :] <= block_positions[:, None]
        weights = jnp.where(allowed, jnp.exp(scores), 0.0)
        totals = lax.optimization_barrier(jnp.sum(weights, axis=-1))
        summed = low_back(jnp.einsum('krqt,tkd->qkrd', low(weights), value_vectors, precision=HIGHEST))
        return (summed / jnp.transpose(totals, (2, 0, 1))[..., None]).reshape(rows, H * HD)
    return lax.map(jax.checkpoint(one_block), (grouped, spots)).reshape(LEN, H * HD)

def layer_sequence(inputs, blocks, params):
    attn_gain, query_weight, key_weight, value_weight, query_gain, key_gain, output_weight, mlp_gain, gate_weight, up_weight, down_weight = params
    positions = (blocks[:, None] * BLK + jnp.arange(BLK, dtype=jnp.int32)[None, :]).reshape(LEN)
    cosine, sine = rope_tables(positions)
    cosine = cosine[:, None, :]
    sine = sine[:, None, :]
    normed = low(rms_scale(inputs) * attn_gain)
    queries = low_back(matmul(normed, query_weight)).reshape(LEN, H, HD)
    keys = low_back(matmul(normed, key_weight)).reshape(LEN, KVH, HD)
    value_vectors = low(low_back(matmul(normed, value_weight))).reshape(LEN, KVH, HD)
    queries = rms_scale(queries) * query_gain
    queries = low(queries * cosine + rotate(queries) * sine)
    keys = rms_scale(keys) * key_gain
    keys = low(keys * cosine + rotate(keys) * sine)
    attended = attention(queries, keys, value_vectors, positions)
    branch = low_back(matmul(low(attended), output_weight))
    middle = inputs + branch
    normed_two = low(rms_scale(middle) * mlp_gain)
    gate = low_back(matmul(normed_two, gate_weight))
    upper = low_back(matmul(normed_two, up_weight))
    hidden = low(jax.nn.silu(gate) * upper)
    return middle + matmul(hidden, down_weight)

def reference(tokens, cotangent, block_map, attn_gain, query_weight, key_weight, value_weight, query_gain, key_gain, output_weight, mlp_gain, gate_weight, up_weight, down_weight):
    params = (attn_gain.astype(jnp.float32), query_weight.astype(jnp.float32), key_weight.astype(jnp.float32), value_weight.astype(jnp.float32), query_gain.astype(jnp.float32), key_gain.astype(jnp.float32), output_weight.astype(jnp.float32), mlp_gain.astype(jnp.float32), gate_weight.astype(jnp.float32), up_weight.astype(jnp.float32), down_weight.astype(jnp.float32))

    def whole(inputs, weights):

        def advance(carry, pair):
            return (carry, jax.checkpoint(layer_sequence)(pair[0], pair[1], weights))
        unused, outputs = lax.scan(advance, jnp.zeros((), jnp.float32), (inputs, block_map))
        return outputs
    outputs, pullback = jax.vjp(whole, tokens.astype(jnp.float32), params)
    grad_inputs, grads = pullback(cotangent.astype(jnp.float32))
    grad_attn, grad_query, grad_key, grad_value, grad_qgain, grad_kgain, grad_output, grad_mlp, grad_gate, grad_upper, grad_down = grads
    return (outputs.astype(jnp.bfloat16), grad_inputs.astype(jnp.bfloat16), grad_attn, grad_query, grad_key, grad_value, grad_qgain, grad_kgain, grad_output, grad_mlp, grad_gate, grad_upper, grad_down)
```

```python
import functools
import math

import jax
import jax.numpy as jnp
from jax import lax
from jax.experimental import pallas as pl
from jax.experimental.pallas import tpu as pltpu
from jax.sharding import PartitionSpec as P

MESH = pl.DeviceIdType.MESH
ANY = pl.BlockSpec(memory_space=pl.ANY)


H = 16
KVH = 8
HD = 128
BLK = 128


EPSILON = 1e-06
ROPE_BASE = 1000000.0


def rope_tables(positions):
    half = HD // 2
    freqs = jnp.exp(jnp.arange(half, dtype=jnp.float32) * (-2.0 * math.log(ROPE_BASE) / HD))
    angles = positions.astype(jnp.float32)[..., None] * freqs
    cosine = jnp.cos(angles)
    sine = jnp.sin(angles)
    return (jnp.concatenate([cosine, cosine], axis=-1), jnp.concatenate([sine, sine], axis=-1))


def rotate(value_vectors):
    half = value_vectors.shape[-1] // 2
    return jnp.concatenate([-value_vectors[..., half:], value_vectors[..., :half]], axis=-1)


def unrotate(value_vectors):
    half = value_vectors.shape[-1] // 2
    return jnp.concatenate([value_vectors[..., half:], -value_vectors[..., :half]], axis=-1)


def left_dot(left, right):
    return lax.dot_general(
        left, right, (((0,), (0,)), ((), ())), preferred_element_type=jnp.float32
    )


def right_dot(left, right):
    return lax.dot_general(
        left, right, (((1,), (1,)), ((), ())), preferred_element_type=jnp.float32
    )


def plain_dot(left, right):
    return jnp.dot(left, right, preferred_element_type=jnp.float32)


def norm_back(grad_normed, unit, inverse, gain):
    scaled = grad_normed * gain
    return inverse * (scaled - unit * jnp.mean(scaled * unit, axis=-1, keepdims=True))


class Grid:
    def __init__(self, ctx, fsdp):
        self.sizes = {"a": ctx // 4, "b": 2, "core": 2, "f": fsdp}
        self.stride = {"a": 4, "b": 2, "core": 1}

    def enter(self):
        self.c = lax.axis_index("ctx")
        self.at = {
            "a": self.c // 4,
            "b": (self.c // 2) % 2,
            "core": self.c % 2,
            "f": lax.axis_index("fsdp"),
        }

    def peer(self, axis, place):
        if axis == "f":
            return {"fsdp": place}
        return {"ctx": self.c + (place - self.at[axis]) * self.stride[axis]}

    def sources(self, axis):
        n, p = self.sizes[axis], self.at[axis]
        if n == 2:
            return [(None, 1 - p, None, None)]
        found = []
        for step in range(1, n):
            for way in (1, -1):
                origin = p - way * step
                onward = p + way
                found.append(
                    (
                        jnp.logical_and(origin >= 0, origin < n),
                        origin,
                        onward,
                        jnp.logical_and(
                            jnp.logical_and(origin >= 0, origin < n),
                            jnp.logical_and(onward >= 0, onward < n),
                        ),
                    )
                )
        return found

    def around(self, axis):
        n, p = self.sizes[axis], self.at[axis]
        if n == 2:
            return [(None, 1 - p)]
        return [(p + 1 < n, p + 1), (p >= 1, p - 1)]

    def nearest(self, axis):
        n, p = self.sizes[axis], self.at[axis]
        if n == 2:
            return [p, 1 - p]
        order = [0]
        for step in range(1, n):
            for way in (step, n - step):
                if way not in order:
                    order.append(way)
        return [lax.rem(p + s, n) for s in order]


class Pool:
    def __init__(self, ref):
        self.ref, self.used = ref, 0

    def take(self, count):
        first = self.used
        self.used += count
        return self.ref.at[pl.ds(first, count)]


def guarded(cond, body):
    if cond is None:
        body()
    else:
        pl.when(cond)(body)


class Gather:
    def __init__(self, grid, order, src, dst, columns, send_sem, recv_sem, layout_axes):
        self.grid, self.order, self.src, self.dst = grid, order, src, dst
        self.columns, self.send_sem, self.recv_sem = columns, send_sem, recv_sem
        self.layout_axes = layout_axes
        self.sends = 0
        self.pending = []

    @staticmethod
    def semaphores(grid, order):
        near = {x: 1 if grid.sizes[x] == 2 else 2 for x in order}
        far = {x: 0 if grid.sizes[x] == 2 else 2 * (grid.sizes[x] - 1) for x in order}
        sends = near[order[0]] + far[order[0]] + sum(near[x] for x in order[1:])
        inner = 1
        for level in range(1, len(order)):
            axis = order[level]
            onward = sum(near[x] for x in order[level + 1 :])
            sends += inner * (far[axis] + max(far[axis], 1) * onward)
            inner *= grid.sizes[axis]
        return sends, grid.sizes[order[0]] + inner

    def view(self, places):
        idx = tuple(places.get(x, slice(None)) for x in self.layout_axes)
        return self.dst.at[idx + (slice(None), self.columns)]

    def unit_number(self, places):
        number = 0
        for x in self.order[1:]:
            number = number * self.grid.sizes[x] + places[x]
        return number

    def start(self, cond, view, axis, place, sem):
        slot = self.sends
        self.sends += 1

        def make():
            return pltpu.make_async_remote_copy(
                src_ref=view[0],
                dst_ref=view[1],
                send_sem=self.send_sem.at[slot],
                recv_sem=self.recv_sem.at[sem],
                device_id=self.grid.peer(axis, place),
                device_id_type=MESH,
            )

        guarded(cond, lambda: make().start())
        self.pending.append((cond, make))

    def wait_recv(self, view, sem):
        pltpu.make_async_remote_copy(
            src_ref=view,
            dst_ref=view,
            send_sem=self.send_sem.at[0],
            recv_sem=self.recv_sem.at[sem],
            device_id={},
            device_id_type=MESH,
        ).wait_recv()

    def own_places(self):
        return {x: self.grid.at[x] for x in self.order}

    def open(self):
        axis = self.order[0]
        own = self.view(self.own_places())
        src = self.src.at[:, self.columns]
        for cond, place in self.grid.around(axis):
            self.start(cond, (src, own), axis, place, self.grid.at[axis])

    def first(self):
        axis = self.order[0]
        for cond, origin, onward, more in self.grid.sources(axis):
            view = self.view({**self.own_places(), axis: origin})
            guarded(cond, lambda: self.wait_recv(view, origin))
            if onward is not None:
                self.start(more, (view, view), axis, onward, origin)
        self.pass_on(None, 1, {x: self.grid.at[x] for x in self.order[1:]})

    def pass_on(self, cond, level, places):
        n1 = self.grid.sizes[self.order[0]]
        sem = n1 + self.unit_number(places)
        view = self.view(places)
        for axis in self.order[level:]:
            for near, place in self.grid.around(axis):
                both = near if cond is None else cond if near is None else jnp.logical_and(cond, near)
                self.start(both, (view, view), axis, place, sem)

    def arrivals(self, level):
        n1 = self.grid.sizes[self.order[0]]
        axis = self.order[level]
        inner = [{}]
        for x in self.order[1:level]:
            inner = [{**places, x: j} for places in inner for j in self.grid.nearest(x)]
        fixed = {x: self.grid.at[x] for x in self.order[level + 1 :]}
        for places in inner:
            for cond, origin, onward, more in self.grid.sources(axis):
                unit = {**places, **fixed, axis: origin}
                view = self.view(unit)
                sem = n1 + self.unit_number(unit)
                guarded(cond, lambda: self.wait_recv(view, sem))
                if onward is not None:
                    self.start(more, (view, view), axis, onward, sem)
                self.pass_on(cond, level + 1, unit)

    def close(self):
        for cond, make in self.pending:
            guarded(cond, lambda: make().wait_send())


def add_into(total, term, out=None):
    shape = total.shape
    rows = min(16, shape[-2])
    steps = shape[-2] // rows
    lead = math.prod(shape[:-2])

    def body(i, carry):
        index = ()
        rest = i // steps
        for n in reversed(shape[:-2]):
            index = (lax.rem(rest, n),) + index
            rest = rest // n
        at = index + (pl.ds(pl.multiple_of(lax.rem(i, steps) * rows, rows), rows), slice(None))
        value = total[at].astype(jnp.float32)
        if term is not None:
            value = value + term[at].astype(jnp.float32)
        if out is None:
            total[at] = value.astype(total.dtype)
        else:
            out[at] = value.astype(out.dtype)
        return carry

    lax.fori_loop(0, lead * steps, body, 0)


class Scatter:
    def __init__(self, grid, order, src, columns, own, recvs, load_sem, send_sem, recv_sem, out, layout_axes):
        self.grid, self.order, self.src, self.columns = grid, order, src, columns
        self.own, self.recvs, self.out = own, recvs, out
        self.load_sem, self.send_sem, self.recv_sem = load_sem, send_sem, recv_sem
        self.layout_axes = layout_axes
        self.sends = 0
        self.pending = []
        self.base = {}
        number = 0
        for level in range(len(order) - 1, -1, -1):
            self.base[level] = number
            number += self.slots(grid, order, level)

    @staticmethod
    def inner(grid, order, level):
        return [grid.sizes[x] for x in order[1:level]]

    @staticmethod
    def slots(grid, order, level):
        n = grid.sizes[order[level]]
        lines = 1 if n == 2 else 2 * n
        return lines * math.prod(Scatter.inner(grid, order, level))

    @staticmethod
    def scratch(grid, order, rows, columns, dtype):
        n1 = grid.sizes[order[0]]
        own = tuple(grid.sizes[x] for x in order[1:-1]) + (n1, rows, columns)
        recvs = []
        for level in range(len(order)):
            n = grid.sizes[order[level]]
            lead = () if n == 2 else (2, n)
            block = (rows, columns) if level == 0 else (n1, rows, columns)
            recvs.append(lead + tuple(Scatter.inner(grid, order, level)) + block)
        return [pltpu.VMEM(s, dtype) for s in [own] + recvs]

    @staticmethod
    def semaphores(grid, order):
        loads = math.prod(grid.sizes[x] for x in order[1:-1])
        slots = [Scatter.slots(grid, order, level) for level in range(len(order))]
        sends = [
            (1 if grid.sizes[x] == 2 else 2 * (grid.sizes[x] - 1))
            * math.prod(Scatter.inner(grid, order, level))
            for level, x in enumerate(order)
        ]
        return loads, sum(sends), sum(slots)

    def hbm(self, places):
        idx = tuple(places.get(x, slice(None)) for x in self.layout_axes)
        return self.src.at[idx + (slice(None), self.columns)]

    def units(self, level, first=None):
        found = [{}]
        for x in self.order[1:level]:
            found = [{**places, x: j} for places in found for j in reversed(self.grid.nearest(x))]
        return found

    def mine(self, places):
        idx = tuple(places.get(x, self.grid.at[x]) for x in self.order[1:-1])
        return self.own.at[idx]

    def number(self, places, axes):
        value = 0
        for x in axes:
            value = value * self.grid.sizes[x] + places[x]
        return value

    def slot(self, level, places, way=None, target=None):
        axes = self.order[1:level]
        idx = tuple(places[x] for x in axes)
        inner = math.prod(self.grid.sizes[x] for x in axes)
        number = self.number(places, axes)
        if way is not None:
            idx = (way, target) + idx
            number = (way * self.grid.sizes[self.order[level]] + target) * inner + number
        ref = self.recvs[level]
        return (ref.at[idx] if idx else ref), self.recv_sem.at[self.base[level] + number]

    def send(self, cond, view, landing, axis, place):
        slot = self.sends
        self.sends += 1
        ref, sem = landing

        def make():
            return pltpu.make_async_remote_copy(
                src_ref=view,
                dst_ref=ref,
                send_sem=self.send_sem.at[slot],
                recv_sem=sem,
                device_id=self.grid.peer(axis, place),
                device_id_type=MESH,
            )

        guarded(cond, lambda: make().start())
        self.pending.append((cond, make))

    def take(self, cond, landing, total, out=None):
        ref, sem = landing

        def body():
            pltpu.make_async_remote_copy(
                src_ref=ref,
                dst_ref=ref,
                send_sem=self.send_sem.at[0],
                recv_sem=sem,
                device_id={},
                device_id_type=MESH,
            ).wait_recv()
            add_into(total, ref, out)

        guarded(cond, body)

    def load(self, places):
        axes = self.order[1:-1]
        here = {**places, self.order[-1]: self.grid.at[self.order[-1]]}
        return pltpu.make_async_copy(
            self.hbm(here), self.mine(places), self.load_sem.at[self.number(places, axes)]
        )

    def open(self):
        top = len(self.order) - 1
        axis = self.order[top]
        there = 1 - self.grid.at[axis]
        for places in self.units(top):
            self.send(None, self.hbm({**places, axis: there}), self.slot(top, places), axis, there)
            self.load(places).start()

    def settle(self, level, places):
        above = level + 1
        top = len(self.order) - 1
        total = self.mine(places)
        if above == top:
            self.load(places).wait()
            self.take(None, self.slot(above, places), total)
            return
        axis = self.order[above]
        n, p = self.grid.sizes[axis], self.grid.at[axis]
        if n == 2:
            self.take(None, self.slot(above, places), total)
        else:
            self.take(p >= 1, self.slot(above, places, 0, p), total)
            self.take(p + 1 < n, self.slot(above, places, 1, p), total)

    def step(self, level):
        axis = self.order[level]
        n, p = self.grid.sizes[axis], self.grid.at[axis]
        if level == 0:
            self.settle(0, {})
            whole = self.mine({})
            self.along(level, {}, lambda t: whole.at[t])
            return
        for places in self.units(level):
            self.along(level, places, lambda t: self.mine({**places, axis: t}))
            self.settle(level, {**places, axis: p})

    def along(self, level, places, view):
        axis = self.order[level]
        n, p = self.grid.sizes[axis], self.grid.at[axis]
        if n == 2:
            if level:
                self.settle(level, {**places, axis: 1 - p})
            self.send(None, view(1 - p), self.slot(level, places), axis, 1 - p)
            return
        for s in range(n - 1):
            for way, t in ((0, n - 1 - s), (1, s)):
                wanted = (t > p) if way == 0 else (t < p)
                behind = (p >= 1) if way == 0 else (p + 1 < n)
                if level:
                    pl.when(wanted)(lambda: self.settle(level, {**places, axis: t}))
                self.take(jnp.logical_and(wanted, behind), self.slot(level, places, way, t), view(t))
                self.send(wanted, view(t), self.slot(level, places, way, t), axis, p + (1 if way == 0 else -1))

    def finish(self):
        axis = self.order[0]
        n, p = self.grid.sizes[axis], self.grid.at[axis]
        total = self.mine({}).at[p]
        if n == 2:
            self.take(None, self.slot(0, {}), total, self.out)
            return
        self.take(p >= 1, self.slot(0, {}, 0, p), total)
        self.take(p + 1 < n, self.slot(0, {}, 1, p), total)
        add_into(total, None, self.out)

    def close(self):
        for cond, make in self.pending:
            guarded(cond, lambda: make().wait_send())


def half_pairs(ref, s):
    rows = pl.ds(s * BLK, BLK)
    return jnp.concatenate([ref[rows, :HD], ref[rows, HD:]], axis=0)


def items(table, pairs):
    high_slot, high = table[pairs * 2], table[pairs * 2 + 1]
    low_block = 2 * pairs - 1 - high
    split = high // 2
    found = []
    for w in range(pairs - 1):
        upper = w < split
        found.append((jnp.where(upper, high_slot, 1 - high_slot), jnp.where(upper, w, w - split), None))
    found.append((high_slot, split, high))
    found.append((1 - high_slot, low_block // 2, low_block))
    return found


def chunk_of(ref, table, c):
    return jnp.concatenate(
        [ref[pl.ds(pl.multiple_of(table[2 * c + i] * BLK, BLK), BLK), :] for i in range(2)], axis=0
    )


def row_contract(left, right):
    return lax.dot_general(left, right, (((1,), (1,)), ((), ())), preferred_element_type=jnp.float32)


def attention_kernel(pairs, table, q_ref, k_ref, v_ref, o_ref, low_ref, t_ref, qs, acc, tot):
    for s in range(2):
        qs[s] = half_pairs(q_ref, s)
    acc[...] = jnp.zeros_like(acc)
    tot[...] = jnp.zeros_like(tot)
    for s, c, block in items(table, pairs):
        keys = chunk_of(k_ref, table, c)
        vals = chunk_of(v_ref, table, c)
        scores = row_contract(qs[s], keys) * (HD ** (-0.5) * math.log2(math.e))
        weights = jnp.exp2(scores)
        if block is not None:
            rows = lax.broadcasted_iota(jnp.int32, (2 * BLK, 2 * BLK), 0)
            cols = lax.broadcasted_iota(jnp.int32, (2 * BLK, 2 * BLK), 1)
            allowed = cols <= lax.rem(rows, BLK) + (block - 2 * c) * BLK
            weights = jnp.where(allowed, weights, 0.0)
        tot[s] += weights[:, :HD] + weights[:, HD:]
        acc[s] += jnp.dot(weights.astype(jnp.bfloat16), vals, preferred_element_type=jnp.float32)
    for s in range(2):
        total = tot[s]
        value = acc[s] / jnp.sum(total, axis=1, keepdims=True)
        rows = pl.ds(s * BLK, BLK)
        for i in range(2):
            part = value[i * BLK : (i + 1) * BLK]
            o_ref[rows, i * HD : (i + 1) * HD] = part
            low_ref[rows, i * HD : (i + 1) * HD] = part.astype(jnp.bfloat16)
        t_ref[0, s : s + 1, :] = jnp.sum(total.T, axis=0, keepdims=True)


def attention(table, pairs, queries, keys, values):
    rows, length = queries.shape[0], keys.shape[0]
    head = pl.BlockSpec((rows, 2 * HD), lambda h, t: (0, h))
    side = pl.BlockSpec((length, HD), lambda h, t: (0, h))
    stats = pl.BlockSpec((1, 2, 2 * BLK), lambda h, t: (h, 0, 0))
    return pl.pallas_call(
        functools.partial(attention_kernel, pairs),
        grid_spec=pltpu.PrefetchScalarGridSpec(
            num_scalar_prefetch=1,
            grid=(KVH,),
            in_specs=[head, side, side],
            out_specs=[head, head, stats],
            scratch_shapes=[
                pltpu.VMEM((2, 2 * BLK, HD), jnp.bfloat16),
                pltpu.VMEM((2, 2 * BLK, HD), jnp.float32),
                pltpu.VMEM((2, 2 * BLK, HD), jnp.float32),
            ],
        ),
        out_shape=[
            jax.ShapeDtypeStruct((rows, H * HD), jnp.float32),
            jax.ShapeDtypeStruct((rows, H * HD), jnp.bfloat16),
            jax.ShapeDtypeStruct((KVH, 2, 2 * BLK), jnp.float32),
        ],
        name="attention",
    )(table, queries, keys, values)


def attention_back_kernel(
    pairs, table, q_ref, k_ref, v_ref, g_ref, d_ref, dq_ref, dk_ref, dv_ref, qs, gs, dq, dk, dv
):
    scale = HD ** (-0.5)
    for s in range(2):
        qs[s] = half_pairs(q_ref, s)
        gs[s] = half_pairs(g_ref, s)
    for total in (dq, dk, dv):
        total[...] = jnp.zeros_like(total)
    for s, c, block in items(table, pairs):
        keys = chunk_of(k_ref, table, c)
        vals = chunk_of(v_ref, table, c)
        queries, grads = qs[s], gs[s]
        weights = jnp.exp2(row_contract(keys, queries) * (scale * math.log2(math.e)))
        if block is not None:
            rows = lax.broadcasted_iota(jnp.int32, (2 * BLK, 2 * BLK), 0)
            cols = lax.broadcasted_iota(jnp.int32, (2 * BLK, 2 * BLK), 1)
            allowed = rows <= lax.rem(cols, BLK) + (block - 2 * c) * BLK
            weights = jnp.where(allowed, weights, 0.0)
        through = row_contract(vals, grads)
        scores = (weights * (through - d_ref[0, pl.ds(s, 1), :])).astype(jnp.bfloat16)
        to_values = jnp.dot(weights.astype(jnp.bfloat16), grads, preferred_element_type=jnp.float32)
        to_keys = jnp.dot(scores, queries, preferred_element_type=jnp.float32)
        for i in range(2):
            at = pl.ds(pl.multiple_of(table[2 * c + i] * BLK, BLK), BLK)
            dv[at, :] += to_values[i * BLK : (i + 1) * BLK]
            dk[at, :] += to_keys[i * BLK : (i + 1) * BLK]
        dq[s] += left_dot(scores, keys)
    dk_ref[...] = (dk[...] * scale).astype(jnp.bfloat16)
    dv_ref[...] = dv[...].astype(jnp.bfloat16)
    for s in range(2):
        for i in range(2):
            dq_ref[pl.ds(s * BLK, BLK), i * HD : (i + 1) * HD] = dq[s, i * BLK : (i + 1) * BLK] * scale


def attention_back(table, pairs, queries, keys, values, grads, drift):
    rows, length = queries.shape[0], keys.shape[0]
    head = pl.BlockSpec((rows, 2 * HD), lambda h, t: (0, h))
    side = pl.BlockSpec((length, HD), lambda h, t: (0, h))
    stats = pl.BlockSpec((1, 2, 2 * BLK), lambda h, t: (h, 0, 0))
    return pl.pallas_call(
        functools.partial(attention_back_kernel, pairs),
        grid_spec=pltpu.PrefetchScalarGridSpec(
            num_scalar_prefetch=1,
            grid=(KVH,),
            in_specs=[head, side, side, head, stats],
            out_specs=[head, side, side],
            scratch_shapes=[
                pltpu.VMEM((2, 2 * BLK, HD), jnp.bfloat16),
                pltpu.VMEM((2, 2 * BLK, HD), jnp.bfloat16),
                pltpu.VMEM((2, 2 * BLK, HD), jnp.float32),
                pltpu.VMEM((length, HD), jnp.float32),
                pltpu.VMEM((length, HD), jnp.float32),
            ],
        ),
        out_shape=[
            jax.ShapeDtypeStruct((rows, H * HD), jnp.float32),
            jax.ShapeDtypeStruct((length, KVH * HD), jnp.bfloat16),
            jax.ShapeDtypeStruct((length, KVH * HD), jnp.bfloat16),
        ],
        name="attention_back",
    )(table, queries, keys, values, grads, drift)


ALL_AXES = ("a", "b", "core", "f")
SLOT_AXES = ("a", "b", "core")
BFA, AFB = ("b", "f", "a", "core"), ("a", "f", "b", "core")
FAB, FBA = ("f", "a", "b", "core"), ("f", "b", "a", "core")
AB, BA = ("a", "b", "core"), ("b", "a", "core")


def gather_kernel(grid, portions, layout, n, *refs):
    srcs, dsts, held = refs[:n], refs[n : 2 * n], refs[2 * n : 3 * n]
    send, recv, local = refs[3 * n :]
    grid.enter()
    send, recv = Pool(send), Pool(recv)
    mine = tuple(grid.at[x] for x in layout)
    for i in range(n):
        pltpu.make_async_copy(srcs[i], held[i], local.at[i]).start()
    parts = []
    for i, low, high, order in portions:
        sends, takes = Gather.semaphores(grid, order)
        columns = pl.ds(low, high - low)
        parts.append(
            Gather(grid, order, srcs[i], dsts[i], columns, send.take(sends), recv.take(takes), layout)
        )
        parts[-1].open()
    for i in range(n):
        pltpu.make_async_copy(srcs[i], held[i], local.at[i]).wait()
        pltpu.make_async_copy(held[i], dsts[i].at[mine], local.at[i]).start()
    for i in range(n):
        pltpu.make_async_copy(held[i], dsts[i].at[mine], local.at[i]).wait()
    for part in parts:
        part.first()
    for level in range(1, len(layout)):
        for part in parts:
            part.arrivals(level)
    for part in parts:
        part.close()


def gather(grid, layout, portions, name, *blocks):
    n = len(blocks)
    sends, takes = [sum(x) for x in zip(*[Gather.semaphores(grid, p[3]) for p in portions])]
    places = tuple(grid.sizes[x] for x in layout)
    total = math.prod(places)
    outs = pl.pallas_call(
        functools.partial(gather_kernel, grid, portions, layout, n),
        out_shape=[jax.ShapeDtypeStruct(places + x.shape, x.dtype) for x in blocks],
        in_specs=[ANY] * n,
        out_specs=[ANY] * n,
        scratch_shapes=[pltpu.VMEM(x.shape, x.dtype) for x in blocks]
        + [
            pltpu.SemaphoreType.DMA((sends,)),
            pltpu.SemaphoreType.DMA((takes,)),
            pltpu.SemaphoreType.DMA((n,)),
        ],
        compiler_params=pltpu.CompilerParams(has_side_effects=True),
        name=name,
    )(*blocks)
    return [x.reshape(total * x.shape[-2], x.shape[-1]) for x in outs]


def scatter_kernel(grid, portions, layout, n, *refs):
    srcs, outs, scratch = refs[:n], refs[n : 2 * n], list(refs[2 * n : -3])
    load, send, recv = [Pool(x) for x in refs[-3:]]
    grid.enter()
    parts = []
    for i, low, high, order in portions:
        loads, sends, takes = Scatter.semaphores(grid, order)
        own, *recvs = scratch[: 1 + len(order)]
        del scratch[: 1 + len(order)]
        parts.append(
            Scatter(
                grid,
                order,
                srcs[i],
                pl.ds(low, high - low),
                own,
                recvs,
                load.take(loads),
                send.take(sends),
                recv.take(takes),
                outs[i].at[:, low:high],
                layout,
            )
        )
        parts[-1].open()
    for level in range(len(layout) - 2, -1, -1):
        for part in parts:
            part.step(level)
    for part in parts:
        part.finish()
    for part in parts:
        part.close()


def scatter(grid, layout, portions, name, dtypes, *sums):
    n = len(sums)
    places = tuple(grid.sizes[x] for x in layout)
    total = math.prod(places)
    blocks = [x.reshape(places + (x.shape[0] // total, x.shape[1])) for x in sums]
    loads, sends, takes = [sum(x) for x in zip(*[Scatter.semaphores(grid, p[3]) for p in portions])]
    scratch = []
    for i, low, high, order in portions:
        scratch += Scatter.scratch(grid, order, blocks[i].shape[-2], high - low, blocks[i].dtype)
    return pl.pallas_call(
        functools.partial(scatter_kernel, grid, portions, layout, n),
        out_shape=[jax.ShapeDtypeStruct(x.shape[-2:], t) for x, t in zip(blocks, dtypes)],
        in_specs=[ANY] * n,
        out_specs=[pl.BlockSpec(memory_space=pltpu.VMEM)] * n,
        scratch_shapes=scratch
        + [
            pltpu.SemaphoreType.DMA((loads,)),
            pltpu.SemaphoreType.DMA((sends,)),
            pltpu.SemaphoreType.DMA((takes,)),
        ],
        compiler_params=pltpu.CompilerParams(has_side_effects=True, vmem_limit_bytes=60 * 2**20),
        name=name,
    )(*blocks)


def padded(x, rows):
    return jnp.pad(x, ((0, rows - x.shape[0]), (0, 128 - x.shape[1])))


def gain_rows(total, *gains):
    pieces = [x.reshape(total, 1, -1) for x in gains]
    pieces = [jnp.pad(x, ((0, 0), (0, 0), (0, 128 - x.shape[2]))) for x in pieces]
    block = jnp.concatenate(pieces, axis=1)
    return jnp.pad(block, ((0, 0), (0, 8 - len(gains)), (0, 0))).reshape(total * 8, 128)


def on_device(
    tokens,
    cotangent,
    block_map,
    attn_gain,
    query_weight,
    key_weight,
    value_weight,
    query_gain,
    key_gain,
    output_weight,
    mlp_gain,
    gate_weight,
    up_weight,
    down_weight,
):
    grid = Grid(lax.axis_size("ctx"), lax.axis_size("fsdp"))
    total = lax.axis_size("ctx") * lax.axis_size("fsdp")
    groups, rows, width = tokens.shape
    pairs = block_map.shape[1] // 2
    ratio = H // KVH
    low = jnp.bfloat16

    gains = jnp.concatenate(
        [padded(x.reshape(1, -1), 1) for x in (attn_gain, mlp_gain, query_gain, key_gain)], axis=0
    )
    hidden_width = gate_weight.shape[1]
    wqkv = jnp.concatenate([query_weight, key_weight, value_weight], axis=1)
    wgu = jnp.concatenate([gate_weight, up_weight], axis=1)
    half = wqkv.shape[1] // 2
    full_qkv, full_output, full_gu, full_down, all_gains = gather(
        grid,
        ALL_AXES,
        [
            (0, 0, half, BFA),
            (0, half, 2 * half, AFB),
            (1, 0, width // 2, FAB),
            (1, width // 2, width, FBA),
            (2, 0, hidden_width, BFA),
            (2, hidden_width, 2 * hidden_width, AFB),
            (3, 0, width // 2, FAB),
            (3, width // 2, width, FBA),
            (4, 0, 128, FAB),
        ],
        "gather_weights",
        wqkv,
        output_weight,
        wgu,
        down_weight,
        padded(gains, 16),
    )
    all_gains = all_gains.reshape(total, 16, 128)
    gain_one, gain_two, query_scale, key_scale = [
        all_gains[:, i, : x.shape[0]].reshape(-1).astype(jnp.float32)
        for i, x in enumerate((attn_gain, mlp_gain, query_gain, key_gain))
    ]

    place = lax.axis_index("ctx")
    blocks = block_map.reshape(-1)
    own_blocks = lax.dynamic_slice_in_dim(blocks, 2 * place, 2, 0)
    slots = jnp.argsort(blocks).astype(jnp.int32)
    high_slot = (own_blocks[1] > own_blocks[0]).astype(jnp.int32)
    table = jnp.concatenate([slots, high_slot[None], jnp.max(own_blocks)[None]]).astype(jnp.int32)

    spots = (own_blocks[:, None] * BLK + jnp.arange(BLK, dtype=jnp.int32)).reshape(rows)
    cosine, sine = rope_tables(spots)
    cosine = cosine.reshape(rows, 1, HD)
    sine = sine.reshape(rows, 1, HD)
    inputs = tokens.reshape(rows, width).astype(jnp.float32)
    inverse_one = lax.rsqrt(jnp.mean(inputs * inputs, axis=-1, keepdims=True) + EPSILON)
    normal_one = inputs * inverse_one
    normed = (normal_one * gain_one).astype(low)
    raw = plain_dot(normed, full_qkv)
    query_raw = raw[:, : H * HD].reshape(rows, H, HD)
    key_raw = raw[:, H * HD : (H + KVH) * HD].reshape(rows, KVH, HD)
    value_low = raw[:, (H + KVH) * HD :].astype(low)
    query_inverse = lax.rsqrt(jnp.mean(query_raw * query_raw, axis=-1, keepdims=True) + EPSILON)
    query_unit = query_raw * query_inverse
    query_normed = query_unit * query_scale
    query_low = (query_normed * cosine + rotate(query_normed) * sine).astype(low).reshape(rows, H * HD)
    key_inverse = lax.rsqrt(jnp.mean(key_raw * key_raw, axis=-1, keepdims=True) + EPSILON)
    key_unit = key_raw * key_inverse
    key_normed = key_unit * key_scale
    key_low = (key_normed * cosine + rotate(key_normed) * sine).astype(low).reshape(rows, KVH * HD)
    key_all, value_all = gather(
        grid,
        SLOT_AXES,
        [(0, 0, KVH * HD, AB), (1, 0, KVH * HD, BA)],
        "gather_keys",
        key_low,
        value_low,
    )
    attended, attended_low, totals = attention(table, pairs, query_low, key_all, value_all)
    row_totals = totals.reshape(KVH, 2, ratio, BLK).transpose(1, 3, 0, 2).reshape(rows, H, 1)
    middle = inputs + plain_dot(attended_low, full_output)
    inverse_two = lax.rsqrt(jnp.mean(middle * middle, axis=-1, keepdims=True) + EPSILON)
    normal_two = middle * inverse_two
    normed_two = (normal_two * gain_two).astype(low)
    both = plain_dot(normed_two, full_gu)
    gate, upper = both[:, :hidden_width], both[:, hidden_width:]
    sigmoid_gate = jax.nn.sigmoid(gate)
    activated = gate * sigmoid_gate
    hidden = (activated * upper).astype(low)
    output = (middle + plain_dot(hidden, full_down)).astype(low).reshape(groups, rows, width)

    upstream = cotangent.reshape(rows, width)
    grad_hidden = right_dot(upstream, full_down)
    grad_gate = (grad_hidden * upper * sigmoid_gate * (1.0 + gate * (1.0 - sigmoid_gate))).astype(low)
    grad_upper = (grad_hidden * activated).astype(low)
    grad_both = jnp.concatenate([grad_gate, grad_upper], axis=1)
    grad_down = left_dot(hidden, upstream).astype(low)
    grad_gu = left_dot(normed_two, grad_both).astype(low)
    grad_normed_two = right_dot(grad_both, full_gu)
    grad_gain_two = jnp.sum(grad_normed_two * normal_two, axis=0)
    grad_middle = upstream.astype(jnp.float32) + norm_back(grad_normed_two, normal_two, inverse_two, gain_two)
    f32 = jnp.float32
    out_gu, out_down, out_gain_two = scatter(
        grid,
        ALL_AXES,
        [
            (0, 0, hidden_width, BFA),
            (0, hidden_width, 2 * hidden_width, AFB),
            (1, 0, width // 2, FAB),
            (1, width // 2, width, FBA),
            (2, 0, 128, FAB),
        ],
        "scatter_mlp",
        (f32, f32, f32),
        grad_gu,
        grad_down,
        gain_rows(total, grad_gain_two),
    )
    branch_grad = grad_middle.astype(low)
    grad_woutput = left_dot(attended_low, branch_grad).astype(low)
    grad_attended = right_dot(branch_grad, full_output).reshape(rows, H, HD)
    grad_summed = (grad_attended / row_totals).astype(low).reshape(rows, H * HD)
    drift = jnp.sum(grad_attended * attended.reshape(rows, H, HD), axis=-1) / row_totals[..., 0]
    drift = drift.reshape(2, BLK, KVH, ratio).transpose(2, 0, 3, 1).reshape(KVH, 2, ratio * BLK)
    grad_query, grad_keys, grad_values = attention_back(
        table, pairs, query_low, key_all, value_all, grad_summed, drift
    )
    own_keys, own_values = scatter(
        grid,
        SLOT_AXES,
        [(0, 0, KVH * HD, AB), (1, 0, KVH * HD, BA)],
        "scatter_keys",
        (f32, low),
        grad_keys,
        grad_values,
    )
    grad_qrot = grad_query.reshape(rows, H, HD)
    grad_qnormed = grad_qrot * cosine + unrotate(grad_qrot) * sine
    grad_qscale = jnp.sum(grad_qnormed * query_unit, axis=(0, 1))
    grad_qraw = norm_back(grad_qnormed, query_unit, query_inverse, query_scale)
    grad_krot = own_keys.reshape(rows, KVH, HD)
    grad_knormed = grad_krot * cosine + unrotate(grad_krot) * sine
    grad_kscale = jnp.sum(grad_knormed * key_unit, axis=(0, 1))
    grad_kraw = norm_back(grad_knormed, key_unit, key_inverse, key_scale)
    grad_raw = jnp.concatenate(
        [
            grad_qraw.reshape(rows, H * HD).astype(low),
            grad_kraw.reshape(rows, KVH * HD).astype(low),
            own_values,
        ],
        axis=1,
    )
    grad_wqkv = left_dot(normed, grad_raw).astype(low)
    grad_normed = right_dot(grad_raw, full_qkv)
    grad_gain_one = jnp.sum(grad_normed * normal_one, axis=0)
    grad_inputs = grad_middle + norm_back(grad_normed, normal_one, inverse_one, gain_one)
    out_qkv, out_output, out_gains = scatter(
        grid,
        ALL_AXES,
        [
            (0, 0, half, BFA),
            (0, half, 2 * half, AFB),
            (1, 0, width // 2, FAB),
            (1, width // 2, width, FBA),
            (2, 0, 128, FAB),
        ],
        "scatter_attention",
        (f32, f32, f32),
        grad_wqkv,
        grad_woutput,
        gain_rows(total, grad_gain_one, grad_qscale, grad_kscale),
    )
    return (
        output,
        grad_inputs.astype(low).reshape(groups, rows, width),
        out_gains[0, : attn_gain.shape[0]],
        out_qkv[:, : H * HD],
        out_qkv[:, H * HD : (H + KVH) * HD],
        out_qkv[:, (H + KVH) * HD :],
        out_gains[1, : query_gain.shape[0]],
        out_gains[2, : key_gain.shape[0]],
        out_output,
        out_gain_two[0, : mlp_gain.shape[0]],
        out_gu[:, :hidden_width],
        out_gu[:, hidden_width:],
        out_down,
    )


def solution(mesh):
    return jax.shard_map(
        on_device,
        mesh=mesh,
        in_specs=(
            P("fsdp", "ctx", None),
            P("fsdp", "ctx", None),
            P("fsdp", None),
            P(("ctx", "fsdp")),
            P(("ctx", "fsdp"), None),
            P(("ctx", "fsdp"), None),
            P(("ctx", "fsdp"), None),
            P(("ctx", "fsdp")),
            P(("ctx", "fsdp")),
            P(("ctx", "fsdp"), None),
            P(("ctx", "fsdp")),
            P(("ctx", "fsdp"), None),
            P(("ctx", "fsdp"), None),
            P(("ctx", "fsdp"), None),
        ),
        out_specs=(
            P("fsdp", "ctx", None),
            P("fsdp", "ctx", None),
            P(("ctx", "fsdp")),
            P(("ctx", "fsdp"), None),
            P(("ctx", "fsdp"), None),
            P(("ctx", "fsdp"), None),
            P(("ctx", "fsdp")),
            P(("ctx", "fsdp")),
            P(("ctx", "fsdp"), None),
            P(("ctx", "fsdp")),
            P(("ctx", "fsdp"), None),
            P(("ctx", "fsdp"), None),
            P(("ctx", "fsdp"), None),
        ),
        check_vma=False,
    )
```

```python
import functools
import math

import jax
import jax.numpy as jnp
from jax import lax
from jax.experimental import pallas as pl
from jax.experimental.pallas import tpu as pltpu
from jax.sharding import PartitionSpec as P

MESH = pl.DeviceIdType.MESH
ANY = pl.BlockSpec(memory_space=pl.ANY)


H = 16
KVH = 8
HD = 128
BLK = 128


EPSILON = 1e-06
ROPE_BASE = 1000000.0


def rope_tables(positions):
    half = HD // 2
    freqs = jnp.exp(jnp.arange(half, dtype=jnp.float32) * (-2.0 * math.log(ROPE_BASE) / HD))
    angles = positions.astype(jnp.float32)[..., None] * freqs
    cosine = jnp.cos(angles)
    sine = jnp.sin(angles)
    return (jnp.concatenate([cosine, cosine], axis=-1), jnp.concatenate([sine, sine], axis=-1))


def rotate(value_vectors):
    half = value_vectors.shape[-1] // 2
    return jnp.concatenate([-value_vectors[..., half:], value_vectors[..., :half]], axis=-1)


def unrotate(value_vectors):
    half = value_vectors.shape[-1] // 2
    return jnp.concatenate([value_vectors[..., half:], -value_vectors[..., :half]], axis=-1)


def left_dot(left, right):
    return lax.dot_general(
        left, right, (((0,), (0,)), ((), ())), preferred_element_type=jnp.float32
    )


def right_dot(left, right):
    return lax.dot_general(
        left, right, (((1,), (1,)), ((), ())), preferred_element_type=jnp.float32
    )


def plain_dot(left, right):
    return jnp.dot(left, right, preferred_element_type=jnp.float32)


def norm_back(grad_normed, unit, inverse, gain):
    scaled = grad_normed * gain
    return inverse * (scaled - unit * jnp.mean(scaled * unit, axis=-1, keepdims=True))


class Grid:
    def __init__(self, ctx, fsdp):
        self.sizes = {"a": ctx // 4, "b": 2, "core": 2, "f": fsdp}
        self.stride = {"a": 4, "b": 2, "core": 1}

    def enter(self):
        self.c = lax.axis_index("ctx")
        self.at = {
            "a": self.c // 4,
            "b": (self.c // 2) % 2,
            "core": self.c % 2,
            "f": lax.axis_index("fsdp"),
        }

    def barrier(self):
        sem = pltpu.get_barrier_semaphore()
        count = 0
        for axis in ("core", "b", "a", "f"):
            n, p = self.sizes[axis], self.at[axis]
            for step in (1,) if n == 2 else (1, n - 1):
                pl.semaphore_signal(
                    sem, inc=1, device_id=self.peer(axis, lax.rem(p + step, n)), device_id_type=MESH
                )
                count += 1
        pl.semaphore_wait(sem, count)

    def peer(self, axis, place):
        if axis == "f":
            return {"fsdp": place}
        return {"ctx": self.c + (place - self.at[axis]) * self.stride[axis]}

    def sources(self, axis):
        n, p = self.sizes[axis], self.at[axis]
        if n == 2:
            return [(None, 1 - p, None, None)]
        found = []
        for step in range(1, n):
            for way in (1, -1):
                origin = p - way * step
                onward = p + way
                found.append(
                    (
                        jnp.logical_and(origin >= 0, origin < n),
                        origin,
                        onward,
                        jnp.logical_and(
                            jnp.logical_and(origin >= 0, origin < n),
                            jnp.logical_and(onward >= 0, onward < n),
                        ),
                    )
                )
        return found

    def around(self, axis):
        n, p = self.sizes[axis], self.at[axis]
        if n == 2:
            return [(None, 1 - p)]
        return [(p + 1 < n, p + 1), (p >= 1, p - 1)]

    def nearest(self, axis):
        n, p = self.sizes[axis], self.at[axis]
        if n == 2:
            return [p, 1 - p]
        order = [0]
        for step in range(1, n):
            for way in (step, n - step):
                if way not in order:
                    order.append(way)
        return [lax.rem(p + s, n) for s in order]


class Pool:
    def __init__(self, ref):
        self.ref, self.used = ref, 0

    def take(self, count):
        first = self.used
        self.used += count
        return self.ref.at[pl.ds(first, count)]


def guarded(cond, body):
    if cond is None:
        body()
    else:
        pl.when(cond)(body)


class Gather:
    def __init__(self, grid, order, src, dst, columns, send_sem, recv_sem, layout_axes):
        self.grid, self.order, self.src, self.dst = grid, order, src, dst
        self.columns, self.send_sem, self.recv_sem = columns, send_sem, recv_sem
        self.layout_axes = layout_axes
        self.sends = 0
        self.pending = []

    @staticmethod
    def semaphores(grid, order):
        near = {x: 1 if grid.sizes[x] == 2 else 2 for x in order}
        far = {x: 0 if grid.sizes[x] == 2 else 2 * (grid.sizes[x] - 1) for x in order}
        sends = near[order[0]] + far[order[0]] + sum(near[x] for x in order[1:])
        inner = 1
        for level in range(1, len(order)):
            axis = order[level]
            onward = sum(near[x] for x in order[level + 1 :])
            sends += inner * (far[axis] + max(far[axis], 1) * onward)
            inner *= grid.sizes[axis]
        return sends, grid.sizes[order[0]] + inner

    def view(self, places):
        idx = tuple(places.get(x, slice(None)) for x in self.layout_axes)
        return self.dst.at[idx + (slice(None), self.columns)]

    def unit_number(self, places):
        number = 0
        for x in self.order[1:]:
            number = number * self.grid.sizes[x] + places[x]
        return number

    def start(self, cond, view, axis, place, sem):
        slot = self.sends
        self.sends += 1

        def make():
            return pltpu.make_async_remote_copy(
                src_ref=view[0],
                dst_ref=view[1],
                send_sem=self.send_sem.at[slot],
                recv_sem=self.recv_sem.at[sem],
                device_id=self.grid.peer(axis, place),
                device_id_type=MESH,
            )

        guarded(cond, lambda: make().start())
        self.pending.append((cond, make))

    def wait_recv(self, view, sem):
        pltpu.make_async_remote_copy(
            src_ref=view,
            dst_ref=view,
            send_sem=self.send_sem.at[0],
            recv_sem=self.recv_sem.at[sem],
            device_id={},
            device_id_type=MESH,
        ).wait_recv()

    def own_places(self):
        return {x: self.grid.at[x] for x in self.order}

    def open(self):
        axis = self.order[0]
        own = self.view(self.own_places())
        for cond, place in self.grid.around(axis):
            self.start(cond, (self.src, own), axis, place, self.grid.at[axis])

    def first(self):
        axis = self.order[0]
        for cond, origin, onward, more in self.grid.sources(axis):
            view = self.view({**self.own_places(), axis: origin})
            guarded(cond, lambda: self.wait_recv(view, origin))
            if onward is not None:
                self.start(more, (view, view), axis, onward, origin)
        self.pass_on(None, 1, {x: self.grid.at[x] for x in self.order[1:]})

    def pass_on(self, cond, level, places):
        n1 = self.grid.sizes[self.order[0]]
        sem = n1 + self.unit_number(places)
        view = self.view(places)
        for axis in self.order[level:]:
            for near, place in self.grid.around(axis):
                both = near if cond is None else cond if near is None else jnp.logical_and(cond, near)
                self.start(both, (view, view), axis, place, sem)

    def arrivals(self, level):
        n1 = self.grid.sizes[self.order[0]]
        axis = self.order[level]
        inner = [{}]
        for x in self.order[1:level]:
            inner = [{**places, x: j} for places in inner for j in self.grid.nearest(x)]
        fixed = {x: self.grid.at[x] for x in self.order[level + 1 :]}
        for places in inner:
            for cond, origin, onward, more in self.grid.sources(axis):
                unit = {**places, **fixed, axis: origin}
                view = self.view(unit)
                sem = n1 + self.unit_number(unit)
                guarded(cond, lambda: self.wait_recv(view, sem))
                if onward is not None:
                    self.start(more, (view, view), axis, onward, sem)
                self.pass_on(cond, level + 1, unit)

    def close(self):
        for cond, make in self.pending:
            guarded(cond, lambda: make().wait_send())


def add_into(total, term, out=None):
    shape = total.shape
    rows = min(16, shape[-2])
    steps = shape[-2] // rows
    lead = math.prod(shape[:-2])

    def body(i, carry):
        index = ()
        rest = i // steps
        for n in reversed(shape[:-2]):
            index = (lax.rem(rest, n),) + index
            rest = rest // n
        at = index + (pl.ds(pl.multiple_of(lax.rem(i, steps) * rows, rows), rows), slice(None))
        value = total[at].astype(jnp.float32)
        if term is not None:
            value = value + term[at].astype(jnp.float32)
        if out is None:
            total[at] = value.astype(total.dtype)
        else:
            out[at] = value.astype(out.dtype)
        return carry

    lax.fori_loop(0, lead * steps, body, 0)


class Scatter:
    def __init__(self, grid, order, src, columns, own, recvs, load_sem, send_sem, recv_sem, out, layout_axes):
        self.grid, self.order, self.src, self.columns = grid, order, src, columns
        self.own, self.recvs, self.out = own, recvs, out
        self.load_sem, self.send_sem, self.recv_sem = load_sem, send_sem, recv_sem
        self.layout_axes = layout_axes
        self.sends = 0
        self.pending = []
        self.base = {}
        number = 0
        for level in range(len(order) - 1, -1, -1):
            self.base[level] = number
            number += self.slots(grid, order, level)

    @staticmethod
    def kept(grid, order):
        return order[1:-1] if grid.sizes[order[-1]] == 2 else order[1:]

    @staticmethod
    def inner(grid, order, level):
        return [grid.sizes[x] for x in order[1:level]]

    @staticmethod
    def slots(grid, order, level):
        n = grid.sizes[order[level]]
        lines = 1 if n == 2 else n + 1
        return lines * math.prod(Scatter.inner(grid, order, level))

    @staticmethod
    def scratch(grid, order, rows, columns, dtype):
        n1 = grid.sizes[order[0]]
        own = tuple(grid.sizes[x] for x in Scatter.kept(grid, order)) + (n1, rows, columns)
        recvs = []
        for level in range(len(order)):
            n = grid.sizes[order[level]]
            lead = () if n == 2 else (n + 1,)
            block = (rows, columns) if level == 0 else (n1, rows, columns)
            recvs.append(lead + tuple(Scatter.inner(grid, order, level)) + block)
        return [pltpu.VMEM(s, dtype) for s in [own] + recvs]

    @staticmethod
    def semaphores(grid, order):
        loads = math.prod(grid.sizes[x] for x in Scatter.kept(grid, order))
        slots = [Scatter.slots(grid, order, level) for level in range(len(order))]
        sends = [
            (1 if grid.sizes[x] == 2 else 2 * (grid.sizes[x] - 1))
            * math.prod(Scatter.inner(grid, order, level))
            for level, x in enumerate(order)
        ]
        return loads, sum(sends), sum(slots)

    def hbm(self, places):
        idx = tuple(places.get(x, slice(None)) for x in self.layout_axes)
        return self.src.at[idx + (slice(None), self.columns)]

    def units(self, level, first=None):
        found = [{}]
        for x in self.order[1:level]:
            found = [{**places, x: j} for places in found for j in reversed(self.grid.nearest(x))]
        return found

    def mine(self, places):
        idx = tuple(places.get(x, self.grid.at[x]) for x in self.kept(self.grid, self.order))
        return self.own.at[idx]

    def number(self, places, axes):
        value = 0
        for x in axes:
            value = value * self.grid.sizes[x] + places[x]
        return value

    def slot(self, level, places, way=None, target=None):
        axes = self.order[1:level]
        idx = tuple(places[x] for x in axes)
        inner = math.prod(self.grid.sizes[x] for x in axes)
        number = self.number(places, axes)
        if way is not None:
            line = target + 1 - way
            idx = (line,) + idx
            number = line * inner + number
        ref = self.recvs[level]
        return (ref.at[idx] if idx else ref), self.recv_sem.at[self.base[level] + number]

    def send(self, cond, view, landing, axis, place):
        slot = self.sends
        self.sends += 1
        ref, sem = landing

        def make():
            return pltpu.make_async_remote_copy(
                src_ref=view,
                dst_ref=ref,
                send_sem=self.send_sem.at[slot],
                recv_sem=sem,
                device_id=self.grid.peer(axis, place),
                device_id_type=MESH,
            )

        guarded(cond, lambda: make().start())
        self.pending.append((cond, make))

    def take(self, cond, landing, total, out=None):
        ref, sem = landing

        def body():
            pltpu.make_async_remote_copy(
                src_ref=ref,
                dst_ref=ref,
                send_sem=self.send_sem.at[0],
                recv_sem=sem,
                device_id={},
                device_id_type=MESH,
            ).wait_recv()
            add_into(total, ref, out)

        guarded(cond, body)

    def load(self, places):
        axes = self.kept(self.grid, self.order)
        here = {self.order[-1]: self.grid.at[self.order[-1]], **places}
        return pltpu.make_async_copy(
            self.hbm(here), self.mine(places), self.load_sem.at[self.number(places, axes)]
        )

    def open(self):
        top = len(self.order) - 1
        axis = self.order[top]
        if self.grid.sizes[axis] > 2:
            for places in self.units(top + 1):
                self.load(places).start()
            return
        there = 1 - self.grid.at[axis]
        for places in self.units(top):
            self.send(None, self.hbm({**places, axis: there}), self.slot(top, places), axis, there)
            self.load(places).start()

    def settle(self, level, places):
        above = level + 1
        top = len(self.order) - 1
        total = self.mine(places)
        if above > top:
            self.load(places).wait()
            return
        if above == top and self.grid.sizes[self.order[top]] == 2:
            self.load(places).wait()
            self.take(None, self.slot(above, places), total)
            return
        axis = self.order[above]
        n, p = self.grid.sizes[axis], self.grid.at[axis]
        if n == 2:
            self.take(None, self.slot(above, places), total)
        else:
            self.take(p >= 1, self.slot(above, places, 0, p), total)
            self.take(p + 1 < n, self.slot(above, places, 1, p), total)

    def levels(self):
        top = len(self.order) - 1
        return top if self.grid.sizes[self.order[top]] == 2 else top + 1

    def step(self, level):
        axis = self.order[level]
        n, p = self.grid.sizes[axis], self.grid.at[axis]
        if level == 0:
            self.settle(0, {})
            whole = self.mine({})
            self.along(level, {}, lambda t: whole.at[t])
            return
        for places in self.units(level):
            self.along(level, places, lambda t: self.mine({**places, axis: t}))
            self.settle(level, {**places, axis: p})

    def along(self, level, places, view):
        axis = self.order[level]
        n, p = self.grid.sizes[axis], self.grid.at[axis]
        if n == 2:
            if level:
                self.settle(level, {**places, axis: 1 - p})
            self.send(None, view(1 - p), self.slot(level, places), axis, 1 - p)
            return
        for s in range(n - 1):
            for way, t in ((0, n - 1 - s), (1, s)):
                wanted = (t > p) if way == 0 else (t < p)
                behind = (p >= 1) if way == 0 else (p + 1 < n)
                if level:
                    pl.when(wanted)(lambda: self.settle(level, {**places, axis: t}))
                self.take(jnp.logical_and(wanted, behind), self.slot(level, places, way, t), view(t))
                self.send(wanted, view(t), self.slot(level, places, way, t), axis, p + (1 if way == 0 else -1))

    def finish(self):
        axis = self.order[0]
        n, p = self.grid.sizes[axis], self.grid.at[axis]
        total = self.mine({}).at[p]
        if n == 2:
            self.take(None, self.slot(0, {}), total, self.out)
            return
        self.take(p >= 1, self.slot(0, {}, 0, p), total)
        self.take(p + 1 < n, self.slot(0, {}, 1, p), total)
        add_into(total, None, self.out)

    def close(self):
        for cond, make in self.pending:
            guarded(cond, lambda: make().wait_send())


def half_pairs(ref, s):
    rows = pl.ds(s * BLK, BLK)
    return jnp.concatenate([ref[rows, :HD], ref[rows, HD:]], axis=0)


def items(table, pairs):
    high_slot, high = table[pairs * 2], table[pairs * 2 + 1]
    low_block = 2 * pairs - 1 - high
    split = high // 2
    found = []
    for w in range(pairs - 1):
        upper = w < split
        found.append((jnp.where(upper, high_slot, 1 - high_slot), jnp.where(upper, w, w - split), None))
    found.append((high_slot, split, high))
    found.append((1 - high_slot, low_block // 2, low_block))
    return found


def chunk_of(ref, table, c):
    return jnp.concatenate(
        [ref[pl.ds(pl.multiple_of(table[2 * c + i] * BLK, BLK), BLK), :] for i in range(2)], axis=0
    )


def row_contract(left, right):
    return lax.dot_general(left, right, (((1,), (1,)), ((), ())), preferred_element_type=jnp.float32)


def attention_kernel(pairs, table, q_ref, k_ref, v_ref, o_ref, low_ref, t_ref, qs, acc, tot):
    for s in range(2):
        qs[s] = half_pairs(q_ref, s)
    acc[...] = jnp.zeros_like(acc)
    tot[...] = jnp.zeros_like(tot)
    for s, c, block in items(table, pairs):
        keys = chunk_of(k_ref, table, c)
        vals = chunk_of(v_ref, table, c)
        scores = row_contract(qs[s], keys) * (HD ** (-0.5) * math.log2(math.e))
        weights = jnp.exp2(scores)
        if block is not None:
            rows = lax.broadcasted_iota(jnp.int32, (2 * BLK, 2 * BLK), 0)
            cols = lax.broadcasted_iota(jnp.int32, (2 * BLK, 2 * BLK), 1)
            allowed = cols <= lax.rem(rows, BLK) + (block - 2 * c) * BLK
            weights = jnp.where(allowed, weights, 0.0)
        tot[s] += weights[:, :HD] + weights[:, HD:]
        acc[s] += jnp.dot(weights.astype(jnp.bfloat16), vals, preferred_element_type=jnp.float32)
    for s in range(2):
        total = tot[s]
        value = acc[s] / jnp.sum(total, axis=1, keepdims=True)
        rows = pl.ds(s * BLK, BLK)
        for i in range(2):
            part = value[i * BLK : (i + 1) * BLK]
            o_ref[rows, i * HD : (i + 1) * HD] = part
            low_ref[rows, i * HD : (i + 1) * HD] = part.astype(jnp.bfloat16)
        t_ref[0, s : s + 1, :] = jnp.sum(total.T, axis=0, keepdims=True)


def attention(table, pairs, queries, keys, values):
    rows, length = queries.shape[0], keys.shape[0]
    head = pl.BlockSpec((rows, 2 * HD), lambda h, t: (0, h))
    side = pl.BlockSpec((length, HD), lambda h, t: (0, h))
    stats = pl.BlockSpec((1, 2, 2 * BLK), lambda h, t: (h, 0, 0))
    return pl.pallas_call(
        functools.partial(attention_kernel, pairs),
        grid_spec=pltpu.PrefetchScalarGridSpec(
            num_scalar_prefetch=1,
            grid=(KVH,),
            in_specs=[head, side, side],
            out_specs=[head, head, stats],
            scratch_shapes=[
                pltpu.VMEM((2, 2 * BLK, HD), jnp.bfloat16),
                pltpu.VMEM((2, 2 * BLK, HD), jnp.float32),
                pltpu.VMEM((2, 2 * BLK, HD), jnp.float32),
            ],
        ),
        out_shape=[
            jax.ShapeDtypeStruct((rows, H * HD), jnp.float32),
            jax.ShapeDtypeStruct((rows, H * HD), jnp.bfloat16),
            jax.ShapeDtypeStruct((KVH, 2, 2 * BLK), jnp.float32),
        ],
        name="attention",
    )(table, queries, keys, values)


def attention_back_kernel(
    pairs, table, q_ref, k_ref, v_ref, g_ref, d_ref, dq_ref, dk_ref, dv_ref, qs, gs, dq, dk, dv
):
    scale = HD ** (-0.5)
    for s in range(2):
        qs[s] = half_pairs(q_ref, s)
        gs[s] = half_pairs(g_ref, s)
    for total in (dq, dk, dv):
        total[...] = jnp.zeros_like(total)
    for s, c, block in items(table, pairs):
        keys = chunk_of(k_ref, table, c)
        vals = chunk_of(v_ref, table, c)
        queries, grads = qs[s], gs[s]
        weights = jnp.exp2(row_contract(keys, queries) * (scale * math.log2(math.e)))
        if block is not None:
            rows = lax.broadcasted_iota(jnp.int32, (2 * BLK, 2 * BLK), 0)
            cols = lax.broadcasted_iota(jnp.int32, (2 * BLK, 2 * BLK), 1)
            allowed = rows <= lax.rem(cols, BLK) + (block - 2 * c) * BLK
            weights = jnp.where(allowed, weights, 0.0)
        through = row_contract(vals, grads)
        scores = (weights * (through - d_ref[0, pl.ds(s, 1), :])).astype(jnp.bfloat16)
        to_values = jnp.dot(weights.astype(jnp.bfloat16), grads, preferred_element_type=jnp.float32)
        to_keys = jnp.dot(scores, queries, preferred_element_type=jnp.float32)
        for i in range(2):
            at = pl.ds(pl.multiple_of(table[2 * c + i] * BLK, BLK), BLK)
            dv[at, :] += to_values[i * BLK : (i + 1) * BLK]
            dk[at, :] += to_keys[i * BLK : (i + 1) * BLK]
        dq[s] += left_dot(scores, keys)
    dk_ref[...] = (dk[...] * scale).astype(jnp.bfloat16)
    dv_ref[...] = dv[...].astype(jnp.bfloat16)
    for s in range(2):
        for i in range(2):
            dq_ref[pl.ds(s * BLK, BLK), i * HD : (i + 1) * HD] = dq[s, i * BLK : (i + 1) * BLK] * scale


def attention_back(table, pairs, queries, keys, values, grads, drift):
    rows, length = queries.shape[0], keys.shape[0]
    head = pl.BlockSpec((rows, 2 * HD), lambda h, t: (0, h))
    side = pl.BlockSpec((length, HD), lambda h, t: (0, h))
    stats = pl.BlockSpec((1, 2, 2 * BLK), lambda h, t: (h, 0, 0))
    return pl.pallas_call(
        functools.partial(attention_back_kernel, pairs),
        grid_spec=pltpu.PrefetchScalarGridSpec(
            num_scalar_prefetch=1,
            grid=(KVH,),
            in_specs=[head, side, side, head, stats],
            out_specs=[head, side, side],
            scratch_shapes=[
                pltpu.VMEM((2, 2 * BLK, HD), jnp.bfloat16),
                pltpu.VMEM((2, 2 * BLK, HD), jnp.bfloat16),
                pltpu.VMEM((2, 2 * BLK, HD), jnp.float32),
                pltpu.VMEM((length, HD), jnp.float32),
                pltpu.VMEM((length, HD), jnp.float32),
            ],
        ),
        out_shape=[
            jax.ShapeDtypeStruct((rows, H * HD), jnp.float32),
            jax.ShapeDtypeStruct((length, KVH * HD), jnp.bfloat16),
            jax.ShapeDtypeStruct((length, KVH * HD), jnp.bfloat16),
        ],
        name="attention_back",
    )(table, queries, keys, values, grads, drift)


ALL_AXES = ("a", "b", "core", "f")
SLOT_AXES = ("a", "b", "core")
CHIP_AXES = ("a", "b", "f")
BFA, AFB, FAB, FBA = ("b", "f", "a"), ("a", "f", "b"), ("f", "a", "b"), ("f", "b", "a")
AB, BA = ("a", "b", "core"), ("b", "a", "core")
CORE = ("core",)


FRONT_SRC = ("q", "k", "v", "o", "g", "u", "d", "gains")


def front_kernel(grid, plan, *refs):
    n = len(FRONT_SRC)
    src = dict(zip(FRONT_SRC, refs[:n]))
    tokens_ref, cosine_ref, sine_ref = refs[n : n + 3]
    outs = refs[n + 3 : n + 15]
    wqkv_ref, wo_ref, wgu_ref, wd_ref, allgains_ref, k_out, v_out = outs[:7]
    normed_ref, gains_ref, raw_ref, qlow_ref, inv_ref = outs[7:]
    scratch = refs[n + 15 :]
    held = dict(zip(FRONT_SRC, scratch[:n]))
    weights, klow, vlow, gbuf = scratch[n : n + 4]
    send, recv, local, load = scratch[n + 4 :]
    grid.enter()
    grid.barrier()
    send, recv = Pool(send), Pool(recv)
    width = tokens_ref.shape[1]
    rows = tokens_ref.shape[0]
    spans = {"q": (wqkv_ref, 0), "k": (wqkv_ref, H * HD), "v": (wqkv_ref, (H + KVH) * HD)}
    hidden = src["g"].shape[1]
    spans.update({"o": (wo_ref, 0), "g": (wgu_ref, 0), "u": (wgu_ref, hidden), "d": (wd_ref, 0)})
    spans["gains"] = (allgains_ref, 0)
    mine = tuple(grid.at[x] for x in ALL_AXES)

    def own_copy(i, name):
        dst, at = spans[name]
        return pltpu.make_async_copy(
            held[name], dst.at[mine + (slice(None), pl.ds(at, src[name].shape[1]))], local.at[i]
        )

    for i, name in enumerate(FRONT_SRC):
        pltpu.make_async_copy(src[name], held[name], local.at[i]).start()

    def part(name, low, high, order):
        dst, at = spans[name]
        sends, takes = Gather.semaphores(grid, order)
        columns = pl.ds(at + low, high - low)
        return Gather(
            grid, order, src[name].at[:, low:high], dst, columns, send.take(sends), recv.take(takes), ALL_AXES
        )

    early = [part(*p) for p in plan[0]]
    late = [part(*p) for p in plan[1]]
    for p in early:
        p.open()
    for p in late:
        p.open()
    for i, name in enumerate(FRONT_SRC):
        pltpu.make_async_copy(src[name], held[name], local.at[i]).wait()
        own_copy(i, name).start()
    inputs = tokens_ref[...].astype(jnp.float32)
    inverse = lax.rsqrt(jnp.mean(inputs * inputs, axis=-1, keepdims=True) + EPSILON)
    inv_ref[...] = jnp.broadcast_to(inverse, (rows, 128))
    for i, name in enumerate(FRONT_SRC):
        own_copy(i, name).wait()

    for p in early:
        p.first()
    for level in (1, 2):
        for p in early:
            p.arrivals(level)
    pump = []
    for p in late:
        pump.append(p.first)
    for level in (1, 2, 3):
        for p in late:
            pump.append(functools.partial(p.arrivals, level))

    def step(count):
        for _ in range(count):
            if pump:
                pump.pop(0)()

    step(len(late))
    for p in early:
        p.arrivals(3)

    places = math.prod(grid.sizes[x] for x in ALL_AXES)
    copy = pltpu.make_async_copy(allgains_ref, gbuf, load.at[0])
    copy.start()
    big = pltpu.make_async_copy(wqkv_ref, weights, load.at[1])
    big.start()
    copy.wait()
    blocks = gbuf[...].reshape((places,) + gbuf.shape[-2:]).astype(jnp.float32)
    gains = jnp.sum(blocks, axis=0)
    gains_ref[...] = gains
    lanes = width // 128
    for j in range(lanes):
        cols = slice(j * 128, (j + 1) * 128)
        part_of = tokens_ref[:, cols].astype(jnp.float32) * inv_ref[...] * gains_ref[j : j + 1, :]
        normed_ref[:, cols] = part_of.astype(jnp.bfloat16)
    big.wait()
    step(1)
    flat = weights.reshape(width, weights.shape[-1])
    normed = normed_ref[...]
    chunk = 2 * HD

    def heads(low_out, gain_row, out_at, raw_at, c):
        at = pl.ds(pl.multiple_of(raw_at + c * chunk, chunk), chunk)
        raw = jnp.dot(normed, flat[:, at], preferred_element_type=jnp.float32)
        raw_ref[:, at] = raw
        done = []
        for i in range(2):
            one = raw[:, i * HD : (i + 1) * HD]
            unit = one * lax.rsqrt(jnp.mean(one * one, axis=-1, keepdims=True) + EPSILON)
            unit = unit * gains_ref[gain_row : gain_row + 1, :]
            done.append(unit * cosine_ref[...] + pltpu.roll(unit, HD // 2, 1) * sine_ref[...])
        to = pl.ds(pl.multiple_of(out_at + c * chunk, chunk), chunk)
        low_out[:, to] = jnp.concatenate(done, axis=1).astype(jnp.bfloat16)

    def loop(count, body):
        def once(c, carry):
            body(c)
            return carry

        lax.fori_loop(0, count, once, 0)

    def to_values(c):
        at = pl.ds(pl.multiple_of((H + KVH) * HD + c * chunk, chunk), chunk)
        to = pl.ds(pl.multiple_of(c * chunk, chunk), chunk)
        raw = jnp.dot(normed, flat[:, at], preferred_element_type=jnp.float32)
        vlow[:, to] = raw.astype(jnp.bfloat16)

    loop(KVH // 2, functools.partial(heads, klow, 2 * lanes + 1, 0, H * HD))
    loop(KVH // 2, to_values)

    def pair(source, dst, order):
        sends, takes = Gather.semaphores(grid, order)
        return Gather(
            grid, order, source, dst, pl.ds(0, KVH * HD), send.take(sends), recv.take(takes), SLOT_AXES
        )

    slot = tuple(grid.at[x] for x in SLOT_AXES)
    slabs = [pair(klow, k_out, AB), pair(vlow, v_out, BA)]
    saves = [
        pltpu.make_async_copy(klow, k_out.at[slot], load.at[0]),
        pltpu.make_async_copy(vlow, v_out.at[slot], load.at[1]),
    ]
    for p, save in zip(slabs, saves):
        p.open()
        save.start()
    step(2)
    loop(KVH // 2, functools.partial(heads, qlow_ref, 2 * lanes, 0, 0))
    for p, save in zip(slabs, saves):
        save.wait()
        p.first()
    step(2)
    loop(KVH // 2, functools.partial(heads, qlow_ref, 2 * lanes, H * HD // 2, H * HD // 2))
    for p in slabs:
        p.arrivals(1)
    step(len(pump))
    for p in slabs:
        p.arrivals(2)
    for p in early + late + slabs:
        p.close()


def front(grid, plan, blocks, tokens, cosine, sine):
    n = len(FRONT_SRC)
    rows, width = tokens.shape
    places = tuple(grid.sizes[x] for x in ALL_AXES)
    slots = tuple(grid.sizes[x] for x in SLOT_AXES)
    by = dict(zip(FRONT_SRC, blocks))
    low, f32 = jnp.bfloat16, jnp.float32
    full = (H + 2 * KVH) * HD
    counts = [Gather.semaphores(grid, p[3]) for p in plan[0] + plan[1]]
    counts += [Gather.semaphores(grid, AB), Gather.semaphores(grid, BA)]
    sends, takes = [sum(x) for x in zip(*counts)]
    shape = jax.ShapeDtypeStruct
    vmem = pl.BlockSpec(memory_space=pltpu.VMEM)
    outs = pl.pallas_call(
        functools.partial(front_kernel, grid, plan),
        out_shape=[
            shape(places + (by["q"].shape[0], full), low),
            shape(places + by["o"].shape, low),
            shape(places + (by["g"].shape[0], 2 * by["g"].shape[1]), low),
            shape(places + by["d"].shape, low),
            shape(places + by["gains"].shape, low),
            shape(slots + (rows, KVH * HD), low),
            shape(slots + (rows, KVH * HD), low),
            shape((rows, width), low),
            shape(by["gains"].shape, f32),
            shape((rows, (H + KVH) * HD), f32),
            shape((rows, H * HD), low),
            shape((rows, 128), f32),
        ],
        in_specs=[ANY] * n + [vmem] * 3,
        out_specs=[ANY] * 7 + [vmem] * 5,
        scratch_shapes=[pltpu.VMEM(x.shape, x.dtype) for x in blocks]
        + [
            pltpu.VMEM(places + (by["q"].shape[0], full), low),
            pltpu.VMEM((rows, KVH * HD), low),
            pltpu.VMEM((rows, KVH * HD), low),
            pltpu.VMEM(places + by["gains"].shape, low),
            pltpu.SemaphoreType.DMA((sends,)),
            pltpu.SemaphoreType.DMA((takes,)),
            pltpu.SemaphoreType.DMA((n,)),
            pltpu.SemaphoreType.DMA((2,)),
        ],
        compiler_params=pltpu.CompilerParams(
            has_side_effects=True, vmem_limit_bytes=60 * 2**20, collective_id=0
        ),
        name="front",
    )(*blocks, tokens, cosine, sine)
    wqkv, wo, wgu, wd, _, keys, vals, normed, gains, raw, qlow, inverse = outs
    flat = [x.reshape(-1, x.shape[-1]) for x in (wqkv, wo, wgu, wd, keys, vals)]
    return flat + [normed, gains, raw, qlow, inverse]


def scatter_kernel(grid, portions, layouts, n, *refs):
    srcs, outs, scratch = refs[:n], refs[n : 2 * n], list(refs[2 * n : -3])
    load, send, recv = [Pool(x) for x in refs[-3:]]
    grid.enter()
    parts = []
    for i, low, high, order in portions:
        loads, sends, takes = Scatter.semaphores(grid, order)
        own, *recvs = scratch[: 1 + len(order)]
        del scratch[: 1 + len(order)]
        parts.append(
            Scatter(
                grid,
                order,
                srcs[i],
                pl.ds(low, high - low),
                own,
                recvs,
                load.take(loads),
                send.take(sends),
                recv.take(takes),
                outs[i].at[:, low:high],
                layouts[i],
            )
        )
        parts[-1].open()
    for level in (2, 1, 0):
        for part in parts:
            if level < part.levels():
                part.step(level)
    for part in parts:
        part.finish()
    for part in parts:
        part.close()


def scatter(grid, layouts, portions, name, dtypes, *sums):
    n = len(sums)
    blocks = []
    for layout, x in zip(layouts, sums):
        places = tuple(grid.sizes[axis] for axis in layout)
        blocks.append(x.reshape(places + (x.shape[0] // math.prod(places), x.shape[1])))
    loads, sends, takes = [sum(x) for x in zip(*[Scatter.semaphores(grid, p[3]) for p in portions])]
    scratch = []
    for i, low, high, order in portions:
        scratch += Scatter.scratch(grid, order, blocks[i].shape[-2], high - low, blocks[i].dtype)
    return pl.pallas_call(
        functools.partial(scatter_kernel, grid, portions, layouts, n),
        out_shape=[jax.ShapeDtypeStruct(x.shape[-2:], t) for x, t in zip(blocks, dtypes)],
        in_specs=[ANY] * n,
        out_specs=[pl.BlockSpec(memory_space=pltpu.VMEM)] * n,
        scratch_shapes=scratch
        + [
            pltpu.SemaphoreType.DMA((loads,)),
            pltpu.SemaphoreType.DMA((sends,)),
            pltpu.SemaphoreType.DMA((takes,)),
        ],
        compiler_params=pltpu.CompilerParams(has_side_effects=True, vmem_limit_bytes=60 * 2**20),
        name=name,
    )(*blocks)


def gain_rows(total, *gains):
    pieces = [x.reshape(total, 1, -1) for x in gains]
    pieces = [jnp.pad(x, ((0, 0), (0, 0), (0, 128 - x.shape[2]))) for x in pieces]
    block = jnp.concatenate(pieces, axis=1)
    return jnp.pad(block, ((0, 0), (0, 8 - len(gains)), (0, 0))).reshape(total * 8, 128)


def swapped(x):
    count = lax.axis_size("ctx")
    return lax.ppermute(x, "ctx", [(i, i ^ 1) for i in range(count)])


def chip_sums(left, right, right_other):
    core = lax.axis_index("ctx") % 2
    rows, width = left.shape
    split = left.reshape(rows, lax.axis_size("ctx") // 2, 2, -1)
    mine = lax.dynamic_index_in_dim(split, core, 2, False).reshape(rows, width // 2)
    theirs = lax.dynamic_index_in_dim(split, 1 - core, 2, False).reshape(rows, width // 2)
    both = jnp.concatenate([mine, swapped(theirs)], axis=0)
    return left_dot(both, jnp.concatenate([right, right_other], axis=0)).astype(jnp.bfloat16)


def on_device(
    tokens,
    cotangent,
    block_map,
    attn_gain,
    query_weight,
    key_weight,
    value_weight,
    query_gain,
    key_gain,
    output_weight,
    mlp_gain,
    gate_weight,
    up_weight,
    down_weight,
):
    grid = Grid(lax.axis_size("ctx"), lax.axis_size("fsdp"))
    total = lax.axis_size("ctx") * lax.axis_size("fsdp")
    groups, rows, width = tokens.shape
    pairs = block_map.shape[1] // 2
    ratio = H // KVH
    low = jnp.bfloat16

    device = lax.axis_index("ctx") * lax.axis_size("fsdp") + lax.axis_index("fsdp")
    gains = jnp.zeros((width // 128 * 2 + 16) * 128, low)
    for at, x in ((0, attn_gain), (width, mlp_gain), (2 * width, query_gain), (2 * width + HD, key_gain)):
        gains = lax.dynamic_update_slice_in_dim(gains, x, at + device * x.shape[0], 0)
    gains = gains.reshape(-1, 128)
    hidden_width = gate_weight.shape[1]

    place = lax.axis_index("ctx")
    blocks = block_map.reshape(-1)
    own_blocks = lax.dynamic_slice_in_dim(blocks, 2 * place, 2, 0)
    numbers = jnp.arange(2 * pairs, dtype=jnp.int32)
    slots = jnp.sum(jnp.where(blocks[None, :] == numbers[:, None], numbers[None, :], 0), axis=1)
    high_slot = (own_blocks[1] > own_blocks[0]).astype(jnp.int32)
    table = jnp.concatenate([slots, high_slot[None], jnp.max(own_blocks)[None]]).astype(jnp.int32)

    spots = (own_blocks[:, None] * BLK + jnp.arange(BLK, dtype=jnp.int32)).reshape(rows)
    cosine, sine = rope_tables(spots)
    turned = jnp.concatenate([-sine[:, : HD // 2], sine[:, HD // 2 :]], axis=1)
    half_q, half_k = H * HD // 2, KVH * HD // 2
    half = half_q + 2 * half_k
    plan = (
        (
            ("gains", 0, 128, FAB + CORE),
            ("q", 0, half_q, FAB + CORE),
            ("q", half_q, 2 * half_q, FBA + CORE),
            ("k", 0, 2 * half_k, BFA + CORE),
            ("v", 0, 2 * half_k, AFB + CORE),
        ),
        (
            ("o", 0, width // 2, BFA + CORE),
            ("o", width // 2, width, AFB + CORE),
            ("g", 0, hidden_width, BFA + CORE),
            ("u", 0, hidden_width, AFB + CORE),
            ("d", 0, width // 2, BFA + CORE),
            ("d", width // 2, width, AFB + CORE),
        ),
    )
    (
        full_qkv,
        full_output,
        full_gu,
        full_down,
        key_all,
        value_all,
        normed,
        gains,
        raw,
        query_low,
        inverse_one,
    ) = front(
        grid,
        plan,
        (query_weight, key_weight, value_weight, output_weight, gate_weight, up_weight, down_weight, gains),
        tokens.reshape(rows, width),
        cosine,
        turned,
    )
    attended, attended_low, totals = attention(table, pairs, query_low, key_all, value_all)
    lanes = width // 128
    gain_one, gain_two = gains[:lanes].reshape(-1), gains[lanes : 2 * lanes].reshape(-1)
    query_scale, key_scale = gains[2 * lanes], gains[2 * lanes + 1]
    inverse_one = inverse_one[:, :1]
    inputs = tokens.reshape(rows, width).astype(jnp.float32)
    normal_one = inputs * inverse_one
    cosine = cosine.reshape(rows, 1, HD)
    sine = sine.reshape(rows, 1, HD)
    query_raw = raw[:, : H * HD].reshape(rows, H, HD)
    key_raw = raw[:, H * HD :].reshape(rows, KVH, HD)
    query_inverse = lax.rsqrt(jnp.mean(query_raw * query_raw, axis=-1, keepdims=True) + EPSILON)
    query_unit = query_raw * query_inverse
    key_inverse = lax.rsqrt(jnp.mean(key_raw * key_raw, axis=-1, keepdims=True) + EPSILON)
    key_unit = key_raw * key_inverse
    row_totals = totals.reshape(KVH, 2, ratio, BLK).transpose(1, 3, 0, 2).reshape(rows, H, 1)
    middle = inputs + plain_dot(attended_low, full_output)
    inverse_two = lax.rsqrt(jnp.mean(middle * middle, axis=-1, keepdims=True) + EPSILON)
    normal_two = middle * inverse_two
    normed_two = (normal_two * gain_two).astype(low)
    both = plain_dot(normed_two, full_gu)
    gate, upper = both[:, :hidden_width], both[:, hidden_width:]
    sigmoid_gate = jax.nn.sigmoid(gate)
    activated = gate * sigmoid_gate
    hidden = (activated * upper).astype(low)
    output = (middle + plain_dot(hidden, full_down)).astype(low).reshape(groups, rows, width)

    upstream = cotangent.reshape(rows, width)
    grad_hidden = right_dot(upstream, full_down)
    grad_gate = (grad_hidden * upper * sigmoid_gate * (1.0 + gate * (1.0 - sigmoid_gate))).astype(low)
    grad_upper = (grad_hidden * activated).astype(low)
    grad_both = jnp.concatenate([grad_gate, grad_upper], axis=1)
    grad_down = chip_sums(hidden, upstream, swapped(upstream))
    grad_gu = chip_sums(normed_two, grad_both, swapped(grad_both))
    grad_normed_two = right_dot(grad_both, full_gu)
    grad_gain_two = jnp.sum(grad_normed_two * normal_two, axis=0)
    grad_middle = upstream.astype(jnp.float32) + norm_back(grad_normed_two, normal_two, inverse_two, gain_two)
    f32 = jnp.float32
    branch_grad = grad_middle.astype(low)
    grad_woutput = chip_sums(attended_low, branch_grad, swapped(branch_grad))
    grad_attended = right_dot(branch_grad, full_output).reshape(rows, H, HD)
    grad_summed = (grad_attended / row_totals).astype(low).reshape(rows, H * HD)
    drift = jnp.sum(grad_attended * attended.reshape(rows, H, HD), axis=-1) / row_totals[..., 0]
    drift = drift.reshape(2, BLK, KVH, ratio).transpose(2, 0, 3, 1).reshape(KVH, 2, ratio * BLK)
    grad_query, grad_keys, grad_values = attention_back(
        table, pairs, query_low, key_all, value_all, grad_summed, drift
    )
    f32 = jnp.float32
    own_keys, own_values, out_gu, out_down, out_output = scatter(
        grid,
        [SLOT_AXES] * 2 + [CHIP_AXES] * 3,
        [
            (0, 0, KVH * HD, AB),
            (1, 0, KVH * HD, BA),
            (2, 0, hidden_width, BFA),
            (2, hidden_width, 2 * hidden_width, AFB),
            (3, 0, width // 2, BFA),
            (3, width // 2, width, AFB),
            (4, 0, width // 2, BFA),
            (4, width // 2, width, AFB),
        ],
        "scatter_mlp",
        (f32, low, f32, f32, f32),
        grad_keys,
        grad_values,
        grad_gu,
        grad_down,
        grad_woutput,
    )
    grad_qrot = grad_query.reshape(rows, H, HD)
    grad_qnormed = grad_qrot * cosine + unrotate(grad_qrot) * sine
    grad_qscale = jnp.sum(grad_qnormed * query_unit, axis=(0, 1))
    grad_qraw = norm_back(grad_qnormed, query_unit, query_inverse, query_scale)
    grad_krot = own_keys.reshape(rows, KVH, HD)
    grad_knormed = grad_krot * cosine + unrotate(grad_krot) * sine
    grad_kscale = jnp.sum(grad_knormed * key_unit, axis=(0, 1))
    grad_kraw = norm_back(grad_knormed, key_unit, key_inverse, key_scale)
    grad_raw = jnp.concatenate(
        [
            grad_qraw.reshape(rows, H * HD).astype(low),
            grad_kraw.reshape(rows, KVH * HD).astype(low),
            own_values,
        ],
        axis=1,
    )
    grad_wqkv = chip_sums(normed, grad_raw, swapped(grad_raw))
    grad_normed = right_dot(grad_raw, full_qkv)
    grad_gain_one = jnp.sum(grad_normed * normal_one, axis=0)
    grad_inputs = grad_middle + norm_back(grad_normed, normal_one, inverse_one, gain_one)
    out_qkv, out_gains = scatter(
        grid,
        [CHIP_AXES, ALL_AXES],
        [
            (0, 0, half // 2, FAB),
            (0, half // 2, half, FBA),
            (0, half, 3 * half // 2, BFA),
            (0, 3 * half // 2, 2 * half, AFB),
            (1, 0, 128, FAB + CORE),
        ],
        "scatter_attention",
        (f32, f32),
        grad_wqkv,
        gain_rows(total, grad_gain_one, grad_qscale, grad_kscale, grad_gain_two),
    )
    return (
        output,
        grad_inputs.astype(low).reshape(groups, rows, width),
        out_gains[0, : attn_gain.shape[0]],
        out_qkv[:, : H * HD],
        out_qkv[:, H * HD : (H + KVH) * HD],
        out_qkv[:, (H + KVH) * HD :],
        out_gains[1, : query_gain.shape[0]],
        out_gains[2, : key_gain.shape[0]],
        out_output,
        out_gains[3, : mlp_gain.shape[0]],
        out_gu[:, :hidden_width],
        out_gu[:, hidden_width:],
        out_down,
    )


def solution(mesh):
    return jax.shard_map(
        on_device,
        mesh=mesh,
        in_specs=(
            P("fsdp", "ctx", None),
            P("fsdp", "ctx", None),
            P("fsdp", None),
            P(("ctx", "fsdp")),
            P(("ctx", "fsdp"), None),
            P(("ctx", "fsdp"), None),
            P(("ctx", "fsdp"), None),
            P(("ctx", "fsdp")),
            P(("ctx", "fsdp")),
            P(("ctx", "fsdp"), None),
            P(("ctx", "fsdp")),
            P(("ctx", "fsdp"), None),
            P(("ctx", "fsdp"), None),
            P(("ctx", "fsdp"), None),
        ),
        out_specs=(
            P("fsdp", "ctx", None),
            P("fsdp", "ctx", None),
            P(("ctx", "fsdp")),
            P(("ctx", "fsdp"), None),
            P(("ctx", "fsdp"), None),
            P(("ctx", "fsdp"), None),
            P(("ctx", "fsdp")),
            P(("ctx", "fsdp")),
            P(("ctx", "fsdp"), None),
            P(("ctx", "fsdp")),
            P(("ctx", "fsdp"), None),
            P(("ctx", "fsdp"), None),
            P(("ctx", "fsdp"), None),
        ),
        check_vma=False,
    )
```

```python
import functools
import math

import jax
import jax.numpy as jnp
from jax import lax
from jax.experimental import pallas as pl
from jax.experimental.pallas import tpu as pltpu
from jax.sharding import PartitionSpec as P

MESH = pl.DeviceIdType.MESH
ANY = pl.BlockSpec(memory_space=pl.ANY)


H = 16
KVH = 8
HD = 128
BLK = 128


EPSILON = 1e-06
ROPE_BASE = 1000000.0


def rope_tables(positions):
    half = HD // 2
    freqs = jnp.exp(jnp.arange(half, dtype=jnp.float32) * (-2.0 * math.log(ROPE_BASE) / HD))
    angles = positions.astype(jnp.float32)[..., None] * freqs
    cosine = jnp.cos(angles)
    sine = jnp.sin(angles)
    return (jnp.concatenate([cosine, cosine], axis=-1), jnp.concatenate([sine, sine], axis=-1))


def rotate(value_vectors):
    half = value_vectors.shape[-1] // 2
    return jnp.concatenate([-value_vectors[..., half:], value_vectors[..., :half]], axis=-1)


def unrotate(value_vectors):
    half = value_vectors.shape[-1] // 2
    return jnp.concatenate([value_vectors[..., half:], -value_vectors[..., :half]], axis=-1)


def left_dot(left, right):
    return lax.dot_general(
        left, right, (((0,), (0,)), ((), ())), preferred_element_type=jnp.float32
    )


def right_dot(left, right):
    return lax.dot_general(
        left, right, (((1,), (1,)), ((), ())), preferred_element_type=jnp.float32
    )


def plain_dot(left, right):
    return jnp.dot(left, right, preferred_element_type=jnp.float32)


def norm_back(grad_normed, unit, inverse, gain):
    scaled = grad_normed * gain
    return inverse * (scaled - unit * jnp.mean(scaled * unit, axis=-1, keepdims=True))


class Grid:
    def __init__(self, ctx, fsdp):
        self.sizes = {"a": ctx // 4, "b": 2, "core": 2, "f": fsdp}
        self.stride = {"a": 4, "b": 2, "core": 1}

    def enter(self):
        self.c = lax.axis_index("ctx")
        self.at = {
            "a": self.c // 4,
            "b": (self.c // 2) % 2,
            "core": self.c % 2,
            "f": lax.axis_index("fsdp"),
        }

    def barrier(self):
        sem = pltpu.get_barrier_semaphore()
        count = 0
        for axis in ("core", "b", "a", "f"):
            n, p = self.sizes[axis], self.at[axis]
            for step in (1,) if n == 2 else (1, n - 1):
                pl.semaphore_signal(
                    sem, inc=1, device_id=self.peer(axis, lax.rem(p + step, n)), device_id_type=MESH
                )
                count += 1
        pl.semaphore_wait(sem, count)

    def peer(self, axis, place):
        if axis == "f":
            return {"fsdp": place}
        return {"ctx": self.c + (place - self.at[axis]) * self.stride[axis]}

    def sources(self, axis):
        n, p = self.sizes[axis], self.at[axis]
        if n == 2:
            return [(None, 1 - p, None, None)]
        found = []
        for step in range(1, n):
            for way in (1, -1):
                origin = p - way * step
                onward = p + way
                found.append(
                    (
                        jnp.logical_and(origin >= 0, origin < n),
                        origin,
                        onward,
                        jnp.logical_and(
                            jnp.logical_and(origin >= 0, origin < n),
                            jnp.logical_and(onward >= 0, onward < n),
                        ),
                    )
                )
        return found

    def around(self, axis):
        n, p = self.sizes[axis], self.at[axis]
        if n == 2:
            return [(None, 1 - p)]
        return [(p + 1 < n, p + 1), (p >= 1, p - 1)]

    def nearest(self, axis):
        n, p = self.sizes[axis], self.at[axis]
        if n == 2:
            return [p, 1 - p]
        order = [0]
        for step in range(1, n):
            for way in (step, n - step):
                if way not in order:
                    order.append(way)
        return [lax.rem(p + s, n) for s in order]


class Pool:
    def __init__(self, ref):
        self.ref, self.used = ref, 0

    def take(self, count):
        first = self.used
        self.used += count
        return self.ref.at[pl.ds(first, count)]


def guarded(cond, body):
    if cond is None:
        body()
    else:
        pl.when(cond)(body)


class Gather:
    def __init__(self, grid, order, src, dst, columns, send_sem, recv_sem, layout_axes):
        self.grid, self.order, self.src, self.dst = grid, order, src, dst
        self.columns, self.send_sem, self.recv_sem = columns, send_sem, recv_sem
        self.layout_axes = layout_axes
        self.sends = 0
        self.pending = []

    @staticmethod
    def semaphores(grid, order):
        near = {x: 1 if grid.sizes[x] == 2 else 2 for x in order}
        far = {x: 0 if grid.sizes[x] == 2 else 2 * (grid.sizes[x] - 1) for x in order}
        sends = near[order[0]] + far[order[0]] + sum(near[x] for x in order[1:])
        inner = 1
        for level in range(1, len(order)):
            axis = order[level]
            onward = sum(near[x] for x in order[level + 1 :])
            sends += inner * (far[axis] + max(far[axis], 1) * onward)
            inner *= grid.sizes[axis]
        return sends, grid.sizes[order[0]] + inner

    def view(self, places):
        idx = tuple(places.get(x, slice(None)) for x in self.layout_axes)
        return self.dst.at[idx + (slice(None), self.columns)]

    def unit_number(self, places):
        number = 0
        for x in self.order[1:]:
            number = number * self.grid.sizes[x] + places[x]
        return number

    def start(self, cond, view, axis, place, sem):
        slot = self.sends
        self.sends += 1

        def make():
            return pltpu.make_async_remote_copy(
                src_ref=view[0],
                dst_ref=view[1],
                send_sem=self.send_sem.at[slot],
                recv_sem=self.recv_sem.at[sem],
                device_id=self.grid.peer(axis, place),
                device_id_type=MESH,
            )

        guarded(cond, lambda: make().start())
        self.pending.append((cond, make))

    def wait_recv(self, view, sem):
        pltpu.make_async_remote_copy(
            src_ref=view,
            dst_ref=view,
            send_sem=self.send_sem.at[0],
            recv_sem=self.recv_sem.at[sem],
            device_id={},
            device_id_type=MESH,
        ).wait_recv()

    def own_places(self):
        return {x: self.grid.at[x] for x in self.order}

    def open(self):
        axis = self.order[0]
        own = self.view(self.own_places())
        for cond, place in self.grid.around(axis):
            self.start(cond, (self.src, own), axis, place, self.grid.at[axis])

    def first(self):
        axis = self.order[0]
        for cond, origin, onward, more in self.grid.sources(axis):
            view = self.view({**self.own_places(), axis: origin})
            guarded(cond, lambda: self.wait_recv(view, origin))
            if onward is not None:
                self.start(more, (view, view), axis, onward, origin)
        self.pass_on(None, 1, {x: self.grid.at[x] for x in self.order[1:]})

    def pass_on(self, cond, level, places):
        n1 = self.grid.sizes[self.order[0]]
        sem = n1 + self.unit_number(places)
        view = self.view(places)
        for axis in self.order[level:]:
            for near, place in self.grid.around(axis):
                both = near if cond is None else cond if near is None else jnp.logical_and(cond, near)
                self.start(both, (view, view), axis, place, sem)

    def arrivals(self, level):
        n1 = self.grid.sizes[self.order[0]]
        axis = self.order[level]
        inner = [{}]
        for x in self.order[1:level]:
            inner = [{**places, x: j} for places in inner for j in self.grid.nearest(x)]
        fixed = {x: self.grid.at[x] for x in self.order[level + 1 :]}
        for places in inner:
            for cond, origin, onward, more in self.grid.sources(axis):
                unit = {**places, **fixed, axis: origin}
                view = self.view(unit)
                sem = n1 + self.unit_number(unit)
                guarded(cond, lambda: self.wait_recv(view, sem))
                if onward is not None:
                    self.start(more, (view, view), axis, onward, sem)
                self.pass_on(cond, level + 1, unit)

    def close(self):
        for cond, make in self.pending:
            guarded(cond, lambda: make().wait_send())


def add_into(total, term, out=None):
    shape = total.shape
    rows = min(16, shape[-2])
    steps = shape[-2] // rows
    lead = math.prod(shape[:-2])

    def body(i, carry):
        index = ()
        rest = i // steps
        for n in reversed(shape[:-2]):
            index = (lax.rem(rest, n),) + index
            rest = rest // n
        at = index + (pl.ds(pl.multiple_of(lax.rem(i, steps) * rows, rows), rows), slice(None))
        value = total[at].astype(jnp.float32)
        if term is not None:
            value = value + term[at].astype(jnp.float32)
        if out is None:
            total[at] = value.astype(total.dtype)
        else:
            out[at] = value.astype(out.dtype)
        return carry

    lax.fori_loop(0, lead * steps, body, 0)


class Scatter:
    def __init__(self, grid, order, src, columns, own, recvs, load_sem, send_sem, recv_sem, out, layout_axes):
        self.grid, self.order, self.src, self.columns = grid, order, src, columns
        self.own, self.recvs, self.out = own, recvs, out
        self.load_sem, self.send_sem, self.recv_sem = load_sem, send_sem, recv_sem
        self.layout_axes = layout_axes
        self.sends = 0
        self.pending = []
        self.base = {}
        number = 0
        for level in range(len(order) - 1, -1, -1):
            self.base[level] = number
            number += self.slots(grid, order, level)

    @staticmethod
    def kept(grid, order):
        return order[1:-1] if grid.sizes[order[-1]] == 2 else order[1:]

    @staticmethod
    def inner(grid, order, level):
        return [grid.sizes[x] for x in order[1:level]]

    @staticmethod
    def slots(grid, order, level):
        n = grid.sizes[order[level]]
        lines = 1 if n == 2 else n + 1
        return lines * math.prod(Scatter.inner(grid, order, level))

    @staticmethod
    def scratch(grid, order, rows, columns, dtype):
        n1 = grid.sizes[order[0]]
        own = tuple(grid.sizes[x] for x in Scatter.kept(grid, order)) + (n1, rows, columns)
        recvs = []
        for level in range(len(order)):
            n = grid.sizes[order[level]]
            lead = () if n == 2 else (n + 1,)
            block = (rows, columns) if level == 0 else (n1, rows, columns)
            recvs.append(lead + tuple(Scatter.inner(grid, order, level)) + block)
        return [pltpu.VMEM(s, dtype) for s in [own] + recvs]

    @staticmethod
    def semaphores(grid, order):
        loads = math.prod(grid.sizes[x] for x in Scatter.kept(grid, order))
        slots = [Scatter.slots(grid, order, level) for level in range(len(order))]
        sends = [
            (1 if grid.sizes[x] == 2 else 2 * (grid.sizes[x] - 1))
            * math.prod(Scatter.inner(grid, order, level))
            for level, x in enumerate(order)
        ]
        return loads, sum(sends), sum(slots)

    def hbm(self, places):
        idx = tuple(places.get(x, slice(None)) for x in self.layout_axes)
        return self.src.at[idx + (slice(None), self.columns)]

    def units(self, level, first=None):
        found = [{}]
        for x in self.order[1:level]:
            found = [{**places, x: j} for places in found for j in reversed(self.grid.nearest(x))]
        return found

    def mine(self, places):
        idx = tuple(places.get(x, self.grid.at[x]) for x in self.kept(self.grid, self.order))
        return self.own.at[idx]

    def number(self, places, axes):
        value = 0
        for x in axes:
            value = value * self.grid.sizes[x] + places[x]
        return value

    def slot(self, level, places, way=None, target=None):
        axes = self.order[1:level]
        idx = tuple(places[x] for x in axes)
        inner = math.prod(self.grid.sizes[x] for x in axes)
        number = self.number(places, axes)
        if way is not None:
            line = target + 1 - way
            idx = (line,) + idx
            number = line * inner + number
        ref = self.recvs[level]
        return (ref.at[idx] if idx else ref), self.recv_sem.at[self.base[level] + number]

    def send(self, cond, view, landing, axis, place):
        slot = self.sends
        self.sends += 1
        ref, sem = landing

        def make():
            return pltpu.make_async_remote_copy(
                src_ref=view,
                dst_ref=ref,
                send_sem=self.send_sem.at[slot],
                recv_sem=sem,
                device_id=self.grid.peer(axis, place),
                device_id_type=MESH,
            )

        guarded(cond, lambda: make().start())
        self.pending.append((cond, make))

    def take(self, cond, landing, total, out=None):
        ref, sem = landing

        def body():
            pltpu.make_async_remote_copy(
                src_ref=ref,
                dst_ref=ref,
                send_sem=self.send_sem.at[0],
                recv_sem=sem,
                device_id={},
                device_id_type=MESH,
            ).wait_recv()
            add_into(total, ref, out)

        guarded(cond, body)

    def load(self, places):
        axes = self.kept(self.grid, self.order)
        here = {self.order[-1]: self.grid.at[self.order[-1]], **places}
        return pltpu.make_async_copy(
            self.hbm(here), self.mine(places), self.load_sem.at[self.number(places, axes)]
        )

    def open(self):
        top = len(self.order) - 1
        axis = self.order[top]
        if self.grid.sizes[axis] > 2:
            for places in self.units(top + 1):
                self.load(places).start()
            return
        there = 1 - self.grid.at[axis]
        for places in self.units(top):
            self.send(None, self.hbm({**places, axis: there}), self.slot(top, places), axis, there)
            self.load(places).start()

    def settle(self, level, places):
        above = level + 1
        top = len(self.order) - 1
        total = self.mine(places)
        if above > top:
            self.load(places).wait()
            return
        if above == top and self.grid.sizes[self.order[top]] == 2:
            self.load(places).wait()
            self.take(None, self.slot(above, places), total)
            return
        axis = self.order[above]
        n, p = self.grid.sizes[axis], self.grid.at[axis]
        if n == 2:
            self.take(None, self.slot(above, places), total)
        else:
            self.take(p >= 1, self.slot(above, places, 0, p), total)
            self.take(p + 1 < n, self.slot(above, places, 1, p), total)

    def levels(self):
        top = len(self.order) - 1
        return top if self.grid.sizes[self.order[top]] == 2 else top + 1

    def step(self, level):
        axis = self.order[level]
        n, p = self.grid.sizes[axis], self.grid.at[axis]
        if level == 0:
            self.settle(0, {})
            whole = self.mine({})
            self.along(level, {}, lambda t: whole.at[t])
            return
        for places in self.units(level):
            self.along(level, places, lambda t: self.mine({**places, axis: t}))
            self.settle(level, {**places, axis: p})

    def along(self, level, places, view):
        axis = self.order[level]
        n, p = self.grid.sizes[axis], self.grid.at[axis]
        if n == 2:
            if level:
                self.settle(level, {**places, axis: 1 - p})
            self.send(None, view(1 - p), self.slot(level, places), axis, 1 - p)
            return
        for s in range(n - 1):
            for way, t in ((0, n - 1 - s), (1, s)):
                wanted = (t > p) if way == 0 else (t < p)
                behind = (p >= 1) if way == 0 else (p + 1 < n)
                if level:
                    pl.when(wanted)(lambda: self.settle(level, {**places, axis: t}))
                self.take(jnp.logical_and(wanted, behind), self.slot(level, places, way, t), view(t))
                self.send(wanted, view(t), self.slot(level, places, way, t), axis, p + (1 if way == 0 else -1))

    def finish(self):
        axis = self.order[0]
        n, p = self.grid.sizes[axis], self.grid.at[axis]
        total = self.mine({}).at[p]
        if n == 2:
            self.take(None, self.slot(0, {}), total, self.out)
            return
        self.take(p >= 1, self.slot(0, {}, 0, p), total)
        self.take(p + 1 < n, self.slot(0, {}, 1, p), total)
        add_into(total, None, self.out)

    def close(self):
        for cond, make in self.pending:
            guarded(cond, lambda: make().wait_send())


def half_pairs(ref, s):
    rows = pl.ds(s * BLK, BLK)
    return jnp.concatenate([ref[rows, :HD], ref[rows, HD:]], axis=0)


def items(table, pairs):
    high_slot, high = table[pairs * 2], table[pairs * 2 + 1]
    low_block = 2 * pairs - 1 - high
    split = high // 2
    found = []
    for w in range(pairs - 1):
        upper = w < split
        found.append((jnp.where(upper, high_slot, 1 - high_slot), jnp.where(upper, w, w - split), None))
    found.append((high_slot, split, high))
    found.append((1 - high_slot, low_block // 2, low_block))
    return found


def chunk_of(ref, table, c):
    return jnp.concatenate(
        [ref[pl.ds(pl.multiple_of(table[2 * c + i] * BLK, BLK), BLK), :] for i in range(2)], axis=0
    )


def row_contract(left, right):
    return lax.dot_general(left, right, (((1,), (1,)), ((), ())), preferred_element_type=jnp.float32)


def attention_kernel(pairs, table, q_ref, k_ref, v_ref, o_ref, low_ref, t_ref, qs, acc, tot):
    for s in range(2):
        qs[s] = half_pairs(q_ref, s)
    acc[...] = jnp.zeros_like(acc)
    tot[...] = jnp.zeros_like(tot)
    for s, c, block in items(table, pairs):
        keys = chunk_of(k_ref, table, c)
        vals = chunk_of(v_ref, table, c)
        scores = row_contract(qs[s], keys) * (HD ** (-0.5) * math.log2(math.e))
        weights = jnp.exp2(scores)
        if block is not None:
            rows = lax.broadcasted_iota(jnp.int32, (2 * BLK, 2 * BLK), 0)
            cols = lax.broadcasted_iota(jnp.int32, (2 * BLK, 2 * BLK), 1)
            allowed = cols <= lax.rem(rows, BLK) + (block - 2 * c) * BLK
            weights = jnp.where(allowed, weights, 0.0)
        tot[s] += weights[:, :HD] + weights[:, HD:]
        acc[s] += jnp.dot(weights.astype(jnp.bfloat16), vals, preferred_element_type=jnp.float32)
    for s in range(2):
        total = tot[s]
        value = acc[s] / jnp.sum(total, axis=1, keepdims=True)
        rows = pl.ds(s * BLK, BLK)
        for i in range(2):
            part = value[i * BLK : (i + 1) * BLK]
            o_ref[rows, i * HD : (i + 1) * HD] = part
            low_ref[rows, i * HD : (i + 1) * HD] = part.astype(jnp.bfloat16)
        t_ref[0, s : s + 1, :] = jnp.sum(total.T, axis=0, keepdims=True)


def attention(table, pairs, queries, keys, values):
    rows, length = queries.shape[0], keys.shape[0]
    head = pl.BlockSpec((rows, 2 * HD), lambda h, t: (0, h))
    side = pl.BlockSpec((length, HD), lambda h, t: (0, h))
    stats = pl.BlockSpec((1, 2, 2 * BLK), lambda h, t: (h, 0, 0))
    return pl.pallas_call(
        functools.partial(attention_kernel, pairs),
        grid_spec=pltpu.PrefetchScalarGridSpec(
            num_scalar_prefetch=1,
            grid=(KVH,),
            in_specs=[head, side, side],
            out_specs=[head, head, stats],
            scratch_shapes=[
                pltpu.VMEM((2, 2 * BLK, HD), jnp.bfloat16),
                pltpu.VMEM((2, 2 * BLK, HD), jnp.float32),
                pltpu.VMEM((2, 2 * BLK, HD), jnp.float32),
            ],
        ),
        out_shape=[
            jax.ShapeDtypeStruct((rows, H * HD), jnp.float32),
            jax.ShapeDtypeStruct((rows, H * HD), jnp.bfloat16),
            jax.ShapeDtypeStruct((KVH, 2, 2 * BLK), jnp.float32),
        ],
        name="attention",
    )(table, queries, keys, values)


def attention_back_kernel(
    pairs, table, q_ref, k_ref, v_ref, g_ref, d_ref, dq_ref, dk_ref, dv_ref, qs, gs, dq, dk, dv
):
    scale = HD ** (-0.5)
    for s in range(2):
        qs[s] = half_pairs(q_ref, s)
        gs[s] = half_pairs(g_ref, s)
    for total in (dq, dk, dv):
        total[...] = jnp.zeros_like(total)
    for s, c, block in items(table, pairs):
        keys = chunk_of(k_ref, table, c)
        vals = chunk_of(v_ref, table, c)
        queries, grads = qs[s], gs[s]
        weights = jnp.exp2(row_contract(keys, queries) * (scale * math.log2(math.e)))
        if block is not None:
            rows = lax.broadcasted_iota(jnp.int32, (2 * BLK, 2 * BLK), 0)
            cols = lax.broadcasted_iota(jnp.int32, (2 * BLK, 2 * BLK), 1)
            allowed = rows <= lax.rem(cols, BLK) + (block - 2 * c) * BLK
            weights = jnp.where(allowed, weights, 0.0)
        through = row_contract(vals, grads)
        scores = (weights * (through - d_ref[0, pl.ds(s, 1), :])).astype(jnp.bfloat16)
        to_values = jnp.dot(weights.astype(jnp.bfloat16), grads, preferred_element_type=jnp.float32)
        to_keys = jnp.dot(scores, queries, preferred_element_type=jnp.float32)
        for i in range(2):
            at = pl.ds(pl.multiple_of(table[2 * c + i] * BLK, BLK), BLK)
            dv[at, :] += to_values[i * BLK : (i + 1) * BLK]
            dk[at, :] += to_keys[i * BLK : (i + 1) * BLK]
        dq[s] += left_dot(scores, keys)
    dk_ref[...] = (dk[...] * scale).astype(jnp.bfloat16)
    dv_ref[...] = dv[...].astype(jnp.bfloat16)
    for s in range(2):
        for i in range(2):
            dq_ref[pl.ds(s * BLK, BLK), i * HD : (i + 1) * HD] = dq[s, i * BLK : (i + 1) * BLK] * scale


def attention_back(table, pairs, queries, keys, values, grads, drift):
    rows, length = queries.shape[0], keys.shape[0]
    head = pl.BlockSpec((rows, 2 * HD), lambda h, t: (0, h))
    side = pl.BlockSpec((length, HD), lambda h, t: (0, h))
    stats = pl.BlockSpec((1, 2, 2 * BLK), lambda h, t: (h, 0, 0))
    return pl.pallas_call(
        functools.partial(attention_back_kernel, pairs),
        grid_spec=pltpu.PrefetchScalarGridSpec(
            num_scalar_prefetch=1,
            grid=(KVH,),
            in_specs=[head, side, side, head, stats],
            out_specs=[head, side, side],
            scratch_shapes=[
                pltpu.VMEM((2, 2 * BLK, HD), jnp.bfloat16),
                pltpu.VMEM((2, 2 * BLK, HD), jnp.bfloat16),
                pltpu.VMEM((2, 2 * BLK, HD), jnp.float32),
                pltpu.VMEM((length, HD), jnp.float32),
                pltpu.VMEM((length, HD), jnp.float32),
            ],
        ),
        out_shape=[
            jax.ShapeDtypeStruct((rows, H * HD), jnp.float32),
            jax.ShapeDtypeStruct((length, KVH * HD), jnp.bfloat16),
            jax.ShapeDtypeStruct((length, KVH * HD), jnp.bfloat16),
        ],
        name="attention_back",
    )(table, queries, keys, values, grads, drift)


ALL_AXES = ("a", "b", "core", "f")
SLOT_AXES = ("a", "b", "core")
CHIP_AXES = ("a", "b", "f")
BFA, AFB, FAB, FBA = ("b", "f", "a"), ("a", "f", "b"), ("f", "a", "b"), ("f", "b", "a")
ABF, BAF = ("a", "b", "f"), ("b", "a", "f")
AB, BA = ("a", "b", "core"), ("b", "a", "core")
CORE = ("core",)


FRONT_SRC = ("q", "k", "v", "o", "g", "u", "d", "gains")


def front_kernel(grid, plan, *refs):
    n = len(FRONT_SRC)
    src = dict(zip(FRONT_SRC, refs[:n]))
    tokens_ref, cosine_ref, sine_ref = refs[n : n + 3]
    outs = refs[n + 3 : n + 15]
    wqkv_ref, wo_ref, wgu_ref, wd_ref, allgains_ref, k_out, v_out = outs[:7]
    normed_ref, gains_ref, raw_ref, qlow_ref, inv_ref = outs[7:]
    scratch = refs[n + 15 :]
    held = dict(zip(FRONT_SRC, scratch[:n]))
    weights, klow, vlow, gbuf = scratch[n : n + 4]
    send, recv, local, load = scratch[n + 4 :]
    grid.enter()
    grid.barrier()
    send, recv = Pool(send), Pool(recv)
    width = tokens_ref.shape[1]
    rows = tokens_ref.shape[0]
    spans = {"q": (wqkv_ref, 0), "k": (wqkv_ref, H * HD), "v": (wqkv_ref, (H + KVH) * HD)}
    hidden = src["g"].shape[1]
    spans.update({"o": (wo_ref, 0), "g": (wgu_ref, 0), "u": (wgu_ref, hidden), "d": (wd_ref, 0)})
    spans["gains"] = (allgains_ref, 0)
    mine = tuple(grid.at[x] for x in ALL_AXES)

    def own_copy(i, name):
        dst, at = spans[name]
        return pltpu.make_async_copy(
            held[name], dst.at[mine + (slice(None), pl.ds(at, src[name].shape[1]))], local.at[i]
        )

    for i, name in enumerate(FRONT_SRC):
        pltpu.make_async_copy(src[name], held[name], local.at[i]).start()

    def part(name, low, high, order):
        dst, at = spans[name]
        sends, takes = Gather.semaphores(grid, order)
        columns = pl.ds(at + low, high - low)
        return Gather(
            grid, order, src[name].at[:, low:high], dst, columns, send.take(sends), recv.take(takes), ALL_AXES
        )

    early = [part(*p) for p in plan[0]]
    late = [part(*p) for p in plan[1]]
    for p in early:
        p.open()
    for p in late:
        p.open()
    for i, name in enumerate(FRONT_SRC):
        pltpu.make_async_copy(src[name], held[name], local.at[i]).wait()
        own_copy(i, name).start()
    inputs = tokens_ref[...].astype(jnp.float32)
    inverse = lax.rsqrt(jnp.mean(inputs * inputs, axis=-1, keepdims=True) + EPSILON)
    inv_ref[...] = jnp.broadcast_to(inverse, (rows, 128))
    for i, name in enumerate(FRONT_SRC):
        own_copy(i, name).wait()

    for p in early:
        p.first()
    for level in (1, 2):
        for p in early:
            p.arrivals(level)
    pump = []
    for p in late:
        pump.append(p.first)
    for level in (1, 2, 3):
        for p in late:
            pump.append(functools.partial(p.arrivals, level))

    def step(count):
        for _ in range(count):
            if pump:
                pump.pop(0)()

    step(len(late))
    for p in early:
        p.arrivals(3)

    places = math.prod(grid.sizes[x] for x in ALL_AXES)
    copy = pltpu.make_async_copy(allgains_ref, gbuf, load.at[0])
    copy.start()
    big = pltpu.make_async_copy(wqkv_ref, weights, load.at[1])
    big.start()
    copy.wait()
    blocks = gbuf[...].reshape((places,) + gbuf.shape[-2:]).astype(jnp.float32)
    gains = jnp.sum(blocks, axis=0)
    gains_ref[...] = gains
    lanes = width // 128
    for j in range(lanes):
        cols = slice(j * 128, (j + 1) * 128)
        part_of = tokens_ref[:, cols].astype(jnp.float32) * inv_ref[...] * gains_ref[j : j + 1, :]
        normed_ref[:, cols] = part_of.astype(jnp.bfloat16)
    big.wait()
    step(1)
    flat = weights.reshape(width, weights.shape[-1])
    normed = normed_ref[...]
    chunk = 2 * HD

    def heads(low_out, gain_row, out_at, raw_at, c):
        at = pl.ds(pl.multiple_of(raw_at + c * chunk, chunk), chunk)
        raw = jnp.dot(normed, flat[:, at], preferred_element_type=jnp.float32)
        raw_ref[:, at] = raw
        done = []
        for i in range(2):
            one = raw[:, i * HD : (i + 1) * HD]
            unit = one * lax.rsqrt(jnp.mean(one * one, axis=-1, keepdims=True) + EPSILON)
            unit = unit * gains_ref[gain_row : gain_row + 1, :]
            done.append(unit * cosine_ref[...] + pltpu.roll(unit, HD // 2, 1) * sine_ref[...])
        to = pl.ds(pl.multiple_of(out_at + c * chunk, chunk), chunk)
        low_out[:, to] = jnp.concatenate(done, axis=1).astype(jnp.bfloat16)

    def loop(count, body):
        def once(c, carry):
            body(c)
            return carry

        lax.fori_loop(0, count, once, 0)

    def to_values(c):
        at = pl.ds(pl.multiple_of((H + KVH) * HD + c * chunk, chunk), chunk)
        to = pl.ds(pl.multiple_of(c * chunk, chunk), chunk)
        raw = jnp.dot(normed, flat[:, at], preferred_element_type=jnp.float32)
        vlow[:, to] = raw.astype(jnp.bfloat16)

    loop(KVH // 2, functools.partial(heads, klow, 2 * lanes + 1, 0, H * HD))
    loop(KVH // 2, to_values)

    def pair(source, dst, order):
        sends, takes = Gather.semaphores(grid, order)
        return Gather(
            grid, order, source, dst, pl.ds(0, KVH * HD), send.take(sends), recv.take(takes), SLOT_AXES
        )

    slot = tuple(grid.at[x] for x in SLOT_AXES)
    slabs = [pair(klow, k_out, AB), pair(vlow, v_out, BA)]
    saves = [
        pltpu.make_async_copy(klow, k_out.at[slot], load.at[0]),
        pltpu.make_async_copy(vlow, v_out.at[slot], load.at[1]),
    ]
    for p, save in zip(slabs, saves):
        p.open()
        save.start()
    step(2)
    loop(KVH // 2, functools.partial(heads, qlow_ref, 2 * lanes, 0, 0))
    for p, save in zip(slabs, saves):
        save.wait()
        p.first()
    step(2)
    loop(KVH // 2, functools.partial(heads, qlow_ref, 2 * lanes, H * HD // 2, H * HD // 2))
    for p in slabs:
        p.arrivals(1)
    step(len(pump))
    for p in slabs:
        p.arrivals(2)
    for p in early + late + slabs:
        p.close()


def front(grid, plan, blocks, tokens, cosine, sine):
    n = len(FRONT_SRC)
    rows, width = tokens.shape
    places = tuple(grid.sizes[x] for x in ALL_AXES)
    slots = tuple(grid.sizes[x] for x in SLOT_AXES)
    by = dict(zip(FRONT_SRC, blocks))
    low, f32 = jnp.bfloat16, jnp.float32
    full = (H + 2 * KVH) * HD
    counts = [Gather.semaphores(grid, p[3]) for p in plan[0] + plan[1]]
    counts += [Gather.semaphores(grid, AB), Gather.semaphores(grid, BA)]
    sends, takes = [sum(x) for x in zip(*counts)]
    shape = jax.ShapeDtypeStruct
    vmem = pl.BlockSpec(memory_space=pltpu.VMEM)
    outs = pl.pallas_call(
        functools.partial(front_kernel, grid, plan),
        out_shape=[
            shape(places + (by["q"].shape[0], full), low),
            shape(places + by["o"].shape, low),
            shape(places + (by["g"].shape[0], 2 * by["g"].shape[1]), low),
            shape(places + by["d"].shape, low),
            shape(places + by["gains"].shape, low),
            shape(slots + (rows, KVH * HD), low),
            shape(slots + (rows, KVH * HD), low),
            shape((rows, width), low),
            shape(by["gains"].shape, f32),
            shape((rows, (H + KVH) * HD), f32),
            shape((rows, H * HD), low),
            shape((rows, 128), f32),
        ],
        in_specs=[ANY] * n + [vmem] * 3,
        out_specs=[ANY] * 7 + [vmem] * 5,
        scratch_shapes=[pltpu.VMEM(x.shape, x.dtype) for x in blocks]
        + [
            pltpu.VMEM(places + (by["q"].shape[0], full), low),
            pltpu.VMEM((rows, KVH * HD), low),
            pltpu.VMEM((rows, KVH * HD), low),
            pltpu.VMEM(places + by["gains"].shape, low),
            pltpu.SemaphoreType.DMA((sends,)),
            pltpu.SemaphoreType.DMA((takes,)),
            pltpu.SemaphoreType.DMA((n,)),
            pltpu.SemaphoreType.DMA((2,)),
        ],
        compiler_params=pltpu.CompilerParams(
            has_side_effects=True, vmem_limit_bytes=60 * 2**20, collective_id=0
        ),
        name="front",
    )(*blocks, tokens, cosine, sine)
    wqkv, wo, wgu, wd, _, keys, vals, normed, gains, raw, qlow, inverse = outs
    flat = [x.reshape(-1, x.shape[-1]) for x in (wqkv, wo, wgu, wd, keys, vals)]
    return flat + [normed, gains, raw, qlow, inverse]


def sums_kernel(core, left, left_other, right, right_other, out):
    lhs = jnp.concatenate([left[...], left_other[...]], axis=0)
    rhs = jnp.concatenate([right[...], right_other[...]], axis=0)
    out[...] = left_dot(lhs, rhs).astype(out.dtype)


def chip_sums(left, left_other, right, right_other):
    rows, width = left.shape
    count = lax.axis_size("ctx")
    block = width // count
    tile = min(1024, right.shape[1])
    if block % 128:
        place = lax.axis_index("ctx") % 2
        halves = [
            lax.dynamic_index_in_dim(x.reshape(rows, count // 2, 2, block), place, 2, False)
            for x in (left, left_other)
        ]
        lhs = jnp.concatenate(halves, axis=0).reshape(2 * rows, width // 2)
        return left_dot(lhs, jnp.concatenate([right, right_other], axis=0)).astype(jnp.bfloat16)
    core = (lax.axis_index("ctx") % 2).astype(jnp.int32)[None]
    lhs = pl.BlockSpec((rows, block), lambda n, j, c: (0, 2 * j + c[0]))
    rhs = pl.BlockSpec((rows, tile), lambda n, j, c: (0, n))
    return pl.pallas_call(
        sums_kernel,
        grid_spec=pltpu.PrefetchScalarGridSpec(
            num_scalar_prefetch=1,
            grid=(right.shape[1] // tile, count // 2),
            in_specs=[lhs, lhs, rhs, rhs],
            out_specs=pl.BlockSpec((block, tile), lambda n, j, c: (j, n)),
        ),
        out_shape=jax.ShapeDtypeStruct((width // 2, right.shape[1]), jnp.bfloat16),
        name="chip_sums",
    )(core, left, left_other, right, right_other)


BACK_SUMS = ("g", "u", "d", "o")


def back_kernel(grid, plan, *refs):
    refs = list(refs)

    def take(n):
        found = refs[:n]
        del refs[:n]
        return found

    src = dict(zip(BACK_SUMS, take(len(BACK_SUMS))))
    gk_ref, gv_ref, wqkv_ref = take(3)
    dq_ref, raw_ref, cos_ref, turn_ref, gains_ref, normed_ref, tokens_ref, inv_ref, mid_ref, gain2_ref = take(10)
    outs = dict(zip(BACK_SUMS + ("q", "k", "v"), take(len(BACK_SUMS) + 3)))
    din_ref, gsum_ref, sums_ref, gall_ref = take(4)
    weights, both_normed, both_raw, own_k, own_v, stage, acc, gbuf, gblock = take(9)
    load, send, recv, misc = [Pool(x) for x in refs[-4:]]
    del refs[-4:]
    scratch = refs
    grid.enter()
    grid.barrier()
    rows, width = tokens_ref.shape
    lanes = width // 128
    core = grid.at["core"]
    chunk = 2 * HD
    misc_sem = [misc.take(1).at[0] for _ in range(12)]

    def make(source, columns, order, out, layout):
        loads, sends, takes = Scatter.semaphores(grid, order)
        own, *recvs = scratch[: 1 + len(order)]
        del scratch[: 1 + len(order)]
        return Scatter(
            grid, order, source, columns, own, recvs,
            load.take(loads), send.take(sends), recv.take(takes), out, layout,
        )

    def portions(group):
        found = []
        for name, low, high, order in group:
            found.append(
                make(src[name], pl.ds(low, high - low), order, outs[name].at[:, low:high], CHIP_AXES)
            )
        return found

    slabs = [
        make(gk_ref, pl.ds(0, KVH * HD), AB, own_k, SLOT_AXES),
        make(gv_ref, pl.ds(0, KVH * HD), BA, own_v, SLOT_AXES),
    ]
    early, late = portions(plan[0]), portions(plan[1])
    last = []
    for name, at, low, high, order in plan[2]:
        last.append(
            make(sums_ref, pl.ds(at + low, high - low), order, outs[name].at[:, low:high], CHIP_AXES)
        )

    def sibling(source, dst, k):
        return pltpu.make_async_remote_copy(
            src_ref=source, dst_ref=dst, send_sem=misc_sem[2 * k], recv_sem=misc_sem[2 * k + 1],
            device_id=grid.peer("core", 1 - core), device_id_type=MESH,
        )

    for p in slabs + early:
        p.open()
    swap_normed = sibling(normed_ref, both_normed.at[1], 0)
    swap_normed.start()
    both_normed[0] = normed_ref[...]
    gblock[...] = jnp.zeros_like(gblock)
    gblock[lanes : 2 * lanes, :] = gain2_ref[...]

    def loop(count, body):
        def once(c, carry):
            body(c)
            return carry

        lax.fori_loop(0, count, once, 0)

    def heads(source, in_at, raw_at, gain_row, c):
        at = pl.ds(pl.multiple_of(raw_at + c * chunk, chunk), chunk)
        grads = source[:, pl.ds(pl.multiple_of(in_at + c * chunk, chunk), chunk)]
        raw = raw_ref[:, at]
        gain = gains_ref[gain_row : gain_row + 1, :]
        done = []
        for i in range(2):
            g = grads[:, i * HD : (i + 1) * HD]
            g = g * cos_ref[...] - pltpu.roll(g, HD // 2, 1) * turn_ref[...]
            one = raw[:, i * HD : (i + 1) * HD]
            inverse = lax.rsqrt(jnp.mean(one * one, axis=-1, keepdims=True) + EPSILON)
            unit = one * inverse
            gblock[gain_row : gain_row + 1, :] += jnp.sum(g * unit, axis=0, keepdims=True)
            done.append(norm_back(g, unit, inverse, gain))
        both_raw[0, :, at] = jnp.concatenate(done, axis=1).astype(jnp.bfloat16)

    loop(H // 4, functools.partial(heads, dq_ref, 0, 0, 2 * lanes))
    for p in slabs:
        p.step(1)
    for p in late[: len(late) // 2]:
        p.open()
    half_q = H * HD // 2
    loop(H // 4, functools.partial(heads, dq_ref, half_q, half_q, 2 * lanes))
    q_cols, kv_cols = pl.ds(0, H * HD), pl.ds(H * HD, 2 * KVH * HD)
    swap_q = sibling(both_raw.at[0, :, q_cols], both_raw.at[1, :, q_cols], 1)
    swap_q.start()
    for p in slabs:
        p.step(0)
    for p in late[len(late) // 2 :]:
        p.open()
    for p in early:
        for level in range(p.levels() - 1, 0, -1):
            p.step(level)
    for p in slabs:
        p.finish()
    loop(KVH // 2, functools.partial(heads, own_k, 0, H * HD, 2 * lanes + 1))
    at = (H + KVH) * HD
    both_raw[0, :, at : at + KVH * HD] = own_v[...].astype(jnp.bfloat16)
    swap_kv = sibling(both_raw.at[0, :, kv_cols], both_raw.at[1, :, kv_cols], 2)
    swap_kv.start()
    for p in late[: len(late) // 2]:
        p.step(1)
    swap_normed.wait()
    swap_q.wait()
    swap_kv.wait()
    flat_normed = both_normed.reshape(2 * rows, width)
    flat_raw = both_raw.reshape(2 * rows, both_raw.shape[-1])
    count = grid.sizes["a"] * grid.sizes["b"]
    block = width // (2 * count)
    piece = block // grid.sizes["f"]
    full = both_raw.shape[-1]
    tile = 512

    for j in range(count):
        if j >= 2:
            pltpu.make_async_copy(
                stage.at[j % 2], sums_ref.at[(j - 2) // 2, (j - 2) % 2], misc_sem[9 + j % 2]
            ).wait()
        lhs = flat_normed[:, pl.ds(pl.multiple_of((2 * j + core) * block, block), block)]

        def sums(c):
            cols = pl.ds(pl.multiple_of(c * tile, tile), tile)
            value = left_dot(lhs, flat_raw[:, cols]).astype(jnp.bfloat16)
            stage[j % 2, :, :, cols] = value.reshape(grid.sizes["f"], piece, tile)

        loop(full // tile, sums)
        pltpu.make_async_copy(stage.at[j % 2], sums_ref.at[j // 2, j % 2], misc_sem[9 + j % 2]).start()
    for j in range(count - 2, count):
        pltpu.make_async_copy(stage.at[j % 2], sums_ref.at[j // 2, j % 2], misc_sem[9 + j % 2]).wait()
    for p in last:
        p.open()
    for p in late[len(late) // 2 :]:
        p.step(1)
    tiles = [
        pltpu.make_async_copy(
            wqkv_ref.at[:, c * tile : (c + 1) * tile], weights.at[c % 2], misc_sem[6 + c % 2]
        )
        for c in range(full // tile)
    ]
    tiles[0].start()
    for c in range(full // tile):
        if c + 1 < full // tile:
            tiles[c + 1].start()
        tiles[c].wait()
        value = right_dot(both_raw[0, :, c * tile : (c + 1) * tile], weights[c % 2])
        acc[...] = value if c == 0 else acc[...] + value
    inverse = inv_ref[...]
    for j in range(lanes):
        cols = slice(j * 128, (j + 1) * 128)
        normal = tokens_ref[:, cols].astype(jnp.float32) * inverse
        gblock[j : j + 1, :] = jnp.sum(acc[:, cols] * normal, axis=0, keepdims=True)
    copy = pltpu.make_async_copy(gblock, gbuf, misc_sem[11])
    copy.start()
    copy.wait()
    order = FAB + CORE
    sends, takes = Gather.semaphores(grid, order)
    spread = Gather(
        grid, order, gbuf, gall_ref, slice(None), send.take(sends), recv.take(takes), ALL_AXES
    )
    spread.open()
    mine = tuple(grid.at[x] for x in ALL_AXES)
    gall_ref[mine] = gblock[...]
    for p in early + late:
        p.step(0)
    for p in last:
        p.step(1)
    spread.first()
    dots = jnp.zeros((rows, 1), jnp.float32)
    for j in range(lanes):
        cols = slice(j * 128, (j + 1) * 128)
        normal = tokens_ref[:, cols].astype(jnp.float32) * inverse
        dots += jnp.sum(acc[:, cols] * gains_ref[j : j + 1, :] * normal, axis=1, keepdims=True)
    dots = dots / width
    for j in range(lanes):
        cols = slice(j * 128, (j + 1) * 128)
        normal = tokens_ref[:, cols].astype(jnp.float32) * inverse
        grad = inverse * (acc[:, cols] * gains_ref[j : j + 1, :] - normal * dots)
        din_ref[:, cols] = (mid_ref[:, cols] + grad).astype(jnp.bfloat16)
    spread.arrivals(1)
    for p in early + late:
        p.finish()
    for p in last:
        p.step(0)
    spread.arrivals(2)
    spread.arrivals(3)
    places = math.prod(grid.sizes[x] for x in ALL_AXES)
    gsum_ref[...] = jnp.sum(gall_ref.reshape((places,) + gblock.shape)[...], axis=0)
    for p in last:
        p.finish()
    for p in slabs + early + late + last:
        p.close()
    spread.close()


def back_scratch(grid, plan, pieces, rows, width):
    low = jnp.bfloat16
    scratch, counts = [], []
    for order in (AB, BA):
        scratch += Scatter.scratch(grid, order, rows, KVH * HD, low)
        counts.append(Scatter.semaphores(grid, order))
    for name, begin, end, order in plan[0] + plan[1] + tuple((p[0],) + p[2:] for p in plan[2]):
        scratch += Scatter.scratch(grid, order, pieces[name], end - begin, low)
        counts.append(Scatter.semaphores(grid, order))
    return scratch, [sum(x) for x in zip(*counts)]


def back_fits(grid, plan, rows, width, hidden, total):
    pieces = {name: width // total for name in ("g", "u", "q", "k", "v")}
    pieces.update({"d": hidden // total, "o": H * HD // total})
    scratch = back_scratch(grid, plan, pieces, rows, width)[0]
    taken = sum(2 * math.prod(x.shape) for x in scratch)
    held = 2 * rows * (11 * width + 3 * (H + 2 * KVH) * HD + 4 * (H + KVH) * HD) + 6 * 2**20
    return taken + held < 62 * 2**20


def back(grid, plan, sums, gk, gv, wqkv, dq, raw, cosine, turned, gains, normed, tokens, inverse, middle, gain2):
    low, f32 = jnp.bfloat16, jnp.float32
    rows, width = tokens.shape
    chips = tuple(grid.sizes[x] for x in CHIP_AXES)
    places = tuple(grid.sizes[x] for x in ALL_AXES)
    slots = tuple(grid.sizes[x] for x in SLOT_AXES)
    blocks = [x.reshape(chips + (x.shape[0] // math.prod(chips), x.shape[1])) for x in sums]
    shape = jax.ShapeDtypeStruct
    vmem = pl.BlockSpec(memory_space=pltpu.VMEM)
    piece = width // math.prod(places)
    pieces = dict(zip(BACK_SUMS, [x.shape[-2] for x in blocks]))
    pieces.update({"q": piece, "k": piece, "v": piece})
    scratch, (loads, sends, takes) = back_scratch(grid, plan, pieces, rows, width)
    more = Gather.semaphores(grid, FAB + CORE)
    full = wqkv.shape[1]
    count = grid.sizes["a"] * grid.sizes["b"]
    outs = pl.pallas_call(
        functools.partial(back_kernel, grid, plan),
        out_shape=[shape(x.shape[-2:], f32) for x in blocks]
        + [shape((piece, n), f32) for n in (H * HD, KVH * HD, KVH * HD)]
        + [
            shape((rows, width), low),
            shape(gains.shape, f32),
            shape(chips + (piece, full), low),
        ],
        in_specs=[ANY] * (len(blocks) + 3) + [vmem] * 10,
        out_specs=[vmem] * (len(blocks) + 5) + [ANY],
        scratch_shapes=[
            pltpu.VMEM(places + gains.shape, f32),
            pltpu.VMEM((2, width, 512), low),
            pltpu.VMEM((2, rows, width), low),
            pltpu.VMEM((2, rows, full), low),
            pltpu.VMEM((rows, KVH * HD), f32),
            pltpu.VMEM((rows, KVH * HD), f32),
            pltpu.VMEM((2, grid.sizes["f"], piece, full), low),
            pltpu.VMEM((rows, width), f32),
            pltpu.VMEM(gains.shape, f32),
            pltpu.VMEM(gains.shape, f32),
        ]
        + scratch
        + [
            pltpu.SemaphoreType.DMA((loads,)),
            pltpu.SemaphoreType.DMA((sends + more[0],)),
            pltpu.SemaphoreType.DMA((takes + more[1],)),
            pltpu.SemaphoreType.DMA((12,)),
        ],
        compiler_params=pltpu.CompilerParams(
            has_side_effects=True, vmem_limit_bytes=63 * 2**20, collective_id=1
        ),
        name="back",
    )(
        *blocks,
        gk.reshape(slots + (rows, KVH * HD)),
        gv.reshape(slots + (rows, KVH * HD)),
        wqkv, dq, raw, cosine, turned, gains, normed, tokens, inverse, middle, gain2,
    )
    return outs


def scatter_kernel(grid, portions, layouts, n, *refs):
    srcs, outs, scratch = refs[:n], refs[n : 2 * n], list(refs[2 * n : -3])
    load, send, recv = [Pool(x) for x in refs[-3:]]
    grid.enter()
    parts = []
    for i, low, high, order in portions:
        loads, sends, takes = Scatter.semaphores(grid, order)
        own, *recvs = scratch[: 1 + len(order)]
        del scratch[: 1 + len(order)]
        parts.append(
            Scatter(
                grid,
                order,
                srcs[i],
                pl.ds(low, high - low),
                own,
                recvs,
                load.take(loads),
                send.take(sends),
                recv.take(takes),
                outs[i].at[:, low:high],
                layouts[i],
            )
        )
        parts[-1].open()
    for level in (2, 1, 0):
        for part in parts:
            if level < part.levels():
                part.step(level)
    for part in parts:
        part.finish()
    for part in parts:
        part.close()


def scatter(grid, layouts, portions, name, dtypes, *sums):
    n = len(sums)
    blocks = []
    for layout, x in zip(layouts, sums):
        places = tuple(grid.sizes[axis] for axis in layout)
        blocks.append(x.reshape(places + (x.shape[0] // math.prod(places), x.shape[1])))
    loads, sends, takes = [sum(x) for x in zip(*[Scatter.semaphores(grid, p[3]) for p in portions])]
    scratch = []
    for i, low, high, order in portions:
        scratch += Scatter.scratch(grid, order, blocks[i].shape[-2], high - low, blocks[i].dtype)
    return pl.pallas_call(
        functools.partial(scatter_kernel, grid, portions, layouts, n),
        out_shape=[jax.ShapeDtypeStruct(x.shape[-2:], t) for x, t in zip(blocks, dtypes)],
        in_specs=[ANY] * n,
        out_specs=[pl.BlockSpec(memory_space=pltpu.VMEM)] * n,
        scratch_shapes=scratch
        + [
            pltpu.SemaphoreType.DMA((loads,)),
            pltpu.SemaphoreType.DMA((sends,)),
            pltpu.SemaphoreType.DMA((takes,)),
        ],
        compiler_params=pltpu.CompilerParams(has_side_effects=True, vmem_limit_bytes=60 * 2**20),
        name=name,
    )(*blocks)


def gain_rows(total, *gains):
    pieces = [x.reshape(total, 1, -1) for x in gains]
    pieces = [jnp.pad(x, ((0, 0), (0, 0), (0, 128 - x.shape[2]))) for x in pieces]
    block = jnp.concatenate(pieces, axis=1)
    return jnp.pad(block, ((0, 0), (0, 8 - len(gains)), (0, 0))).reshape(total * 8, 128)


def swapped(x):
    count = lax.axis_size("ctx")
    return lax.ppermute(x, "ctx", [(i, i ^ 1) for i in range(count)])


def on_device(
    tokens,
    cotangent,
    block_map,
    attn_gain,
    query_weight,
    key_weight,
    value_weight,
    query_gain,
    key_gain,
    output_weight,
    mlp_gain,
    gate_weight,
    up_weight,
    down_weight,
):
    grid = Grid(lax.axis_size("ctx"), lax.axis_size("fsdp"))
    total = lax.axis_size("ctx") * lax.axis_size("fsdp")
    groups, rows, width = tokens.shape
    pairs = block_map.shape[1] // 2
    ratio = H // KVH
    low = jnp.bfloat16

    device = lax.axis_index("ctx") * lax.axis_size("fsdp") + lax.axis_index("fsdp")
    gains = jnp.zeros((width // 128 * 2 + 16) * 128, low)
    for at, x in ((0, attn_gain), (width, mlp_gain), (2 * width, query_gain), (2 * width + HD, key_gain)):
        gains = lax.dynamic_update_slice_in_dim(gains, x, at + device * x.shape[0], 0)
    gains = gains.reshape(-1, 128)
    hidden_width = gate_weight.shape[1]

    place = lax.axis_index("ctx")
    blocks = block_map.reshape(-1)
    own_blocks = lax.dynamic_slice_in_dim(blocks, 2 * place, 2, 0)
    numbers = jnp.arange(2 * pairs, dtype=jnp.int32)
    slots = jnp.sum(jnp.where(blocks[None, :] == numbers[:, None], numbers[None, :], 0), axis=1)
    high_slot = (own_blocks[1] > own_blocks[0]).astype(jnp.int32)
    table = jnp.concatenate([slots, high_slot[None], jnp.max(own_blocks)[None]]).astype(jnp.int32)

    spots = (own_blocks[:, None] * BLK + jnp.arange(BLK, dtype=jnp.int32)).reshape(rows)
    cosine, sine = rope_tables(spots)
    turned = jnp.concatenate([-sine[:, : HD // 2], sine[:, HD // 2 :]], axis=1)
    half_q, half_k = H * HD // 2, KVH * HD // 2
    half = half_q + 2 * half_k
    plan = (
        (
            ("gains", 0, 128, FAB + CORE),
            ("q", 0, half_q, FAB + CORE),
            ("q", half_q, 2 * half_q, FBA + CORE),
            ("k", 0, 2 * half_k, BFA + CORE),
            ("v", 0, 2 * half_k, AFB + CORE),
        ),
        (
            ("o", 0, width // 2, BFA + CORE),
            ("o", width // 2, width, AFB + CORE),
            ("g", 0, hidden_width, BFA + CORE),
            ("u", 0, hidden_width, AFB + CORE),
            ("d", 0, width // 2, BFA + CORE),
            ("d", width // 2, width, AFB + CORE),
        ),
    )
    (
        full_qkv,
        full_output,
        full_gu,
        full_down,
        key_all,
        value_all,
        normed,
        gains,
        raw,
        query_low,
        inverse_one,
    ) = front(
        grid,
        plan,
        (query_weight, key_weight, value_weight, output_weight, gate_weight, up_weight, down_weight, gains),
        tokens.reshape(rows, width),
        cosine,
        turned,
    )
    attended, attended_low, totals = attention(table, pairs, query_low, key_all, value_all)
    lanes = width // 128
    gain_one, gain_two = gains[:lanes].reshape(-1), gains[lanes : 2 * lanes].reshape(-1)
    query_scale, key_scale = gains[2 * lanes], gains[2 * lanes + 1]
    inverse_rows = inverse_one
    inverse_one = inverse_one[:, :1]
    inputs = tokens.reshape(rows, width).astype(jnp.float32)
    normal_one = inputs * inverse_one
    cosine = cosine.reshape(rows, 1, HD)
    sine = sine.reshape(rows, 1, HD)
    query_raw = raw[:, : H * HD].reshape(rows, H, HD)
    key_raw = raw[:, H * HD :].reshape(rows, KVH, HD)
    query_inverse = lax.rsqrt(jnp.mean(query_raw * query_raw, axis=-1, keepdims=True) + EPSILON)
    query_unit = query_raw * query_inverse
    key_inverse = lax.rsqrt(jnp.mean(key_raw * key_raw, axis=-1, keepdims=True) + EPSILON)
    key_unit = key_raw * key_inverse
    row_totals = totals.reshape(KVH, 2, ratio, BLK).transpose(1, 3, 0, 2).reshape(rows, H, 1)
    middle = inputs + plain_dot(attended_low, full_output)
    inverse_two = lax.rsqrt(jnp.mean(middle * middle, axis=-1, keepdims=True) + EPSILON)
    normal_two = middle * inverse_two
    normed_two = (normal_two * gain_two).astype(low)
    both = plain_dot(normed_two, full_gu)
    gate, upper = both[:, :hidden_width], both[:, hidden_width:]
    sigmoid_gate = jax.nn.sigmoid(gate)
    activated = gate * sigmoid_gate
    hidden = (activated * upper).astype(low)
    output = (middle + plain_dot(hidden, full_down)).astype(low).reshape(groups, rows, width)

    upstream = cotangent.reshape(rows, width)
    grad_hidden = right_dot(upstream, full_down)
    grad_gate = (grad_hidden * upper * sigmoid_gate * (1.0 + gate * (1.0 - sigmoid_gate))).astype(low)
    grad_upper = (grad_hidden * activated).astype(low)
    grad_both = jnp.concatenate([grad_gate, grad_upper], axis=1)
    normed_other, upstream_other = swapped(normed_two), swapped(upstream)
    grad_down = chip_sums(hidden, swapped(hidden), upstream, upstream_other)
    grad_g = chip_sums(normed_two, normed_other, grad_gate, swapped(grad_gate))
    grad_u = chip_sums(normed_two, normed_other, grad_upper, swapped(grad_upper))
    grad_normed_two = right_dot(grad_both, full_gu)
    grad_gain_two = jnp.sum(grad_normed_two * normal_two, axis=0)
    grad_middle = upstream.astype(jnp.float32) + norm_back(grad_normed_two, normal_two, inverse_two, gain_two)
    f32 = jnp.float32
    branch_grad = grad_middle.astype(low)
    grad_woutput = chip_sums(attended_low, swapped(attended_low), branch_grad, swapped(branch_grad))
    grad_attended = right_dot(branch_grad, full_output).reshape(rows, H, HD)
    grad_summed = (grad_attended / row_totals).astype(low).reshape(rows, H * HD)
    drift = jnp.sum(grad_attended * attended.reshape(rows, H, HD), axis=-1) / row_totals[..., 0]
    drift = drift.reshape(2, BLK, KVH, ratio).transpose(2, 0, 3, 1).reshape(KVH, 2, ratio * BLK)
    grad_query, grad_keys, grad_values = attention_back(
        table, pairs, query_low, key_all, value_all, grad_summed, drift
    )
    back_plan = (
        (("d", 0, width // 2, ABF), ("d", width // 2, width, BAF)),
        (
            ("g", 0, hidden_width, FAB),
            ("u", 0, hidden_width, FBA),
            ("o", 0, width // 2, FAB),
            ("o", width // 2, width, FBA),
        ),
        (
            ("q", 0, 0, half_q, FAB),
            ("q", 0, half_q, 2 * half_q, FBA),
            ("k", H * HD, 0, 2 * half_k, BFA),
            ("v", (H + KVH) * HD, 0, 2 * half_k, AFB),
        ),
    )
    if back_fits(grid, back_plan, rows, width, hidden_width, total):
        out_g, out_u, out_down, out_output, out_q, out_k, out_v, grad_tokens, gain_sums, _ = back(
            grid,
            back_plan,
            (grad_g, grad_u, grad_down, grad_woutput),
            grad_keys,
            grad_values,
            full_qkv,
            grad_query,
            raw,
            cosine.reshape(rows, HD),
            turned,
            gains,
            normed,
            tokens.reshape(rows, width),
            inverse_rows,
            grad_middle,
            grad_gain_two.reshape(lanes, 128),
        )
        flat_sums = gain_sums.reshape(-1)

        def own_piece(at, x):
            return lax.dynamic_slice_in_dim(flat_sums, at + device * x.shape[0], x.shape[0], 0)

        return (
            output,
            grad_tokens.reshape(groups, rows, width),
            own_piece(0, attn_gain),
            out_q,
            out_k,
            out_v,
            own_piece(2 * width, query_gain),
            own_piece(2 * width + HD, key_gain),
            out_output,
            own_piece(width, mlp_gain),
            out_g,
            out_u,
            out_down,
        )
    f32 = jnp.float32
    own_keys, own_values, out_g, out_u, out_down, out_output = scatter(
        grid,
        [SLOT_AXES] * 2 + [CHIP_AXES] * 4,
        [
            (0, 0, KVH * HD, AB),
            (1, 0, KVH * HD, BA),
            (2, 0, hidden_width, BFA),
            (3, 0, hidden_width, AFB),
            (4, 0, width // 2, BFA),
            (4, width // 2, width, AFB),
            (5, 0, width // 2, BFA),
            (5, width // 2, width, AFB),
        ],
        "scatter_mlp",
        (f32, low, f32, f32, f32, f32),
        grad_keys,
        grad_values,
        grad_g,
        grad_u,
        grad_down,
        grad_woutput,
    )
    grad_qrot = grad_query.reshape(rows, H, HD)
    grad_qnormed = grad_qrot * cosine + unrotate(grad_qrot) * sine
    grad_qscale = jnp.sum(grad_qnormed * query_unit, axis=(0, 1))
    grad_qraw = norm_back(grad_qnormed, query_unit, query_inverse, query_scale)
    grad_krot = own_keys.reshape(rows, KVH, HD)
    grad_knormed = grad_krot * cosine + unrotate(grad_krot) * sine
    grad_kscale = jnp.sum(grad_knormed * key_unit, axis=(0, 1))
    grad_kraw = norm_back(grad_knormed, key_unit, key_inverse, key_scale)
    grad_raw = jnp.concatenate(
        [
            grad_qraw.reshape(rows, H * HD).astype(low),
            grad_kraw.reshape(rows, KVH * HD).astype(low),
            own_values,
        ],
        axis=1,
    )
    grad_wqkv = chip_sums(normed, swapped(normed), grad_raw, swapped(grad_raw))
    grad_normed = right_dot(grad_raw, full_qkv)
    grad_gain_one = jnp.sum(grad_normed * normal_one, axis=0)
    grad_inputs = grad_middle + norm_back(grad_normed, normal_one, inverse_one, gain_one)
    out_qkv, out_gains = scatter(
        grid,
        [CHIP_AXES, ALL_AXES],
        [
            (0, 0, half // 2, FAB),
            (0, half // 2, half, FBA),
            (0, half, 3 * half // 2, BFA),
            (0, 3 * half // 2, 2 * half, AFB),
            (1, 0, 128, FAB + CORE),
        ],
        "scatter_attention",
        (f32, f32),
        grad_wqkv,
        gain_rows(total, grad_gain_one, grad_qscale, grad_kscale, grad_gain_two),
    )
    return (
        output,
        grad_inputs.astype(low).reshape(groups, rows, width),
        out_gains[0, : attn_gain.shape[0]],
        out_qkv[:, : H * HD],
        out_qkv[:, H * HD : (H + KVH) * HD],
        out_qkv[:, (H + KVH) * HD :],
        out_gains[1, : query_gain.shape[0]],
        out_gains[2, : key_gain.shape[0]],
        out_output,
        out_gains[3, : mlp_gain.shape[0]],
        out_g,
        out_u,
        out_down,
    )


def solution(mesh):
    return jax.shard_map(
        on_device,
        mesh=mesh,
        in_specs=(
            P("fsdp", "ctx", None),
            P("fsdp", "ctx", None),
            P("fsdp", None),
            P(("ctx", "fsdp")),
            P(("ctx", "fsdp"), None),
            P(("ctx", "fsdp"), None),
            P(("ctx", "fsdp"), None),
            P(("ctx", "fsdp")),
            P(("ctx", "fsdp")),
            P(("ctx", "fsdp"), None),
            P(("ctx", "fsdp")),
            P(("ctx", "fsdp"), None),
            P(("ctx", "fsdp"), None),
            P(("ctx", "fsdp"), None),
        ),
        out_specs=(
            P("fsdp", "ctx", None),
            P("fsdp", "ctx", None),
            P(("ctx", "fsdp")),
            P(("ctx", "fsdp"), None),
            P(("ctx", "fsdp"), None),
            P(("ctx", "fsdp"), None),
            P(("ctx", "fsdp")),
            P(("ctx", "fsdp")),
            P(("ctx", "fsdp"), None),
            P(("ctx", "fsdp")),
            P(("ctx", "fsdp"), None),
            P(("ctx", "fsdp"), None),
            P(("ctx", "fsdp"), None),
        ),
        check_vma=False,
    )
```

```python
import functools
import itertools
import math

import jax
import jax.numpy as jnp
from jax import lax
from jax.experimental import pallas as pl
from jax.experimental.pallas import tpu as pltpu
from jax.sharding import PartitionSpec as P

MESH = pl.DeviceIdType.MESH
ANY = pl.BlockSpec(memory_space=pl.ANY)


H = 16
KVH = 8
HD = 128
BLK = 128


EPSILON = 1e-06
ROPE_BASE = 1000000.0


def rope_tables(positions):
    half = HD // 2
    freqs = jnp.exp(jnp.arange(half, dtype=jnp.float32) * (-2.0 * math.log(ROPE_BASE) / HD))
    angles = positions.astype(jnp.float32)[..., None] * freqs
    cosine = jnp.cos(angles)
    sine = jnp.sin(angles)
    return (jnp.concatenate([cosine, cosine], axis=-1), jnp.concatenate([sine, sine], axis=-1))


def rotate(value_vectors):
    half = value_vectors.shape[-1] // 2
    return jnp.concatenate([-value_vectors[..., half:], value_vectors[..., :half]], axis=-1)


def unrotate(value_vectors):
    half = value_vectors.shape[-1] // 2
    return jnp.concatenate([value_vectors[..., half:], -value_vectors[..., :half]], axis=-1)


def left_dot(left, right):
    return lax.dot_general(
        left, right, (((0,), (0,)), ((), ())), preferred_element_type=jnp.float32
    )


def right_dot(left, right):
    return lax.dot_general(
        left, right, (((1,), (1,)), ((), ())), preferred_element_type=jnp.float32
    )


def plain_dot(left, right):
    return jnp.dot(left, right, preferred_element_type=jnp.float32)


def norm_back(grad_normed, unit, inverse, gain):
    scaled = grad_normed * gain
    return inverse * (scaled - unit * jnp.mean(scaled * unit, axis=-1, keepdims=True))


class Grid:
    def __init__(self, ctx, fsdp):
        self.sizes = {"a": ctx // 4, "b": 2, "core": 2, "f": fsdp}
        self.stride = {"a": 4, "b": 2, "core": 1}

    def enter(self):
        self.c = lax.axis_index("ctx")
        self.at = {
            "a": self.c // 4,
            "b": (self.c // 2) % 2,
            "core": self.c % 2,
            "f": lax.axis_index("fsdp"),
        }

    def barrier(self):
        sem = pltpu.get_barrier_semaphore()
        count = 0
        for axis in ("core", "b", "a", "f"):
            n, p = self.sizes[axis], self.at[axis]
            for step in range(1, n):
                pl.semaphore_signal(
                    sem, inc=1, device_id=self.peer(axis, lax.rem(p + step, n)), device_id_type=MESH
                )
                count += 1
        pl.semaphore_wait(sem, count)

    def peer(self, axis, place):
        if axis == "f":
            return {"fsdp": place}
        return {"ctx": self.c + (place - self.at[axis]) * self.stride[axis]}

    def sources(self, axis):
        n, p = self.sizes[axis], self.at[axis]
        if n == 2:
            return [(None, 1 - p, None, None)]
        found = []
        for step in range(1, n):
            for way in (1, -1):
                origin = p - way * step
                onward = p + way
                found.append(
                    (
                        jnp.logical_and(origin >= 0, origin < n),
                        origin,
                        onward,
                        jnp.logical_and(
                            jnp.logical_and(origin >= 0, origin < n),
                            jnp.logical_and(onward >= 0, onward < n),
                        ),
                    )
                )
        return found

    def around(self, axis):
        n, p = self.sizes[axis], self.at[axis]
        if n == 2:
            return [(None, 1 - p)]
        return [(p + 1 < n, p + 1), (p >= 1, p - 1)]

    def spread(self, axis):
        n, p = self.sizes[axis], self.at[axis]
        if n == 2:
            return [p, 1 - p]
        order = [0]
        for step in range(1, n):
            for way in (step, n - step):
                if way not in order:
                    order.append(way)
        return [lax.rem(p + s, n) for s in order]

    def others(self, axis):
        n, p = self.sizes[axis], self.at[axis]
        return [1 - p] if n == 2 else [lax.rem(p + step, n) for step in range(1, n)]

    def nearest(self, axis):
        return [self.at[axis]] + self.others(axis)


class Pool:
    def __init__(self, ref):
        self.ref, self.used = ref, 0

    def take(self, count):
        first = self.used
        self.used += count
        return self.ref.at[pl.ds(first, count)]


def guarded(cond, body):
    if cond is None:
        body()
    else:
        pl.when(cond)(body)


class Gather:
    def __init__(self, grid, order, src, dst, columns, send_sem, recv_sem, layout_axes):
        self.grid, self.order, self.src, self.dst = grid, order, src, dst
        self.columns, self.send_sem, self.recv_sem = columns, send_sem, recv_sem
        self.layout_axes = layout_axes
        self.sends = 0
        self.pending = []

    @staticmethod
    def semaphores(grid, order):
        near = {x: 1 if grid.sizes[x] == 2 else 2 for x in order}
        far = {x: 0 if grid.sizes[x] == 2 else 2 * (grid.sizes[x] - 1) for x in order}
        sends = near[order[0]] + far[order[0]] + sum(near[x] for x in order[1:])
        inner = 1
        for level in range(1, len(order)):
            axis = order[level]
            onward = sum(near[x] for x in order[level + 1 :])
            sends += inner * (far[axis] + max(far[axis], 1) * onward)
            inner *= grid.sizes[axis]
        return sends, grid.sizes[order[0]] + inner

    def view(self, places):
        idx = tuple(places.get(x, slice(None)) for x in self.layout_axes)
        return self.dst.at[idx + (slice(None), self.columns)]

    def unit_number(self, places):
        number = 0
        for x in self.order[1:]:
            number = number * self.grid.sizes[x] + places[x]
        return number

    def start(self, cond, view, axis, place, sem):
        slot = self.sends
        self.sends += 1

        def make():
            return pltpu.make_async_remote_copy(
                src_ref=view[0],
                dst_ref=view[1],
                send_sem=self.send_sem.at[slot],
                recv_sem=self.recv_sem.at[sem],
                device_id=self.grid.peer(axis, place),
                device_id_type=MESH,
            )

        guarded(cond, lambda: make().start())
        self.pending.append((cond, make))

    def wait_recv(self, view, sem):
        pltpu.make_async_remote_copy(
            src_ref=view,
            dst_ref=view,
            send_sem=self.send_sem.at[0],
            recv_sem=self.recv_sem.at[sem],
            device_id={},
            device_id_type=MESH,
        ).wait_recv()

    def own_places(self):
        return {x: self.grid.at[x] for x in self.order}

    def open(self):
        axis = self.order[0]
        own = self.view(self.own_places())
        for cond, place in self.grid.around(axis):
            self.start(cond, (self.src, own), axis, place, self.grid.at[axis])

    def first(self):
        axis = self.order[0]
        for cond, origin, onward, more in self.grid.sources(axis):
            view = self.view({**self.own_places(), axis: origin})
            guarded(cond, lambda: self.wait_recv(view, origin))
            if onward is not None:
                self.start(more, (view, view), axis, onward, origin)
        self.pass_on(None, 1, {x: self.grid.at[x] for x in self.order[1:]})

    def pass_on(self, cond, level, places):
        n1 = self.grid.sizes[self.order[0]]
        sem = n1 + self.unit_number(places)
        view = self.view(places)
        for axis in self.order[level:]:
            for near, place in self.grid.around(axis):
                both = near if cond is None else cond if near is None else jnp.logical_and(cond, near)
                self.start(both, (view, view), axis, place, sem)

    def arrivals(self, level):
        n1 = self.grid.sizes[self.order[0]]
        axis = self.order[level]
        inner = [{}]
        for x in self.order[1:level]:
            inner = [{**places, x: j} for places in inner for j in self.grid.spread(x)]
        fixed = {x: self.grid.at[x] for x in self.order[level + 1 :]}
        for places in inner:
            for cond, origin, onward, more in self.grid.sources(axis):
                unit = {**places, **fixed, axis: origin}
                view = self.view(unit)
                sem = n1 + self.unit_number(unit)
                guarded(cond, lambda: self.wait_recv(view, sem))
                if onward is not None:
                    self.start(more, (view, view), axis, onward, sem)
                self.pass_on(cond, level + 1, unit)

    def close(self):
        for cond, make in self.pending:
            guarded(cond, lambda: make().wait_send())


def add_into(total, terms, out=None):
    shape = total.shape
    rows = min(16, shape[-2])
    steps = shape[-2] // rows
    lead = math.prod(shape[:-2])

    def body(i, carry):
        index = ()
        rest = i // steps
        for n in reversed(shape[:-2]):
            index = (lax.rem(rest, n),) + index
            rest = rest // n
        at = index + (pl.ds(pl.multiple_of(lax.rem(i, steps) * rows, rows), rows), slice(None))
        value = total[at].astype(jnp.float32)
        for term in terms:
            value = value + term[at].astype(jnp.float32)
        if out is None:
            total[at] = value.astype(total.dtype)
        else:
            out[at] = value.astype(out.dtype)
        return carry

    lax.fori_loop(0, lead * steps, body, 0)


class Scatter:
    def __init__(self, grid, order, src, columns, own, recvs, load_sem, send_sem, recv_sem, out, layout_axes):
        self.grid, self.order, self.src, self.columns = grid, order, src, columns
        self.own, self.recvs, self.out = own, recvs, out
        self.load_sem, self.send_sem, self.recv_sem = load_sem, send_sem, recv_sem
        self.layout_axes = layout_axes
        self.pending = []
        self.base = {}
        self.top = len(order) - 1
        number = 0
        for level in range(self.top, -1, -1):
            self.base[level] = number
            number += self.slots(grid, order, level)

    @staticmethod
    def inner(grid, order, level):
        return [grid.sizes[x] for x in order[1:level]]

    @staticmethod
    def slots(grid, order, level):
        return (grid.sizes[order[level]] - 1) * math.prod(Scatter.inner(grid, order, level))

    @staticmethod
    def scratch(grid, order, rows, columns, dtype):
        n1 = grid.sizes[order[0]]
        shapes = [tuple(grid.sizes[x] for x in order[1:-1]) + (n1, rows, columns)]
        for level, axis in enumerate(order):
            block = (rows, columns) if level == 0 else (n1, rows, columns)
            shapes.append((grid.sizes[axis] - 1,) + tuple(Scatter.inner(grid, order, level)) + block)
        return [pltpu.VMEM(x, dtype) for x in shapes]

    @staticmethod
    def semaphores(grid, order):
        loads = math.prod(grid.sizes[x] for x in order[1:-1])
        slots = sum(Scatter.slots(grid, order, level) for level in range(len(order)))
        return loads, slots, slots

    def hbm(self, places):
        idx = tuple(places.get(x, slice(None)) for x in self.layout_axes)
        return self.src.at[idx + (slice(None), self.columns)]

    def units(self, level):
        found = [{}]
        for x in self.order[1:level]:
            found = [{**places, x: j} for places in found for j in reversed(self.grid.nearest(x))]
        return found

    def mine(self, places):
        return self.own.at[tuple(places.get(x, self.grid.at[x]) for x in self.order[1:-1])]

    def number(self, places, axes):
        value = 0
        for x in axes:
            value = value * self.grid.sizes[x] + places[x]
        return value

    def slot(self, level, places, line):
        axes = self.order[1:level]
        number = line * math.prod(self.grid.sizes[x] for x in axes) + self.number(places, axes)
        ref = self.recvs[level].at[(line,) + tuple(places[x] for x in axes)]
        return ref, self.recv_sem.at[self.base[level] + number]

    def send(self, level, places, step, place, view):
        axis = self.order[level]
        ref, sem = self.slot(level, places, self.grid.sizes[axis] - 1 - step)
        copy = pltpu.make_async_remote_copy(
            src_ref=view,
            dst_ref=ref,
            send_sem=self.send_sem.at[len(self.pending)],
            recv_sem=sem,
            device_id=self.grid.peer(axis, place),
            device_id_type=MESH,
        )
        copy.start()
        self.pending.append(copy)

    def take(self, level, places, total, out=None):
        lines = self.grid.sizes[self.order[level]] - 1
        terms = []
        for line in range(lines):
            ref, sem = self.slot(level, places, line)
            pltpu.make_async_remote_copy(
                src_ref=ref,
                dst_ref=ref,
                send_sem=self.send_sem.at[0],
                recv_sem=sem,
                device_id={},
                device_id_type=MESH,
            ).wait_recv()
            terms.append(ref)
        add_into(total, terms, out)

    def load(self, places):
        here = {**places, self.order[-1]: self.grid.at[self.order[-1]]}
        number = self.number(places, self.order[1:-1])
        return pltpu.make_async_copy(self.hbm(here), self.mine(places), self.load_sem.at[number])

    def open(self):
        axis = self.order[self.top]
        for places in self.units(self.top):
            for step, place in enumerate(self.grid.others(axis), 1):
                self.send(self.top, places, step, place, self.hbm({**places, axis: place}))
            self.load(places).start()

    def settle(self, level, places):
        if level + 1 == self.top:
            self.load(places).wait()
        self.take(level + 1, places, self.mine(places))

    def step(self, level):
        axis = self.order[level]
        if level == 0:
            self.settle(0, {})
            for step, place in enumerate(self.grid.others(axis), 1):
                self.send(0, {}, step, place, self.mine({}).at[place])
            return
        for places in self.units(level):
            for step, place in enumerate(self.grid.others(axis), 1):
                unit = {**places, axis: place}
                self.settle(level, unit)
                self.send(level, places, step, place, self.mine(unit))
            self.settle(level, {**places, axis: self.grid.at[axis]})

    def finish(self):
        self.take(0, {}, self.mine({}).at[self.grid.at[self.order[0]]], self.out)

    def close(self):
        for copy in self.pending:
            copy.wait_send()


def half_pairs(ref, s):
    rows = pl.ds(s * BLK, BLK)
    return jnp.concatenate([ref[rows, :HD], ref[rows, HD:]], axis=0)


def items(table, pairs):
    high_slot, high = table[pairs * 2], table[pairs * 2 + 1]
    low_block = 2 * pairs - 1 - high
    split = high // 2
    found = []
    for w in range(pairs - 1):
        upper = w < split
        found.append((jnp.where(upper, high_slot, 1 - high_slot), jnp.where(upper, w, w - split), None))
    found.append((high_slot, split, high))
    found.append((1 - high_slot, low_block // 2, low_block))
    return found


def chunk_of(ref, table, c):
    return jnp.concatenate(
        [ref[pl.ds(pl.multiple_of(table[2 * c + i] * BLK, BLK), BLK), :] for i in range(2)], axis=0
    )


def row_contract(left, right):
    return lax.dot_general(left, right, (((1,), (1,)), ((), ())), preferred_element_type=jnp.float32)


def attention_kernel(pairs, table, q_ref, k_ref, v_ref, o_ref, low_ref, t_ref, qs, acc, tot):
    for s in range(2):
        qs[s] = half_pairs(q_ref, s)
    acc[...] = jnp.zeros_like(acc)
    tot[...] = jnp.zeros_like(tot)
    for s, c, block in items(table, pairs):
        keys = chunk_of(k_ref, table, c)
        vals = chunk_of(v_ref, table, c)
        scores = row_contract(qs[s], keys) * (HD ** (-0.5) * math.log2(math.e))
        weights = jnp.exp2(scores)
        if block is not None:
            rows = lax.broadcasted_iota(jnp.int32, (2 * BLK, 2 * BLK), 0)
            cols = lax.broadcasted_iota(jnp.int32, (2 * BLK, 2 * BLK), 1)
            allowed = cols <= lax.rem(rows, BLK) + (block - 2 * c) * BLK
            weights = jnp.where(allowed, weights, 0.0)
        tot[s] += weights[:, :HD] + weights[:, HD:]
        acc[s] += jnp.dot(weights.astype(jnp.bfloat16), vals, preferred_element_type=jnp.float32)
    for s in range(2):
        total = tot[s]
        value = acc[s] / jnp.sum(total, axis=1, keepdims=True)
        rows = pl.ds(s * BLK, BLK)
        for i in range(2):
            part = value[i * BLK : (i + 1) * BLK]
            o_ref[rows, i * HD : (i + 1) * HD] = part
            low_ref[rows, i * HD : (i + 1) * HD] = part.astype(jnp.bfloat16)
        t_ref[0, s : s + 1, :] = jnp.sum(total.T, axis=0, keepdims=True)


def attention(table, pairs, queries, keys, values):
    rows, length = queries.shape[0], keys.shape[0]
    head = pl.BlockSpec((rows, 2 * HD), lambda h, t: (0, h))
    side = pl.BlockSpec((length, HD), lambda h, t: (0, h))
    stats = pl.BlockSpec((1, 2, 2 * BLK), lambda h, t: (h, 0, 0))
    return pl.pallas_call(
        functools.partial(attention_kernel, pairs),
        grid_spec=pltpu.PrefetchScalarGridSpec(
            num_scalar_prefetch=1,
            grid=(KVH,),
            in_specs=[head, side, side],
            out_specs=[head, head, stats],
            scratch_shapes=[
                pltpu.VMEM((2, 2 * BLK, HD), jnp.bfloat16),
                pltpu.VMEM((2, 2 * BLK, HD), jnp.float32),
                pltpu.VMEM((2, 2 * BLK, HD), jnp.float32),
            ],
        ),
        out_shape=[
            jax.ShapeDtypeStruct((rows, H * HD), jnp.float32),
            jax.ShapeDtypeStruct((rows, H * HD), jnp.bfloat16),
            jax.ShapeDtypeStruct((KVH, 2, 2 * BLK), jnp.float32),
        ],
        name="attention",
    )(table, queries, keys, values)


def attention_back_kernel(
    pairs, table, q_ref, k_ref, v_ref, g_ref, d_ref, dq_ref, dk_ref, dv_ref, qs, gs, dq, dk, dv
):
    scale = HD ** (-0.5)
    for s in range(2):
        qs[s] = half_pairs(q_ref, s)
        gs[s] = half_pairs(g_ref, s)
    for total in (dq, dk, dv):
        total[...] = jnp.zeros_like(total)
    for s, c, block in items(table, pairs):
        keys = chunk_of(k_ref, table, c)
        vals = chunk_of(v_ref, table, c)
        queries, grads = qs[s], gs[s]
        weights = jnp.exp2(row_contract(keys, queries) * (scale * math.log2(math.e)))
        if block is not None:
            rows = lax.broadcasted_iota(jnp.int32, (2 * BLK, 2 * BLK), 0)
            cols = lax.broadcasted_iota(jnp.int32, (2 * BLK, 2 * BLK), 1)
            allowed = rows <= lax.rem(cols, BLK) + (block - 2 * c) * BLK
            weights = jnp.where(allowed, weights, 0.0)
        through = row_contract(vals, grads)
        scores = (weights * (through - d_ref[0, pl.ds(s, 1), :])).astype(jnp.bfloat16)
        to_values = jnp.dot(weights.astype(jnp.bfloat16), grads, preferred_element_type=jnp.float32)
        to_keys = jnp.dot(scores, queries, preferred_element_type=jnp.float32)
        for i in range(2):
            at = pl.ds(pl.multiple_of(table[2 * c + i] * BLK, BLK), BLK)
            dv[at, :] += to_values[i * BLK : (i + 1) * BLK]
            dk[at, :] += to_keys[i * BLK : (i + 1) * BLK]
        dq[s] += left_dot(scores, keys)
    dk_ref[...] = (dk[...] * scale).astype(jnp.bfloat16)
    dv_ref[...] = dv[...].astype(jnp.bfloat16)
    for s in range(2):
        for i in range(2):
            dq_ref[pl.ds(s * BLK, BLK), i * HD : (i + 1) * HD] = dq[s, i * BLK : (i + 1) * BLK] * scale


def attention_back(table, pairs, queries, keys, values, grads, drift):
    rows, length = queries.shape[0], keys.shape[0]
    head = pl.BlockSpec((rows, 2 * HD), lambda h, t: (0, h))
    side = pl.BlockSpec((length, HD), lambda h, t: (0, h))
    stats = pl.BlockSpec((1, 2, 2 * BLK), lambda h, t: (h, 0, 0))
    return pl.pallas_call(
        functools.partial(attention_back_kernel, pairs),
        grid_spec=pltpu.PrefetchScalarGridSpec(
            num_scalar_prefetch=1,
            grid=(KVH,),
            in_specs=[head, side, side, head, stats],
            out_specs=[head, side, side],
            scratch_shapes=[
                pltpu.VMEM((2, 2 * BLK, HD), jnp.bfloat16),
                pltpu.VMEM((2, 2 * BLK, HD), jnp.bfloat16),
                pltpu.VMEM((2, 2 * BLK, HD), jnp.float32),
                pltpu.VMEM((length, HD), jnp.float32),
                pltpu.VMEM((length, HD), jnp.float32),
            ],
        ),
        out_shape=[
            jax.ShapeDtypeStruct((rows, H * HD), jnp.float32),
            jax.ShapeDtypeStruct((length, KVH * HD), jnp.bfloat16),
            jax.ShapeDtypeStruct((length, KVH * HD), jnp.bfloat16),
        ],
        name="attention_back",
    )(table, queries, keys, values, grads, drift)


ALL_AXES = ("a", "b", "core", "f")
SLOT_AXES = ("a", "b", "core")
CHIP_AXES = ("a", "b", "f")
BFA, AFB, FAB, FBA = ("b", "f", "a"), ("a", "f", "b"), ("f", "a", "b"), ("f", "b", "a")
ABF, BAF = ("a", "b", "f"), ("b", "a", "f")
AB, BA = ("a", "b", "core"), ("b", "a", "core")
CORE = ("core",)


FRONT_SRC = ("q", "k", "v", "o", "g", "u", "d", "gains")


def front_kernel(grid, plan, *refs):
    n = len(FRONT_SRC)
    src = dict(zip(FRONT_SRC, refs[:n]))
    tokens_ref, cosine_ref, sine_ref = refs[n : n + 3]
    outs = refs[n + 3 : n + 15]
    wqkv_ref, wo_ref, wgu_ref, wd_ref, allgains_ref, k_out, v_out = outs[:7]
    normed_ref, gains_ref, raw_ref, qlow_ref, inv_ref = outs[7:]
    scratch = refs[n + 15 :]
    held = dict(zip(FRONT_SRC, scratch[:n]))
    weights, klow, vlow, gbuf = scratch[n : n + 4]
    send, recv, local, load = scratch[n + 4 :]
    grid.enter()
    grid.barrier()
    send, recv = Pool(send), Pool(recv)
    width = tokens_ref.shape[1]
    rows = tokens_ref.shape[0]
    spans = {"q": (wqkv_ref, 0), "k": (wqkv_ref, H * HD), "v": (wqkv_ref, (H + KVH) * HD)}
    hidden = src["g"].shape[1]
    spans.update({"o": (wo_ref, 0), "g": (wgu_ref, 0), "u": (wgu_ref, hidden), "d": (wd_ref, 0)})
    spans["gains"] = (allgains_ref, 0)
    mine = tuple(grid.at[x] for x in ALL_AXES)

    def own_copy(i, name):
        dst, at = spans[name]
        return pltpu.make_async_copy(
            held[name], dst.at[mine + (slice(None), pl.ds(at, src[name].shape[1]))], local.at[i]
        )

    for i, name in enumerate(FRONT_SRC):
        pltpu.make_async_copy(src[name], held[name], local.at[i]).start()

    def part(name, low, high, order):
        dst, at = spans[name]
        sends, takes = Gather.semaphores(grid, order)
        columns = pl.ds(at + low, high - low)
        return Gather(
            grid, order, src[name].at[:, low:high], dst, columns, send.take(sends), recv.take(takes), ALL_AXES
        )

    early = [part(*p) for p in plan[0]]
    late = [part(*p) for p in plan[1]]
    for p in early:
        p.open()
    for p in late:
        p.open()
    for i, name in enumerate(FRONT_SRC):
        pltpu.make_async_copy(src[name], held[name], local.at[i]).wait()
        own_copy(i, name).start()
    inputs = tokens_ref[...].astype(jnp.float32)
    inverse = lax.rsqrt(jnp.mean(inputs * inputs, axis=-1, keepdims=True) + EPSILON)
    inv_ref[...] = jnp.broadcast_to(inverse, (rows, 128))
    for i, name in enumerate(FRONT_SRC):
        own_copy(i, name).wait()

    for p in early:
        p.first()
    for level in (1, 2):
        for p in early:
            p.arrivals(level)
    pump = []
    for p in late:
        pump.append(p.first)
    for level in (1, 2, 3):
        for p in late:
            pump.append(functools.partial(p.arrivals, level))

    def step(count):
        for _ in range(count):
            if pump:
                pump.pop(0)()

    step(len(late))
    for p in early:
        p.arrivals(3)

    places = math.prod(grid.sizes[x] for x in ALL_AXES)
    copy = pltpu.make_async_copy(allgains_ref, gbuf, load.at[0])
    copy.start()
    big = pltpu.make_async_copy(wqkv_ref, weights, load.at[1])
    big.start()
    copy.wait()
    blocks = gbuf[...].reshape((places,) + gbuf.shape[-2:]).astype(jnp.float32)
    gains = jnp.sum(blocks, axis=0)
    gains_ref[...] = gains
    lanes = width // 128
    for j in range(lanes):
        cols = slice(j * 128, (j + 1) * 128)
        part_of = tokens_ref[:, cols].astype(jnp.float32) * inv_ref[...] * gains_ref[j : j + 1, :]
        normed_ref[:, cols] = part_of.astype(jnp.bfloat16)
    big.wait()
    step(1)
    flat = weights.reshape(width, weights.shape[-1])
    normed = normed_ref[...]
    chunk = 2 * HD

    def heads(low_out, gain_row, out_at, raw_at, c):
        at = pl.ds(pl.multiple_of(raw_at + c * chunk, chunk), chunk)
        raw = jnp.dot(normed, flat[:, at], preferred_element_type=jnp.float32)
        raw_ref[:, at] = raw
        done = []
        for i in range(2):
            one = raw[:, i * HD : (i + 1) * HD]
            unit = one * lax.rsqrt(jnp.mean(one * one, axis=-1, keepdims=True) + EPSILON)
            unit = unit * gains_ref[gain_row : gain_row + 1, :]
            done.append(unit * cosine_ref[...] + pltpu.roll(unit, HD // 2, 1) * sine_ref[...])
        to = pl.ds(pl.multiple_of(out_at + c * chunk, chunk), chunk)
        low_out[:, to] = jnp.concatenate(done, axis=1).astype(jnp.bfloat16)

    def loop(count, body):
        def once(c, carry):
            body(c)
            return carry

        lax.fori_loop(0, count, once, 0)

    def to_values(c):
        at = pl.ds(pl.multiple_of((H + KVH) * HD + c * chunk, chunk), chunk)
        to = pl.ds(pl.multiple_of(c * chunk, chunk), chunk)
        raw = jnp.dot(normed, flat[:, at], preferred_element_type=jnp.float32)
        vlow[:, to] = raw.astype(jnp.bfloat16)

    loop(KVH // 2, functools.partial(heads, klow, 2 * lanes + 1, 0, H * HD))
    loop(KVH // 2, to_values)

    def pair(source, dst, order):
        sends, takes = Gather.semaphores(grid, order)
        return Gather(
            grid, order, source, dst, pl.ds(0, KVH * HD), send.take(sends), recv.take(takes), SLOT_AXES
        )

    slot = tuple(grid.at[x] for x in SLOT_AXES)
    slabs = [pair(klow, k_out, AB), pair(vlow, v_out, BA)]
    saves = [
        pltpu.make_async_copy(klow, k_out.at[slot], load.at[0]),
        pltpu.make_async_copy(vlow, v_out.at[slot], load.at[1]),
    ]
    for p, save in zip(slabs, saves):
        p.open()
        save.start()
    step(2)
    loop(KVH // 2, functools.partial(heads, qlow_ref, 2 * lanes, 0, 0))
    for p, save in zip(slabs, saves):
        save.wait()
        p.first()
    step(2)
    loop(KVH // 2, functools.partial(heads, qlow_ref, 2 * lanes, H * HD // 2, H * HD // 2))
    for p in slabs:
        p.arrivals(1)
    step(len(pump))
    for p in slabs:
        p.arrivals(2)
    for p in early + late + slabs:
        p.close()


def front(grid, plan, blocks, tokens, cosine, sine):
    n = len(FRONT_SRC)
    rows, width = tokens.shape
    places = tuple(grid.sizes[x] for x in ALL_AXES)
    slots = tuple(grid.sizes[x] for x in SLOT_AXES)
    by = dict(zip(FRONT_SRC, blocks))
    low, f32 = jnp.bfloat16, jnp.float32
    full = (H + 2 * KVH) * HD
    counts = [Gather.semaphores(grid, p[3]) for p in plan[0] + plan[1]]
    counts += [Gather.semaphores(grid, AB), Gather.semaphores(grid, BA)]
    sends, takes = [sum(x) for x in zip(*counts)]
    shape = jax.ShapeDtypeStruct
    vmem = pl.BlockSpec(memory_space=pltpu.VMEM)
    outs = pl.pallas_call(
        functools.partial(front_kernel, grid, plan),
        out_shape=[
            shape(places + (by["q"].shape[0], full), low),
            shape(places + by["o"].shape, low),
            shape(places + (by["g"].shape[0], 2 * by["g"].shape[1]), low),
            shape(places + by["d"].shape, low),
            shape(places + by["gains"].shape, low),
            shape(slots + (rows, KVH * HD), low),
            shape(slots + (rows, KVH * HD), low),
            shape((rows, width), low),
            shape(by["gains"].shape, f32),
            shape((rows, (H + KVH) * HD), f32),
            shape((rows, H * HD), low),
            shape((rows, 128), f32),
        ],
        in_specs=[ANY] * n + [vmem] * 3,
        out_specs=[ANY] * 7 + [vmem] * 5,
        scratch_shapes=[pltpu.VMEM(x.shape, x.dtype) for x in blocks]
        + [
            pltpu.VMEM(places + (by["q"].shape[0], full), low),
            pltpu.VMEM((rows, KVH * HD), low),
            pltpu.VMEM((rows, KVH * HD), low),
            pltpu.VMEM(places + by["gains"].shape, low),
            pltpu.SemaphoreType.DMA((sends,)),
            pltpu.SemaphoreType.DMA((takes,)),
            pltpu.SemaphoreType.DMA((n,)),
            pltpu.SemaphoreType.DMA((2,)),
        ],
        compiler_params=pltpu.CompilerParams(
            has_side_effects=True, vmem_limit_bytes=60 * 2**20, collective_id=0
        ),
        name="front",
    )(*blocks, tokens, cosine, sine)
    wqkv, wo, wgu, wd, _, keys, vals, normed, gains, raw, qlow, inverse = outs
    flat = [x.reshape(-1, x.shape[-1]) for x in (wqkv, wo, wgu, wd, keys, vals)]
    return flat + [normed, gains, raw, qlow, inverse]


def sums_kernel(core, left, left_other, right, right_other, out):
    lhs = jnp.concatenate([left[...], left_other[...]], axis=0)
    rhs = jnp.concatenate([right[...], right_other[...]], axis=0)
    out[...] = left_dot(lhs, rhs).astype(out.dtype)


def chip_sums(left, left_other, right, right_other):
    rows, width = left.shape
    count = lax.axis_size("ctx")
    block = width // count
    tile = min(1024, right.shape[1])
    if block % 128:
        place = lax.axis_index("ctx") % 2
        halves = [
            lax.dynamic_index_in_dim(x.reshape(rows, count // 2, 2, block), place, 2, False)
            for x in (left, left_other)
        ]
        lhs = jnp.concatenate(halves, axis=0).reshape(2 * rows, width // 2)
        return left_dot(lhs, jnp.concatenate([right, right_other], axis=0)).astype(jnp.bfloat16)
    core = (lax.axis_index("ctx") % 2).astype(jnp.int32)[None]
    lhs = pl.BlockSpec((rows, block), lambda n, j, c: (0, 2 * j + c[0]))
    rhs = pl.BlockSpec((rows, tile), lambda n, j, c: (0, n))
    return pl.pallas_call(
        sums_kernel,
        grid_spec=pltpu.PrefetchScalarGridSpec(
            num_scalar_prefetch=1,
            grid=(right.shape[1] // tile, count // 2),
            in_specs=[lhs, lhs, rhs, rhs],
            out_specs=pl.BlockSpec((block, tile), lambda n, j, c: (j, n)),
        ),
        out_shape=jax.ShapeDtypeStruct((width // 2, right.shape[1]), jnp.bfloat16),
        name="chip_sums",
    )(core, left, left_other, right, right_other)


def handed_kernel(*refs):
    for source, out in zip(refs[: len(refs) // 2], refs[len(refs) // 2 :]):
        out[...] = source[...]


def handed(*results):
    vmem = pl.BlockSpec(memory_space=pltpu.VMEM)
    return pl.pallas_call(
        handed_kernel,
        out_shape=[jax.ShapeDtypeStruct(x.shape, x.dtype) for x in results],
        in_specs=[vmem] * len(results),
        out_specs=[vmem] * len(results),
        name="handed",
    )(*results)


BACK_SUMS = ("g", "u", "d", "o")


def back_kernel(grid, plan, *refs):
    refs = list(refs)

    def take(n):
        found = refs[:n]
        del refs[:n]
        return found

    src = dict(zip(BACK_SUMS, take(len(BACK_SUMS))))
    gk_ref, gv_ref, wqkv_ref = take(3)
    dq_ref, raw_ref, cos_ref, turn_ref, gains_ref, normed_ref, tokens_ref, inv_ref, mid_ref, gain2_ref = take(10)
    outs = dict(zip(BACK_SUMS + ("q", "k", "v"), take(len(BACK_SUMS) + 3)))
    din_ref, gsum_ref, sums_ref, gall_ref = take(4)
    weights, both_normed, both_raw, own_k, own_v, stage, acc, gbuf, gblock = take(9)
    load, send, recv, misc = [Pool(x) for x in refs[-4:]]
    del refs[-4:]
    scratch = refs
    grid.enter()
    grid.barrier()
    rows, width = tokens_ref.shape
    lanes = width // 128
    core = grid.at["core"]
    chunk = 2 * HD
    misc_sem = [misc.take(1).at[0] for _ in range(12)]

    def make(source, columns, order, out, layout):
        loads, sends, takes = Scatter.semaphores(grid, order)
        own, *recvs = scratch[: 1 + len(order)]
        del scratch[: 1 + len(order)]
        return Scatter(
            grid, order, source, columns, own, recvs,
            load.take(loads), send.take(sends), recv.take(takes), out, layout,
        )

    def portions(group):
        found = []
        for name, low, high, order in group:
            found.append(
                make(src[name], pl.ds(low, high - low), order, outs[name].at[:, low:high], CHIP_AXES)
            )
        return found

    slabs = [
        make(gk_ref, pl.ds(0, KVH * HD), AB, own_k, SLOT_AXES),
        make(gv_ref, pl.ds(0, KVH * HD), BA, own_v, SLOT_AXES),
    ]
    early, waves = portions(plan[0]), [portions(group) for group in plan[1]]
    late = [p for wave in waves for p in wave]
    last = []
    for name, at, low, high, order in plan[2]:
        last.append(
            make(sums_ref, pl.ds(at + low, high - low), order, outs[name].at[:, low:high], CHIP_AXES)
        )

    def sibling(source, dst, k):
        return pltpu.make_async_remote_copy(
            src_ref=source, dst_ref=dst, send_sem=misc_sem[2 * k], recv_sem=misc_sem[2 * k + 1],
            device_id=grid.peer("core", 1 - core), device_id_type=MESH,
        )

    for p in slabs + early:
        p.open()
    swap_normed = sibling(normed_ref, both_normed.at[1], 0)
    swap_normed.start()
    both_normed[0] = normed_ref[...]
    gblock[...] = jnp.zeros_like(gblock)
    gblock[lanes : 2 * lanes, :] = gain2_ref[...]

    def loop(count, body):
        def once(c, carry):
            body(c)
            return carry

        lax.fori_loop(0, count, once, 0)

    def heads(source, in_at, raw_at, gain_row, c):
        at = pl.ds(pl.multiple_of(raw_at + c * chunk, chunk), chunk)
        grads = source[:, pl.ds(pl.multiple_of(in_at + c * chunk, chunk), chunk)]
        raw = raw_ref[:, at]
        gain = gains_ref[gain_row : gain_row + 1, :]
        done = []
        for i in range(2):
            g = grads[:, i * HD : (i + 1) * HD]
            g = g * cos_ref[...] - pltpu.roll(g, HD // 2, 1) * turn_ref[...]
            one = raw[:, i * HD : (i + 1) * HD]
            inverse = lax.rsqrt(jnp.mean(one * one, axis=-1, keepdims=True) + EPSILON)
            unit = one * inverse
            gblock[gain_row : gain_row + 1, :] += jnp.sum(g * unit, axis=0, keepdims=True)
            done.append(norm_back(g, unit, inverse, gain))
        both_raw[0, :, at] = jnp.concatenate(done, axis=1).astype(jnp.bfloat16)

    half_q = H * HD // 2
    q_cols, kv_cols = pl.ds(0, H * HD), pl.ds(H * HD, 2 * KVH * HD)
    loop(H // 4, functools.partial(heads, dq_ref, 0, 0, 2 * lanes))
    for p in slabs:
        p.step(1)
    loop(H // 4, functools.partial(heads, dq_ref, half_q, half_q, 2 * lanes))
    swap_q = sibling(both_raw.at[0, :, q_cols], both_raw.at[1, :, q_cols], 1)
    swap_q.start()
    for p in slabs:
        p.step(0)
    def every(group, what, *args):
        for p in group:
            getattr(p, what)(*args)

    every(waves[0], "open")
    for p in slabs:
        p.finish()
    loop(KVH // 2, functools.partial(heads, own_k, 0, H * HD, 2 * lanes + 1))
    at = (H + KVH) * HD
    both_raw[0, :, at : at + KVH * HD] = own_v[...].astype(jnp.bfloat16)
    swap_kv = sibling(both_raw.at[0, :, kv_cols], both_raw.at[1, :, kv_cols], 2)
    swap_kv.start()
    every(waves[1], "open")
    swap_normed.wait()
    swap_q.wait()
    swap_kv.wait()
    flat_normed = both_normed.reshape(2 * rows, width)
    flat_raw = both_raw.reshape(2 * rows, both_raw.shape[-1])
    count = grid.sizes["a"] * grid.sizes["b"]
    block = width // (2 * count)
    piece = block // grid.sizes["f"]
    full = both_raw.shape[-1]
    tile = 512

    def stored(j):
        return pltpu.make_async_copy(stage.at[j % 2], sums_ref.at[j // 2, j % 2], misc_sem[9 + j % 2])

    for j in range(count):
        if j >= 2:
            stored(j - 2).wait()
        lhs = flat_normed[:, pl.ds(pl.multiple_of((2 * j + core) * block, block), block)]

        def sums(c):
            cols = pl.ds(pl.multiple_of(c * tile, tile), tile)
            value = left_dot(lhs, flat_raw[:, cols]).astype(jnp.bfloat16)
            stage[j % 2, :, :, cols] = value.reshape(grid.sizes["f"], piece, tile)

        loop(full // tile, sums)
        stored(j).start()
    for j in range(count - 2, count):
        stored(j).wait()
    every(waves[0], "step", 1)
    every(last, "open")
    every(waves[2], "open")
    every(early, "step", 1)
    every(waves[1], "step", 1)
    every(waves[0], "step", 0)
    tiles = [
        pltpu.make_async_copy(
            wqkv_ref.at[:, c * tile : (c + 1) * tile], weights.at[c % 2], misc_sem[6 + c % 2]
        )
        for c in range(full // tile)
    ]
    tiles[0].start()
    for c in range(full // tile):
        if c + 1 < full // tile:
            tiles[c + 1].start()
        tiles[c].wait()
        value = right_dot(both_raw[0, :, c * tile : (c + 1) * tile], weights[c % 2])
        acc[...] = value if c == 0 else acc[...] + value
    inverse = inv_ref[...]
    for j in range(lanes):
        cols = slice(j * 128, (j + 1) * 128)
        normal = tokens_ref[:, cols].astype(jnp.float32) * inverse
        gblock[j : j + 1, :] = jnp.sum(acc[:, cols] * normal, axis=0, keepdims=True)
    copy = pltpu.make_async_copy(gblock, gbuf, misc_sem[11])
    copy.start()
    copy.wait()
    order = FAB + CORE
    sends, takes = Gather.semaphores(grid, order)
    spread = Gather(
        grid, order, gbuf, gall_ref, slice(None), send.take(sends), recv.take(takes), ALL_AXES
    )
    spread.open()
    mine = tuple(grid.at[x] for x in ALL_AXES)
    gall_ref[mine] = gblock[...]
    every(early, "step", 0)
    every(last, "step", 1)
    every(waves[2], "step", 1)
    every(waves[1], "step", 0)
    spread.first()
    dots = jnp.zeros((rows, 1), jnp.float32)
    for j in range(lanes):
        cols = slice(j * 128, (j + 1) * 128)
        normal = tokens_ref[:, cols].astype(jnp.float32) * inverse
        dots += jnp.sum(acc[:, cols] * gains_ref[j : j + 1, :] * normal, axis=1, keepdims=True)
    dots = dots / width
    for j in range(lanes):
        cols = slice(j * 128, (j + 1) * 128)
        normal = tokens_ref[:, cols].astype(jnp.float32) * inverse
        grad = inverse * (acc[:, cols] * gains_ref[j : j + 1, :] - normal * dots)
        din_ref[:, cols] = (mid_ref[:, cols] + grad).astype(jnp.bfloat16)
    spread.arrivals(1)
    every(last, "step", 0)
    every(waves[2], "step", 0)
    spread.arrivals(2)
    every(waves[0] + early + waves[1], "finish")
    spread.arrivals(3)
    every(last + waves[2], "finish")
    places = math.prod(grid.sizes[x] for x in ALL_AXES)
    gsum_ref[...] = jnp.sum(gall_ref.reshape((places,) + gblock.shape)[...], axis=0)
    for p in slabs + early + late + last:
        p.close()
    spread.close()


def back_scratch(grid, plan, pieces, rows, width):
    low = jnp.bfloat16
    scratch, counts = [], []
    for order in (AB, BA):
        scratch += Scatter.scratch(grid, order, rows, KVH * HD, low)
        counts.append(Scatter.semaphores(grid, order))
    for name, begin, end, order in plan[0] + sum(plan[1], ()) + tuple((p[0],) + p[2:] for p in plan[2]):
        scratch += Scatter.scratch(grid, order, pieces[name], end - begin, low)
        counts.append(Scatter.semaphores(grid, order))
    return scratch, [sum(x) for x in zip(*counts)]


def back_fits(grid, plan, rows, width, hidden, total):
    pieces = {name: width // total for name in ("g", "u", "q", "k", "v")}
    pieces.update({"d": hidden // total, "o": H * HD // total})
    scratch = back_scratch(grid, plan, pieces, rows, width)[0]
    taken = sum(2 * math.prod(x.shape) for x in scratch)
    held = 2 * rows * (11 * width + 3 * (H + 2 * KVH) * HD + 4 * (H + KVH) * HD) + 6 * 2**20
    return taken + held < 62 * 2**20


def back(grid, plan, sums, gk, gv, wqkv, dq, raw, cosine, turned, gains, normed, tokens, inverse, middle, gain2):
    low, f32 = jnp.bfloat16, jnp.float32
    rows, width = tokens.shape
    chips = tuple(grid.sizes[x] for x in CHIP_AXES)
    places = tuple(grid.sizes[x] for x in ALL_AXES)
    slots = tuple(grid.sizes[x] for x in SLOT_AXES)
    blocks = [x.reshape(chips + (x.shape[0] // math.prod(chips), x.shape[1])) for x in sums]
    shape = jax.ShapeDtypeStruct
    vmem = pl.BlockSpec(memory_space=pltpu.VMEM)
    piece = width // math.prod(places)
    pieces = dict(zip(BACK_SUMS, [x.shape[-2] for x in blocks]))
    pieces.update({"q": piece, "k": piece, "v": piece})
    scratch, (loads, sends, takes) = back_scratch(grid, plan, pieces, rows, width)
    more = Gather.semaphores(grid, FAB + CORE)
    full = wqkv.shape[1]
    count = grid.sizes["a"] * grid.sizes["b"]
    outs = pl.pallas_call(
        functools.partial(back_kernel, grid, plan),
        out_shape=[shape(x.shape[-2:], f32) for x in blocks]
        + [shape((piece, n), f32) for n in (H * HD, KVH * HD, KVH * HD)]
        + [
            shape((rows, width), low),
            shape(gains.shape, f32),
            shape(chips + (piece, full), low),
        ],
        in_specs=[ANY] * (len(blocks) + 3) + [vmem] * 10,
        out_specs=[vmem] * (len(blocks) + 5) + [ANY],
        scratch_shapes=[
            pltpu.VMEM(places + gains.shape, f32),
            pltpu.VMEM((2, width, 512), low),
            pltpu.VMEM((2, rows, width), low),
            pltpu.VMEM((2, rows, full), low),
            pltpu.VMEM((rows, KVH * HD), f32),
            pltpu.VMEM((rows, KVH * HD), f32),
            pltpu.VMEM((2, grid.sizes["f"], piece, full), low),
            pltpu.VMEM((rows, width), f32),
            pltpu.VMEM(gains.shape, f32),
            pltpu.VMEM(gains.shape, f32),
        ]
        + scratch
        + [
            pltpu.SemaphoreType.DMA((loads,)),
            pltpu.SemaphoreType.DMA((sends + more[0],)),
            pltpu.SemaphoreType.DMA((takes + more[1],)),
            pltpu.SemaphoreType.DMA((12,)),
        ],
        compiler_params=pltpu.CompilerParams(
            has_side_effects=True, vmem_limit_bytes=63 * 2**20, collective_id=1
        ),
        name="back",
    )(
        *blocks,
        gk.reshape(slots + (rows, KVH * HD)),
        gv.reshape(slots + (rows, KVH * HD)),
        wqkv, dq, raw, cosine, turned, gains, normed, tokens, inverse, middle, gain2,
    )
    return outs


def scatter_kernel(grid, portions, layouts, n, *refs):
    srcs, outs, scratch = refs[:n], refs[n : 2 * n], list(refs[2 * n : -3])
    load, send, recv = [Pool(x) for x in refs[-3:]]
    grid.enter()
    parts = []
    for i, low, high, order in portions:
        loads, sends, takes = Scatter.semaphores(grid, order)
        own, *recvs = scratch[: 1 + len(order)]
        del scratch[: 1 + len(order)]
        parts.append(
            Scatter(
                grid,
                order,
                srcs[i],
                pl.ds(low, high - low),
                own,
                recvs,
                load.take(loads),
                send.take(sends),
                recv.take(takes),
                outs[i].at[:, low:high],
                layouts[i],
            )
        )
        parts[-1].open()
    for level in (2, 1, 0):
        for part in parts:
            if level < part.top:
                part.step(level)
    for part in parts:
        part.finish()
    for part in parts:
        part.close()


def scatter(grid, layouts, portions, name, dtypes, *sums):
    n = len(sums)
    blocks = []
    for layout, x in zip(layouts, sums):
        places = tuple(grid.sizes[axis] for axis in layout)
        blocks.append(x.reshape(places + (x.shape[0] // math.prod(places), x.shape[1])))
    loads, sends, takes = [sum(x) for x in zip(*[Scatter.semaphores(grid, p[3]) for p in portions])]
    scratch = []
    for i, low, high, order in portions:
        scratch += Scatter.scratch(grid, order, blocks[i].shape[-2], high - low, blocks[i].dtype)
    return pl.pallas_call(
        functools.partial(scatter_kernel, grid, portions, layouts, n),
        out_shape=[jax.ShapeDtypeStruct(x.shape[-2:], t) for x, t in zip(blocks, dtypes)],
        in_specs=[ANY] * n,
        out_specs=[pl.BlockSpec(memory_space=pltpu.VMEM)] * n,
        scratch_shapes=scratch
        + [
            pltpu.SemaphoreType.DMA((loads,)),
            pltpu.SemaphoreType.DMA((sends,)),
            pltpu.SemaphoreType.DMA((takes,)),
        ],
        compiler_params=pltpu.CompilerParams(has_side_effects=True, vmem_limit_bytes=60 * 2**20),
        name=name,
    )(*blocks)


def gain_rows(total, *gains):
    pieces = [x.reshape(total, 1, -1) for x in gains]
    pieces = [jnp.pad(x, ((0, 0), (0, 0), (0, 128 - x.shape[2]))) for x in pieces]
    block = jnp.concatenate(pieces, axis=1)
    return jnp.pad(block, ((0, 0), (0, 8 - len(gains)), (0, 0))).reshape(total * 8, 128)


def swapped(x):
    count = lax.axis_size("ctx")
    return lax.ppermute(x, "ctx", [(i, i ^ 1) for i in range(count)])


def on_device(
    tokens,
    cotangent,
    block_map,
    attn_gain,
    query_weight,
    key_weight,
    value_weight,
    query_gain,
    key_gain,
    output_weight,
    mlp_gain,
    gate_weight,
    up_weight,
    down_weight,
):
    grid = Grid(lax.axis_size("ctx"), lax.axis_size("fsdp"))
    total = lax.axis_size("ctx") * lax.axis_size("fsdp")
    groups, rows, width = tokens.shape
    pairs = block_map.shape[1] // 2
    ratio = H // KVH
    low = jnp.bfloat16

    device = lax.axis_index("ctx") * lax.axis_size("fsdp") + lax.axis_index("fsdp")
    gains = jnp.zeros((width // 128 * 2 + 16) * 128, low)
    for at, x in ((0, attn_gain), (width, mlp_gain), (2 * width, query_gain), (2 * width + HD, key_gain)):
        gains = lax.dynamic_update_slice_in_dim(gains, x, at + device * x.shape[0], 0)
    gains = gains.reshape(-1, 128)
    hidden_width = gate_weight.shape[1]

    place = lax.axis_index("ctx")
    blocks = block_map.reshape(-1)
    own_blocks = lax.dynamic_slice_in_dim(blocks, 2 * place, 2, 0)
    numbers = jnp.arange(2 * pairs, dtype=jnp.int32)
    slots = jnp.sum(jnp.where(blocks[None, :] == numbers[:, None], numbers[None, :], 0), axis=1)
    high_slot = (own_blocks[1] > own_blocks[0]).astype(jnp.int32)
    table = jnp.concatenate([slots, high_slot[None], jnp.max(own_blocks)[None]]).astype(jnp.int32)

    spots = (own_blocks[:, None] * BLK + jnp.arange(BLK, dtype=jnp.int32)).reshape(rows)
    cosine, sine = rope_tables(spots)
    turned = jnp.concatenate([-sine[:, : HD // 2], sine[:, HD // 2 :]], axis=1)
    half_q, half_k = H * HD // 2, KVH * HD // 2
    half = half_q + 2 * half_k
    plan = (
        (
            ("gains", 0, 128, FAB + CORE),
            ("q", 0, half_q, FAB + CORE),
            ("q", half_q, 2 * half_q, FBA + CORE),
            ("k", 0, 2 * half_k, BFA + CORE),
            ("v", 0, 2 * half_k, AFB + CORE),
        ),
        (
            ("o", 0, width // 2, ABF + CORE),
            ("o", width // 2, width, BAF + CORE),
            ("g", 0, hidden_width, BFA + CORE),
            ("u", 0, hidden_width, AFB + CORE),
            ("d", 0, width // 2, BFA + CORE),
            ("d", width // 2, width, AFB + CORE),
        ),
    )
    (
        full_qkv,
        full_output,
        full_gu,
        full_down,
        key_all,
        value_all,
        normed,
        gains,
        raw,
        query_low,
        inverse_one,
    ) = front(
        grid,
        plan,
        (query_weight, key_weight, value_weight, output_weight, gate_weight, up_weight, down_weight, gains),
        tokens.reshape(rows, width),
        cosine,
        turned,
    )
    attended, attended_low, totals = attention(table, pairs, query_low, key_all, value_all)
    lanes = width // 128
    gain_one, gain_two = gains[:lanes].reshape(-1), gains[lanes : 2 * lanes].reshape(-1)
    query_scale, key_scale = gains[2 * lanes], gains[2 * lanes + 1]
    inverse_rows = inverse_one
    inverse_one = inverse_one[:, :1]
    inputs = tokens.reshape(rows, width).astype(jnp.float32)
    normal_one = inputs * inverse_one
    cosine = cosine.reshape(rows, 1, HD)
    sine = sine.reshape(rows, 1, HD)
    query_raw = raw[:, : H * HD].reshape(rows, H, HD)
    key_raw = raw[:, H * HD :].reshape(rows, KVH, HD)
    query_inverse = lax.rsqrt(jnp.mean(query_raw * query_raw, axis=-1, keepdims=True) + EPSILON)
    query_unit = query_raw * query_inverse
    key_inverse = lax.rsqrt(jnp.mean(key_raw * key_raw, axis=-1, keepdims=True) + EPSILON)
    key_unit = key_raw * key_inverse
    row_totals = totals.reshape(KVH, 2, ratio, BLK).transpose(1, 3, 0, 2).reshape(rows, H, 1)
    middle = inputs + plain_dot(attended_low, full_output)
    inverse_two = lax.rsqrt(jnp.mean(middle * middle, axis=-1, keepdims=True) + EPSILON)
    normal_two = middle * inverse_two
    normed_two = (normal_two * gain_two).astype(low)
    both = plain_dot(normed_two, full_gu)
    gate, upper = both[:, :hidden_width], both[:, hidden_width:]
    sigmoid_gate = jax.nn.sigmoid(gate)
    activated = gate * sigmoid_gate
    hidden = (activated * upper).astype(low)
    output = (middle + plain_dot(hidden, full_down)).astype(low).reshape(groups, rows, width)

    upstream = cotangent.reshape(rows, width)
    grad_hidden = right_dot(upstream, full_down)
    grad_gate = (grad_hidden * upper * sigmoid_gate * (1.0 + gate * (1.0 - sigmoid_gate))).astype(low)
    grad_upper = (grad_hidden * activated).astype(low)
    grad_both = jnp.concatenate([grad_gate, grad_upper], axis=1)
    normed_other, upstream_other = swapped(normed_two), swapped(upstream)
    grad_down = chip_sums(hidden, swapped(hidden), upstream, upstream_other)
    grad_g = chip_sums(normed_two, normed_other, grad_gate, swapped(grad_gate))
    grad_u = chip_sums(normed_two, normed_other, grad_upper, swapped(grad_upper))
    grad_normed_two = right_dot(grad_both, full_gu)
    grad_gain_two = jnp.sum(grad_normed_two * normal_two, axis=0)
    grad_middle = upstream.astype(jnp.float32) + norm_back(grad_normed_two, normal_two, inverse_two, gain_two)
    f32 = jnp.float32
    branch_grad = grad_middle.astype(low)
    grad_woutput = chip_sums(attended_low, swapped(attended_low), branch_grad, swapped(branch_grad))
    grad_attended = right_dot(branch_grad, full_output).reshape(rows, H, HD)
    grad_summed = (grad_attended / row_totals).astype(low).reshape(rows, H * HD)
    drift = jnp.sum(grad_attended * attended.reshape(rows, H, HD), axis=-1) / row_totals[..., 0]
    drift = drift.reshape(2, BLK, KVH, ratio).transpose(2, 0, 3, 1).reshape(KVH, 2, ratio * BLK)
    grad_query, grad_keys, grad_values = attention_back(
        table, pairs, query_low, key_all, value_all, grad_summed, drift
    )
    back_plan = (
        (("d", 0, width // 2, ABF), ("d", width // 2, width, BAF)),
        (
            (("g", 0, hidden_width // 2, FAB), ("g", hidden_width // 2, hidden_width, FBA)),
            (("u", 0, hidden_width // 2, FAB), ("u", hidden_width // 2, hidden_width, FBA)),
            (("o", 0, width // 2, FAB), ("o", width // 2, width, FBA)),
        ),
        (
            ("q", 0, 0, half_q, ABF),
            ("q", 0, half_q, 2 * half_q, BAF),
            ("k", H * HD, 0, 2 * half_k, FAB),
            ("v", (H + KVH) * HD, 0, 2 * half_k, FBA),
        ),
    )
    if back_fits(grid, back_plan, rows, width, hidden_width, total):
        out_g, out_u, out_down, out_output, out_q, out_k, out_v, grad_tokens, gain_sums, _ = back(
            grid,
            back_plan,
            (grad_g, grad_u, grad_down, grad_woutput),
            grad_keys,
            grad_values,
            full_qkv,
            grad_query,
            raw,
            cosine.reshape(rows, HD),
            turned,
            gains,
            normed,
            tokens.reshape(rows, width),
            inverse_rows,
            grad_middle,
            grad_gain_two.reshape(lanes, 128),
        )
        out_g, out_u, out_down, out_output, out_q, out_k, out_v, grad_tokens = handed(
            out_g, out_u, out_down, out_output, out_q, out_k, out_v, grad_tokens
        )
        flat_sums = gain_sums.reshape(-1)

        def own_piece(at, x):
            return lax.dynamic_slice_in_dim(flat_sums, at + device * x.shape[0], x.shape[0], 0)

        return (
            output,
            grad_tokens.reshape(groups, rows, width),
            own_piece(0, attn_gain),
            out_q,
            out_k,
            out_v,
            own_piece(2 * width, query_gain),
            own_piece(2 * width + HD, key_gain),
            out_output,
            own_piece(width, mlp_gain),
            out_g,
            out_u,
            out_down,
        )
    f32 = jnp.float32
    own_keys, own_values, out_g, out_u, out_down, out_output = scatter(
        grid,
        [SLOT_AXES] * 2 + [CHIP_AXES] * 4,
        [
            (0, 0, KVH * HD, AB),
            (1, 0, KVH * HD, BA),
            (2, 0, hidden_width, BFA),
            (3, 0, hidden_width, AFB),
            (4, 0, width // 2, BFA),
            (4, width // 2, width, AFB),
            (5, 0, width // 2, BFA),
            (5, width // 2, width, AFB),
        ],
        "scatter_mlp",
        (f32, low, f32, f32, f32, f32),
        grad_keys,
        grad_values,
        grad_g,
        grad_u,
        grad_down,
        grad_woutput,
    )
    grad_qrot = grad_query.reshape(rows, H, HD)
    grad_qnormed = grad_qrot * cosine + unrotate(grad_qrot) * sine
    grad_qscale = jnp.sum(grad_qnormed * query_unit, axis=(0, 1))
    grad_qraw = norm_back(grad_qnormed, query_unit, query_inverse, query_scale)
    grad_krot = own_keys.reshape(rows, KVH, HD)
    grad_knormed = grad_krot * cosine + unrotate(grad_krot) * sine
    grad_kscale = jnp.sum(grad_knormed * key_unit, axis=(0, 1))
    grad_kraw = norm_back(grad_knormed, key_unit, key_inverse, key_scale)
    grad_raw = jnp.concatenate(
        [
            grad_qraw.reshape(rows, H * HD).astype(low),
            grad_kraw.reshape(rows, KVH * HD).astype(low),
            own_values,
        ],
        axis=1,
    )
    grad_wqkv = chip_sums(normed, swapped(normed), grad_raw, swapped(grad_raw))
    grad_normed = right_dot(grad_raw, full_qkv)
    grad_gain_one = jnp.sum(grad_normed * normal_one, axis=0)
    grad_inputs = grad_middle + norm_back(grad_normed, normal_one, inverse_one, gain_one)
    out_qkv, out_gains = scatter(
        grid,
        [CHIP_AXES, ALL_AXES],
        [
            (0, 0, half // 2, FAB),
            (0, half // 2, half, FBA),
            (0, half, 3 * half // 2, BFA),
            (0, 3 * half // 2, 2 * half, AFB),
            (1, 0, 128, FAB + CORE),
        ],
        "scatter_attention",
        (f32, f32),
        grad_wqkv,
        gain_rows(total, grad_gain_one, grad_qscale, grad_kscale, grad_gain_two),
    )
    return (
        output,
        grad_inputs.astype(low).reshape(groups, rows, width),
        out_gains[0, : attn_gain.shape[0]],
        out_qkv[:, : H * HD],
        out_qkv[:, H * HD : (H + KVH) * HD],
        out_qkv[:, (H + KVH) * HD :],
        out_gains[1, : query_gain.shape[0]],
        out_gains[2, : key_gain.shape[0]],
        out_output,
        out_gains[3, : mlp_gain.shape[0]],
        out_g,
        out_u,
        out_down,
    )


def solution(mesh):
    return jax.shard_map(
        on_device,
        mesh=mesh,
        in_specs=(
            P("fsdp", "ctx", None),
            P("fsdp", "ctx", None),
            P("fsdp", None),
            P(("ctx", "fsdp")),
            P(("ctx", "fsdp"), None),
            P(("ctx", "fsdp"), None),
            P(("ctx", "fsdp"), None),
            P(("ctx", "fsdp")),
            P(("ctx", "fsdp")),
            P(("ctx", "fsdp"), None),
            P(("ctx", "fsdp")),
            P(("ctx", "fsdp"), None),
            P(("ctx", "fsdp"), None),
            P(("ctx", "fsdp"), None),
        ),
        out_specs=(
            P("fsdp", "ctx", None),
            P("fsdp", "ctx", None),
            P(("ctx", "fsdp")),
            P(("ctx", "fsdp"), None),
            P(("ctx", "fsdp"), None),
            P(("ctx", "fsdp"), None),
            P(("ctx", "fsdp")),
            P(("ctx", "fsdp")),
            P(("ctx", "fsdp"), None),
            P(("ctx", "fsdp")),
            P(("ctx", "fsdp"), None),
            P(("ctx", "fsdp"), None),
            P(("ctx", "fsdp"), None),
        ),
        check_vma=False,
    )
```

```python
import functools
import itertools
import math

import jax
import jax.numpy as jnp
from jax import lax
from jax.experimental import pallas as pl
from jax.experimental.pallas import tpu as pltpu
from jax.sharding import PartitionSpec as P

MESH = pl.DeviceIdType.MESH
ANY = pl.BlockSpec(memory_space=pl.ANY)


H = 16
KVH = 8
HD = 128
BLK = 128


EPSILON = 1e-06
ROPE_BASE = 1000000.0


def rope_tables(positions):
    half = HD // 2
    freqs = jnp.exp(jnp.arange(half, dtype=jnp.float32) * (-2.0 * math.log(ROPE_BASE) / HD))
    angles = positions.astype(jnp.float32)[..., None] * freqs
    cosine = jnp.cos(angles)
    sine = jnp.sin(angles)
    return (jnp.concatenate([cosine, cosine], axis=-1), jnp.concatenate([sine, sine], axis=-1))


def rotate(value_vectors):
    half = value_vectors.shape[-1] // 2
    return jnp.concatenate([-value_vectors[..., half:], value_vectors[..., :half]], axis=-1)


def unrotate(value_vectors):
    half = value_vectors.shape[-1] // 2
    return jnp.concatenate([value_vectors[..., half:], -value_vectors[..., :half]], axis=-1)


def left_dot(left, right):
    return lax.dot_general(
        left, right, (((0,), (0,)), ((), ())), preferred_element_type=jnp.float32
    )


def right_dot(left, right):
    return lax.dot_general(
        left, right, (((1,), (1,)), ((), ())), preferred_element_type=jnp.float32
    )


def plain_dot(left, right):
    return jnp.dot(left, right, preferred_element_type=jnp.float32)


def norm_back(grad_normed, unit, inverse, gain):
    scaled = grad_normed * gain
    return inverse * (scaled - unit * jnp.mean(scaled * unit, axis=-1, keepdims=True))


class Grid:
    def __init__(self, ctx, fsdp):
        self.sizes = {"a": ctx // 4, "b": 2, "core": 2, "f": fsdp}
        self.stride = {"a": 4, "b": 2, "core": 1}

    def enter(self):
        self.c = lax.axis_index("ctx")
        self.at = {
            "a": self.c // 4,
            "b": (self.c // 2) % 2,
            "core": self.c % 2,
            "f": lax.axis_index("fsdp"),
        }

    def barrier(self):
        sem = pltpu.get_barrier_semaphore()
        count = 0
        for axis in ("core", "b", "a", "f"):
            n, p = self.sizes[axis], self.at[axis]
            for step in range(1, n):
                pl.semaphore_signal(
                    sem, inc=1, device_id=self.peer(axis, lax.rem(p + step, n)), device_id_type=MESH
                )
                count += 1
        pl.semaphore_wait(sem, count)

    def peer(self, axis, place):
        if axis == "f":
            return {"fsdp": place}
        return {"ctx": self.c + (place - self.at[axis]) * self.stride[axis]}

    def sources(self, axis):
        n, p = self.sizes[axis], self.at[axis]
        if n == 2:
            return [(None, 1 - p, None, None)]
        found = []
        for step in range(1, n):
            for way in (1, -1):
                origin = p - way * step
                onward = p + way
                found.append(
                    (
                        jnp.logical_and(origin >= 0, origin < n),
                        origin,
                        onward,
                        jnp.logical_and(
                            jnp.logical_and(origin >= 0, origin < n),
                            jnp.logical_and(onward >= 0, onward < n),
                        ),
                    )
                )
        return found

    def around(self, axis):
        n, p = self.sizes[axis], self.at[axis]
        if n == 2:
            return [(None, 1 - p)]
        return [(p + 1 < n, p + 1), (p >= 1, p - 1)]

    def spread(self, axis):
        n, p = self.sizes[axis], self.at[axis]
        if n == 2:
            return [p, 1 - p]
        order = [0]
        for step in range(1, n):
            for way in (step, n - step):
                if way not in order:
                    order.append(way)
        return [lax.rem(p + s, n) for s in order]

    def others(self, axis):
        n, p = self.sizes[axis], self.at[axis]
        return [1 - p] if n == 2 else [lax.rem(p + step, n) for step in range(1, n)]

    def nearest(self, axis):
        return [self.at[axis]] + self.others(axis)


class Pool:
    def __init__(self, ref):
        self.ref, self.used = ref, 0

    def take(self, count):
        first = self.used
        self.used += count
        return self.ref.at[pl.ds(first, count)]


def guarded(cond, body):
    if cond is None:
        body()
    else:
        pl.when(cond)(body)


class Gather:
    def __init__(self, grid, order, src, dst, columns, send_sem, recv_sem, layout_axes):
        self.grid, self.order, self.src, self.dst = grid, order, src, dst
        self.columns, self.send_sem, self.recv_sem = columns, send_sem, recv_sem
        self.layout_axes = layout_axes
        self.sends = 0
        self.pending = []

    @staticmethod
    def semaphores(grid, order):
        near = {x: 1 if grid.sizes[x] == 2 else 2 for x in order}
        far = {x: 0 if grid.sizes[x] == 2 else 2 * (grid.sizes[x] - 1) for x in order}
        sends = near[order[0]] + far[order[0]] + sum(near[x] for x in order[1:])
        inner = 1
        for level in range(1, len(order)):
            axis = order[level]
            onward = sum(near[x] for x in order[level + 1 :])
            sends += inner * (far[axis] + max(far[axis], 1) * onward)
            inner *= grid.sizes[axis]
        return sends, grid.sizes[order[0]] + inner

    def view(self, places):
        idx = tuple(places.get(x, slice(None)) for x in self.layout_axes)
        return self.dst.at[idx + (slice(None), self.columns)]

    def unit_number(self, places):
        number = 0
        for x in self.order[1:]:
            number = number * self.grid.sizes[x] + places[x]
        return number

    def start(self, cond, view, axis, place, sem):
        slot = self.sends
        self.sends += 1

        def make():
            return pltpu.make_async_remote_copy(
                src_ref=view[0],
                dst_ref=view[1],
                send_sem=self.send_sem.at[slot],
                recv_sem=self.recv_sem.at[sem],
                device_id=self.grid.peer(axis, place),
                device_id_type=MESH,
            )

        guarded(cond, lambda: make().start())
        self.pending.append((cond, make))

    def wait_recv(self, view, sem):
        pltpu.make_async_remote_copy(
            src_ref=view,
            dst_ref=view,
            send_sem=self.send_sem.at[0],
            recv_sem=self.recv_sem.at[sem],
            device_id={},
            device_id_type=MESH,
        ).wait_recv()

    def own_places(self):
        return {x: self.grid.at[x] for x in self.order}

    def open(self):
        axis = self.order[0]
        own = self.view(self.own_places())
        for cond, place in self.grid.around(axis):
            self.start(cond, (self.src, own), axis, place, self.grid.at[axis])

    def first(self):
        axis = self.order[0]
        for cond, origin, onward, more in self.grid.sources(axis):
            view = self.view({**self.own_places(), axis: origin})
            guarded(cond, lambda: self.wait_recv(view, origin))
            if onward is not None:
                self.start(more, (view, view), axis, onward, origin)
        self.pass_on(None, 1, {x: self.grid.at[x] for x in self.order[1:]})

    def pass_on(self, cond, level, places):
        n1 = self.grid.sizes[self.order[0]]
        sem = n1 + self.unit_number(places)
        view = self.view(places)
        for axis in self.order[level:]:
            for near, place in self.grid.around(axis):
                both = near if cond is None else cond if near is None else jnp.logical_and(cond, near)
                self.start(both, (view, view), axis, place, sem)

    def arrivals(self, level):
        n1 = self.grid.sizes[self.order[0]]
        axis = self.order[level]
        inner = [{}]
        for x in self.order[1:level]:
            inner = [{**places, x: j} for places in inner for j in self.grid.spread(x)]
        fixed = {x: self.grid.at[x] for x in self.order[level + 1 :]}
        for places in inner:
            for cond, origin, onward, more in self.grid.sources(axis):
                unit = {**places, **fixed, axis: origin}
                view = self.view(unit)
                sem = n1 + self.unit_number(unit)
                guarded(cond, lambda: self.wait_recv(view, sem))
                if onward is not None:
                    self.start(more, (view, view), axis, onward, sem)
                self.pass_on(cond, level + 1, unit)

    def close(self):
        for cond, make in self.pending:
            guarded(cond, lambda: make().wait_send())


def add_into(total, terms, out=None):
    shape = total.shape
    rows = min(16, shape[-2])
    steps = shape[-2] // rows
    lead = math.prod(shape[:-2])

    def body(i, carry):
        index = ()
        rest = i // steps
        for n in reversed(shape[:-2]):
            index = (lax.rem(rest, n),) + index
            rest = rest // n
        at = index + (pl.ds(pl.multiple_of(lax.rem(i, steps) * rows, rows), rows), slice(None))
        value = total[at].astype(jnp.float32)
        for term in terms:
            value = value + term[at].astype(jnp.float32)
        if out is None:
            total[at] = value.astype(total.dtype)
        else:
            out[at] = value.astype(out.dtype)
        return carry

    lax.fori_loop(0, lead * steps, body, 0)


class Scatter:
    def __init__(self, grid, order, src, columns, own, recvs, load_sem, send_sem, recv_sem, out, layout_axes):
        self.grid, self.order, self.src, self.columns = grid, order, src, columns
        self.own, self.recvs, self.out = own, recvs, out
        self.load_sem, self.send_sem, self.recv_sem = load_sem, send_sem, recv_sem
        self.layout_axes = layout_axes
        self.pending = []
        self.base = {}
        self.top = len(order) - 1
        number = 0
        for level in range(self.top, -1, -1):
            self.base[level] = number
            number += self.slots(grid, order, level)

    @staticmethod
    def inner(grid, order, level):
        return [grid.sizes[x] for x in order[1:level]]

    @staticmethod
    def slots(grid, order, level):
        return (grid.sizes[order[level]] - 1) * math.prod(Scatter.inner(grid, order, level))

    @staticmethod
    def scratch(grid, order, rows, columns, dtype):
        n1 = grid.sizes[order[0]]
        shapes = [tuple(grid.sizes[x] for x in order[1:-1]) + (n1, rows, columns)]
        for level, axis in enumerate(order):
            block = (rows, columns) if level == 0 else (n1, rows, columns)
            shapes.append((grid.sizes[axis] - 1,) + tuple(Scatter.inner(grid, order, level)) + block)
        return [pltpu.VMEM(x, dtype) for x in shapes]

    @staticmethod
    def semaphores(grid, order):
        loads = math.prod(grid.sizes[x] for x in order[1:-1])
        slots = sum(Scatter.slots(grid, order, level) for level in range(len(order)))
        return loads, slots, slots

    def hbm(self, places):
        idx = tuple(places.get(x, slice(None)) for x in self.layout_axes)
        return self.src.at[idx + (slice(None), self.columns)]

    def units(self, level):
        found = [{}]
        for x in self.order[1:level]:
            found = [{**places, x: j} for places in found for j in reversed(self.grid.nearest(x))]
        return found

    def mine(self, places):
        return self.own.at[tuple(places.get(x, self.grid.at[x]) for x in self.order[1:-1])]

    def number(self, places, axes):
        value = 0
        for x in axes:
            value = value * self.grid.sizes[x] + places[x]
        return value

    def slot(self, level, places, line):
        axes = self.order[1:level]
        number = line * math.prod(self.grid.sizes[x] for x in axes) + self.number(places, axes)
        ref = self.recvs[level].at[(line,) + tuple(places[x] for x in axes)]
        return ref, self.recv_sem.at[self.base[level] + number]

    def send(self, level, places, step, place, view):
        axis = self.order[level]
        ref, sem = self.slot(level, places, self.grid.sizes[axis] - 1 - step)
        copy = pltpu.make_async_remote_copy(
            src_ref=view,
            dst_ref=ref,
            send_sem=self.send_sem.at[len(self.pending)],
            recv_sem=sem,
            device_id=self.grid.peer(axis, place),
            device_id_type=MESH,
        )
        copy.start()
        self.pending.append(copy)

    def take(self, level, places, total, out=None):
        lines = self.grid.sizes[self.order[level]] - 1
        terms = []
        for line in range(lines):
            ref, sem = self.slot(level, places, line)
            pltpu.make_async_remote_copy(
                src_ref=ref,
                dst_ref=ref,
                send_sem=self.send_sem.at[0],
                recv_sem=sem,
                device_id={},
                device_id_type=MESH,
            ).wait_recv()
            terms.append(ref)
        add_into(total, terms, out)

    def load(self, places):
        here = {**places, self.order[-1]: self.grid.at[self.order[-1]]}
        number = self.number(places, self.order[1:-1])
        return pltpu.make_async_copy(self.hbm(here), self.mine(places), self.load_sem.at[number])

    def open(self):
        axis = self.order[self.top]
        for places in self.units(self.top):
            for step, place in enumerate(self.grid.others(axis), 1):
                self.send(self.top, places, step, place, self.hbm({**places, axis: place}))
            self.load(places).start()

    def settle(self, level, places):
        if level + 1 == self.top:
            self.load(places).wait()
        self.take(level + 1, places, self.mine(places))

    def step(self, level):
        axis = self.order[level]
        if level == 0:
            self.settle(0, {})
            for step, place in enumerate(self.grid.others(axis), 1):
                self.send(0, {}, step, place, self.mine({}).at[place])
            return
        for places in self.units(level):
            for step, place in enumerate(self.grid.others(axis), 1):
                unit = {**places, axis: place}
                self.settle(level, unit)
                self.send(level, places, step, place, self.mine(unit))
            self.settle(level, {**places, axis: self.grid.at[axis]})

    def finish(self):
        self.take(0, {}, self.mine({}).at[self.grid.at[self.order[0]]], self.out)

    def close(self):
        for copy in self.pending:
            copy.wait_send()


def half_pairs(ref, s):
    rows = pl.ds(s * BLK, BLK)
    return jnp.concatenate([ref[rows, :HD], ref[rows, HD:]], axis=0)


def read_map(blocks, table, pairs):
    @pl.when(pl.program_id(0) == 0)
    def _():
        for t in range(2 * pairs):
            table[blocks[t]] = t
        place = lax.axis_index("ctx")
        first, second = blocks[2 * place], blocks[2 * place + 1]
        table[2 * pairs] = jnp.where(second > first, 1, 0)
        table[2 * pairs + 1] = jnp.maximum(first, second)


def items(table, pairs):
    high_slot, high = table[pairs * 2], table[pairs * 2 + 1]
    low_block = 2 * pairs - 1 - high
    split = high // 2
    found = []
    for w in range(pairs - 1):
        upper = w < split
        found.append((jnp.where(upper, high_slot, 1 - high_slot), jnp.where(upper, w, w - split), None))
    found.append((high_slot, split, high))
    found.append((1 - high_slot, low_block // 2, low_block))
    return found


def chunk_of(ref, table, c):
    return jnp.concatenate(
        [ref[pl.ds(pl.multiple_of(table[2 * c + i] * BLK, BLK), BLK), :] for i in range(2)], axis=0
    )


def row_contract(left, right):
    return lax.dot_general(left, right, (((1,), (1,)), ((), ())), preferred_element_type=jnp.float32)


def attention_kernel(pairs, blocks, q_ref, k_ref, v_ref, o_ref, low_ref, over_ref, table, qs, acc, tot):
    read_map(blocks, table, pairs)
    for s in range(2):
        qs[s] = half_pairs(q_ref, s)
    acc[...] = jnp.zeros_like(acc)
    tot[...] = jnp.zeros_like(tot)
    for s, c, block in items(table, pairs):
        keys = chunk_of(k_ref, table, c)
        vals = chunk_of(v_ref, table, c)
        scores = row_contract(qs[s], keys) * (HD ** (-0.5) * math.log2(math.e))
        weights = jnp.exp2(scores)
        if block is not None:
            rows = lax.broadcasted_iota(jnp.int32, (2 * BLK, 2 * BLK), 0)
            cols = lax.broadcasted_iota(jnp.int32, (2 * BLK, 2 * BLK), 1)
            allowed = cols <= lax.rem(rows, BLK) + (block - 2 * c) * BLK
            weights = jnp.where(allowed, weights, 0.0)
        tot[s] += weights[:, :HD] + weights[:, HD:]
        acc[s] += jnp.dot(weights.astype(jnp.bfloat16), vals, preferred_element_type=jnp.float32)
    for s in range(2):
        over = 1.0 / jnp.sum(tot[s], axis=1, keepdims=True)
        value = acc[s] * over
        over = jnp.broadcast_to(over, value.shape)
        rows = pl.ds(s * BLK, BLK)
        for i in range(2):
            part = value[i * BLK : (i + 1) * BLK]
            o_ref[rows, i * HD : (i + 1) * HD] = part
            low_ref[rows, i * HD : (i + 1) * HD] = part.astype(jnp.bfloat16)
            over_ref[rows, i * HD : (i + 1) * HD] = over[i * BLK : (i + 1) * BLK]


def attention(blocks, pairs, queries, keys, values):
    rows, length = queries.shape[0], keys.shape[0]
    head = pl.BlockSpec((rows, 2 * HD), lambda h, t: (0, h))
    side = pl.BlockSpec((length, HD), lambda h, t: (0, h))
    return pl.pallas_call(
        functools.partial(attention_kernel, pairs),
        grid_spec=pltpu.PrefetchScalarGridSpec(
            num_scalar_prefetch=1,
            grid=(KVH,),
            in_specs=[head, side, side],
            out_specs=[head, head, head],
            scratch_shapes=[
                pltpu.SMEM((2 * pairs + 2,), jnp.int32),
                pltpu.VMEM((2, 2 * BLK, HD), jnp.bfloat16),
                pltpu.VMEM((2, 2 * BLK, HD), jnp.float32),
                pltpu.VMEM((2, 2 * BLK, HD), jnp.float32),
            ],
        ),
        out_shape=[
            jax.ShapeDtypeStruct((rows, H * HD), jnp.float32),
            jax.ShapeDtypeStruct((rows, H * HD), jnp.bfloat16),
            jax.ShapeDtypeStruct((rows, H * HD), jnp.float32),
        ],
        name="attention",
    )(blocks, queries, keys, values)


def attention_back_kernel(
    pairs, blocks, q_ref, k_ref, v_ref, g_ref, o_ref, dq_ref, dk_ref, dv_ref, table, qs, gs, drift, dq, dk, dv
):
    read_map(blocks, table, pairs)
    scale = HD ** (-0.5)
    for s in range(2):
        qs[s] = half_pairs(q_ref, s)
        gs[s] = half_pairs(g_ref, s)
        products = gs[s].astype(jnp.float32) * half_pairs(o_ref, s)
        drift[s : s + 1, :] = jnp.sum(products.T, axis=0, keepdims=True)
    for total in (dq, dk, dv):
        total[...] = jnp.zeros_like(total)
    for s, c, block in items(table, pairs):
        keys = chunk_of(k_ref, table, c)
        vals = chunk_of(v_ref, table, c)
        queries, grads = qs[s], gs[s]
        weights = jnp.exp2(row_contract(keys, queries) * (scale * math.log2(math.e)))
        if block is not None:
            rows = lax.broadcasted_iota(jnp.int32, (2 * BLK, 2 * BLK), 0)
            cols = lax.broadcasted_iota(jnp.int32, (2 * BLK, 2 * BLK), 1)
            allowed = rows <= lax.rem(cols, BLK) + (block - 2 * c) * BLK
            weights = jnp.where(allowed, weights, 0.0)
        through = row_contract(vals, grads)
        scores = (weights * (through - drift[pl.ds(s, 1), :])).astype(jnp.bfloat16)
        to_values = jnp.dot(weights.astype(jnp.bfloat16), grads, preferred_element_type=jnp.float32)
        to_keys = jnp.dot(scores, queries, preferred_element_type=jnp.float32)
        for i in range(2):
            at = pl.ds(pl.multiple_of(table[2 * c + i] * BLK, BLK), BLK)
            dv[at, :] += to_values[i * BLK : (i + 1) * BLK]
            dk[at, :] += to_keys[i * BLK : (i + 1) * BLK]
        dq[s] += left_dot(scores, keys)
    dk_ref[...] = (dk[...] * scale).astype(jnp.bfloat16)
    dv_ref[...] = dv[...].astype(jnp.bfloat16)
    for s in range(2):
        for i in range(2):
            dq_ref[pl.ds(s * BLK, BLK), i * HD : (i + 1) * HD] = dq[s, i * BLK : (i + 1) * BLK] * scale


def attention_back(blocks, pairs, queries, keys, values, grads, attended):
    rows, length = queries.shape[0], keys.shape[0]
    head = pl.BlockSpec((rows, 2 * HD), lambda h, t: (0, h))
    side = pl.BlockSpec((length, HD), lambda h, t: (0, h))
    return pl.pallas_call(
        functools.partial(attention_back_kernel, pairs),
        grid_spec=pltpu.PrefetchScalarGridSpec(
            num_scalar_prefetch=1,
            grid=(KVH,),
            in_specs=[head, side, side, head, head],
            out_specs=[head, side, side],
            scratch_shapes=[
                pltpu.SMEM((2 * pairs + 2,), jnp.int32),
                pltpu.VMEM((2, 2 * BLK, HD), jnp.bfloat16),
                pltpu.VMEM((2, 2 * BLK, HD), jnp.bfloat16),
                pltpu.VMEM((2, 2 * BLK), jnp.float32),
                pltpu.VMEM((2, 2 * BLK, HD), jnp.float32),
                pltpu.VMEM((length, HD), jnp.float32),
                pltpu.VMEM((length, HD), jnp.float32),
            ],
        ),
        out_shape=[
            jax.ShapeDtypeStruct((rows, H * HD), jnp.float32),
            jax.ShapeDtypeStruct((length, KVH * HD), jnp.bfloat16),
            jax.ShapeDtypeStruct((length, KVH * HD), jnp.bfloat16),
        ],
        cost_estimate=pl.CostEstimate(
            flops=20 * (pairs + 1) * KVH * (2 * BLK) ** 2 * HD,
            bytes_accessed=14 * rows * H * HD + 8 * length * KVH * HD,
            transcendentals=(pairs + 1) * KVH * (2 * BLK) ** 2,
        ),
        name="attention_back",
    )(blocks, queries, keys, values, grads, attended)


ALL_AXES = ("a", "b", "core", "f")
SLOT_AXES = ("a", "b", "core")
CHIP_AXES = ("a", "b", "f")
BFA, AFB, FAB, FBA = ("b", "f", "a"), ("a", "f", "b"), ("f", "a", "b"), ("f", "b", "a")
ABF, BAF = ("a", "b", "f"), ("b", "a", "f")
AB, BA = ("a", "b", "core"), ("b", "a", "core")
CORE = ("core",)


FRONT_SRC = ("q", "k", "v", "o", "g", "u", "d", "gains")


def front_kernel(grid, plan, pieces, *refs):
    n = len(FRONT_SRC)
    src = dict(zip(FRONT_SRC, refs[:n]))
    tokens_ref, cosine_ref, sine_ref = refs[n : n + 3]
    rows_of = refs[n - 1]
    outs = refs[n + 3 : n + 15]
    wqkv_ref, wo_ref, wgu_ref, wd_ref, allgains_ref, k_out, v_out = outs[:7]
    normed_ref, gains_ref, raw_ref, qlow_ref, inv_ref = outs[7:]
    scratch = refs[n + 15 :]
    held = dict(zip(FRONT_SRC, scratch[:n]))
    weights, klow, vlow, gbuf, gmine = scratch[n : n + 5]
    send, recv, local, load = scratch[n + 5 :]
    grid.enter()
    grid.barrier()
    send, recv = Pool(send), Pool(recv)
    device = grid.c * grid.sizes["f"] + grid.at["f"]
    block_rows = lax.broadcasted_iota(jnp.int32, gmine.shape, 0)
    block = jnp.zeros(gmine.shape, jnp.float32)
    for i, (at, size) in enumerate(pieces):
        spot = at + device * size
        line = jnp.broadcast_to(rows_of[i : i + 1, :], (8, 128))
        line = pltpu.roll(line, lax.rem(spot, 128), 1)[:1]
        block = jnp.where(block_rows == spot // 128, line, block)
    gmine[...] = block.astype(gmine.dtype)
    copy = pltpu.make_async_copy(gmine, held["gains"], local.at[n - 1])
    copy.start()
    copy.wait()
    src["gains"] = held["gains"]
    width = tokens_ref.shape[1]
    rows = tokens_ref.shape[0]
    spans = {"q": (wqkv_ref, 0), "k": (wqkv_ref, H * HD), "v": (wqkv_ref, (H + KVH) * HD)}
    hidden = src["g"].shape[1]
    spans.update({"o": (wo_ref, 0), "g": (wgu_ref, 0), "u": (wgu_ref, hidden), "d": (wd_ref, 0)})
    spans["gains"] = (allgains_ref, 0)
    mine = tuple(grid.at[x] for x in ALL_AXES)

    def own_copy(i, name):
        dst, at = spans[name]
        return pltpu.make_async_copy(
            held[name], dst.at[mine + (slice(None), pl.ds(at, src[name].shape[1]))], local.at[i]
        )

    for i, name in enumerate(FRONT_SRC[:-1]):
        pltpu.make_async_copy(src[name], held[name], local.at[i]).start()

    def part(name, low, high, order):
        dst, at = spans[name]
        sends, takes = Gather.semaphores(grid, order)
        columns = pl.ds(at + low, high - low)
        return Gather(
            grid, order, src[name].at[:, low:high], dst, columns, send.take(sends), recv.take(takes), ALL_AXES
        )

    early = [part(*p) for p in plan[0]]
    late = [part(*p) for p in plan[1]]
    for p in early:
        p.open()
    for p in late:
        p.open()
    for i, name in enumerate(FRONT_SRC):
        if name != "gains":
            pltpu.make_async_copy(src[name], held[name], local.at[i]).wait()
        own_copy(i, name).start()
    inputs = tokens_ref[...].astype(jnp.float32)
    inverse = lax.rsqrt(jnp.mean(inputs * inputs, axis=-1, keepdims=True) + EPSILON)
    inv_ref[...] = jnp.broadcast_to(inverse, (rows, 128))
    for i, name in enumerate(FRONT_SRC):
        own_copy(i, name).wait()

    for p in early:
        p.first()
    for level in (1, 2):
        for p in early:
            p.arrivals(level)
    pump = []
    for p in late:
        pump.append(p.first)
    for level in (1, 2, 3):
        for p in late:
            pump.append(functools.partial(p.arrivals, level))

    def step(count):
        for _ in range(count):
            if pump:
                pump.pop(0)()

    step(len(late))
    for p in early:
        p.arrivals(3)

    places = math.prod(grid.sizes[x] for x in ALL_AXES)
    copy = pltpu.make_async_copy(allgains_ref, gbuf, load.at[0])
    copy.start()
    big = pltpu.make_async_copy(wqkv_ref, weights, load.at[1])
    big.start()
    copy.wait()
    blocks = gbuf[...].reshape((places,) + gbuf.shape[-2:]).astype(jnp.float32)
    gains = jnp.sum(blocks, axis=0)
    gains_ref[...] = gains
    lanes = width // 128
    for j in range(lanes):
        cols = slice(j * 128, (j + 1) * 128)
        part_of = tokens_ref[:, cols].astype(jnp.float32) * inv_ref[...] * gains_ref[j : j + 1, :]
        normed_ref[:, cols] = part_of.astype(jnp.bfloat16)
    big.wait()
    step(1)
    flat = weights.reshape(width, weights.shape[-1])
    normed = normed_ref[...]
    chunk = 2 * HD

    def heads(low_out, gain_row, out_at, raw_at, c):
        at = pl.ds(pl.multiple_of(raw_at + c * chunk, chunk), chunk)
        raw = jnp.dot(normed, flat[:, at], preferred_element_type=jnp.float32)
        raw_ref[:, at] = raw
        done = []
        for i in range(2):
            one = raw[:, i * HD : (i + 1) * HD]
            unit = one * lax.rsqrt(jnp.mean(one * one, axis=-1, keepdims=True) + EPSILON)
            unit = unit * gains_ref[gain_row : gain_row + 1, :]
            done.append(unit * cosine_ref[...] + pltpu.roll(unit, HD // 2, 1) * sine_ref[...])
        to = pl.ds(pl.multiple_of(out_at + c * chunk, chunk), chunk)
        low_out[:, to] = jnp.concatenate(done, axis=1).astype(jnp.bfloat16)

    def loop(count, body):
        def once(c, carry):
            body(c)
            return carry

        lax.fori_loop(0, count, once, 0)

    def to_values(c):
        at = pl.ds(pl.multiple_of((H + KVH) * HD + c * chunk, chunk), chunk)
        to = pl.ds(pl.multiple_of(c * chunk, chunk), chunk)
        raw = jnp.dot(normed, flat[:, at], preferred_element_type=jnp.float32)
        vlow[:, to] = raw.astype(jnp.bfloat16)

    loop(KVH // 2, functools.partial(heads, klow, 2 * lanes + 1, 0, H * HD))
    loop(KVH // 2, to_values)

    def pair(source, dst, order):
        sends, takes = Gather.semaphores(grid, order)
        return Gather(
            grid, order, source, dst, pl.ds(0, KVH * HD), send.take(sends), recv.take(takes), SLOT_AXES
        )

    slot = tuple(grid.at[x] for x in SLOT_AXES)
    slabs = [pair(klow, k_out, AB), pair(vlow, v_out, BA)]
    saves = [
        pltpu.make_async_copy(klow, k_out.at[slot], load.at[0]),
        pltpu.make_async_copy(vlow, v_out.at[slot], load.at[1]),
    ]
    for p, save in zip(slabs, saves):
        p.open()
        save.start()
    step(2)
    loop(KVH // 2, functools.partial(heads, qlow_ref, 2 * lanes, 0, 0))
    for p, save in zip(slabs, saves):
        save.wait()
        p.first()
    step(2)
    loop(KVH // 2, functools.partial(heads, qlow_ref, 2 * lanes, H * HD // 2, H * HD // 2))
    for p in slabs:
        p.arrivals(1)
    step(len(pump))
    for p in slabs:
        p.arrivals(2)
    for p in early + late + slabs:
        p.close()


def front(grid, plan, pieces, blocks, gain_rows, tokens, cosine, sine):
    n = len(FRONT_SRC)
    rows, width = tokens.shape
    places = tuple(grid.sizes[x] for x in ALL_AXES)
    slots = tuple(grid.sizes[x] for x in SLOT_AXES)
    gains = jax.ShapeDtypeStruct((width // 128 * 2 + 16, 128), jnp.bfloat16)
    blocks = tuple(blocks) + (gains,)
    by = dict(zip(FRONT_SRC, blocks))
    low, f32 = jnp.bfloat16, jnp.float32
    full = (H + 2 * KVH) * HD
    counts = [Gather.semaphores(grid, p[3]) for p in plan[0] + plan[1]]
    counts += [Gather.semaphores(grid, AB), Gather.semaphores(grid, BA)]
    sends, takes = [sum(x) for x in zip(*counts)]
    shape = jax.ShapeDtypeStruct
    vmem = pl.BlockSpec(memory_space=pltpu.VMEM)
    outs = pl.pallas_call(
        functools.partial(front_kernel, grid, plan, pieces),
        out_shape=[
            shape(places + (by["q"].shape[0], full), low),
            shape(places + by["o"].shape, low),
            shape(places + (by["g"].shape[0], 2 * by["g"].shape[1]), low),
            shape(places + by["d"].shape, low),
            shape(places + by["gains"].shape, low),
            shape(slots + (rows, KVH * HD), low),
            shape(slots + (rows, KVH * HD), low),
            shape((rows, width), low),
            shape(by["gains"].shape, f32),
            shape((rows, (H + KVH) * HD), f32),
            shape((rows, H * HD), low),
            shape((rows, 128), f32),
        ],
        in_specs=[ANY] * (n - 1) + [vmem] * 4,
        out_specs=[ANY] * 7 + [vmem] * 5,
        scratch_shapes=[pltpu.VMEM(x.shape, x.dtype) for x in blocks]
        + [
            pltpu.VMEM(places + (by["q"].shape[0], full), low),
            pltpu.VMEM((rows, KVH * HD), low),
            pltpu.VMEM((rows, KVH * HD), low),
            pltpu.VMEM(places + by["gains"].shape, low),
            pltpu.VMEM(by["gains"].shape, low),
            pltpu.SemaphoreType.DMA((sends,)),
            pltpu.SemaphoreType.DMA((takes,)),
            pltpu.SemaphoreType.DMA((n,)),
            pltpu.SemaphoreType.DMA((2,)),
        ],
        compiler_params=pltpu.CompilerParams(
            has_side_effects=True, vmem_limit_bytes=60 * 2**20, collective_id=0
        ),
        name="front",
    )(*blocks[:-1], gain_rows, tokens, cosine, sine)
    wqkv, wo, wgu, wd, _, keys, vals, normed, gains, raw, qlow, inverse = outs
    flat = [x.reshape(-1, x.shape[-1]) for x in (wqkv, wo, wgu, wd, keys, vals)]
    return flat + [normed, gains, raw, qlow, inverse]


def sums_kernel(count, core, left, left_other, right, right_other, out, turned):
    rows, width = left.shape
    block = width // count

    @pl.when(pl.program_id(0) == 0)
    def _():
        for j in range(count // 2):
            at = pl.ds(pl.multiple_of((2 * j + core[0]) * block, block), block)
            for k, ref in enumerate((left, left_other)):
                turned[j * block : (j + 1) * block, k * rows : (k + 1) * rows] = ref[:, at].T

    rhs = jnp.concatenate([right[...], right_other[...]], axis=0)
    out[...] = jnp.dot(turned[...], rhs, preferred_element_type=jnp.float32).astype(out.dtype)


def chip_sums(left, left_other, right, right_other):
    rows, width = left.shape
    count = lax.axis_size("ctx")
    block = width // count
    tile = 512
    if block % 128:
        place = lax.axis_index("ctx") % 2
        halves = [
            lax.dynamic_index_in_dim(x.reshape(rows, count // 2, 2, block), place, 2, False)
            for x in (left, left_other)
        ]
        lhs = jnp.concatenate(halves, axis=0).reshape(2 * rows, width // 2)
        return left_dot(lhs, jnp.concatenate([right, right_other], axis=0)).astype(jnp.bfloat16)
    core = (lax.axis_index("ctx") % 2).astype(jnp.int32)[None]
    lhs = pl.BlockSpec((rows, width), lambda n, c: (0, 0))
    rhs = pl.BlockSpec((rows, tile), lambda n, c: (0, n))
    return pl.pallas_call(
        functools.partial(sums_kernel, count),
        grid_spec=pltpu.PrefetchScalarGridSpec(
            num_scalar_prefetch=1,
            grid=(right.shape[1] // tile,),
            in_specs=[lhs, lhs, rhs, rhs],
            out_specs=pl.BlockSpec((width // 2, tile), lambda n, c: (0, n)),
            scratch_shapes=[pltpu.VMEM((width // 2, 2 * rows), jnp.bfloat16)],
        ),
        out_shape=jax.ShapeDtypeStruct((width // 2, right.shape[1]), jnp.bfloat16),
        name="chip_sums",
    )(core, left, left_other, right, right_other)


def handed_kernel(*refs):
    for source, out in zip(refs[: len(refs) // 2], refs[len(refs) // 2 :]):
        out[...] = source[...]


def handed(*results):
    vmem = pl.BlockSpec(memory_space=pltpu.VMEM)
    return pl.pallas_call(
        handed_kernel,
        out_shape=[jax.ShapeDtypeStruct(x.shape, x.dtype) for x in results],
        in_specs=[vmem] * len(results),
        out_specs=[vmem] * len(results),
        name="handed",
    )(*results)


BACK_SUMS = ("g", "u", "d", "o")


def back_kernel(grid, plan, *refs):
    refs = list(refs)

    def take(n):
        found = refs[:n]
        del refs[:n]
        return found

    src = dict(zip(BACK_SUMS, take(len(BACK_SUMS))))
    gk_ref, gv_ref, wqkv_ref = take(3)
    dq_ref, raw_ref, cos_ref, turn_ref, gains_ref, normed_ref, tokens_ref, inv_ref, mid_ref, gain2_ref = take(10)
    outs = dict(zip(BACK_SUMS + ("q", "k", "v"), take(len(BACK_SUMS) + 3)))
    din_ref, gsum_ref, sums_ref, gall_ref = take(4)
    weights, both_normed, both_raw, own_k, own_v, stage, acc, gbuf, gblock = take(9)
    load, send, recv, misc = [Pool(x) for x in refs[-4:]]
    del refs[-4:]
    scratch = refs
    grid.enter()
    grid.barrier()
    rows, width = tokens_ref.shape
    lanes = width // 128
    core = grid.at["core"]
    chunk = 2 * HD
    misc_sem = [misc.take(1).at[0] for _ in range(12)]

    def make(source, columns, order, out, layout):
        loads, sends, takes = Scatter.semaphores(grid, order)
        own, *recvs = scratch[: 1 + len(order)]
        del scratch[: 1 + len(order)]
        return Scatter(
            grid, order, source, columns, own, recvs,
            load.take(loads), send.take(sends), recv.take(takes), out, layout,
        )

    def portions(group):
        found = []
        for name, low, high, order in group:
            found.append(
                make(src[name], pl.ds(low, high - low), order, outs[name].at[:, low:high], CHIP_AXES)
            )
        return found

    slabs = [
        make(gk_ref, pl.ds(0, KVH * HD), AB, own_k, SLOT_AXES),
        make(gv_ref, pl.ds(0, KVH * HD), BA, own_v, SLOT_AXES),
    ]
    early, waves = portions(plan[0]), [portions(group) for group in plan[1]]
    late = [p for wave in waves for p in wave]
    last = []
    for name, at, low, high, order in plan[2]:
        last.append(
            make(sums_ref, pl.ds(at + low, high - low), order, outs[name].at[:, low:high], CHIP_AXES)
        )

    def sibling(source, dst, k):
        return pltpu.make_async_remote_copy(
            src_ref=source, dst_ref=dst, send_sem=misc_sem[2 * k], recv_sem=misc_sem[2 * k + 1],
            device_id=grid.peer("core", 1 - core), device_id_type=MESH,
        )

    for p in slabs + early:
        p.open()
    swap_normed = sibling(normed_ref, both_normed.at[1], 0)
    swap_normed.start()
    both_normed[0] = normed_ref[...]
    gblock[...] = jnp.zeros_like(gblock)
    gblock[lanes : 2 * lanes, :] = gain2_ref[...]

    def loop(count, body):
        def once(c, carry):
            body(c)
            return carry

        lax.fori_loop(0, count, once, 0)

    def heads(source, in_at, raw_at, gain_row, c):
        at = pl.ds(pl.multiple_of(raw_at + c * chunk, chunk), chunk)
        grads = source[:, pl.ds(pl.multiple_of(in_at + c * chunk, chunk), chunk)]
        raw = raw_ref[:, at]
        gain = gains_ref[gain_row : gain_row + 1, :]
        done = []
        for i in range(2):
            g = grads[:, i * HD : (i + 1) * HD]
            g = g * cos_ref[...] - pltpu.roll(g, HD // 2, 1) * turn_ref[...]
            one = raw[:, i * HD : (i + 1) * HD]
            inverse = lax.rsqrt(jnp.mean(one * one, axis=-1, keepdims=True) + EPSILON)
            unit = one * inverse
            gblock[gain_row : gain_row + 1, :] += jnp.sum(g * unit, axis=0, keepdims=True)
            done.append(norm_back(g, unit, inverse, gain))
        both_raw[0, :, at] = jnp.concatenate(done, axis=1).astype(jnp.bfloat16)

    half_q = H * HD // 2
    q_cols, kv_cols = pl.ds(0, H * HD), pl.ds(H * HD, 2 * KVH * HD)
    loop(H // 4, functools.partial(heads, dq_ref, 0, 0, 2 * lanes))
    for p in slabs:
        p.step(1)
    loop(H // 4, functools.partial(heads, dq_ref, half_q, half_q, 2 * lanes))
    swap_q = sibling(both_raw.at[0, :, q_cols], both_raw.at[1, :, q_cols], 1)
    swap_q.start()
    for p in slabs:
        p.step(0)
    def every(group, what, *args):
        for p in group:
            getattr(p, what)(*args)

    every(waves[0], "open")
    for p in slabs:
        p.finish()
    loop(KVH // 2, functools.partial(heads, own_k, 0, H * HD, 2 * lanes + 1))
    at = (H + KVH) * HD
    both_raw[0, :, at : at + KVH * HD] = own_v[...].astype(jnp.bfloat16)
    swap_kv = sibling(both_raw.at[0, :, kv_cols], both_raw.at[1, :, kv_cols], 2)
    swap_kv.start()
    every(waves[1], "open")
    swap_normed.wait()
    swap_q.wait()
    swap_kv.wait()
    flat_normed = both_normed.reshape(2 * rows, width)
    flat_raw = both_raw.reshape(2 * rows, both_raw.shape[-1])
    count = grid.sizes["a"] * grid.sizes["b"]
    block = width // (2 * count)
    piece = block // grid.sizes["f"]
    full = both_raw.shape[-1]
    tile = 512

    def stored(j):
        return pltpu.make_async_copy(stage.at[j % 2], sums_ref.at[j // 2, j % 2], misc_sem[9 + j % 2])

    for j in range(count):
        if j >= 2:
            stored(j - 2).wait()
        lhs = flat_normed[:, pl.ds(pl.multiple_of((2 * j + core) * block, block), block)]

        def sums(c):
            cols = pl.ds(pl.multiple_of(c * tile, tile), tile)
            value = left_dot(lhs, flat_raw[:, cols]).astype(jnp.bfloat16)
            stage[j % 2, :, :, cols] = value.reshape(grid.sizes["f"], piece, tile)

        loop(full // tile, sums)
        stored(j).start()
    for j in range(count - 2, count):
        stored(j).wait()
    every(waves[0], "step", 1)
    every(last, "open")
    every(waves[2], "open")
    every(early, "step", 1)
    every(waves[1], "step", 1)
    every(waves[0], "step", 0)
    tiles = [
        pltpu.make_async_copy(
            wqkv_ref.at[:, c * tile : (c + 1) * tile], weights.at[c % 2], misc_sem[6 + c % 2]
        )
        for c in range(full // tile)
    ]
    tiles[0].start()
    for c in range(full // tile):
        if c + 1 < full // tile:
            tiles[c + 1].start()
        tiles[c].wait()
        value = right_dot(both_raw[0, :, c * tile : (c + 1) * tile], weights[c % 2])
        acc[...] = value if c == 0 else acc[...] + value
    inverse = inv_ref[...]
    for j in range(lanes):
        cols = slice(j * 128, (j + 1) * 128)
        normal = tokens_ref[:, cols].astype(jnp.float32) * inverse
        gblock[j : j + 1, :] = jnp.sum(acc[:, cols] * normal, axis=0, keepdims=True)
    copy = pltpu.make_async_copy(gblock, gbuf, misc_sem[11])
    copy.start()
    copy.wait()
    order = FAB + CORE
    sends, takes = Gather.semaphores(grid, order)
    spread = Gather(
        grid, order, gbuf, gall_ref, slice(None), send.take(sends), recv.take(takes), ALL_AXES
    )
    spread.open()
    mine = tuple(grid.at[x] for x in ALL_AXES)
    gall_ref[mine] = gblock[...]
    every(early, "step", 0)
    every(last, "step", 1)
    every(waves[2], "step", 1)
    every(waves[1], "step", 0)
    spread.first()
    dots = jnp.zeros((rows, 1), jnp.float32)
    for j in range(lanes):
        cols = slice(j * 128, (j + 1) * 128)
        normal = tokens_ref[:, cols].astype(jnp.float32) * inverse
        dots += jnp.sum(acc[:, cols] * gains_ref[j : j + 1, :] * normal, axis=1, keepdims=True)
    dots = dots / width
    for j in range(lanes):
        cols = slice(j * 128, (j + 1) * 128)
        normal = tokens_ref[:, cols].astype(jnp.float32) * inverse
        grad = inverse * (acc[:, cols] * gains_ref[j : j + 1, :] - normal * dots)
        din_ref[:, cols] = (mid_ref[:, cols] + grad).astype(jnp.bfloat16)
    spread.arrivals(1)
    every(last, "step", 0)
    every(waves[2], "step", 0)
    spread.arrivals(2)
    every(waves[0] + early + waves[1], "finish")
    spread.arrivals(3)
    every(last + waves[2], "finish")
    places = math.prod(grid.sizes[x] for x in ALL_AXES)
    gsum_ref[...] = jnp.sum(gall_ref.reshape((places,) + gblock.shape)[...], axis=0)
    for p in slabs + early + late + last:
        p.close()
    spread.close()


def back_scratch(grid, plan, pieces, rows, width):
    low = jnp.bfloat16
    scratch, counts = [], []
    for order in (AB, BA):
        scratch += Scatter.scratch(grid, order, rows, KVH * HD, low)
        counts.append(Scatter.semaphores(grid, order))
    for name, begin, end, order in plan[0] + sum(plan[1], ()) + tuple((p[0],) + p[2:] for p in plan[2]):
        scratch += Scatter.scratch(grid, order, pieces[name], end - begin, low)
        counts.append(Scatter.semaphores(grid, order))
    return scratch, [sum(x) for x in zip(*counts)]


def back_fits(grid, plan, rows, width, hidden, total):
    pieces = {name: width // total for name in ("g", "u", "q", "k", "v")}
    pieces.update({"d": hidden // total, "o": H * HD // total})
    scratch = back_scratch(grid, plan, pieces, rows, width)[0]
    taken = sum(2 * math.prod(x.shape) for x in scratch)
    held = 2 * rows * (11 * width + 3 * (H + 2 * KVH) * HD + 4 * (H + KVH) * HD) + 6 * 2**20
    return taken + held < 62 * 2**20


def back(grid, plan, sums, gk, gv, wqkv, dq, raw, cosine, turned, gains, normed, tokens, inverse, middle, gain2):
    low, f32 = jnp.bfloat16, jnp.float32
    rows, width = tokens.shape
    chips = tuple(grid.sizes[x] for x in CHIP_AXES)
    places = tuple(grid.sizes[x] for x in ALL_AXES)
    slots = tuple(grid.sizes[x] for x in SLOT_AXES)
    blocks = [x.reshape(chips + (x.shape[0] // math.prod(chips), x.shape[1])) for x in sums]
    shape = jax.ShapeDtypeStruct
    vmem = pl.BlockSpec(memory_space=pltpu.VMEM)
    piece = width // math.prod(places)
    pieces = dict(zip(BACK_SUMS, [x.shape[-2] for x in blocks]))
    pieces.update({"q": piece, "k": piece, "v": piece})
    scratch, (loads, sends, takes) = back_scratch(grid, plan, pieces, rows, width)
    more = Gather.semaphores(grid, FAB + CORE)
    full = wqkv.shape[1]
    count = grid.sizes["a"] * grid.sizes["b"]
    outs = pl.pallas_call(
        functools.partial(back_kernel, grid, plan),
        out_shape=[shape(x.shape[-2:], f32) for x in blocks]
        + [shape((piece, n), f32) for n in (H * HD, KVH * HD, KVH * HD)]
        + [
            shape((rows, width), low),
            shape(gains.shape, f32),
            shape(chips + (piece, full), low),
        ],
        in_specs=[ANY] * (len(blocks) + 3) + [vmem] * 10,
        out_specs=[vmem] * (len(blocks) + 5) + [ANY],
        scratch_shapes=[
            pltpu.VMEM(places + gains.shape, f32),
            pltpu.VMEM((2, width, 512), low),
            pltpu.VMEM((2, rows, width), low),
            pltpu.VMEM((2, rows, full), low),
            pltpu.VMEM((rows, KVH * HD), f32),
            pltpu.VMEM((rows, KVH * HD), f32),
            pltpu.VMEM((2, grid.sizes["f"], piece, full), low),
            pltpu.VMEM((rows, width), f32),
            pltpu.VMEM(gains.shape, f32),
            pltpu.VMEM(gains.shape, f32),
        ]
        + scratch
        + [
            pltpu.SemaphoreType.DMA((loads,)),
            pltpu.SemaphoreType.DMA((sends + more[0],)),
            pltpu.SemaphoreType.DMA((takes + more[1],)),
            pltpu.SemaphoreType.DMA((12,)),
        ],
        compiler_params=pltpu.CompilerParams(
            has_side_effects=True, vmem_limit_bytes=63 * 2**20, collective_id=1
        ),
        name="back",
    )(
        *blocks,
        gk.reshape(slots + (rows, KVH * HD)),
        gv.reshape(slots + (rows, KVH * HD)),
        wqkv, dq, raw, cosine, turned, gains, normed, tokens, inverse, middle, gain2,
    )
    return outs


def middle_kernel(
    steps, alow_ref, over_ref, wo_ref, wg_ref, wu_ref, wd_ref, tokens_ref, cot_ref, gains_ref,
    out_ref, hidden_ref, gg_ref, gu_ref, normed_ref, mid_ref, branch_ref, gain_ref, gs_ref,
    middle, total, back, inv,
):
    c = pl.program_id(0)
    rows, width = tokens_ref.shape
    lanes = width // 128
    low = jnp.bfloat16

    @pl.when(c == 0)
    def _():
        value = tokens_ref[...].astype(jnp.float32) + plain_dot(alow_ref[...], wo_ref[...])
        inverse = lax.rsqrt(jnp.mean(value * value, axis=-1, keepdims=True) + EPSILON)
        inv[...] = jnp.broadcast_to(inverse, inv.shape)
        middle[...] = value
        total[...] = value
        for j in range(lanes):
            cols = slice(j * 128, (j + 1) * 128)
            gain = gains_ref[lanes + j : lanes + j + 1, :]
            normed_ref[:, cols] = (middle[:, cols] * inv[...] * gain).astype(low)
        back[...] = jnp.zeros_like(back)

    normed = normed_ref[...]
    gate = plain_dot(normed, wg_ref[...])
    upper = plain_dot(normed, wu_ref[...])
    grads = right_dot(cot_ref[...], wd_ref[...])
    sig = jax.nn.sigmoid(gate)
    activated = gate * sig
    hidden = (activated * upper).astype(low)
    grad_gate = (grads * upper * sig * (1.0 + gate * (1.0 - sig))).astype(low)
    grad_upper = (grads * activated).astype(low)
    hidden_ref[...] = hidden
    gg_ref[...] = grad_gate
    gu_ref[...] = grad_upper
    total[...] += plain_dot(hidden, wd_ref[...])
    back[...] += right_dot(grad_gate, wg_ref[...]) + right_dot(grad_upper, wu_ref[...])

    @pl.when(c == steps - 1)
    def _():
        out_ref[...] = total[...].astype(low)
        inverse = inv[...]
        dots = jnp.zeros((rows, 1), jnp.float32)
        for j in range(lanes):
            cols = slice(j * 128, (j + 1) * 128)
            normal = middle[:, cols] * inverse
            gain_ref[j : j + 1, :] = jnp.sum(back[:, cols] * normal, axis=0, keepdims=True)
            gain = gains_ref[lanes + j : lanes + j + 1, :]
            dots += jnp.sum(back[:, cols] * gain * normal, axis=1, keepdims=True)
        dots = dots / width
        for j in range(lanes):
            cols = slice(j * 128, (j + 1) * 128)
            gain = gains_ref[lanes + j : lanes + j + 1, :]
            normal = middle[:, cols] * inverse
            grad = cot_ref[:, cols].astype(jnp.float32) + inverse * (back[:, cols] * gain - normal * dots)
            mid_ref[:, cols] = grad
            branch_ref[:, cols] = grad.astype(low)
        tile = 512
        for j in range(gs_ref.shape[1] // tile):
            cols = slice(j * tile, (j + 1) * tile)
            attended = right_dot(branch_ref[...], wo_ref[cols, :])
            gs_ref[:, cols] = (attended * over_ref[:, cols]).astype(low)


def middle_part(alow, over, wo, wgu, wd, tokens, cotangent, gains):
    low, f32 = jnp.bfloat16, jnp.float32
    rows, width = tokens.shape
    hidden = wd.shape[0]
    tile = 512
    steps = hidden // tile
    shape = jax.ShapeDtypeStruct

    def whole(x):
        return pl.BlockSpec(x.shape, lambda c: (0,) * len(x.shape))

    def columns(at):
        return pl.BlockSpec((width, tile), lambda c: (0, at + c))

    chunk = pl.BlockSpec((rows, tile), lambda c: (0, c))
    outs = [
        shape((rows, width), low),
        shape((rows, hidden), low),
        shape((rows, hidden), low),
        shape((rows, hidden), low),
        shape((rows, width), low),
        shape((rows, width), f32),
        shape((rows, width), low),
        shape((width // 128, 128), f32),
        shape(alow.shape, low),
    ]
    return pl.pallas_call(
        functools.partial(middle_kernel, steps),
        grid=(steps,),
        in_specs=[
            whole(alow),
            whole(over),
            whole(wo),
            columns(0),
            columns(steps),
            pl.BlockSpec((tile, width), lambda c: (c, 0)),
            whole(tokens),
            whole(cotangent),
            whole(gains),
        ],
        out_specs=[whole(outs[0])] + [chunk] * 3 + [whole(x) for x in outs[4:]],
        out_shape=outs,
        scratch_shapes=[pltpu.VMEM((rows, width), f32)] * 3 + [pltpu.VMEM((rows, 128), f32)],
        compiler_params=pltpu.CompilerParams(vmem_limit_bytes=60 * 2**20),
        name="middle",
    )(alow, over, wo, wgu, wgu, wd, tokens, cotangent, gains)


def scatter_kernel(grid, portions, layouts, n, *refs):
    srcs, outs, scratch = refs[:n], refs[n : 2 * n], list(refs[2 * n : -3])
    load, send, recv = [Pool(x) for x in refs[-3:]]
    grid.enter()
    parts = []
    for i, low, high, order in portions:
        loads, sends, takes = Scatter.semaphores(grid, order)
        own, *recvs = scratch[: 1 + len(order)]
        del scratch[: 1 + len(order)]
        parts.append(
            Scatter(
                grid,
                order,
                srcs[i],
                pl.ds(low, high - low),
                own,
                recvs,
                load.take(loads),
                send.take(sends),
                recv.take(takes),
                outs[i].at[:, low:high],
                layouts[i],
            )
        )
        parts[-1].open()
    for level in (2, 1, 0):
        for part in parts:
            if level < part.top:
                part.step(level)
    for part in parts:
        part.finish()
    for part in parts:
        part.close()


def scatter(grid, layouts, portions, name, dtypes, *sums):
    n = len(sums)
    blocks = []
    for layout, x in zip(layouts, sums):
        places = tuple(grid.sizes[axis] for axis in layout)
        blocks.append(x.reshape(places + (x.shape[0] // math.prod(places), x.shape[1])))
    loads, sends, takes = [sum(x) for x in zip(*[Scatter.semaphores(grid, p[3]) for p in portions])]
    scratch = []
    for i, low, high, order in portions:
        scratch += Scatter.scratch(grid, order, blocks[i].shape[-2], high - low, blocks[i].dtype)
    return pl.pallas_call(
        functools.partial(scatter_kernel, grid, portions, layouts, n),
        out_shape=[jax.ShapeDtypeStruct(x.shape[-2:], t) for x, t in zip(blocks, dtypes)],
        in_specs=[ANY] * n,
        out_specs=[pl.BlockSpec(memory_space=pltpu.VMEM)] * n,
        scratch_shapes=scratch
        + [
            pltpu.SemaphoreType.DMA((loads,)),
            pltpu.SemaphoreType.DMA((sends,)),
            pltpu.SemaphoreType.DMA((takes,)),
        ],
        compiler_params=pltpu.CompilerParams(has_side_effects=True, vmem_limit_bytes=60 * 2**20),
        name=name,
    )(*blocks)


def gain_rows(total, *gains):
    pieces = [x.reshape(total, 1, -1) for x in gains]
    pieces = [jnp.pad(x, ((0, 0), (0, 0), (0, 128 - x.shape[2]))) for x in pieces]
    block = jnp.concatenate(pieces, axis=1)
    return jnp.pad(block, ((0, 0), (0, 8 - len(gains)), (0, 0))).reshape(total * 8, 128)


def swapped(x):
    count = lax.axis_size("ctx")
    return lax.ppermute(x, "ctx", [(i, i ^ 1) for i in range(count)])


def on_device(
    tokens,
    cotangent,
    block_map,
    attn_gain,
    query_weight,
    key_weight,
    value_weight,
    query_gain,
    key_gain,
    output_weight,
    mlp_gain,
    gate_weight,
    up_weight,
    down_weight,
):
    grid = Grid(lax.axis_size("ctx"), lax.axis_size("fsdp"))
    total = lax.axis_size("ctx") * lax.axis_size("fsdp")
    groups, rows, width = tokens.shape
    pairs = block_map.shape[1] // 2
    ratio = H // KVH
    low = jnp.bfloat16

    device = lax.axis_index("ctx") * lax.axis_size("fsdp") + lax.axis_index("fsdp")
    gain_pieces = [
        (at, x.shape[0])
        for at, x in ((0, attn_gain), (width, mlp_gain), (2 * width, query_gain), (2 * width + HD, key_gain))
    ]
    gain_lines = jnp.concatenate(
        [
            jnp.pad(x.astype(jnp.float32).reshape(1, -1), ((0, 0), (0, 128 - x.shape[0])))
            for x in (attn_gain, mlp_gain, query_gain, key_gain)
        ]
    )
    hidden_width = gate_weight.shape[1]

    place = lax.axis_index("ctx")
    blocks = block_map.reshape(-1)
    own_blocks = lax.dynamic_slice_in_dim(blocks, 2 * place, 2, 0)
    spots = (own_blocks[:, None] * BLK + jnp.arange(BLK, dtype=jnp.int32)).reshape(rows)
    cosine, sine = rope_tables(spots)
    turned = jnp.concatenate([-sine[:, : HD // 2], sine[:, HD // 2 :]], axis=1)
    half_q, half_k = H * HD // 2, KVH * HD // 2
    half = half_q + 2 * half_k
    plan = (
        (
            ("gains", 0, 128, FAB + CORE),
            ("q", 0, half_q, FAB + CORE),
            ("q", half_q, 2 * half_q, FBA + CORE),
            ("k", 0, 2 * half_k, BFA + CORE),
            ("v", 0, 2 * half_k, AFB + CORE),
        ),
        (
            ("o", 0, width // 2, ABF + CORE),
            ("o", width // 2, width, BAF + CORE),
            ("g", 0, hidden_width, BFA + CORE),
            ("u", 0, hidden_width, AFB + CORE),
            ("d", 0, width // 2, BFA + CORE),
            ("d", width // 2, width, AFB + CORE),
        ),
    )
    (
        full_qkv,
        full_output,
        full_gu,
        full_down,
        key_all,
        value_all,
        normed,
        gains,
        raw,
        query_low,
        inverse_one,
    ) = front(
        grid,
        plan,
        gain_pieces,
        (query_weight, key_weight, value_weight, output_weight, gate_weight, up_weight, down_weight),
        gain_lines,
        tokens.reshape(rows, width),
        cosine,
        turned,
    )
    attended, attended_low, over_totals = attention(blocks, pairs, query_low, key_all, value_all)
    lanes = width // 128
    gain_one = gains[:lanes].reshape(-1)
    query_scale, key_scale = gains[2 * lanes], gains[2 * lanes + 1]
    inverse_rows = inverse_one
    inverse_one = inverse_one[:, :1]
    inputs = tokens.reshape(rows, width).astype(jnp.float32)
    normal_one = inputs * inverse_one
    cosine = cosine.reshape(rows, 1, HD)
    sine = sine.reshape(rows, 1, HD)
    query_raw = raw[:, : H * HD].reshape(rows, H, HD)
    key_raw = raw[:, H * HD :].reshape(rows, KVH, HD)
    query_inverse = lax.rsqrt(jnp.mean(query_raw * query_raw, axis=-1, keepdims=True) + EPSILON)
    query_unit = query_raw * query_inverse
    key_inverse = lax.rsqrt(jnp.mean(key_raw * key_raw, axis=-1, keepdims=True) + EPSILON)
    key_unit = key_raw * key_inverse
    upstream = cotangent.reshape(rows, width)
    (
        output,
        hidden,
        grad_gate,
        grad_upper,
        normed_two,
        grad_middle,
        branch_grad,
        grad_gain_two,
        grad_summed,
    ) = middle_part(
        attended_low, over_totals, full_output, full_gu, full_down, tokens.reshape(rows, width), upstream, gains
    )
    output = output.reshape(groups, rows, width)
    grad_gain_two = grad_gain_two.reshape(width)
    normed_other, upstream_other = swapped(normed_two), swapped(upstream)
    grad_down = chip_sums(hidden, swapped(hidden), upstream, upstream_other)
    grad_g = chip_sums(normed_two, normed_other, grad_gate, swapped(grad_gate))
    grad_u = chip_sums(normed_two, normed_other, grad_upper, swapped(grad_upper))
    grad_woutput = chip_sums(attended_low, swapped(attended_low), branch_grad, swapped(branch_grad))
    grad_query, grad_keys, grad_values = attention_back(
        blocks, pairs, query_low, key_all, value_all, grad_summed, attended
    )
    back_plan = (
        (("d", 0, width // 2, ABF), ("d", width // 2, width, BAF)),
        (
            (("g", 0, hidden_width // 2, FAB), ("g", hidden_width // 2, hidden_width, FBA)),
            (("u", 0, hidden_width // 2, FAB), ("u", hidden_width // 2, hidden_width, FBA)),
            (("o", 0, width // 2, FAB), ("o", width // 2, width, FBA)),
        ),
        (
            ("q", 0, 0, half_q, ABF),
            ("q", 0, half_q, 2 * half_q, BAF),
            ("k", H * HD, 0, 2 * half_k, FAB),
            ("v", (H + KVH) * HD, 0, 2 * half_k, FBA),
        ),
    )
    if back_fits(grid, back_plan, rows, width, hidden_width, total):
        out_g, out_u, out_down, out_output, out_q, out_k, out_v, grad_tokens, gain_sums, _ = back(
            grid,
            back_plan,
            (grad_g, grad_u, grad_down, grad_woutput),
            grad_keys,
            grad_values,
            full_qkv,
            grad_query,
            raw,
            cosine.reshape(rows, HD),
            turned,
            gains,
            normed,
            tokens.reshape(rows, width),
            inverse_rows,
            grad_middle,
            grad_gain_two.reshape(lanes, 128),
        )
        out_g, out_u, out_down, out_output, out_q, out_k, out_v, grad_tokens = handed(
            out_g, out_u, out_down, out_output, out_q, out_k, out_v, grad_tokens
        )
        flat_sums = gain_sums.reshape(-1)

        def own_piece(at, x):
            return lax.dynamic_slice_in_dim(flat_sums, at + device * x.shape[0], x.shape[0], 0)

        return (
            output,
            grad_tokens.reshape(groups, rows, width),
            own_piece(0, attn_gain),
            out_q,
            out_k,
            out_v,
            own_piece(2 * width, query_gain),
            own_piece(2 * width + HD, key_gain),
            out_output,
            own_piece(width, mlp_gain),
            out_g,
            out_u,
            out_down,
        )
    f32 = jnp.float32
    own_keys, own_values, out_g, out_u, out_down, out_output = scatter(
        grid,
        [SLOT_AXES] * 2 + [CHIP_AXES] * 4,
        [
            (0, 0, KVH * HD, AB),
            (1, 0, KVH * HD, BA),
            (2, 0, hidden_width, BFA),
            (3, 0, hidden_width, AFB),
            (4, 0, width // 2, BFA),
            (4, width // 2, width, AFB),
            (5, 0, width // 2, BFA),
            (5, width // 2, width, AFB),
        ],
        "scatter_mlp",
        (f32, low, f32, f32, f32, f32),
        grad_keys,
        grad_values,
        grad_g,
        grad_u,
        grad_down,
        grad_woutput,
    )
    grad_qrot = grad_query.reshape(rows, H, HD)
    grad_qnormed = grad_qrot * cosine + unrotate(grad_qrot) * sine
    grad_qscale = jnp.sum(grad_qnormed * query_unit, axis=(0, 1))
    grad_qraw = norm_back(grad_qnormed, query_unit, query_inverse, query_scale)
    grad_krot = own_keys.reshape(rows, KVH, HD)
    grad_knormed = grad_krot * cosine + unrotate(grad_krot) * sine
    grad_kscale = jnp.sum(grad_knormed * key_unit, axis=(0, 1))
    grad_kraw = norm_back(grad_knormed, key_unit, key_inverse, key_scale)
    grad_raw = jnp.concatenate(
        [
            grad_qraw.reshape(rows, H * HD).astype(low),
            grad_kraw.reshape(rows, KVH * HD).astype(low),
            own_values,
        ],
        axis=1,
    )
    grad_wqkv = chip_sums(normed, swapped(normed), grad_raw, swapped(grad_raw))
    grad_normed = right_dot(grad_raw, full_qkv)
    grad_gain_one = jnp.sum(grad_normed * normal_one, axis=0)
    grad_inputs = grad_middle + norm_back(grad_normed, normal_one, inverse_one, gain_one)
    out_qkv, out_gains = scatter(
        grid,
        [CHIP_AXES, ALL_AXES],
        [
            (0, 0, half // 2, FAB),
            (0, half // 2, half, FBA),
            (0, half, 3 * half // 2, BFA),
            (0, 3 * half // 2, 2 * half, AFB),
            (1, 0, 128, FAB + CORE),
        ],
        "scatter_attention",
        (f32, f32),
        grad_wqkv,
        gain_rows(total, grad_gain_one, grad_qscale, grad_kscale, grad_gain_two),
    )
    return (
        output,
        grad_inputs.astype(low).reshape(groups, rows, width),
        out_gains[0, : attn_gain.shape[0]],
        out_qkv[:, : H * HD],
        out_qkv[:, H * HD : (H + KVH) * HD],
        out_qkv[:, (H + KVH) * HD :],
        out_gains[1, : query_gain.shape[0]],
        out_gains[2, : key_gain.shape[0]],
        out_output,
        out_gains[3, : mlp_gain.shape[0]],
        out_g,
        out_u,
        out_down,
    )


def solution(mesh):
    return jax.shard_map(
        on_device,
        mesh=mesh,
        in_specs=(
            P("fsdp", "ctx", None),
            P("fsdp", "ctx", None),
            P("fsdp", None),
            P(("ctx", "fsdp")),
            P(("ctx", "fsdp"), None),
            P(("ctx", "fsdp"), None),
            P(("ctx", "fsdp"), None),
            P(("ctx", "fsdp")),
            P(("ctx", "fsdp")),
            P(("ctx", "fsdp"), None),
            P(("ctx", "fsdp")),
            P(("ctx", "fsdp"), None),
            P(("ctx", "fsdp"), None),
            P(("ctx", "fsdp"), None),
        ),
        out_specs=(
            P("fsdp", "ctx", None),
            P("fsdp", "ctx", None),
            P(("ctx", "fsdp")),
            P(("ctx", "fsdp"), None),
            P(("ctx", "fsdp"), None),
            P(("ctx", "fsdp"), None),
            P(("ctx", "fsdp")),
            P(("ctx", "fsdp")),
            P(("ctx", "fsdp"), None),
            P(("ctx", "fsdp")),
            P(("ctx", "fsdp"), None),
            P(("ctx", "fsdp"), None),
            P(("ctx", "fsdp"), None),
        ),
        check_vma=False,
    )
```

```python
import functools
import itertools
import math

import jax
import jax.numpy as jnp
from jax import lax
from jax.experimental import pallas as pl
from jax.experimental.pallas import tpu as pltpu
from jax.sharding import PartitionSpec as P

MESH = pl.DeviceIdType.MESH
ANY = pl.BlockSpec(memory_space=pl.ANY)


H = 16
KVH = 8
HD = 128
BLK = 128


EPSILON = 1e-06
ROPE_BASE = 1000000.0


def rope_tables(positions):
    half = HD // 2
    freqs = jnp.exp(jnp.arange(half, dtype=jnp.float32) * (-2.0 * math.log(ROPE_BASE) / HD))
    angles = positions.astype(jnp.float32)[..., None] * freqs
    cosine = jnp.cos(angles)
    sine = jnp.sin(angles)
    return (jnp.concatenate([cosine, cosine], axis=-1), jnp.concatenate([sine, sine], axis=-1))


def rotate(value_vectors):
    half = value_vectors.shape[-1] // 2
    return jnp.concatenate([-value_vectors[..., half:], value_vectors[..., :half]], axis=-1)


def unrotate(value_vectors):
    half = value_vectors.shape[-1] // 2
    return jnp.concatenate([value_vectors[..., half:], -value_vectors[..., :half]], axis=-1)


def left_dot(left, right):
    return lax.dot_general(
        left, right, (((0,), (0,)), ((), ())), preferred_element_type=jnp.float32
    )


def right_dot(left, right):
    return lax.dot_general(
        left, right, (((1,), (1,)), ((), ())), preferred_element_type=jnp.float32
    )


def plain_dot(left, right):
    return jnp.dot(left, right, preferred_element_type=jnp.float32)


def norm_back(grad_normed, unit, inverse, gain):
    scaled = grad_normed * gain
    return inverse * (scaled - unit * jnp.mean(scaled * unit, axis=-1, keepdims=True))


class Grid:
    def __init__(self, ctx, fsdp):
        self.sizes = {"a": ctx // 4, "b": 2, "core": 2, "f": fsdp}
        self.stride = {"a": 4, "b": 2, "core": 1}

    def enter(self):
        self.c = lax.axis_index("ctx")
        self.at = {
            "a": self.c // 4,
            "b": (self.c // 2) % 2,
            "core": self.c % 2,
            "f": lax.axis_index("fsdp"),
        }

    def barrier(self):
        sem = pltpu.get_barrier_semaphore()
        count = 0
        for axis in ("core", "b", "a", "f"):
            n, p = self.sizes[axis], self.at[axis]
            for step in range(1, n):
                pl.semaphore_signal(
                    sem, inc=1, device_id=self.peer(axis, lax.rem(p + step, n)), device_id_type=MESH
                )
                count += 1
        pl.semaphore_wait(sem, count)

    def peer(self, axis, place):
        if axis == "f":
            return {"fsdp": place}
        return {"ctx": self.c + (place - self.at[axis]) * self.stride[axis]}

    def others(self, axis):
        n, p = self.sizes[axis], self.at[axis]
        return [1 - p] if n == 2 else [lax.rem(p + step, n) for step in range(1, n)]

    def nearest(self, axis):
        return [self.at[axis]] + self.others(axis)


class Pairs:
    def __init__(self, ctx, fsdp):
        self.bits = {"b": ("b",), "core": ("core",)}
        self.stride = {"b": ("ctx", 2), "core": ("ctx", 1)}
        for axis, name, count, unit in (("a", "ctx", ctx // 4, 4), ("f", "fsdp", fsdp, 1)):
            bits = []
            for k in reversed(range(count.bit_length() - 1)):
                bits.append(f"{axis}{k}")
                self.stride[bits[-1]] = (name, unit << k)
            self.bits[axis] = tuple(bits)
        self.sizes = dict.fromkeys(self.stride, 2)

    def axes(self, order):
        return tuple(bit for axis in order for bit in self.bits[axis])

    def shape(self, order):
        return (2,) * len(self.axes(order))

    def enter(self):
        self.index = {"ctx": lax.axis_index("ctx"), "fsdp": lax.axis_index("fsdp")}
        self.at = {}
        for bit, (name, unit) in self.stride.items():
            self.at[bit] = lax.rem(self.index[name] // unit, 2)

    def barrier(self):
        sem = pltpu.get_barrier_semaphore()
        for bit in self.stride:
            pl.semaphore_signal(
                sem, inc=1, device_id=self.peer(bit, 1 - self.at[bit]), device_id_type=MESH
            )
        pl.semaphore_wait(sem, len(self.stride))

    def peer(self, axis, place):
        name, unit = self.stride[axis]
        return {name: self.index[name] + (place - self.at[axis]) * unit}

    def others(self, axis):
        return [1 - self.at[axis]]

    def nearest(self, axis):
        return [self.at[axis], 1 - self.at[axis]]


class Pool:
    def __init__(self, ref):
        self.ref, self.used = ref, 0

    def take(self, count):
        first = self.used
        self.used += count
        return self.ref.at[pl.ds(first, count)]


class Gather:
    def __init__(self, grid, order, src, dst, columns, send_sem, recv_sem, layout_axes):
        self.grid, self.order, self.src, self.dst = grid, order, src, dst
        self.columns, self.send_sem, self.recv_sem = columns, send_sem, recv_sem
        self.layout_axes = layout_axes
        self.pending = []

    @staticmethod
    def semaphores(grid, order):
        near = {x: grid.sizes[x] - 1 for x in order}
        sends, inner = sum(near.values()), 1
        for level in range(1, len(order)):
            axis = order[level]
            sends += inner * near[axis] * sum(near[x] for x in order[level + 1 :])
            inner *= grid.sizes[axis]
        return sends, grid.sizes[order[0]] + inner

    def view(self, places):
        idx = tuple(places.get(x, slice(None)) for x in self.layout_axes)
        return self.dst.at[idx + (slice(None), self.columns)]

    def unit_number(self, places):
        number = 0
        for x in self.order[1:]:
            number = number * self.grid.sizes[x] + places[x]
        return number

    def start(self, source, view, axis, place, sem):
        copy = pltpu.make_async_remote_copy(
            src_ref=source,
            dst_ref=view,
            send_sem=self.send_sem.at[len(self.pending)],
            recv_sem=self.recv_sem.at[sem],
            device_id=self.grid.peer(axis, place),
            device_id_type=MESH,
        )
        copy.start()
        self.pending.append(copy)

    def wait_recv(self, view, sem):
        pltpu.make_async_remote_copy(
            src_ref=view,
            dst_ref=view,
            send_sem=self.send_sem.at[0],
            recv_sem=self.recv_sem.at[sem],
            device_id={},
            device_id_type=MESH,
        ).wait_recv()

    def own_places(self):
        return {x: self.grid.at[x] for x in self.order}

    def open(self):
        axis = self.order[0]
        for place in self.grid.others(axis):
            self.start(self.src, self.view(self.own_places()), axis, place, self.grid.at[axis])

    def first(self):
        axis = self.order[0]
        for origin in self.grid.others(axis):
            self.wait_recv(self.view({**self.own_places(), axis: origin}), origin)
        self.pass_on(1, {x: self.grid.at[x] for x in self.order[1:]})

    def pass_on(self, level, places):
        sem = self.grid.sizes[self.order[0]] + self.unit_number(places)
        view = self.view(places)
        for axis in self.order[level:]:
            for place in self.grid.others(axis):
                self.start(view, view, axis, place, sem)

    def arrivals(self, level):
        n1 = self.grid.sizes[self.order[0]]
        axis = self.order[level]
        inner = [{}]
        for x in self.order[1:level]:
            inner = [{**places, x: j} for places in inner for j in self.grid.nearest(x)]
        fixed = {x: self.grid.at[x] for x in self.order[level + 1 :]}
        for places in inner:
            for origin in self.grid.others(axis):
                unit = {**places, **fixed, axis: origin}
                self.wait_recv(self.view(unit), n1 + self.unit_number(unit))
                self.pass_on(level + 1, unit)

    def close(self):
        for copy in self.pending:
            copy.wait_send()


def add_into(total, terms, out=None):
    shape = total.shape
    rows = min(16, shape[-2])
    steps = shape[-2] // rows
    lead = math.prod(shape[:-2])

    def body(i, carry):
        index = ()
        rest = i // steps
        for n in reversed(shape[:-2]):
            index = (lax.rem(rest, n),) + index
            rest = rest // n
        at = index + (pl.ds(pl.multiple_of(lax.rem(i, steps) * rows, rows), rows), slice(None))
        value = total[at].astype(jnp.float32)
        for term in terms:
            value = value + term[at].astype(jnp.float32)
        if out is None:
            total[at] = value.astype(total.dtype)
        else:
            out[at] = value.astype(out.dtype)
        return carry

    lax.fori_loop(0, lead * steps, body, 0)


class Scatter:
    def __init__(self, grid, order, src, columns, own, recvs, load_sem, send_sem, recv_sem, out, layout_axes):
        self.grid, self.order, self.src, self.columns = grid, order, src, columns
        self.own, self.recvs, self.out = own, recvs, out
        self.load_sem, self.send_sem, self.recv_sem = load_sem, send_sem, recv_sem
        self.layout_axes = layout_axes
        self.pending = []
        self.base = {}
        self.top = len(order) - 1
        number = 0
        for level in range(self.top, -1, -1):
            self.base[level] = number
            number += self.slots(grid, order, level)

    @staticmethod
    def inner(grid, order, level):
        return [grid.sizes[x] for x in order[1:level]]

    @staticmethod
    def slots(grid, order, level):
        return (grid.sizes[order[level]] - 1) * math.prod(Scatter.inner(grid, order, level))

    @staticmethod
    def scratch(grid, order, rows, columns, dtype):
        n1 = grid.sizes[order[0]]
        shapes = [tuple(grid.sizes[x] for x in order[1:-1]) + (n1, rows, columns)]
        for level, axis in enumerate(order):
            block = (rows, columns) if level == 0 else (n1, rows, columns)
            shapes.append((grid.sizes[axis] - 1,) + tuple(Scatter.inner(grid, order, level)) + block)
        return [pltpu.VMEM(x, dtype) for x in shapes]

    @staticmethod
    def semaphores(grid, order):
        loads = math.prod(grid.sizes[x] for x in order[1:-1])
        slots = sum(Scatter.slots(grid, order, level) for level in range(len(order)))
        return loads, slots, slots

    def hbm(self, places):
        idx = tuple(places.get(x, slice(None)) for x in self.layout_axes)
        return self.src.at[idx + (slice(None), self.columns)]

    def units(self, level):
        found = [{}]
        for x in self.order[1:level]:
            found = [{**places, x: j} for places in found for j in reversed(self.grid.nearest(x))]
        return found

    def mine(self, places):
        return self.own.at[tuple(places.get(x, self.grid.at[x]) for x in self.order[1:-1])]

    def number(self, places, axes):
        value = 0
        for x in axes:
            value = value * self.grid.sizes[x] + places[x]
        return value

    def slot(self, level, places, line):
        axes = self.order[1:level]
        number = line * math.prod(self.grid.sizes[x] for x in axes) + self.number(places, axes)
        ref = self.recvs[level].at[(line,) + tuple(places[x] for x in axes)]
        return ref, self.recv_sem.at[self.base[level] + number]

    def send(self, level, places, step, place, view):
        axis = self.order[level]
        ref, sem = self.slot(level, places, self.grid.sizes[axis] - 1 - step)
        copy = pltpu.make_async_remote_copy(
            src_ref=view,
            dst_ref=ref,
            send_sem=self.send_sem.at[len(self.pending)],
            recv_sem=sem,
            device_id=self.grid.peer(axis, place),
            device_id_type=MESH,
        )
        copy.start()
        self.pending.append(copy)

    def take(self, level, places, total, out=None):
        lines = self.grid.sizes[self.order[level]] - 1
        terms = []
        for line in range(lines):
            ref, sem = self.slot(level, places, line)
            pltpu.make_async_remote_copy(
                src_ref=ref,
                dst_ref=ref,
                send_sem=self.send_sem.at[0],
                recv_sem=sem,
                device_id={},
                device_id_type=MESH,
            ).wait_recv()
            terms.append(ref)
        add_into(total, terms, out)

    def load(self, places):
        here = {**places, self.order[-1]: self.grid.at[self.order[-1]]}
        number = self.number(places, self.order[1:-1])
        return pltpu.make_async_copy(self.hbm(here), self.mine(places), self.load_sem.at[number])

    def open(self):
        axis = self.order[self.top]
        for places in self.units(self.top):
            for step, place in enumerate(self.grid.others(axis), 1):
                self.send(self.top, places, step, place, self.hbm({**places, axis: place}))
            self.load(places).start()

    def settle(self, level, places):
        if level + 1 == self.top:
            self.load(places).wait()
        self.take(level + 1, places, self.mine(places))

    def step(self, level):
        axis = self.order[level]
        if level == 0:
            self.settle(0, {})
            for step, place in enumerate(self.grid.others(axis), 1):
                self.send(0, {}, step, place, self.mine({}).at[place])
            return
        for places in self.units(level):
            for step, place in enumerate(self.grid.others(axis), 1):
                unit = {**places, axis: place}
                self.settle(level, unit)
                self.send(level, places, step, place, self.mine(unit))
            self.settle(level, {**places, axis: self.grid.at[axis]})

    def finish(self):
        self.take(0, {}, self.mine({}).at[self.grid.at[self.order[0]]], self.out)

    def close(self):
        for copy in self.pending:
            copy.wait_send()


def half_pairs(ref, s):
    rows = pl.ds(s * BLK, BLK)
    return jnp.concatenate([ref[rows, :HD], ref[rows, HD:]], axis=0)


def read_map(blocks, table, pairs):
    @pl.when(pl.program_id(0) == 0)
    def _():
        for t in range(2 * pairs):
            table[blocks[t]] = t
        place = lax.axis_index("ctx")
        first, second = blocks[2 * place], blocks[2 * place + 1]
        table[2 * pairs] = jnp.where(second > first, 1, 0)
        table[2 * pairs + 1] = jnp.maximum(first, second)


def items(table, pairs):
    high_slot, high = table[pairs * 2], table[pairs * 2 + 1]
    low_block = 2 * pairs - 1 - high
    split = high // 2
    found = []
    for w in range(pairs - 1):
        upper = w < split
        found.append((jnp.where(upper, high_slot, 1 - high_slot), jnp.where(upper, w, w - split), None))
    found.append((high_slot, split, high))
    found.append((1 - high_slot, low_block // 2, low_block))
    return found


def chunk_of(ref, table, c):
    return jnp.concatenate(
        [ref[pl.ds(pl.multiple_of(table[2 * c + i] * BLK, BLK), BLK), :] for i in range(2)], axis=0
    )


def row_contract(left, right):
    return lax.dot_general(left, right, (((1,), (1,)), ((), ())), preferred_element_type=jnp.float32)


def attention_kernel(pairs, blocks, q_ref, k_ref, v_ref, o_ref, low_ref, over_ref, table, qs, acc, tot):
    read_map(blocks, table, pairs)
    for s in range(2):
        qs[s] = half_pairs(q_ref, s)
    acc[...] = jnp.zeros_like(acc)
    tot[...] = jnp.zeros_like(tot)
    for s, c, block in items(table, pairs):
        keys = chunk_of(k_ref, table, c)
        vals = chunk_of(v_ref, table, c)
        scores = row_contract(qs[s], keys) * (HD ** (-0.5) * math.log2(math.e))
        weights = jnp.exp2(scores)
        if block is not None:
            rows = lax.broadcasted_iota(jnp.int32, (2 * BLK, 2 * BLK), 0)
            cols = lax.broadcasted_iota(jnp.int32, (2 * BLK, 2 * BLK), 1)
            allowed = cols <= lax.rem(rows, BLK) + (block - 2 * c) * BLK
            weights = jnp.where(allowed, weights, 0.0)
        tot[s] += weights[:, :HD] + weights[:, HD:]
        acc[s] += jnp.dot(weights.astype(jnp.bfloat16), vals, preferred_element_type=jnp.float32)
    for s in range(2):
        over = 1.0 / jnp.sum(tot[s], axis=1, keepdims=True)
        value = acc[s] * over
        over = jnp.broadcast_to(over, value.shape)
        rows = pl.ds(s * BLK, BLK)
        for i in range(2):
            part = value[i * BLK : (i + 1) * BLK]
            o_ref[rows, i * HD : (i + 1) * HD] = part
            low_ref[rows, i * HD : (i + 1) * HD] = part.astype(jnp.bfloat16)
            over_ref[rows, i * HD : (i + 1) * HD] = over[i * BLK : (i + 1) * BLK]


def attention(blocks, pairs, queries, keys, values):
    rows, length = queries.shape[0], keys.shape[0]
    head = pl.BlockSpec((rows, 2 * HD), lambda h, t: (0, h))
    side = pl.BlockSpec((length, HD), lambda h, t: (0, h))
    return pl.pallas_call(
        functools.partial(attention_kernel, pairs),
        grid_spec=pltpu.PrefetchScalarGridSpec(
            num_scalar_prefetch=1,
            grid=(KVH,),
            in_specs=[head, side, side],
            out_specs=[head, head, head],
            scratch_shapes=[
                pltpu.SMEM((2 * pairs + 2,), jnp.int32),
                pltpu.VMEM((2, 2 * BLK, HD), jnp.bfloat16),
                pltpu.VMEM((2, 2 * BLK, HD), jnp.float32),
                pltpu.VMEM((2, 2 * BLK, HD), jnp.float32),
            ],
        ),
        out_shape=[
            jax.ShapeDtypeStruct((rows, H * HD), jnp.float32),
            jax.ShapeDtypeStruct((rows, H * HD), jnp.bfloat16),
            jax.ShapeDtypeStruct((rows, H * HD), jnp.float32),
        ],
        name="attention",
    )(blocks, queries, keys, values)


def attention_back_kernel(
    pairs, blocks, q_ref, k_ref, v_ref, g_ref, o_ref, dq_ref, dk_ref, dv_ref, table, qs, gs, drift, dq, dk, dv
):
    read_map(blocks, table, pairs)
    scale = HD ** (-0.5)
    for s in range(2):
        qs[s] = half_pairs(q_ref, s)
        gs[s] = half_pairs(g_ref, s)
        products = gs[s].astype(jnp.float32) * half_pairs(o_ref, s)
        drift[s : s + 1, :] = jnp.sum(products.T, axis=0, keepdims=True)
    for total in (dq, dk, dv):
        total[...] = jnp.zeros_like(total)
    for s, c, block in items(table, pairs):
        keys = chunk_of(k_ref, table, c)
        vals = chunk_of(v_ref, table, c)
        queries, grads = qs[s], gs[s]
        weights = jnp.exp2(row_contract(keys, queries) * (scale * math.log2(math.e)))
        if block is not None:
            rows = lax.broadcasted_iota(jnp.int32, (2 * BLK, 2 * BLK), 0)
            cols = lax.broadcasted_iota(jnp.int32, (2 * BLK, 2 * BLK), 1)
            allowed = rows <= lax.rem(cols, BLK) + (block - 2 * c) * BLK
            weights = jnp.where(allowed, weights, 0.0)
        through = row_contract(vals, grads)
        scores = (weights * (through - drift[pl.ds(s, 1), :])).astype(jnp.bfloat16)
        to_values = jnp.dot(weights.astype(jnp.bfloat16), grads, preferred_element_type=jnp.float32)
        to_keys = jnp.dot(scores, queries, preferred_element_type=jnp.float32)
        for i in range(2):
            at = pl.ds(pl.multiple_of(table[2 * c + i] * BLK, BLK), BLK)
            dv[at, :] += to_values[i * BLK : (i + 1) * BLK]
            dk[at, :] += to_keys[i * BLK : (i + 1) * BLK]
        dq[s] += left_dot(scores, keys)
    dk_ref[...] = (dk[...] * scale).astype(jnp.bfloat16)
    dv_ref[...] = dv[...].astype(jnp.bfloat16)
    for s in range(2):
        for i in range(2):
            dq_ref[pl.ds(s * BLK, BLK), i * HD : (i + 1) * HD] = dq[s, i * BLK : (i + 1) * BLK] * scale


def attention_back(blocks, pairs, queries, keys, values, grads, attended):
    rows, length = queries.shape[0], keys.shape[0]
    head = pl.BlockSpec((rows, 2 * HD), lambda h, t: (0, h))
    side = pl.BlockSpec((length, HD), lambda h, t: (0, h))
    return pl.pallas_call(
        functools.partial(attention_back_kernel, pairs),
        grid_spec=pltpu.PrefetchScalarGridSpec(
            num_scalar_prefetch=1,
            grid=(KVH,),
            in_specs=[head, side, side, head, head],
            out_specs=[head, side, side],
            scratch_shapes=[
                pltpu.SMEM((2 * pairs + 2,), jnp.int32),
                pltpu.VMEM((2, 2 * BLK, HD), jnp.bfloat16),
                pltpu.VMEM((2, 2 * BLK, HD), jnp.bfloat16),
                pltpu.VMEM((2, 2 * BLK), jnp.float32),
                pltpu.VMEM((2, 2 * BLK, HD), jnp.float32),
                pltpu.VMEM((length, HD), jnp.float32),
                pltpu.VMEM((length, HD), jnp.float32),
            ],
        ),
        out_shape=[
            jax.ShapeDtypeStruct((rows, H * HD), jnp.float32),
            jax.ShapeDtypeStruct((length, KVH * HD), jnp.bfloat16),
            jax.ShapeDtypeStruct((length, KVH * HD), jnp.bfloat16),
        ],
        cost_estimate=pl.CostEstimate(
            flops=20 * (pairs + 1) * KVH * (2 * BLK) ** 2 * HD,
            bytes_accessed=14 * rows * H * HD + 8 * length * KVH * HD,
            transcendentals=(pairs + 1) * KVH * (2 * BLK) ** 2,
        ),
        name="attention_back",
    )(blocks, queries, keys, values, grads, attended)


ALL_AXES = ("a", "b", "core", "f")
SLOT_AXES = ("a", "b", "core")
CHIP_AXES = ("a", "b", "f")
BFA, AFB, FAB, FBA = ("b", "f", "a"), ("a", "f", "b"), ("f", "a", "b"), ("f", "b", "a")
ABF, BAF = ("a", "b", "f"), ("b", "a", "f")
AB, BA = ("a", "b", "core"), ("b", "a", "core")
CORE = ("core",)


PUMP = (6, 1, 2, 2)
FRONT_SRC = ("q", "k", "v", "o", "g", "u", "d", "gains")


def front_kernel(grid, plan, pieces, *refs):
    n = len(FRONT_SRC)
    src = dict(zip(FRONT_SRC, refs[:n]))
    tokens_ref, cosine_ref, sine_ref = refs[n : n + 3]
    rows_of = refs[n - 1]
    outs = refs[n + 3 : n + 15]
    wqkv_ref, wo_ref, wgu_ref, wd_ref, allgains_ref, k_out, v_out = outs[:7]
    normed_ref, gains_ref, raw_ref, qlow_ref, inv_ref = outs[7:]
    scratch = refs[n + 15 :]
    held = dict(zip(FRONT_SRC, scratch[:n]))
    weights, klow, vlow, gbuf, gmine = scratch[n : n + 5]
    send, recv, local, load = scratch[n + 5 :]
    grid.enter()
    grid.barrier()
    send, recv = Pool(send), Pool(recv)
    device = grid.index["ctx"] * 2 ** len(grid.bits["f"]) + grid.index["fsdp"]
    block_rows = lax.broadcasted_iota(jnp.int32, gmine.shape, 0)
    block = jnp.zeros(gmine.shape, jnp.float32)
    for i, (at, size) in enumerate(pieces):
        spot = at + device * size
        line = jnp.broadcast_to(rows_of[i : i + 1, :], (8, 128))
        line = pltpu.roll(line, lax.rem(spot, 128), 1)[:1]
        block = jnp.where(block_rows == spot // 128, line, block)
    gmine[...] = block.astype(gmine.dtype)
    copy = pltpu.make_async_copy(gmine, held["gains"], local.at[n - 1])
    copy.start()
    copy.wait()
    src["gains"] = held["gains"]
    width = tokens_ref.shape[1]
    rows = tokens_ref.shape[0]
    spans = {"q": (wqkv_ref, 0), "k": (wqkv_ref, H * HD), "v": (wqkv_ref, (H + KVH) * HD)}
    hidden = src["g"].shape[1]
    spans.update({"o": (wo_ref, 0), "g": (wgu_ref, 0), "u": (wgu_ref, hidden), "d": (wd_ref, 0)})
    spans["gains"] = (allgains_ref, 0)
    mine = tuple(grid.at[x] for x in grid.axes(ALL_AXES))

    def own_copy(i, name):
        dst, at = spans[name]
        return pltpu.make_async_copy(
            held[name], dst.at[mine + (slice(None), pl.ds(at, src[name].shape[1]))], local.at[i]
        )

    for i, name in enumerate(FRONT_SRC[:-1]):
        pltpu.make_async_copy(src[name], held[name], local.at[i]).start()

    def part(name, low, high, order):
        dst, at = spans[name]
        order = grid.axes(order)
        sends, takes = Gather.semaphores(grid, order)
        columns = pl.ds(at + low, high - low)
        return Gather(
            grid, order, src[name].at[:, low:high], dst, columns, send.take(sends), recv.take(takes),
            grid.axes(ALL_AXES),
        )

    early = [part(*p) for p in plan[0]]
    late = [part(*p) for p in plan[1]]
    for p in early:
        p.open()
    for p in late:
        p.open()
    for i, name in enumerate(FRONT_SRC):
        if name != "gains":
            pltpu.make_async_copy(src[name], held[name], local.at[i]).wait()
        own_copy(i, name).start()
    inputs = tokens_ref[...].astype(jnp.float32)
    inverse = lax.rsqrt(jnp.mean(inputs * inputs, axis=-1, keepdims=True) + EPSILON)
    inv_ref[...] = jnp.broadcast_to(inverse, (rows, 128))
    for i, name in enumerate(FRONT_SRC):
        own_copy(i, name).wait()

    for p in early:
        p.first()
    levels = len(early[0].order)
    for level in range(1, levels - 1):
        for p in early:
            p.arrivals(level)
    pump = []
    for p in late:
        pump.append(p.first)
    for level in range(1, levels):
        for p in late:
            pump.append(functools.partial(p.arrivals, level))

    def step(count):
        for _ in range(count):
            if pump:
                pump.pop(0)()

    step(PUMP[0])
    for p in early:
        p.arrivals(levels - 1)

    places = math.prod(grid.shape(ALL_AXES))
    copy = pltpu.make_async_copy(allgains_ref, gbuf, load.at[0])
    copy.start()
    big = pltpu.make_async_copy(wqkv_ref, weights, load.at[1])
    big.start()
    copy.wait()
    blocks = gbuf[...].reshape((places,) + gbuf.shape[-2:]).astype(jnp.float32)
    gains = jnp.sum(blocks, axis=0)
    gains_ref[...] = gains
    lanes = width // 128
    for j in range(lanes):
        cols = slice(j * 128, (j + 1) * 128)
        part_of = tokens_ref[:, cols].astype(jnp.float32) * inv_ref[...] * gains_ref[j : j + 1, :]
        normed_ref[:, cols] = part_of.astype(jnp.bfloat16)
    big.wait()
    step(PUMP[1])
    flat = weights.reshape(width, weights.shape[-1])
    normed = normed_ref[...]
    chunk = 2 * HD

    def heads(low_out, gain_row, out_at, raw_at, c):
        at = pl.ds(pl.multiple_of(raw_at + c * chunk, chunk), chunk)
        raw = jnp.dot(normed, flat[:, at], preferred_element_type=jnp.float32)
        raw_ref[:, at] = raw
        done = []
        for i in range(2):
            one = raw[:, i * HD : (i + 1) * HD]
            unit = one * lax.rsqrt(jnp.mean(one * one, axis=-1, keepdims=True) + EPSILON)
            unit = unit * gains_ref[gain_row : gain_row + 1, :]
            done.append(unit * cosine_ref[...] + pltpu.roll(unit, HD // 2, 1) * sine_ref[...])
        to = pl.ds(pl.multiple_of(out_at + c * chunk, chunk), chunk)
        low_out[:, to] = jnp.concatenate(done, axis=1).astype(jnp.bfloat16)

    def loop(count, body):
        def once(c, carry):
            body(c)
            return carry

        lax.fori_loop(0, count, once, 0)

    def to_values(c):
        at = pl.ds(pl.multiple_of((H + KVH) * HD + c * chunk, chunk), chunk)
        to = pl.ds(pl.multiple_of(c * chunk, chunk), chunk)
        raw = jnp.dot(normed, flat[:, at], preferred_element_type=jnp.float32)
        vlow[:, to] = raw.astype(jnp.bfloat16)

    loop(KVH // 2, functools.partial(heads, klow, 2 * lanes + 1, 0, H * HD))
    loop(KVH // 2, to_values)

    def pair(source, dst, order):
        order = grid.axes(order)
        sends, takes = Gather.semaphores(grid, order)
        return Gather(
            grid, order, source, dst, pl.ds(0, KVH * HD), send.take(sends), recv.take(takes),
            grid.axes(SLOT_AXES),
        )

    slot = tuple(grid.at[x] for x in grid.axes(SLOT_AXES))
    slabs = [pair(klow, k_out, AB), pair(vlow, v_out, BA)]
    saves = [
        pltpu.make_async_copy(klow, k_out.at[slot], load.at[0]),
        pltpu.make_async_copy(vlow, v_out.at[slot], load.at[1]),
    ]
    for p, save in zip(slabs, saves):
        p.open()
        save.start()
    step(PUMP[2])
    loop(KVH // 2, functools.partial(heads, qlow_ref, 2 * lanes, 0, 0))
    for p, save in zip(slabs, saves):
        save.wait()
        p.first()
    step(PUMP[3])
    loop(KVH // 2, functools.partial(heads, qlow_ref, 2 * lanes, H * HD // 2, H * HD // 2))
    depth = len(slabs[0].order)
    for level in range(1, depth - 1):
        for p in slabs:
            p.arrivals(level)
    step(len(pump))
    for p in slabs:
        p.arrivals(depth - 1)
    for p in early + late + slabs:
        p.close()


def front(grid, plan, pieces, blocks, gain_rows, tokens, cosine, sine):
    n = len(FRONT_SRC)
    rows, width = tokens.shape
    places = grid.shape(ALL_AXES)
    slots = grid.shape(SLOT_AXES)
    gains = jax.ShapeDtypeStruct((width // 128 * 2 + 16, 128), jnp.bfloat16)
    blocks = tuple(blocks) + (gains,)
    by = dict(zip(FRONT_SRC, blocks))
    low, f32 = jnp.bfloat16, jnp.float32
    full = (H + 2 * KVH) * HD
    counts = [Gather.semaphores(grid, grid.axes(p[3])) for p in plan[0] + plan[1]]
    counts += [Gather.semaphores(grid, grid.axes(x)) for x in (AB, BA)]
    sends, takes = [sum(x) for x in zip(*counts)]
    shape = jax.ShapeDtypeStruct
    vmem = pl.BlockSpec(memory_space=pltpu.VMEM)
    outs = pl.pallas_call(
        functools.partial(front_kernel, grid, plan, pieces),
        out_shape=[
            shape(places + (by["q"].shape[0], full), low),
            shape(places + by["o"].shape, low),
            shape(places + (by["g"].shape[0], 2 * by["g"].shape[1]), low),
            shape(places + by["d"].shape, low),
            shape(places + by["gains"].shape, low),
            shape(slots + (rows, KVH * HD), low),
            shape(slots + (rows, KVH * HD), low),
            shape((rows, width), low),
            shape(by["gains"].shape, f32),
            shape((rows, (H + KVH) * HD), f32),
            shape((rows, H * HD), low),
            shape((rows, 128), f32),
        ],
        in_specs=[ANY] * (n - 1) + [vmem] * 4,
        out_specs=[ANY] * 7 + [vmem] * 5,
        scratch_shapes=[pltpu.VMEM(x.shape, x.dtype) for x in blocks]
        + [
            pltpu.VMEM(places + (by["q"].shape[0], full), low),
            pltpu.VMEM((rows, KVH * HD), low),
            pltpu.VMEM((rows, KVH * HD), low),
            pltpu.VMEM(places + by["gains"].shape, low),
            pltpu.VMEM(by["gains"].shape, low),
            pltpu.SemaphoreType.DMA((sends,)),
            pltpu.SemaphoreType.DMA((takes,)),
            pltpu.SemaphoreType.DMA((n,)),
            pltpu.SemaphoreType.DMA((2,)),
        ],
        compiler_params=pltpu.CompilerParams(
            has_side_effects=True, vmem_limit_bytes=60 * 2**20, collective_id=0
        ),
        name="front",
    )(*blocks[:-1], gain_rows, tokens, cosine, sine)
    wqkv, wo, wgu, wd, _, keys, vals, normed, gains, raw, qlow, inverse = outs
    flat = [x.reshape(-1, x.shape[-1]) for x in (wqkv, wo, wgu, wd, keys, vals)]
    return flat + [normed, gains, raw, qlow, inverse]


def sums_kernel(count, core, left, left_other, right, right_other, out, turned):
    rows, width = left.shape
    block = width // count

    @pl.when(pl.program_id(0) == 0)
    def _():
        for j in range(count // 2):
            at = pl.ds(pl.multiple_of((2 * j + core[0]) * block, block), block)
            for k, ref in enumerate((left, left_other)):
                turned[j * block : (j + 1) * block, k * rows : (k + 1) * rows] = ref[:, at].T

    rhs = jnp.concatenate([right[...], right_other[...]], axis=0)
    out[...] = jnp.dot(turned[...], rhs, preferred_element_type=jnp.float32).astype(out.dtype)


def chip_sums(left, left_other, right, right_other):
    rows, width = left.shape
    count = lax.axis_size("ctx")
    block = width // count
    tile = 512
    if block % 128:
        place = lax.axis_index("ctx") % 2
        halves = [
            lax.dynamic_index_in_dim(x.reshape(rows, count // 2, 2, block), place, 2, False)
            for x in (left, left_other)
        ]
        lhs = jnp.concatenate(halves, axis=0).reshape(2 * rows, width // 2)
        return left_dot(lhs, jnp.concatenate([right, right_other], axis=0)).astype(jnp.bfloat16)
    core = (lax.axis_index("ctx") % 2).astype(jnp.int32)[None]
    lhs = pl.BlockSpec((rows, width), lambda n, c: (0, 0))
    rhs = pl.BlockSpec((rows, tile), lambda n, c: (0, n))
    return pl.pallas_call(
        functools.partial(sums_kernel, count),
        grid_spec=pltpu.PrefetchScalarGridSpec(
            num_scalar_prefetch=1,
            grid=(right.shape[1] // tile,),
            in_specs=[lhs, lhs, rhs, rhs],
            out_specs=pl.BlockSpec((width // 2, tile), lambda n, c: (0, n)),
            scratch_shapes=[pltpu.VMEM((width // 2, 2 * rows), jnp.bfloat16)],
        ),
        out_shape=jax.ShapeDtypeStruct((width // 2, right.shape[1]), jnp.bfloat16),
        name="chip_sums",
    )(core, left, left_other, right, right_other)


def handed_kernel(*refs):
    for source, out in zip(refs[: len(refs) // 2], refs[len(refs) // 2 :]):
        out[...] = source[...]


def handed(*results):
    vmem = pl.BlockSpec(memory_space=pltpu.VMEM)
    return pl.pallas_call(
        handed_kernel,
        out_shape=[jax.ShapeDtypeStruct(x.shape, x.dtype) for x in results],
        in_specs=[vmem] * len(results),
        out_specs=[vmem] * len(results),
        name="handed",
    )(*results)


BACK_SUMS = ("g", "u", "d", "o")


def back_kernel(grid, plan, *refs):
    refs = list(refs)

    def take(n):
        found = refs[:n]
        del refs[:n]
        return found

    src = dict(zip(BACK_SUMS, take(len(BACK_SUMS))))
    gk_ref, gv_ref, wqkv_ref = take(3)
    dq_ref, raw_ref, cos_ref, turn_ref, gains_ref, normed_ref, tokens_ref, inv_ref, mid_ref, gain2_ref = take(10)
    outs = dict(zip(BACK_SUMS + ("q", "k", "v"), take(len(BACK_SUMS) + 3)))
    din_ref, gsum_ref, sums_ref, gall_ref = take(4)
    weights, both_normed, both_raw, own_k, own_v, stage, acc, gbuf, gblock = take(9)
    load, send, recv, misc = [Pool(x) for x in refs[-4:]]
    del refs[-4:]
    scratch = refs
    grid.enter()
    grid.barrier()
    rows, width = tokens_ref.shape
    lanes = width // 128
    core = grid.at["core"]
    chunk = 2 * HD
    misc_sem = [misc.take(1).at[0] for _ in range(12)]

    def make(source, columns, order, out, layout):
        loads, sends, takes = Scatter.semaphores(grid, order)
        own, *recvs = scratch[: 1 + len(order)]
        del scratch[: 1 + len(order)]
        return Scatter(
            grid, order, source, columns, own, recvs,
            load.take(loads), send.take(sends), recv.take(takes), out, layout,
        )

    def portions(group):
        found = []
        for name, low, high, order in group:
            found.append(
                make(src[name], pl.ds(low, high - low), order, outs[name].at[:, low:high], CHIP_AXES)
            )
        return found

    slabs = [
        make(gk_ref, pl.ds(0, KVH * HD), AB, own_k, SLOT_AXES),
        make(gv_ref, pl.ds(0, KVH * HD), BA, own_v, SLOT_AXES),
    ]
    early, waves = portions(plan[0]), [portions(group) for group in plan[1]]
    late = [p for wave in waves for p in wave]
    last = []
    for name, at, low, high, order in plan[2]:
        last.append(
            make(sums_ref, pl.ds(at + low, high - low), order, outs[name].at[:, low:high], CHIP_AXES)
        )

    def sibling(source, dst, k):
        return pltpu.make_async_remote_copy(
            src_ref=source, dst_ref=dst, send_sem=misc_sem[2 * k], recv_sem=misc_sem[2 * k + 1],
            device_id=grid.peer("core", 1 - core), device_id_type=MESH,
        )

    for p in slabs + early:
        p.open()
    swap_normed = sibling(normed_ref, both_normed.at[1], 0)
    swap_normed.start()
    both_normed[0] = normed_ref[...]
    gblock[...] = jnp.zeros_like(gblock)
    gblock[lanes : 2 * lanes, :] = gain2_ref[...]

    def loop(count, body):
        def once(c, carry):
            body(c)
            return carry

        lax.fori_loop(0, count, once, 0)

    def heads(source, in_at, raw_at, gain_row, c):
        at = pl.ds(pl.multiple_of(raw_at + c * chunk, chunk), chunk)
        grads = source[:, pl.ds(pl.multiple_of(in_at + c * chunk, chunk), chunk)]
        raw = raw_ref[:, at]
        gain = gains_ref[gain_row : gain_row + 1, :]
        done = []
        for i in range(2):
            g = grads[:, i * HD : (i + 1) * HD]
            g = g * cos_ref[...] - pltpu.roll(g, HD // 2, 1) * turn_ref[...]
            one = raw[:, i * HD : (i + 1) * HD]
            inverse = lax.rsqrt(jnp.mean(one * one, axis=-1, keepdims=True) + EPSILON)
            unit = one * inverse
            gblock[gain_row : gain_row + 1, :] += jnp.sum(g * unit, axis=0, keepdims=True)
            done.append(norm_back(g, unit, inverse, gain))
        both_raw[0, :, at] = jnp.concatenate(done, axis=1).astype(jnp.bfloat16)

    half_q = H * HD // 2
    q_cols, kv_cols = pl.ds(0, H * HD), pl.ds(H * HD, 2 * KVH * HD)
    loop(H // 4, functools.partial(heads, dq_ref, 0, 0, 2 * lanes))
    for p in slabs:
        p.step(1)
    loop(H // 4, functools.partial(heads, dq_ref, half_q, half_q, 2 * lanes))
    swap_q = sibling(both_raw.at[0, :, q_cols], both_raw.at[1, :, q_cols], 1)
    swap_q.start()
    for p in slabs:
        p.step(0)
    def every(group, what, *args):
        for p in group:
            getattr(p, what)(*args)

    every(waves[0], "open")
    for p in slabs:
        p.finish()
    loop(KVH // 2, functools.partial(heads, own_k, 0, H * HD, 2 * lanes + 1))
    at = (H + KVH) * HD
    both_raw[0, :, at : at + KVH * HD] = own_v[...].astype(jnp.bfloat16)
    swap_kv = sibling(both_raw.at[0, :, kv_cols], both_raw.at[1, :, kv_cols], 2)
    swap_kv.start()
    every(waves[1], "open")
    swap_normed.wait()
    swap_q.wait()
    swap_kv.wait()
    flat_normed = both_normed.reshape(2 * rows, width)
    flat_raw = both_raw.reshape(2 * rows, both_raw.shape[-1])
    count = grid.sizes["a"] * grid.sizes["b"]
    block = width // (2 * count)
    piece = block // grid.sizes["f"]
    full = both_raw.shape[-1]
    tile = 512

    def stored(j):
        return pltpu.make_async_copy(stage.at[j % 2], sums_ref.at[j // 2, j % 2], misc_sem[9 + j % 2])

    for j in range(count):
        if j >= 2:
            stored(j - 2).wait()
        lhs = flat_normed[:, pl.ds(pl.multiple_of((2 * j + core) * block, block), block)]

        def sums(c):
            cols = pl.ds(pl.multiple_of(c * tile, tile), tile)
            value = left_dot(lhs, flat_raw[:, cols]).astype(jnp.bfloat16)
            stage[j % 2, :, :, cols] = value.reshape(grid.sizes["f"], piece, tile)

        loop(full // tile, sums)
        stored(j).start()
    for j in range(count - 2, count):
        stored(j).wait()
    every(waves[0], "step", 1)
    every(last, "open")
    every(waves[2], "open")
    every(early, "step", 1)
    every(waves[1], "step", 1)
    every(waves[0], "step", 0)
    tiles = [
        pltpu.make_async_copy(
            wqkv_ref.at[:, c * tile : (c + 1) * tile], weights.at[c % 2], misc_sem[6 + c % 2]
        )
        for c in range(full // tile)
    ]
    tiles[0].start()
    for c in range(full // tile):
        if c + 1 < full // tile:
            tiles[c + 1].start()
        tiles[c].wait()
        value = right_dot(both_raw[0, :, c * tile : (c + 1) * tile], weights[c % 2])
        acc[...] = value if c == 0 else acc[...] + value
    inverse = inv_ref[...]
    for j in range(lanes):
        cols = slice(j * 128, (j + 1) * 128)
        normal = tokens_ref[:, cols].astype(jnp.float32) * inverse
        gblock[j : j + 1, :] = jnp.sum(acc[:, cols] * normal, axis=0, keepdims=True)
    copy = pltpu.make_async_copy(gblock, gbuf, misc_sem[11])
    copy.start()
    copy.wait()
    order = FAB + CORE
    sends, takes = Gather.semaphores(grid, order)
    spread = Gather(
        grid, order, gbuf, gall_ref, slice(None), send.take(sends), recv.take(takes), ALL_AXES
    )
    spread.open()
    mine = tuple(grid.at[x] for x in ALL_AXES)
    gall_ref[mine] = gblock[...]
    every(early, "step", 0)
    every(last, "step", 1)
    every(waves[2], "step", 1)
    every(waves[1], "step", 0)
    spread.first()
    dots = jnp.zeros((rows, 1), jnp.float32)
    for j in range(lanes):
        cols = slice(j * 128, (j + 1) * 128)
        normal = tokens_ref[:, cols].astype(jnp.float32) * inverse
        dots += jnp.sum(acc[:, cols] * gains_ref[j : j + 1, :] * normal, axis=1, keepdims=True)
    dots = dots / width
    for j in range(lanes):
        cols = slice(j * 128, (j + 1) * 128)
        normal = tokens_ref[:, cols].astype(jnp.float32) * inverse
        grad = inverse * (acc[:, cols] * gains_ref[j : j + 1, :] - normal * dots)
        din_ref[:, cols] = (mid_ref[:, cols] + grad).astype(jnp.bfloat16)
    spread.arrivals(1)
    every(last, "step", 0)
    every(waves[2], "step", 0)
    spread.arrivals(2)
    every(waves[0] + early + waves[1], "finish")
    spread.arrivals(3)
    every(last + waves[2], "finish")
    places = math.prod(grid.sizes[x] for x in ALL_AXES)
    gsum_ref[...] = jnp.sum(gall_ref.reshape((places,) + gblock.shape)[...], axis=0)
    for p in slabs + early + late + last:
        p.close()
    spread.close()


def back_scratch(grid, plan, pieces, rows, width):
    low = jnp.bfloat16
    scratch, counts = [], []
    for order in (AB, BA):
        scratch += Scatter.scratch(grid, order, rows, KVH * HD, low)
        counts.append(Scatter.semaphores(grid, order))
    for name, begin, end, order in plan[0] + sum(plan[1], ()) + tuple((p[0],) + p[2:] for p in plan[2]):
        scratch += Scatter.scratch(grid, order, pieces[name], end - begin, low)
        counts.append(Scatter.semaphores(grid, order))
    return scratch, [sum(x) for x in zip(*counts)]


def back_fits(grid, plan, rows, width, hidden, total):
    pieces = {name: width // total for name in ("g", "u", "q", "k", "v")}
    pieces.update({"d": hidden // total, "o": H * HD // total})
    scratch = back_scratch(grid, plan, pieces, rows, width)[0]
    taken = sum(2 * math.prod(x.shape) for x in scratch)
    held = 2 * rows * (11 * width + 3 * (H + 2 * KVH) * HD + 4 * (H + KVH) * HD) + 6 * 2**20
    return taken + held < 62 * 2**20


def back(grid, plan, sums, gk, gv, wqkv, dq, raw, cosine, turned, gains, normed, tokens, inverse, middle, gain2):
    low, f32 = jnp.bfloat16, jnp.float32
    rows, width = tokens.shape
    chips = tuple(grid.sizes[x] for x in CHIP_AXES)
    places = tuple(grid.sizes[x] for x in ALL_AXES)
    slots = tuple(grid.sizes[x] for x in SLOT_AXES)
    blocks = [x.reshape(chips + (x.shape[0] // math.prod(chips), x.shape[1])) for x in sums]
    shape = jax.ShapeDtypeStruct
    vmem = pl.BlockSpec(memory_space=pltpu.VMEM)
    piece = width // math.prod(places)
    pieces = dict(zip(BACK_SUMS, [x.shape[-2] for x in blocks]))
    pieces.update({"q": piece, "k": piece, "v": piece})
    scratch, (loads, sends, takes) = back_scratch(grid, plan, pieces, rows, width)
    more = Gather.semaphores(grid, FAB + CORE)
    full = wqkv.shape[1]
    count = grid.sizes["a"] * grid.sizes["b"]
    outs = pl.pallas_call(
        functools.partial(back_kernel, grid, plan),
        out_shape=[shape(x.shape[-2:], f32) for x in blocks]
        + [shape((piece, n), f32) for n in (H * HD, KVH * HD, KVH * HD)]
        + [
            shape((rows, width), low),
            shape(gains.shape, f32),
            shape(chips + (piece, full), low),
        ],
        in_specs=[ANY] * (len(blocks) + 3) + [vmem] * 10,
        out_specs=[vmem] * (len(blocks) + 5) + [ANY],
        scratch_shapes=[
            pltpu.VMEM(places + gains.shape, f32),
            pltpu.VMEM((2, width, 512), low),
            pltpu.VMEM((2, rows, width), low),
            pltpu.VMEM((2, rows, full), low),
            pltpu.VMEM((rows, KVH * HD), f32),
            pltpu.VMEM((rows, KVH * HD), f32),
            pltpu.VMEM((2, grid.sizes["f"], piece, full), low),
            pltpu.VMEM((rows, width), f32),
            pltpu.VMEM(gains.shape, f32),
            pltpu.VMEM(gains.shape, f32),
        ]
        + scratch
        + [
            pltpu.SemaphoreType.DMA((loads,)),
            pltpu.SemaphoreType.DMA((sends + more[0],)),
            pltpu.SemaphoreType.DMA((takes + more[1],)),
            pltpu.SemaphoreType.DMA((12,)),
        ],
        compiler_params=pltpu.CompilerParams(
            has_side_effects=True, vmem_limit_bytes=63 * 2**20, collective_id=1
        ),
        name="back",
    )(
        *blocks,
        gk.reshape(slots + (rows, KVH * HD)),
        gv.reshape(slots + (rows, KVH * HD)),
        wqkv, dq, raw, cosine, turned, gains, normed, tokens, inverse, middle, gain2,
    )
    return outs


def middle_kernel(
    steps, alow_ref, over_ref, wo_ref, wg_ref, wu_ref, wd_ref, tokens_ref, cot_ref, gains_ref,
    out_ref, hidden_ref, gg_ref, gu_ref, normed_ref, mid_ref, branch_ref, gain_ref, gs_ref,
    middle, total, back, inv,
):
    c = pl.program_id(0)
    rows, width = tokens_ref.shape
    lanes = width // 128
    low = jnp.bfloat16

    @pl.when(c == 0)
    def _():
        value = tokens_ref[...].astype(jnp.float32) + plain_dot(alow_ref[...], wo_ref[...])
        inverse = lax.rsqrt(jnp.mean(value * value, axis=-1, keepdims=True) + EPSILON)
        inv[...] = jnp.broadcast_to(inverse, inv.shape)
        middle[...] = value
        total[...] = value
        for j in range(lanes):
            cols = slice(j * 128, (j + 1) * 128)
            gain = gains_ref[lanes + j : lanes + j + 1, :]
            normed_ref[:, cols] = (middle[:, cols] * inv[...] * gain).astype(low)
        back[...] = jnp.zeros_like(back)

    normed = normed_ref[...]
    gate = plain_dot(normed, wg_ref[...])
    upper = plain_dot(normed, wu_ref[...])
    grads = right_dot(cot_ref[...], wd_ref[...])
    sig = jax.nn.sigmoid(gate)
    activated = gate * sig
    hidden = (activated * upper).astype(low)
    grad_gate = (grads * upper * sig * (1.0 + gate * (1.0 - sig))).astype(low)
    grad_upper = (grads * activated).astype(low)
    hidden_ref[...] = hidden
    gg_ref[...] = grad_gate
    gu_ref[...] = grad_upper
    total[...] += plain_dot(hidden, wd_ref[...])
    back[...] += right_dot(grad_gate, wg_ref[...]) + right_dot(grad_upper, wu_ref[...])

    @pl.when(c == steps - 1)
    def _():
        out_ref[...] = total[...].astype(low)
        inverse = inv[...]
        dots = jnp.zeros((rows, 1), jnp.float32)
        for j in range(lanes):
            cols = slice(j * 128, (j + 1) * 128)
            normal = middle[:, cols] * inverse
            gain_ref[j : j + 1, :] = jnp.sum(back[:, cols] * normal, axis=0, keepdims=True)
            gain = gains_ref[lanes + j : lanes + j + 1, :]
            dots += jnp.sum(back[:, cols] * gain * normal, axis=1, keepdims=True)
        dots = dots / width
        for j in range(lanes):
            cols = slice(j * 128, (j + 1) * 128)
            gain = gains_ref[lanes + j : lanes + j + 1, :]
            normal = middle[:, cols] * inverse
            grad = cot_ref[:, cols].astype(jnp.float32) + inverse * (back[:, cols] * gain - normal * dots)
            mid_ref[:, cols] = grad
            branch_ref[:, cols] = grad.astype(low)
        tile = 512
        for j in range(gs_ref.shape[1] // tile):
            cols = slice(j * tile, (j + 1) * tile)
            attended = right_dot(branch_ref[...], wo_ref[cols, :])
            gs_ref[:, cols] = (attended * over_ref[:, cols]).astype(low)


def middle_part(alow, over, wo, wgu, wd, tokens, cotangent, gains):
    low, f32 = jnp.bfloat16, jnp.float32
    rows, width = tokens.shape
    hidden = wd.shape[0]
    tile = 512
    steps = hidden // tile
    shape = jax.ShapeDtypeStruct

    def whole(x):
        return pl.BlockSpec(x.shape, lambda c: (0,) * len(x.shape))

    def columns(at):
        return pl.BlockSpec((width, tile), lambda c: (0, at + c))

    chunk = pl.BlockSpec((rows, tile), lambda c: (0, c))
    outs = [
        shape((rows, width), low),
        shape((rows, hidden), low),
        shape((rows, hidden), low),
        shape((rows, hidden), low),
        shape((rows, width), low),
        shape((rows, width), f32),
        shape((rows, width), low),
        shape((width // 128, 128), f32),
        shape(alow.shape, low),
    ]
    return pl.pallas_call(
        functools.partial(middle_kernel, steps),
        grid=(steps,),
        in_specs=[
            whole(alow),
            whole(over),
            whole(wo),
            columns(0),
            columns(steps),
            pl.BlockSpec((tile, width), lambda c: (c, 0)),
            whole(tokens),
            whole(cotangent),
            whole(gains),
        ],
        out_specs=[whole(outs[0])] + [chunk] * 3 + [whole(x) for x in outs[4:]],
        out_shape=outs,
        scratch_shapes=[pltpu.VMEM((rows, width), f32)] * 3 + [pltpu.VMEM((rows, 128), f32)],
        compiler_params=pltpu.CompilerParams(vmem_limit_bytes=60 * 2**20),
        name="middle",
    )(alow, over, wo, wgu, wgu, wd, tokens, cotangent, gains)


def scatter_kernel(grid, portions, layouts, n, *refs):
    srcs, outs, scratch = refs[:n], refs[n : 2 * n], list(refs[2 * n : -3])
    load, send, recv = [Pool(x) for x in refs[-3:]]
    grid.enter()
    parts = []
    for i, low, high, order in portions:
        loads, sends, takes = Scatter.semaphores(grid, order)
        own, *recvs = scratch[: 1 + len(order)]
        del scratch[: 1 + len(order)]
        parts.append(
            Scatter(
                grid,
                order,
                srcs[i],
                pl.ds(low, high - low),
                own,
                recvs,
                load.take(loads),
                send.take(sends),
                recv.take(takes),
                outs[i].at[:, low:high],
                layouts[i],
            )
        )
        parts[-1].open()
    for level in (2, 1, 0):
        for part in parts:
            if level < part.top:
                part.step(level)
    for part in parts:
        part.finish()
    for part in parts:
        part.close()


def scatter(grid, layouts, portions, name, dtypes, *sums):
    n = len(sums)
    blocks = []
    for layout, x in zip(layouts, sums):
        places = tuple(grid.sizes[axis] for axis in layout)
        blocks.append(x.reshape(places + (x.shape[0] // math.prod(places), x.shape[1])))
    loads, sends, takes = [sum(x) for x in zip(*[Scatter.semaphores(grid, p[3]) for p in portions])]
    scratch = []
    for i, low, high, order in portions:
        scratch += Scatter.scratch(grid, order, blocks[i].shape[-2], high - low, blocks[i].dtype)
    return pl.pallas_call(
        functools.partial(scatter_kernel, grid, portions, layouts, n),
        out_shape=[jax.ShapeDtypeStruct(x.shape[-2:], t) for x, t in zip(blocks, dtypes)],
        in_specs=[ANY] * n,
        out_specs=[pl.BlockSpec(memory_space=pltpu.VMEM)] * n,
        scratch_shapes=scratch
        + [
            pltpu.SemaphoreType.DMA((loads,)),
            pltpu.SemaphoreType.DMA((sends,)),
            pltpu.SemaphoreType.DMA((takes,)),
        ],
        compiler_params=pltpu.CompilerParams(has_side_effects=True, vmem_limit_bytes=60 * 2**20),
        name=name,
    )(*blocks)


def gain_rows(total, *gains):
    pieces = [x.reshape(total, 1, -1) for x in gains]
    pieces = [jnp.pad(x, ((0, 0), (0, 0), (0, 128 - x.shape[2]))) for x in pieces]
    block = jnp.concatenate(pieces, axis=1)
    return jnp.pad(block, ((0, 0), (0, 8 - len(gains)), (0, 0))).reshape(total * 8, 128)


def swapped(x):
    count = lax.axis_size("ctx")
    return lax.ppermute(x, "ctx", [(i, i ^ 1) for i in range(count)])


def on_device(
    tokens,
    cotangent,
    block_map,
    attn_gain,
    query_weight,
    key_weight,
    value_weight,
    query_gain,
    key_gain,
    output_weight,
    mlp_gain,
    gate_weight,
    up_weight,
    down_weight,
):
    grid = Grid(lax.axis_size("ctx"), lax.axis_size("fsdp"))
    total = lax.axis_size("ctx") * lax.axis_size("fsdp")
    groups, rows, width = tokens.shape
    pairs = block_map.shape[1] // 2
    ratio = H // KVH
    low = jnp.bfloat16

    device = lax.axis_index("ctx") * lax.axis_size("fsdp") + lax.axis_index("fsdp")
    gain_pieces = [
        (at, x.shape[0])
        for at, x in ((0, attn_gain), (width, mlp_gain), (2 * width, query_gain), (2 * width + HD, key_gain))
    ]
    gain_lines = jnp.concatenate(
        [
            jnp.pad(x.astype(jnp.float32).reshape(1, -1), ((0, 0), (0, 128 - x.shape[0])))
            for x in (attn_gain, mlp_gain, query_gain, key_gain)
        ]
    )
    hidden_width = gate_weight.shape[1]

    place = lax.axis_index("ctx")
    blocks = block_map.reshape(-1)
    own_blocks = lax.dynamic_slice_in_dim(blocks, 2 * place, 2, 0)
    spots = (own_blocks[:, None] * BLK + jnp.arange(BLK, dtype=jnp.int32)).reshape(rows)
    cosine, sine = rope_tables(spots)
    turned = jnp.concatenate([-sine[:, : HD // 2], sine[:, HD // 2 :]], axis=1)
    half_q, half_k = H * HD // 2, KVH * HD // 2
    half = half_q + 2 * half_k
    plan = (
        (
            ("gains", 0, 128, FAB + CORE),
            ("q", 0, half_q, FAB + CORE),
            ("q", half_q, 2 * half_q, FBA + CORE),
            ("k", 0, 2 * half_k, BFA + CORE),
            ("v", 0, 2 * half_k, AFB + CORE),
        ),
        (
            ("o", 0, width // 2, FAB + CORE),
            ("o", width // 2, width, FBA + CORE),
            ("g", 0, hidden_width, BFA + CORE),
            ("u", 0, hidden_width, AFB + CORE),
            ("d", 0, width // 2, BFA + CORE),
            ("d", width // 2, width, AFB + CORE),
        ),
    )
    (
        full_qkv,
        full_output,
        full_gu,
        full_down,
        key_all,
        value_all,
        normed,
        gains,
        raw,
        query_low,
        inverse_one,
    ) = front(
        Pairs(lax.axis_size("ctx"), lax.axis_size("fsdp")),
        plan,
        gain_pieces,
        (query_weight, key_weight, value_weight, output_weight, gate_weight, up_weight, down_weight),
        gain_lines,
        tokens.reshape(rows, width),
        cosine,
        turned,
    )
    attended, attended_low, over_totals = attention(blocks, pairs, query_low, key_all, value_all)
    lanes = width // 128
    gain_one = gains[:lanes].reshape(-1)
    query_scale, key_scale = gains[2 * lanes], gains[2 * lanes + 1]
    inverse_rows = inverse_one
    inverse_one = inverse_one[:, :1]
    inputs = tokens.reshape(rows, width).astype(jnp.float32)
    normal_one = inputs * inverse_one
    cosine = cosine.reshape(rows, 1, HD)
    sine = sine.reshape(rows, 1, HD)
    query_raw = raw[:, : H * HD].reshape(rows, H, HD)
    key_raw = raw[:, H * HD :].reshape(rows, KVH, HD)
    query_inverse = lax.rsqrt(jnp.mean(query_raw * query_raw, axis=-1, keepdims=True) + EPSILON)
    query_unit = query_raw * query_inverse
    key_inverse = lax.rsqrt(jnp.mean(key_raw * key_raw, axis=-1, keepdims=True) + EPSILON)
    key_unit = key_raw * key_inverse
    upstream = cotangent.reshape(rows, width)
    (
        output,
        hidden,
        grad_gate,
        grad_upper,
        normed_two,
        grad_middle,
        branch_grad,
        grad_gain_two,
        grad_summed,
    ) = middle_part(
        attended_low, over_totals, full_output, full_gu, full_down, tokens.reshape(rows, width), upstream, gains
    )
    output = output.reshape(groups, rows, width)
    grad_gain_two = grad_gain_two.reshape(width)
    normed_other, upstream_other = swapped(normed_two), swapped(upstream)
    grad_down = chip_sums(hidden, swapped(hidden), upstream, upstream_other)
    grad_g = chip_sums(normed_two, normed_other, grad_gate, swapped(grad_gate))
    grad_u = chip_sums(normed_two, normed_other, grad_upper, swapped(grad_upper))
    grad_woutput = chip_sums(attended_low, swapped(attended_low), branch_grad, swapped(branch_grad))
    grad_query, grad_keys, grad_values = attention_back(
        blocks, pairs, query_low, key_all, value_all, grad_summed, attended
    )
    back_plan = (
        (("d", 0, width // 2, ABF), ("d", width // 2, width, BAF)),
        (
            (("g", 0, hidden_width // 2, FAB), ("g", hidden_width // 2, hidden_width, FBA)),
            (("u", 0, hidden_width // 2, FAB), ("u", hidden_width // 2, hidden_width, FBA)),
            (("o", 0, width // 2, FAB), ("o", width // 2, width, FBA)),
        ),
        (
            ("q", 0, 0, half_q, ABF),
            ("q", 0, half_q, 2 * half_q, BAF),
            ("k", H * HD, 0, 2 * half_k, FAB),
            ("v", (H + KVH) * HD, 0, 2 * half_k, FBA),
        ),
    )
    if back_fits(grid, back_plan, rows, width, hidden_width, total):
        out_g, out_u, out_down, out_output, out_q, out_k, out_v, grad_tokens, gain_sums, _ = back(
            grid,
            back_plan,
            (grad_g, grad_u, grad_down, grad_woutput),
            grad_keys,
            grad_values,
            full_qkv,
            grad_query,
            raw,
            cosine.reshape(rows, HD),
            turned,
            gains,
            normed,
            tokens.reshape(rows, width),
            inverse_rows,
            grad_middle,
            grad_gain_two.reshape(lanes, 128),
        )
        out_g, out_u, out_down, out_output, out_q, out_k, out_v, grad_tokens = handed(
            out_g, out_u, out_down, out_output, out_q, out_k, out_v, grad_tokens
        )
        flat_sums = gain_sums.reshape(-1)

        def own_piece(at, x):
            return lax.dynamic_slice_in_dim(flat_sums, at + device * x.shape[0], x.shape[0], 0)

        return (
            output,
            grad_tokens.reshape(groups, rows, width),
            own_piece(0, attn_gain),
            out_q,
            out_k,
            out_v,
            own_piece(2 * width, query_gain),
            own_piece(2 * width + HD, key_gain),
            out_output,
            own_piece(width, mlp_gain),
            out_g,
            out_u,
            out_down,
        )
    f32 = jnp.float32
    own_keys, own_values, out_g, out_u, out_down, out_output = scatter(
        grid,
        [SLOT_AXES] * 2 + [CHIP_AXES] * 4,
        [
            (0, 0, KVH * HD, AB),
            (1, 0, KVH * HD, BA),
            (2, 0, hidden_width, BFA),
            (3, 0, hidden_width, AFB),
            (4, 0, width // 2, BFA),
            (4, width // 2, width, AFB),
            (5, 0, width // 2, BFA),
            (5, width // 2, width, AFB),
        ],
        "scatter_mlp",
        (f32, low, f32, f32, f32, f32),
        grad_keys,
        grad_values,
        grad_g,
        grad_u,
        grad_down,
        grad_woutput,
    )
    grad_qrot = grad_query.reshape(rows, H, HD)
    grad_qnormed = grad_qrot * cosine + unrotate(grad_qrot) * sine
    grad_qscale = jnp.sum(grad_qnormed * query_unit, axis=(0, 1))
    grad_qraw = norm_back(grad_qnormed, query_unit, query_inverse, query_scale)
    grad_krot = own_keys.reshape(rows, KVH, HD)
    grad_knormed = grad_krot * cosine + unrotate(grad_krot) * sine
    grad_kscale = jnp.sum(grad_knormed * key_unit, axis=(0, 1))
    grad_kraw = norm_back(grad_knormed, key_unit, key_inverse, key_scale)
    grad_raw = jnp.concatenate(
        [
            grad_qraw.reshape(rows, H * HD).astype(low),
            grad_kraw.reshape(rows, KVH * HD).astype(low),
            own_values,
        ],
        axis=1,
    )
    grad_wqkv = chip_sums(normed, swapped(normed), grad_raw, swapped(grad_raw))
    grad_normed = right_dot(grad_raw, full_qkv)
    grad_gain_one = jnp.sum(grad_normed * normal_one, axis=0)
    grad_inputs = grad_middle + norm_back(grad_normed, normal_one, inverse_one, gain_one)
    out_qkv, out_gains = scatter(
        grid,
        [CHIP_AXES, ALL_AXES],
        [
            (0, 0, half // 2, FAB),
            (0, half // 2, half, FBA),
            (0, half, 3 * half // 2, BFA),
            (0, 3 * half // 2, 2 * half, AFB),
            (1, 0, 128, FAB + CORE),
        ],
        "scatter_attention",
        (f32, f32),
        grad_wqkv,
        gain_rows(total, grad_gain_one, grad_qscale, grad_kscale, grad_gain_two),
    )
    return (
        output,
        grad_inputs.astype(low).reshape(groups, rows, width),
        out_gains[0, : attn_gain.shape[0]],
        out_qkv[:, : H * HD],
        out_qkv[:, H * HD : (H + KVH) * HD],
        out_qkv[:, (H + KVH) * HD :],
        out_gains[1, : query_gain.shape[0]],
        out_gains[2, : key_gain.shape[0]],
        out_output,
        out_gains[3, : mlp_gain.shape[0]],
        out_g,
        out_u,
        out_down,
    )


def solution(mesh):
    return jax.shard_map(
        on_device,
        mesh=mesh,
        in_specs=(
            P("fsdp", "ctx", None),
            P("fsdp", "ctx", None),
            P("fsdp", None),
            P(("ctx", "fsdp")),
            P(("ctx", "fsdp"), None),
            P(("ctx", "fsdp"), None),
            P(("ctx", "fsdp"), None),
            P(("ctx", "fsdp")),
            P(("ctx", "fsdp")),
            P(("ctx", "fsdp"), None),
            P(("ctx", "fsdp")),
            P(("ctx", "fsdp"), None),
            P(("ctx", "fsdp"), None),
            P(("ctx", "fsdp"), None),
        ),
        out_specs=(
            P("fsdp", "ctx", None),
            P("fsdp", "ctx", None),
            P(("ctx", "fsdp")),
            P(("ctx", "fsdp"), None),
            P(("ctx", "fsdp"), None),
            P(("ctx", "fsdp"), None),
            P(("ctx", "fsdp")),
            P(("ctx", "fsdp")),
            P(("ctx", "fsdp"), None),
            P(("ctx", "fsdp")),
            P(("ctx", "fsdp"), None),
            P(("ctx", "fsdp"), None),
            P(("ctx", "fsdp"), None),
        ),
        check_vma=False,
    )
```

```python
import functools
import itertools
import math

import jax
import jax.numpy as jnp
from jax import lax
from jax.experimental import pallas as pl
from jax.experimental.pallas import tpu as pltpu
from jax.sharding import PartitionSpec as P

MESH = pl.DeviceIdType.MESH
ANY = pl.BlockSpec(memory_space=pl.ANY)


H = 16
KVH = 8
HD = 128
BLK = 128


EPSILON = 1e-06
ROPE_BASE = 1000000.0


def rope_tables(positions):
    half = HD // 2
    freqs = jnp.exp(jnp.arange(half, dtype=jnp.float32) * (-2.0 * math.log(ROPE_BASE) / HD))
    angles = positions.astype(jnp.float32)[..., None] * freqs
    cosine = jnp.cos(angles)
    sine = jnp.sin(angles)
    return (jnp.concatenate([cosine, cosine], axis=-1), jnp.concatenate([sine, sine], axis=-1))


def rotate(value_vectors):
    half = value_vectors.shape[-1] // 2
    return jnp.concatenate([-value_vectors[..., half:], value_vectors[..., :half]], axis=-1)


def unrotate(value_vectors):
    half = value_vectors.shape[-1] // 2
    return jnp.concatenate([value_vectors[..., half:], -value_vectors[..., :half]], axis=-1)


def left_dot(left, right):
    return lax.dot_general(
        left, right, (((0,), (0,)), ((), ())), preferred_element_type=jnp.float32
    )


def right_dot(left, right):
    return lax.dot_general(
        left, right, (((1,), (1,)), ((), ())), preferred_element_type=jnp.float32
    )


def plain_dot(left, right):
    return jnp.dot(left, right, preferred_element_type=jnp.float32)


def norm_back(grad_normed, unit, inverse, gain):
    scaled = grad_normed * gain
    return inverse * (scaled - unit * jnp.mean(scaled * unit, axis=-1, keepdims=True))


class Grid:
    def __init__(self, ctx, fsdp):
        self.sizes = {"a": ctx // 4, "b": 2, "core": 2, "f": fsdp}
        self.stride = {"a": 4, "b": 2, "core": 1}

    def enter(self):
        self.c = lax.axis_index("ctx")
        self.at = {
            "a": self.c // 4,
            "b": (self.c // 2) % 2,
            "core": self.c % 2,
            "f": lax.axis_index("fsdp"),
        }

    def barrier(self):
        sem = pltpu.get_barrier_semaphore()
        count = 0
        for axis in ("core", "b", "a", "f"):
            n, p = self.sizes[axis], self.at[axis]
            for step in range(1, n):
                pl.semaphore_signal(
                    sem, inc=1, device_id=self.peer(axis, lax.rem(p + step, n)), device_id_type=MESH
                )
                count += 1
        pl.semaphore_wait(sem, count)

    def peer(self, axis, place):
        if axis == "f":
            return {"fsdp": place}
        return {"ctx": self.c + (place - self.at[axis]) * self.stride[axis]}

    def others(self, axis):
        n, p = self.sizes[axis], self.at[axis]
        return [1 - p] if n == 2 else [lax.rem(p + step, n) for step in range(1, n)]

    def nearest(self, axis):
        return [self.at[axis]] + self.others(axis)


class Pairs:
    def __init__(self, ctx, fsdp):
        self.bits = {"b": ("b",), "core": ("core",)}
        self.stride = {"b": ("ctx", 2), "core": ("ctx", 1)}
        for axis, name, count, unit in (("a", "ctx", ctx // 4, 4), ("f", "fsdp", fsdp, 1)):
            bits = []
            for k in reversed(range(count.bit_length() - 1)):
                bits.append(f"{axis}{k}")
                self.stride[bits[-1]] = (name, unit << k)
            self.bits[axis] = tuple(bits)
        self.sizes = dict.fromkeys(self.stride, 2)

    def axes(self, order):
        return tuple(bit for axis in order for bit in self.bits[axis])

    def shape(self, order):
        return (2,) * len(self.axes(order))

    def enter(self):
        self.index = {"ctx": lax.axis_index("ctx"), "fsdp": lax.axis_index("fsdp")}
        self.at = {}
        for bit, (name, unit) in self.stride.items():
            self.at[bit] = lax.rem(self.index[name] // unit, 2)

    def barrier(self):
        sem = pltpu.get_barrier_semaphore()
        for bit in self.stride:
            pl.semaphore_signal(
                sem, inc=1, device_id=self.peer(bit, 1 - self.at[bit]), device_id_type=MESH
            )
        pl.semaphore_wait(sem, len(self.stride))

    def peer(self, axis, place):
        name, unit = self.stride[axis]
        return {name: self.index[name] + (place - self.at[axis]) * unit}

    def others(self, axis):
        return [1 - self.at[axis]]

    def nearest(self, axis):
        return [self.at[axis], 1 - self.at[axis]]


class Pool:
    def __init__(self, ref):
        self.ref, self.used = ref, 0

    def take(self, count):
        first = self.used
        self.used += count
        return self.ref.at[pl.ds(first, count)]


class Gather:
    def __init__(self, grid, order, src, dst, columns, send_sem, recv_sem, layout_axes):
        self.grid, self.order, self.src, self.dst = grid, order, src, dst
        self.columns, self.send_sem, self.recv_sem = columns, send_sem, recv_sem
        self.layout_axes = layout_axes
        self.pending = []

    @staticmethod
    def semaphores(grid, order):
        near = {x: grid.sizes[x] - 1 for x in order}
        sends, inner = sum(near.values()), 1
        for level in range(1, len(order)):
            axis = order[level]
            sends += inner * near[axis] * sum(near[x] for x in order[level + 1 :])
            inner *= grid.sizes[axis]
        return sends, grid.sizes[order[0]] + inner

    def view(self, places):
        idx = tuple(places.get(x, slice(None)) for x in self.layout_axes)
        return self.dst.at[idx + (slice(None), self.columns)]

    def unit_number(self, places):
        number = 0
        for x in self.order[1:]:
            number = number * self.grid.sizes[x] + places[x]
        return number

    def start(self, source, view, axis, place, sem):
        copy = pltpu.make_async_remote_copy(
            src_ref=source,
            dst_ref=view,
            send_sem=self.send_sem.at[len(self.pending)],
            recv_sem=self.recv_sem.at[sem],
            device_id=self.grid.peer(axis, place),
            device_id_type=MESH,
        )
        copy.start()
        self.pending.append(copy)

    def wait_recv(self, view, sem):
        pltpu.make_async_remote_copy(
            src_ref=view,
            dst_ref=view,
            send_sem=self.send_sem.at[0],
            recv_sem=self.recv_sem.at[sem],
            device_id={},
            device_id_type=MESH,
        ).wait_recv()

    def own_places(self):
        return {x: self.grid.at[x] for x in self.order}

    def open(self):
        axis = self.order[0]
        for place in self.grid.others(axis):
            self.start(self.src, self.view(self.own_places()), axis, place, self.grid.at[axis])

    def first(self):
        axis = self.order[0]
        for origin in self.grid.others(axis):
            self.wait_recv(self.view({**self.own_places(), axis: origin}), origin)
        self.pass_on(1, {x: self.grid.at[x] for x in self.order[1:]})

    def pass_on(self, level, places):
        sem = self.grid.sizes[self.order[0]] + self.unit_number(places)
        view = self.view(places)
        for axis in self.order[level:]:
            for place in self.grid.others(axis):
                self.start(view, view, axis, place, sem)

    def arrivals(self, level):
        n1 = self.grid.sizes[self.order[0]]
        axis = self.order[level]
        inner = [{}]
        for x in self.order[1:level]:
            inner = [{**places, x: j} for places in inner for j in self.grid.nearest(x)]
        fixed = {x: self.grid.at[x] for x in self.order[level + 1 :]}
        for places in inner:
            for origin in self.grid.others(axis):
                unit = {**places, **fixed, axis: origin}
                self.wait_recv(self.view(unit), n1 + self.unit_number(unit))
                self.pass_on(level + 1, unit)

    def close(self):
        for copy in self.pending:
            copy.wait_send()


def add_into(total, terms, out=None):
    shape = total.shape
    rows = min(16, shape[-2])
    steps = shape[-2] // rows
    lead = math.prod(shape[:-2])

    def body(i, carry):
        index = ()
        rest = i // steps
        for n in reversed(shape[:-2]):
            index = (lax.rem(rest, n),) + index
            rest = rest // n
        at = index + (pl.ds(pl.multiple_of(lax.rem(i, steps) * rows, rows), rows), slice(None))
        value = total[at].astype(jnp.float32)
        for term in terms:
            value = value + term[at].astype(jnp.float32)
        if out is None:
            total[at] = value.astype(total.dtype)
        else:
            out[at] = value.astype(out.dtype)
        return carry

    lax.fori_loop(0, lead * steps, body, 0)


class Scatter:
    def __init__(self, grid, order, src, columns, own, recvs, load_sem, send_sem, recv_sem, out, layout_axes):
        self.grid, self.order, self.src, self.columns = grid, order, src, columns
        self.own, self.recvs, self.out = own, recvs, out
        self.load_sem, self.send_sem, self.recv_sem = load_sem, send_sem, recv_sem
        self.layout_axes = layout_axes
        self.pending = []
        self.base = {}
        self.top = len(order) - 1
        number = 0
        for level in range(self.top, -1, -1):
            self.base[level] = number
            number += self.slots(grid, order, level)

    @staticmethod
    def inner(grid, order, level):
        return [grid.sizes[x] for x in order[1:level]]

    @staticmethod
    def slots(grid, order, level):
        return (grid.sizes[order[level]] - 1) * math.prod(Scatter.inner(grid, order, level))

    @staticmethod
    def scratch(grid, order, rows, columns, dtype):
        n1 = grid.sizes[order[0]]
        shapes = [tuple(grid.sizes[x] for x in order[1:-1]) + (n1, rows, columns)]
        for level, axis in enumerate(order):
            block = (rows, columns) if level == 0 else (n1, rows, columns)
            shapes.append((grid.sizes[axis] - 1,) + tuple(Scatter.inner(grid, order, level)) + block)
        return [pltpu.VMEM(x, dtype) for x in shapes]

    @staticmethod
    def semaphores(grid, order):
        loads = math.prod(grid.sizes[x] for x in order[1:-1])
        slots = sum(Scatter.slots(grid, order, level) for level in range(len(order)))
        return loads, slots, slots

    def hbm(self, places):
        idx = tuple(places.get(x, slice(None)) for x in self.layout_axes)
        return self.src.at[idx + (slice(None), self.columns)]

    def units(self, level):
        found = [{}]
        for x in self.order[1:level]:
            found = [{**places, x: j} for places in found for j in reversed(self.grid.nearest(x))]
        return found

    def mine(self, places):
        return self.own.at[tuple(places.get(x, self.grid.at[x]) for x in self.order[1:-1])]

    def number(self, places, axes):
        value = 0
        for x in axes:
            value = value * self.grid.sizes[x] + places[x]
        return value

    def slot(self, level, places, line):
        axes = self.order[1:level]
        number = line * math.prod(self.grid.sizes[x] for x in axes) + self.number(places, axes)
        ref = self.recvs[level].at[(line,) + tuple(places[x] for x in axes)]
        return ref, self.recv_sem.at[self.base[level] + number]

    def send(self, level, places, step, place, view):
        axis = self.order[level]
        ref, sem = self.slot(level, places, self.grid.sizes[axis] - 1 - step)
        copy = pltpu.make_async_remote_copy(
            src_ref=view,
            dst_ref=ref,
            send_sem=self.send_sem.at[len(self.pending)],
            recv_sem=sem,
            device_id=self.grid.peer(axis, place),
            device_id_type=MESH,
        )
        copy.start()
        self.pending.append(copy)

    def take(self, level, places, total, out=None):
        lines = self.grid.sizes[self.order[level]] - 1
        terms = []
        for line in range(lines):
            ref, sem = self.slot(level, places, line)
            pltpu.make_async_remote_copy(
                src_ref=ref,
                dst_ref=ref,
                send_sem=self.send_sem.at[0],
                recv_sem=sem,
                device_id={},
                device_id_type=MESH,
            ).wait_recv()
            terms.append(ref)
        add_into(total, terms, out)

    def load(self, places):
        here = {**places, self.order[-1]: self.grid.at[self.order[-1]]}
        number = self.number(places, self.order[1:-1])
        return pltpu.make_async_copy(self.hbm(here), self.mine(places), self.load_sem.at[number])

    def open(self):
        axis = self.order[self.top]
        for places in self.units(self.top):
            for step, place in enumerate(self.grid.others(axis), 1):
                self.send(self.top, places, step, place, self.hbm({**places, axis: place}))
            self.load(places).start()

    def settle(self, level, places):
        if level + 1 == self.top:
            self.load(places).wait()
        self.take(level + 1, places, self.mine(places))

    def step(self, level):
        axis = self.order[level]
        if level == 0:
            self.settle(0, {})
            for step, place in enumerate(self.grid.others(axis), 1):
                self.send(0, {}, step, place, self.mine({}).at[place])
            return
        for places in self.units(level):
            for step, place in enumerate(self.grid.others(axis), 1):
                unit = {**places, axis: place}
                self.settle(level, unit)
                self.send(level, places, step, place, self.mine(unit))
            self.settle(level, {**places, axis: self.grid.at[axis]})

    def finish(self):
        self.take(0, {}, self.mine({}).at[self.grid.at[self.order[0]]], self.out)

    def close(self):
        for copy in self.pending:
            copy.wait_send()


def half_pairs(ref, s):
    rows = pl.ds(s * BLK, BLK)
    return jnp.concatenate([ref[rows, :HD], ref[rows, HD:]], axis=0)


def read_map(blocks, table, pairs):
    @pl.when(pl.program_id(0) == 0)
    def _():
        for t in range(2 * pairs):
            table[blocks[t]] = t
        place = lax.axis_index("ctx")
        first, second = blocks[2 * place], blocks[2 * place + 1]
        table[2 * pairs] = jnp.where(second > first, 1, 0)
        table[2 * pairs + 1] = jnp.maximum(first, second)


def items(table, pairs):
    high_slot, high = table[pairs * 2], table[pairs * 2 + 1]
    low_block = 2 * pairs - 1 - high
    split = high // 2
    found = []
    for w in range(pairs - 1):
        upper = w < split
        found.append((jnp.where(upper, high_slot, 1 - high_slot), jnp.where(upper, w, w - split), None))
    found.append((high_slot, split, high))
    found.append((1 - high_slot, low_block // 2, low_block))
    return found


def chunk_of(ref, table, c):
    return jnp.concatenate(
        [ref[pl.ds(pl.multiple_of(table[2 * c + i] * BLK, BLK), BLK), :] for i in range(2)], axis=0
    )


def row_contract(left, right):
    return lax.dot_general(left, right, (((1,), (1,)), ((), ())), preferred_element_type=jnp.float32)


def attention_kernel(pairs, blocks, q_ref, k_ref, v_ref, o_ref, low_ref, over_ref, table, qs, acc, tot):
    read_map(blocks, table, pairs)
    for s in range(2):
        qs[s] = half_pairs(q_ref, s)
    acc[...] = jnp.zeros_like(acc)
    tot[...] = jnp.zeros_like(tot)
    for s, c, block in items(table, pairs):
        keys = chunk_of(k_ref, table, c)
        vals = chunk_of(v_ref, table, c)
        scores = row_contract(qs[s], keys) * (HD ** (-0.5) * math.log2(math.e))
        weights = jnp.exp2(scores)
        if block is not None:
            rows = lax.broadcasted_iota(jnp.int32, (2 * BLK, 2 * BLK), 0)
            cols = lax.broadcasted_iota(jnp.int32, (2 * BLK, 2 * BLK), 1)
            allowed = cols <= lax.rem(rows, BLK) + (block - 2 * c) * BLK
            weights = jnp.where(allowed, weights, 0.0)
        tot[s] += weights[:, :HD] + weights[:, HD:]
        acc[s] += jnp.dot(weights.astype(jnp.bfloat16), vals, preferred_element_type=jnp.float32)
    for s in range(2):
        over = 1.0 / jnp.sum(tot[s], axis=1, keepdims=True)
        value = acc[s] * over
        over = jnp.broadcast_to(over, value.shape)
        rows = pl.ds(s * BLK, BLK)
        for i in range(2):
            part = value[i * BLK : (i + 1) * BLK]
            o_ref[rows, i * HD : (i + 1) * HD] = part
            low_ref[rows, i * HD : (i + 1) * HD] = part.astype(jnp.bfloat16)
            over_ref[rows, i * HD : (i + 1) * HD] = over[i * BLK : (i + 1) * BLK]


def attention(blocks, pairs, queries, keys, values):
    rows, length = queries.shape[0], keys.shape[0]
    head = pl.BlockSpec((rows, 2 * HD), lambda h, t: (0, h))
    side = pl.BlockSpec((length, HD), lambda h, t: (0, h))
    return pl.pallas_call(
        functools.partial(attention_kernel, pairs),
        grid_spec=pltpu.PrefetchScalarGridSpec(
            num_scalar_prefetch=1,
            grid=(KVH,),
            in_specs=[head, side, side],
            out_specs=[head, head, head],
            scratch_shapes=[
                pltpu.SMEM((2 * pairs + 2,), jnp.int32),
                pltpu.VMEM((2, 2 * BLK, HD), jnp.bfloat16),
                pltpu.VMEM((2, 2 * BLK, HD), jnp.float32),
                pltpu.VMEM((2, 2 * BLK, HD), jnp.float32),
            ],
        ),
        out_shape=[
            jax.ShapeDtypeStruct((rows, H * HD), jnp.float32),
            jax.ShapeDtypeStruct((rows, H * HD), jnp.bfloat16),
            jax.ShapeDtypeStruct((rows, H * HD), jnp.float32),
        ],
        name="attention",
    )(blocks, queries, keys, values)


def attention_back_kernel(
    pairs, blocks, q_ref, k_ref, v_ref, g_ref, o_ref, dq_ref, dk_ref, dv_ref, table, qs, gs, drift, dq, dk, dv
):
    read_map(blocks, table, pairs)
    scale = HD ** (-0.5)
    for s in range(2):
        qs[s] = half_pairs(q_ref, s)
        gs[s] = half_pairs(g_ref, s)
        products = gs[s].astype(jnp.float32) * half_pairs(o_ref, s)
        drift[s : s + 1, :] = jnp.sum(products.T, axis=0, keepdims=True)
    for total in (dq, dk, dv):
        total[...] = jnp.zeros_like(total)
    for s, c, block in items(table, pairs):
        keys = chunk_of(k_ref, table, c)
        vals = chunk_of(v_ref, table, c)
        queries, grads = qs[s], gs[s]
        weights = jnp.exp2(row_contract(keys, queries) * (scale * math.log2(math.e)))
        if block is not None:
            rows = lax.broadcasted_iota(jnp.int32, (2 * BLK, 2 * BLK), 0)
            cols = lax.broadcasted_iota(jnp.int32, (2 * BLK, 2 * BLK), 1)
            allowed = rows <= lax.rem(cols, BLK) + (block - 2 * c) * BLK
            weights = jnp.where(allowed, weights, 0.0)
        through = row_contract(vals, grads)
        scores = (weights * (through - drift[pl.ds(s, 1), :])).astype(jnp.bfloat16)
        to_values = jnp.dot(weights.astype(jnp.bfloat16), grads, preferred_element_type=jnp.float32)
        to_keys = jnp.dot(scores, queries, preferred_element_type=jnp.float32)
        for i in range(2):
            at = pl.ds(pl.multiple_of(table[2 * c + i] * BLK, BLK), BLK)
            dv[at, :] += to_values[i * BLK : (i + 1) * BLK]
            dk[at, :] += to_keys[i * BLK : (i + 1) * BLK]
        dq[s] += left_dot(scores, keys)
    dk_ref[...] = (dk[...] * scale).astype(jnp.bfloat16)
    dv_ref[...] = dv[...].astype(jnp.bfloat16)
    for s in range(2):
        for i in range(2):
            dq_ref[pl.ds(s * BLK, BLK), i * HD : (i + 1) * HD] = dq[s, i * BLK : (i + 1) * BLK] * scale


def attention_back(blocks, pairs, queries, keys, values, grads, attended):
    rows, length = queries.shape[0], keys.shape[0]
    head = pl.BlockSpec((rows, 2 * HD), lambda h, t: (0, h))
    side = pl.BlockSpec((length, HD), lambda h, t: (0, h))
    return pl.pallas_call(
        functools.partial(attention_back_kernel, pairs),
        grid_spec=pltpu.PrefetchScalarGridSpec(
            num_scalar_prefetch=1,
            grid=(KVH,),
            in_specs=[head, side, side, head, head],
            out_specs=[head, side, side],
            scratch_shapes=[
                pltpu.SMEM((2 * pairs + 2,), jnp.int32),
                pltpu.VMEM((2, 2 * BLK, HD), jnp.bfloat16),
                pltpu.VMEM((2, 2 * BLK, HD), jnp.bfloat16),
                pltpu.VMEM((2, 2 * BLK), jnp.float32),
                pltpu.VMEM((2, 2 * BLK, HD), jnp.float32),
                pltpu.VMEM((length, HD), jnp.float32),
                pltpu.VMEM((length, HD), jnp.float32),
            ],
        ),
        out_shape=[
            jax.ShapeDtypeStruct((rows, H * HD), jnp.float32),
            jax.ShapeDtypeStruct((length, KVH * HD), jnp.bfloat16),
            jax.ShapeDtypeStruct((length, KVH * HD), jnp.bfloat16),
        ],
        cost_estimate=pl.CostEstimate(
            flops=20 * (pairs + 1) * KVH * (2 * BLK) ** 2 * HD,
            bytes_accessed=14 * rows * H * HD + 8 * length * KVH * HD,
            transcendentals=(pairs + 1) * KVH * (2 * BLK) ** 2,
        ),
        name="attention_back",
    )(blocks, queries, keys, values, grads, attended)


ALL_AXES = ("a", "b", "core", "f")
SLOT_AXES = ("a", "b", "core")
CHIP_AXES = ("a", "b", "f")
BFA, AFB, FAB, FBA = ("b", "f", "a"), ("a", "f", "b"), ("f", "a", "b"), ("f", "b", "a")
ABF, BAF = ("a", "b", "f"), ("b", "a", "f")
AB, BA = ("a", "b", "core"), ("b", "a", "core")
CORE = ("core",)


PUMP = (6, 1, 2, 2)
FRONT_SRC = ("q", "k", "v", "o", "g", "u", "d", "gains")


def front_kernel(grid, plan, pieces, *refs):
    n = len(FRONT_SRC)
    src = dict(zip(FRONT_SRC, refs[:n]))
    tokens_ref, cosine_ref, sine_ref = refs[n : n + 3]
    rows_of = refs[n - 1]
    outs = refs[n + 3 : n + 15]
    wqkv_ref, wo_ref, wgu_ref, wd_ref, allgains_ref, k_out, v_out = outs[:7]
    normed_ref, gains_ref, raw_ref, qlow_ref, inv_ref = outs[7:]
    scratch = refs[n + 15 :]
    held = dict(zip(FRONT_SRC, scratch[:n]))
    weights, klow, vlow, gbuf, gmine = scratch[n : n + 5]
    send, recv, local, load = scratch[n + 5 :]
    grid.enter()
    grid.barrier()
    send, recv = Pool(send), Pool(recv)
    device = grid.index["ctx"] * 2 ** len(grid.bits["f"]) + grid.index["fsdp"]
    block_rows = lax.broadcasted_iota(jnp.int32, gmine.shape, 0)
    block = jnp.zeros(gmine.shape, jnp.float32)
    for i, (at, size) in enumerate(pieces):
        spot = at + device * size
        line = jnp.broadcast_to(rows_of[i : i + 1, :], (8, 128))
        line = pltpu.roll(line, lax.rem(spot, 128), 1)[:1]
        block = jnp.where(block_rows == spot // 128, line, block)
    gmine[...] = block.astype(gmine.dtype)
    copy = pltpu.make_async_copy(gmine, held["gains"], local.at[n - 1])
    copy.start()
    copy.wait()
    src["gains"] = held["gains"]
    width = tokens_ref.shape[1]
    rows = tokens_ref.shape[0]
    spans = {"q": (wqkv_ref, 0), "k": (wqkv_ref, H * HD), "v": (wqkv_ref, (H + KVH) * HD)}
    hidden = src["g"].shape[1]
    spans.update({"o": (wo_ref, 0), "g": (wgu_ref, 0), "u": (wgu_ref, hidden), "d": (wd_ref, 0)})
    spans["gains"] = (allgains_ref, 0)
    mine = tuple(grid.at[x] for x in grid.axes(ALL_AXES))

    def own_copy(i, name):
        dst, at = spans[name]
        return pltpu.make_async_copy(
            held[name], dst.at[mine + (slice(None), pl.ds(at, src[name].shape[1]))], local.at[i]
        )

    for i, name in enumerate(FRONT_SRC[:-1]):
        pltpu.make_async_copy(src[name], held[name], local.at[i]).start()

    def part(name, low, high, order):
        dst, at = spans[name]
        order = grid.axes(order)
        sends, takes = Gather.semaphores(grid, order)
        columns = pl.ds(at + low, high - low)
        return Gather(
            grid, order, src[name].at[:, low:high], dst, columns, send.take(sends), recv.take(takes),
            grid.axes(ALL_AXES),
        )

    early = [part(*p) for p in plan[0]]
    late = [part(*p) for p in plan[1]]
    for p in early:
        p.open()
    for p in late:
        p.open()
    for i, name in enumerate(FRONT_SRC):
        if name != "gains":
            pltpu.make_async_copy(src[name], held[name], local.at[i]).wait()
        own_copy(i, name).start()
    inputs = tokens_ref[...].astype(jnp.float32)
    inverse = lax.rsqrt(jnp.mean(inputs * inputs, axis=-1, keepdims=True) + EPSILON)
    inv_ref[...] = jnp.broadcast_to(inverse, (rows, 128))
    for i, name in enumerate(FRONT_SRC):
        own_copy(i, name).wait()

    for p in early:
        p.first()
    levels = len(early[0].order)
    for level in range(1, levels - 1):
        for p in early:
            p.arrivals(level)
    pump = []
    for p in late:
        pump.append(p.first)
    for level in range(1, levels):
        for p in late:
            pump.append(functools.partial(p.arrivals, level))

    def step(count):
        for _ in range(count):
            if pump:
                pump.pop(0)()

    step(PUMP[0])
    for p in early:
        p.arrivals(levels - 1)

    places = math.prod(grid.shape(ALL_AXES))
    copy = pltpu.make_async_copy(allgains_ref, gbuf, load.at[0])
    copy.start()
    big = pltpu.make_async_copy(wqkv_ref, weights, load.at[1])
    big.start()
    copy.wait()
    blocks = gbuf[...].reshape((places,) + gbuf.shape[-2:]).astype(jnp.float32)
    gains = jnp.sum(blocks, axis=0)
    gains_ref[...] = gains
    lanes = width // 128
    for j in range(lanes):
        cols = slice(j * 128, (j + 1) * 128)
        part_of = tokens_ref[:, cols].astype(jnp.float32) * inv_ref[...] * gains_ref[j : j + 1, :]
        normed_ref[:, cols] = part_of.astype(jnp.bfloat16)
    big.wait()
    step(PUMP[1])
    flat = weights.reshape(width, weights.shape[-1])
    normed = normed_ref[...]
    chunk = 2 * HD

    def heads(low_out, gain_row, out_at, raw_at, c):
        at = pl.ds(pl.multiple_of(raw_at + c * chunk, chunk), chunk)
        raw = jnp.dot(normed, flat[:, at], preferred_element_type=jnp.float32)
        raw_ref[:, at] = raw
        done = []
        for i in range(2):
            one = raw[:, i * HD : (i + 1) * HD]
            unit = one * lax.rsqrt(jnp.mean(one * one, axis=-1, keepdims=True) + EPSILON)
            unit = unit * gains_ref[gain_row : gain_row + 1, :]
            done.append(unit * cosine_ref[...] + pltpu.roll(unit, HD // 2, 1) * sine_ref[...])
        to = pl.ds(pl.multiple_of(out_at + c * chunk, chunk), chunk)
        low_out[:, to] = jnp.concatenate(done, axis=1).astype(jnp.bfloat16)

    def loop(count, body):
        def once(c, carry):
            body(c)
            return carry

        lax.fori_loop(0, count, once, 0)

    def to_values(c):
        at = pl.ds(pl.multiple_of((H + KVH) * HD + c * chunk, chunk), chunk)
        to = pl.ds(pl.multiple_of(c * chunk, chunk), chunk)
        raw = jnp.dot(normed, flat[:, at], preferred_element_type=jnp.float32)
        vlow[:, to] = raw.astype(jnp.bfloat16)

    loop(KVH // 2, functools.partial(heads, klow, 2 * lanes + 1, 0, H * HD))
    loop(KVH // 2, to_values)

    def pair(source, dst, order):
        order = grid.axes(order)
        sends, takes = Gather.semaphores(grid, order)
        return Gather(
            grid, order, source, dst, pl.ds(0, KVH * HD), send.take(sends), recv.take(takes),
            grid.axes(SLOT_AXES),
        )

    slot = tuple(grid.at[x] for x in grid.axes(SLOT_AXES))
    slabs = [pair(klow, k_out, AB), pair(vlow, v_out, BA)]
    saves = [
        pltpu.make_async_copy(klow, k_out.at[slot], load.at[0]),
        pltpu.make_async_copy(vlow, v_out.at[slot], load.at[1]),
    ]
    for p, save in zip(slabs, saves):
        p.open()
        save.start()
    step(PUMP[2])
    loop(KVH // 2, functools.partial(heads, qlow_ref, 2 * lanes, 0, 0))
    for p, save in zip(slabs, saves):
        save.wait()
        p.first()
    step(PUMP[3])
    loop(KVH // 2, functools.partial(heads, qlow_ref, 2 * lanes, H * HD // 2, H * HD // 2))
    depth = len(slabs[0].order)
    for level in range(1, depth - 1):
        for p in slabs:
            p.arrivals(level)
    step(len(pump))
    for p in slabs:
        p.arrivals(depth - 1)
    for p in early + late + slabs:
        p.close()


def front(grid, plan, pieces, blocks, gain_rows, tokens, cosine, sine):
    n = len(FRONT_SRC)
    rows, width = tokens.shape
    places = grid.shape(ALL_AXES)
    slots = grid.shape(SLOT_AXES)
    gains = jax.ShapeDtypeStruct((width // 128 * 2 + 16, 128), jnp.bfloat16)
    blocks = tuple(blocks) + (gains,)
    by = dict(zip(FRONT_SRC, blocks))
    low, f32 = jnp.bfloat16, jnp.float32
    full = (H + 2 * KVH) * HD
    counts = [Gather.semaphores(grid, grid.axes(p[3])) for p in plan[0] + plan[1]]
    counts += [Gather.semaphores(grid, grid.axes(x)) for x in (AB, BA)]
    sends, takes = [sum(x) for x in zip(*counts)]
    shape = jax.ShapeDtypeStruct
    vmem = pl.BlockSpec(memory_space=pltpu.VMEM)
    outs = pl.pallas_call(
        functools.partial(front_kernel, grid, plan, pieces),
        out_shape=[
            shape(places + (by["q"].shape[0], full), low),
            shape(places + by["o"].shape, low),
            shape(places + (by["g"].shape[0], 2 * by["g"].shape[1]), low),
            shape(places + by["d"].shape, low),
            shape(places + by["gains"].shape, low),
            shape(slots + (rows, KVH * HD), low),
            shape(slots + (rows, KVH * HD), low),
            shape((rows, width), low),
            shape(by["gains"].shape, f32),
            shape((rows, (H + KVH) * HD), f32),
            shape((rows, H * HD), low),
            shape((rows, 128), f32),
        ],
        in_specs=[ANY] * (n - 1) + [vmem] * 4,
        out_specs=[ANY] * 7 + [vmem] * 5,
        scratch_shapes=[pltpu.VMEM(x.shape, x.dtype) for x in blocks]
        + [
            pltpu.VMEM(places + (by["q"].shape[0], full), low),
            pltpu.VMEM((rows, KVH * HD), low),
            pltpu.VMEM((rows, KVH * HD), low),
            pltpu.VMEM(places + by["gains"].shape, low),
            pltpu.VMEM(by["gains"].shape, low),
            pltpu.SemaphoreType.DMA((sends,)),
            pltpu.SemaphoreType.DMA((takes,)),
            pltpu.SemaphoreType.DMA((n,)),
            pltpu.SemaphoreType.DMA((2,)),
        ],
        compiler_params=pltpu.CompilerParams(
            has_side_effects=True, vmem_limit_bytes=60 * 2**20, collective_id=0
        ),
        name="front",
    )(*blocks[:-1], gain_rows, tokens, cosine, sine)
    wqkv, wo, wgu, wd, _, keys, vals, normed, gains, raw, qlow, inverse = outs
    flat = [x.reshape(-1, x.shape[-1]) for x in (wqkv, wo, wgu, wd, keys, vals)]
    return flat + [normed, gains, raw, qlow, inverse]


def sums_kernel(count, core, left, left_other, right, right_other, out, turned):
    rows, width = left.shape
    block = width // count

    @pl.when(pl.program_id(0) == 0)
    def _():
        for j in range(count // 2):
            at = pl.ds(pl.multiple_of((2 * j + core[0]) * block, block), block)
            for k, ref in enumerate((left, left_other)):
                turned[j * block : (j + 1) * block, k * rows : (k + 1) * rows] = ref[:, at].T

    rhs = jnp.concatenate([right[...], right_other[...]], axis=0)
    out[...] = jnp.dot(turned[...], rhs, preferred_element_type=jnp.float32).astype(out.dtype)


def chip_sums(left, left_other, right, right_other):
    rows, width = left.shape
    count = lax.axis_size("ctx")
    block = width // count
    tile = 512
    if block % 128:
        place = lax.axis_index("ctx") % 2
        halves = [
            lax.dynamic_index_in_dim(x.reshape(rows, count // 2, 2, block), place, 2, False)
            for x in (left, left_other)
        ]
        lhs = jnp.concatenate(halves, axis=0).reshape(2 * rows, width // 2)
        return left_dot(lhs, jnp.concatenate([right, right_other], axis=0)).astype(jnp.bfloat16)
    core = (lax.axis_index("ctx") % 2).astype(jnp.int32)[None]
    lhs = pl.BlockSpec((rows, width), lambda n, c: (0, 0))
    rhs = pl.BlockSpec((rows, tile), lambda n, c: (0, n))
    return pl.pallas_call(
        functools.partial(sums_kernel, count),
        grid_spec=pltpu.PrefetchScalarGridSpec(
            num_scalar_prefetch=1,
            grid=(right.shape[1] // tile,),
            in_specs=[lhs, lhs, rhs, rhs],
            out_specs=pl.BlockSpec((width // 2, tile), lambda n, c: (0, n)),
            scratch_shapes=[pltpu.VMEM((width // 2, 2 * rows), jnp.bfloat16)],
        ),
        out_shape=jax.ShapeDtypeStruct((width // 2, right.shape[1]), jnp.bfloat16),
        name="chip_sums",
    )(core, left, left_other, right, right_other)


def handed_kernel(pieces, count, sums_ref, *refs):
    results, outs = refs[: (len(refs) - len(pieces)) // 2], refs[(len(refs) - len(pieces)) // 2 :]
    for source, out in zip(results, outs):
        out[...] = source[...]
    device = lax.axis_index("ctx") * count + lax.axis_index("fsdp")
    for (at, size), out in zip(pieces, outs[len(results) :]):
        spot = at + device * size
        line = jnp.broadcast_to(sums_ref[pl.ds(spot // 128, 1), :], (8, 128))
        line = pltpu.roll(line, lax.rem(128 - lax.rem(spot, 128), 128), 1)
        out[...] = line[:1, :size]


def handed(pieces, sums, *results):
    vmem = pl.BlockSpec(memory_space=pltpu.VMEM)
    return pl.pallas_call(
        functools.partial(handed_kernel, pieces, lax.axis_size("fsdp")),
        out_shape=[jax.ShapeDtypeStruct(x.shape, x.dtype) for x in results]
        + [jax.ShapeDtypeStruct((1, size), jnp.float32) for _, size in pieces],
        in_specs=[vmem] * (1 + len(results)),
        out_specs=[vmem] * (len(results) + len(pieces)),
        name="handed",
    )(sums, *results)


BACK_SUMS = ("g", "u", "d", "o")


def back_kernel(grid, plan, *refs):
    refs = list(refs)

    def take(n):
        found = refs[:n]
        del refs[:n]
        return found

    src = dict(zip(BACK_SUMS, take(len(BACK_SUMS))))
    gk_ref, gv_ref, wqkv_ref = take(3)
    dq_ref, raw_ref, cos_ref, turn_ref, gains_ref, normed_ref, tokens_ref, inv_ref, mid_ref, gain2_ref = take(10)
    outs = dict(zip(BACK_SUMS + ("q", "k", "v"), take(len(BACK_SUMS) + 3)))
    din_ref, gsum_ref, sums_ref, gall_ref = take(4)
    weights, both_normed, both_raw, own_k, own_v, stage, acc, gbuf, gblock = take(9)
    load, send, recv, misc = [Pool(x) for x in refs[-4:]]
    del refs[-4:]
    scratch = refs
    grid.enter()
    grid.barrier()
    rows, width = tokens_ref.shape
    lanes = width // 128
    core = grid.at["core"]
    chunk = 2 * HD
    misc_sem = [misc.take(1).at[0] for _ in range(12)]

    def make(source, columns, order, out, layout):
        loads, sends, takes = Scatter.semaphores(grid, order)
        own, *recvs = scratch[: 1 + len(order)]
        del scratch[: 1 + len(order)]
        return Scatter(
            grid, order, source, columns, own, recvs,
            load.take(loads), send.take(sends), recv.take(takes), out, layout,
        )

    def portions(group):
        found = []
        for name, low, high, order in group:
            found.append(
                make(src[name], pl.ds(low, high - low), order, outs[name].at[:, low:high], CHIP_AXES)
            )
        return found

    slabs = [
        make(gk_ref, pl.ds(0, KVH * HD), AB, own_k, SLOT_AXES),
        make(gv_ref, pl.ds(0, KVH * HD), BA, own_v, SLOT_AXES),
    ]
    early, waves = portions(plan[0]), [portions(group) for group in plan[1]]
    late = [p for wave in waves for p in wave]
    last = []
    for name, at, low, high, order in plan[2]:
        last.append(
            make(sums_ref, pl.ds(at + low, high - low), order, outs[name].at[:, low:high], CHIP_AXES)
        )

    def sibling(source, dst, k):
        return pltpu.make_async_remote_copy(
            src_ref=source, dst_ref=dst, send_sem=misc_sem[2 * k], recv_sem=misc_sem[2 * k + 1],
            device_id=grid.peer("core", 1 - core), device_id_type=MESH,
        )

    for p in slabs + early:
        p.open()
    swap_normed = sibling(normed_ref, both_normed.at[1], 0)
    swap_normed.start()
    both_normed[0] = normed_ref[...]
    gblock[...] = jnp.zeros_like(gblock)
    gblock[lanes : 2 * lanes, :] = gain2_ref[...]

    def loop(count, body):
        def once(c, carry):
            body(c)
            return carry

        lax.fori_loop(0, count, once, 0)

    def heads(source, in_at, raw_at, gain_row, c):
        at = pl.ds(pl.multiple_of(raw_at + c * chunk, chunk), chunk)
        grads = source[:, pl.ds(pl.multiple_of(in_at + c * chunk, chunk), chunk)]
        raw = raw_ref[:, at]
        gain = gains_ref[gain_row : gain_row + 1, :]
        done = []
        for i in range(2):
            g = grads[:, i * HD : (i + 1) * HD]
            g = g * cos_ref[...] - pltpu.roll(g, HD // 2, 1) * turn_ref[...]
            one = raw[:, i * HD : (i + 1) * HD]
            inverse = lax.rsqrt(jnp.mean(one * one, axis=-1, keepdims=True) + EPSILON)
            unit = one * inverse
            gblock[gain_row : gain_row + 1, :] += jnp.sum(g * unit, axis=0, keepdims=True)
            done.append(norm_back(g, unit, inverse, gain))
        both_raw[0, :, at] = jnp.concatenate(done, axis=1).astype(jnp.bfloat16)

    half_q = H * HD // 2
    q_cols, kv_cols = pl.ds(0, H * HD), pl.ds(H * HD, 2 * KVH * HD)
    loop(H // 4, functools.partial(heads, dq_ref, 0, 0, 2 * lanes))
    for p in slabs:
        p.step(1)
    loop(H // 4, functools.partial(heads, dq_ref, half_q, half_q, 2 * lanes))
    swap_q = sibling(both_raw.at[0, :, q_cols], both_raw.at[1, :, q_cols], 1)
    swap_q.start()
    for p in slabs:
        p.step(0)
    def every(group, what, *args):
        for p in group:
            getattr(p, what)(*args)

    every(waves[0], "open")
    for p in slabs:
        p.finish()
    loop(KVH // 2, functools.partial(heads, own_k, 0, H * HD, 2 * lanes + 1))
    at = (H + KVH) * HD
    both_raw[0, :, at : at + KVH * HD] = own_v[...].astype(jnp.bfloat16)
    swap_kv = sibling(both_raw.at[0, :, kv_cols], both_raw.at[1, :, kv_cols], 2)
    swap_kv.start()
    every(waves[1], "open")
    swap_normed.wait()
    swap_q.wait()
    swap_kv.wait()
    flat_normed = both_normed.reshape(2 * rows, width)
    flat_raw = both_raw.reshape(2 * rows, both_raw.shape[-1])
    count = grid.sizes["a"] * grid.sizes["b"]
    block = width // (2 * count)
    piece = block // grid.sizes["f"]
    full = both_raw.shape[-1]
    tile = 512

    def stored(j):
        return pltpu.make_async_copy(stage.at[j % 2], sums_ref.at[j // 2, j % 2], misc_sem[9 + j % 2])

    for j in range(count):
        if j >= 2:
            stored(j - 2).wait()
        lhs = flat_normed[:, pl.ds(pl.multiple_of((2 * j + core) * block, block), block)]

        def sums(c):
            cols = pl.ds(pl.multiple_of(c * tile, tile), tile)
            value = left_dot(lhs, flat_raw[:, cols]).astype(jnp.bfloat16)
            stage[j % 2, :, :, cols] = value.reshape(grid.sizes["f"], piece, tile)

        loop(full // tile, sums)
        stored(j).start()
    for j in range(count - 2, count):
        stored(j).wait()
    every(waves[0], "step", 1)
    every(last, "open")
    every(waves[2], "open")
    every(early, "step", 1)
    every(waves[1], "step", 1)
    every(waves[0], "step", 0)
    tiles = [
        pltpu.make_async_copy(
            wqkv_ref.at[:, c * tile : (c + 1) * tile], weights.at[c % 2], misc_sem[6 + c % 2]
        )
        for c in range(full // tile)
    ]
    tiles[0].start()
    for c in range(full // tile):
        if c + 1 < full // tile:
            tiles[c + 1].start()
        tiles[c].wait()
        value = right_dot(both_raw[0, :, c * tile : (c + 1) * tile], weights[c % 2])
        acc[...] = value if c == 0 else acc[...] + value
    inverse = inv_ref[...]
    for j in range(lanes):
        cols = slice(j * 128, (j + 1) * 128)
        normal = tokens_ref[:, cols].astype(jnp.float32) * inverse
        gblock[j : j + 1, :] = jnp.sum(acc[:, cols] * normal, axis=0, keepdims=True)
    copy = pltpu.make_async_copy(gblock, gbuf, misc_sem[11])
    copy.start()
    copy.wait()
    order = FAB + CORE
    sends, takes = Gather.semaphores(grid, order)
    spread = Gather(
        grid, order, gbuf, gall_ref, slice(None), send.take(sends), recv.take(takes), ALL_AXES
    )
    spread.open()
    mine = tuple(grid.at[x] for x in ALL_AXES)
    gall_ref[mine] = gblock[...]
    every(early, "step", 0)
    every(last, "step", 1)
    every(waves[2], "step", 1)
    every(waves[1], "step", 0)
    spread.first()
    dots = jnp.zeros((rows, 1), jnp.float32)
    for j in range(lanes):
        cols = slice(j * 128, (j + 1) * 128)
        normal = tokens_ref[:, cols].astype(jnp.float32) * inverse
        dots += jnp.sum(acc[:, cols] * gains_ref[j : j + 1, :] * normal, axis=1, keepdims=True)
    dots = dots / width
    for j in range(lanes):
        cols = slice(j * 128, (j + 1) * 128)
        normal = tokens_ref[:, cols].astype(jnp.float32) * inverse
        grad = inverse * (acc[:, cols] * gains_ref[j : j + 1, :] - normal * dots)
        din_ref[:, cols] = (mid_ref[:, cols] + grad).astype(jnp.bfloat16)
    spread.arrivals(1)
    every(last, "step", 0)
    every(waves[2], "step", 0)
    spread.arrivals(2)
    every(waves[0] + early + waves[1], "finish")
    spread.arrivals(3)
    every(last + waves[2], "finish")
    places = math.prod(grid.sizes[x] for x in ALL_AXES)
    gsum_ref[...] = jnp.sum(gall_ref.reshape((places,) + gblock.shape)[...], axis=0)
    for p in slabs + early + late + last:
        p.close()
    spread.close()


def back_scratch(grid, plan, pieces, rows, width):
    low = jnp.bfloat16
    scratch, counts = [], []
    for order in (AB, BA):
        scratch += Scatter.scratch(grid, order, rows, KVH * HD, low)
        counts.append(Scatter.semaphores(grid, order))
    for name, begin, end, order in plan[0] + sum(plan[1], ()) + tuple((p[0],) + p[2:] for p in plan[2]):
        scratch += Scatter.scratch(grid, order, pieces[name], end - begin, low)
        counts.append(Scatter.semaphores(grid, order))
    return scratch, [sum(x) for x in zip(*counts)]


def back_fits(grid, plan, rows, width, hidden, total):
    pieces = {name: width // total for name in ("g", "u", "q", "k", "v")}
    pieces.update({"d": hidden // total, "o": H * HD // total})
    scratch = back_scratch(grid, plan, pieces, rows, width)[0]
    taken = sum(2 * math.prod(x.shape) for x in scratch)
    held = 2 * rows * (11 * width + 3 * (H + 2 * KVH) * HD + 4 * (H + KVH) * HD) + 6 * 2**20
    return taken + held < 62 * 2**20


def back(grid, plan, sums, gk, gv, wqkv, dq, raw, cosine, turned, gains, normed, tokens, inverse, middle, gain2):
    low, f32 = jnp.bfloat16, jnp.float32
    rows, width = tokens.shape
    chips = tuple(grid.sizes[x] for x in CHIP_AXES)
    places = tuple(grid.sizes[x] for x in ALL_AXES)
    slots = tuple(grid.sizes[x] for x in SLOT_AXES)
    blocks = [x.reshape(chips + (x.shape[0] // math.prod(chips), x.shape[1])) for x in sums]
    shape = jax.ShapeDtypeStruct
    vmem = pl.BlockSpec(memory_space=pltpu.VMEM)
    piece = width // math.prod(places)
    pieces = dict(zip(BACK_SUMS, [x.shape[-2] for x in blocks]))
    pieces.update({"q": piece, "k": piece, "v": piece})
    scratch, (loads, sends, takes) = back_scratch(grid, plan, pieces, rows, width)
    more = Gather.semaphores(grid, FAB + CORE)
    full = wqkv.shape[1]
    count = grid.sizes["a"] * grid.sizes["b"]
    outs = pl.pallas_call(
        functools.partial(back_kernel, grid, plan),
        out_shape=[shape(x.shape[-2:], f32) for x in blocks]
        + [shape((piece, n), f32) for n in (H * HD, KVH * HD, KVH * HD)]
        + [
            shape((rows, width), low),
            shape(gains.shape, f32),
            shape(chips + (piece, full), low),
        ],
        in_specs=[ANY] * (len(blocks) + 3) + [vmem] * 10,
        out_specs=[vmem] * (len(blocks) + 5) + [ANY],
        scratch_shapes=[
            pltpu.VMEM(places + gains.shape, f32),
            pltpu.VMEM((2, width, 512), low),
            pltpu.VMEM((2, rows, width), low),
            pltpu.VMEM((2, rows, full), low),
            pltpu.VMEM((rows, KVH * HD), f32),
            pltpu.VMEM((rows, KVH * HD), f32),
            pltpu.VMEM((2, grid.sizes["f"], piece, full), low),
            pltpu.VMEM((rows, width), f32),
            pltpu.VMEM(gains.shape, f32),
            pltpu.VMEM(gains.shape, f32),
        ]
        + scratch
        + [
            pltpu.SemaphoreType.DMA((loads,)),
            pltpu.SemaphoreType.DMA((sends + more[0],)),
            pltpu.SemaphoreType.DMA((takes + more[1],)),
            pltpu.SemaphoreType.DMA((12,)),
        ],
        compiler_params=pltpu.CompilerParams(
            has_side_effects=True, vmem_limit_bytes=63 * 2**20, collective_id=1
        ),
        name="back",
    )(
        *blocks,
        gk.reshape(slots + (rows, KVH * HD)),
        gv.reshape(slots + (rows, KVH * HD)),
        wqkv, dq, raw, cosine, turned, gains, normed, tokens, inverse, middle, gain2,
    )
    return outs


def middle_kernel(
    steps, alow_ref, over_ref, wo_ref, wg_ref, wu_ref, wd_ref, tokens_ref, cot_ref, gains_ref,
    out_ref, hidden_ref, gg_ref, gu_ref, normed_ref, mid_ref, branch_ref, gain_ref, gs_ref,
    middle, total, back, inv,
):
    c = pl.program_id(0)
    rows, width = tokens_ref.shape
    lanes = width // 128
    low = jnp.bfloat16

    @pl.when(c == 0)
    def _():
        value = tokens_ref[...].astype(jnp.float32) + plain_dot(alow_ref[...], wo_ref[...])
        inverse = lax.rsqrt(jnp.mean(value * value, axis=-1, keepdims=True) + EPSILON)
        inv[...] = jnp.broadcast_to(inverse, inv.shape)
        middle[...] = value
        total[...] = value
        for j in range(lanes):
            cols = slice(j * 128, (j + 1) * 128)
            gain = gains_ref[lanes + j : lanes + j + 1, :]
            normed_ref[:, cols] = (middle[:, cols] * inv[...] * gain).astype(low)
        back[...] = jnp.zeros_like(back)

    normed = normed_ref[...]
    gate = plain_dot(normed, wg_ref[...])
    upper = plain_dot(normed, wu_ref[...])
    grads = right_dot(cot_ref[...], wd_ref[...])
    sig = jax.nn.sigmoid(gate)
    activated = gate * sig
    hidden = (activated * upper).astype(low)
    grad_gate = (grads * upper * sig * (1.0 + gate * (1.0 - sig))).astype(low)
    grad_upper = (grads * activated).astype(low)
    hidden_ref[...] = hidden
    gg_ref[...] = grad_gate
    gu_ref[...] = grad_upper
    total[...] += plain_dot(hidden, wd_ref[...])
    back[...] += right_dot(grad_gate, wg_ref[...]) + right_dot(grad_upper, wu_ref[...])

    @pl.when(c == steps - 1)
    def _():
        out_ref[...] = total[...].astype(low)
        inverse = inv[...]
        dots = jnp.zeros((rows, 1), jnp.float32)
        for j in range(lanes):
            cols = slice(j * 128, (j + 1) * 128)
            normal = middle[:, cols] * inverse
            gain_ref[j : j + 1, :] = jnp.sum(back[:, cols] * normal, axis=0, keepdims=True)
            gain = gains_ref[lanes + j : lanes + j + 1, :]
            dots += jnp.sum(back[:, cols] * gain * normal, axis=1, keepdims=True)
        dots = dots / width
        for j in range(lanes):
            cols = slice(j * 128, (j + 1) * 128)
            gain = gains_ref[lanes + j : lanes + j + 1, :]
            normal = middle[:, cols] * inverse
            grad = cot_ref[:, cols].astype(jnp.float32) + inverse * (back[:, cols] * gain - normal * dots)
            mid_ref[:, cols] = grad
            branch_ref[:, cols] = grad.astype(low)
        tile = 512
        for j in range(gs_ref.shape[1] // tile):
            cols = slice(j * tile, (j + 1) * tile)
            attended = right_dot(branch_ref[...], wo_ref[cols, :])
            gs_ref[:, cols] = (attended * over_ref[:, cols]).astype(low)


def middle_part(alow, over, wo, wgu, wd, tokens, cotangent, gains):
    low, f32 = jnp.bfloat16, jnp.float32
    rows, width = tokens.shape
    hidden = wd.shape[0]
    tile = 512
    steps = hidden // tile
    shape = jax.ShapeDtypeStruct

    def whole(x):
        return pl.BlockSpec(x.shape, lambda c: (0,) * len(x.shape))

    def columns(at):
        return pl.BlockSpec((width, tile), lambda c: (0, at + c))

    chunk = pl.BlockSpec((rows, tile), lambda c: (0, c))
    outs = [
        shape((rows, width), low),
        shape((rows, hidden), low),
        shape((rows, hidden), low),
        shape((rows, hidden), low),
        shape((rows, width), low),
        shape((rows, width), f32),
        shape((rows, width), low),
        shape((width // 128, 128), f32),
        shape(alow.shape, low),
    ]
    return pl.pallas_call(
        functools.partial(middle_kernel, steps),
        grid=(steps,),
        in_specs=[
            whole(alow),
            whole(over),
            whole(wo),
            columns(0),
            columns(steps),
            pl.BlockSpec((tile, width), lambda c: (c, 0)),
            whole(tokens),
            whole(cotangent),
            whole(gains),
        ],
        out_specs=[whole(outs[0])] + [chunk] * 3 + [whole(x) for x in outs[4:]],
        out_shape=outs,
        scratch_shapes=[pltpu.VMEM((rows, width), f32)] * 3 + [pltpu.VMEM((rows, 128), f32)],
        compiler_params=pltpu.CompilerParams(vmem_limit_bytes=60 * 2**20),
        name="middle",
    )(alow, over, wo, wgu, wgu, wd, tokens, cotangent, gains)


def scatter_kernel(grid, portions, layouts, n, *refs):
    srcs, outs, scratch = refs[:n], refs[n : 2 * n], list(refs[2 * n : -3])
    load, send, recv = [Pool(x) for x in refs[-3:]]
    grid.enter()
    parts = []
    for i, low, high, order in portions:
        loads, sends, takes = Scatter.semaphores(grid, order)
        own, *recvs = scratch[: 1 + len(order)]
        del scratch[: 1 + len(order)]
        parts.append(
            Scatter(
                grid,
                order,
                srcs[i],
                pl.ds(low, high - low),
                own,
                recvs,
                load.take(loads),
                send.take(sends),
                recv.take(takes),
                outs[i].at[:, low:high],
                layouts[i],
            )
        )
        parts[-1].open()
    for level in (2, 1, 0):
        for part in parts:
            if level < part.top:
                part.step(level)
    for part in parts:
        part.finish()
    for part in parts:
        part.close()


def scatter(grid, layouts, portions, name, dtypes, *sums):
    n = len(sums)
    blocks = []
    for layout, x in zip(layouts, sums):
        places = tuple(grid.sizes[axis] for axis in layout)
        blocks.append(x.reshape(places + (x.shape[0] // math.prod(places), x.shape[1])))
    loads, sends, takes = [sum(x) for x in zip(*[Scatter.semaphores(grid, p[3]) for p in portions])]
    scratch = []
    for i, low, high, order in portions:
        scratch += Scatter.scratch(grid, order, blocks[i].shape[-2], high - low, blocks[i].dtype)
    return pl.pallas_call(
        functools.partial(scatter_kernel, grid, portions, layouts, n),
        out_shape=[jax.ShapeDtypeStruct(x.shape[-2:], t) for x, t in zip(blocks, dtypes)],
        in_specs=[ANY] * n,
        out_specs=[pl.BlockSpec(memory_space=pltpu.VMEM)] * n,
        scratch_shapes=scratch
        + [
            pltpu.SemaphoreType.DMA((loads,)),
            pltpu.SemaphoreType.DMA((sends,)),
            pltpu.SemaphoreType.DMA((takes,)),
        ],
        compiler_params=pltpu.CompilerParams(has_side_effects=True, vmem_limit_bytes=60 * 2**20),
        name=name,
    )(*blocks)


def gain_rows(total, *gains):
    pieces = [x.reshape(total, 1, -1) for x in gains]
    pieces = [jnp.pad(x, ((0, 0), (0, 0), (0, 128 - x.shape[2]))) for x in pieces]
    block = jnp.concatenate(pieces, axis=1)
    return jnp.pad(block, ((0, 0), (0, 8 - len(gains)), (0, 0))).reshape(total * 8, 128)


def swapped(x):
    count = lax.axis_size("ctx")
    return lax.ppermute(x, "ctx", [(i, i ^ 1) for i in range(count)])


def on_device(
    tokens,
    cotangent,
    block_map,
    attn_gain,
    query_weight,
    key_weight,
    value_weight,
    query_gain,
    key_gain,
    output_weight,
    mlp_gain,
    gate_weight,
    up_weight,
    down_weight,
):
    grid = Grid(lax.axis_size("ctx"), lax.axis_size("fsdp"))
    total = lax.axis_size("ctx") * lax.axis_size("fsdp")
    groups, rows, width = tokens.shape
    pairs = block_map.shape[1] // 2
    ratio = H // KVH
    low = jnp.bfloat16

    device = lax.axis_index("ctx") * lax.axis_size("fsdp") + lax.axis_index("fsdp")
    gain_pieces = [
        (at, x.shape[0])
        for at, x in ((0, attn_gain), (width, mlp_gain), (2 * width, query_gain), (2 * width + HD, key_gain))
    ]
    gain_lines = jnp.concatenate(
        [
            jnp.pad(x.astype(jnp.float32).reshape(1, -1), ((0, 0), (0, 128 - x.shape[0])))
            for x in (attn_gain, mlp_gain, query_gain, key_gain)
        ]
    )
    hidden_width = gate_weight.shape[1]

    place = lax.axis_index("ctx")
    blocks = block_map.reshape(-1)
    own_blocks = lax.dynamic_slice_in_dim(blocks, 2 * place, 2, 0)
    spots = (own_blocks[:, None] * BLK + jnp.arange(BLK, dtype=jnp.int32)).reshape(rows)
    cosine, sine = rope_tables(spots)
    turned = jnp.concatenate([-sine[:, : HD // 2], sine[:, HD // 2 :]], axis=1)
    half_q, half_k = H * HD // 2, KVH * HD // 2
    half = half_q + 2 * half_k
    plan = (
        (
            ("gains", 0, 128, FAB + CORE),
            ("q", 0, half_q, FAB + CORE),
            ("q", half_q, 2 * half_q, FBA + CORE),
            ("k", 0, 2 * half_k, BFA + CORE),
            ("v", 0, 2 * half_k, AFB + CORE),
        ),
        (
            ("o", 0, width // 2, FAB + CORE),
            ("o", width // 2, width, FBA + CORE),
            ("g", 0, hidden_width, BFA + CORE),
            ("u", 0, hidden_width, AFB + CORE),
            ("d", 0, width // 2, ABF + CORE),
            ("d", width // 2, width, BFA + CORE),
        ),
    )
    (
        full_qkv,
        full_output,
        full_gu,
        full_down,
        key_all,
        value_all,
        normed,
        gains,
        raw,
        query_low,
        inverse_one,
    ) = front(
        Pairs(lax.axis_size("ctx"), lax.axis_size("fsdp")),
        plan,
        gain_pieces,
        (query_weight, key_weight, value_weight, output_weight, gate_weight, up_weight, down_weight),
        gain_lines,
        tokens.reshape(rows, width),
        cosine,
        turned,
    )
    attended, attended_low, over_totals = attention(blocks, pairs, query_low, key_all, value_all)
    lanes = width // 128
    gain_one = gains[:lanes].reshape(-1)
    query_scale, key_scale = gains[2 * lanes], gains[2 * lanes + 1]
    inverse_rows = inverse_one
    inverse_one = inverse_one[:, :1]
    inputs = tokens.reshape(rows, width).astype(jnp.float32)
    normal_one = inputs * inverse_one
    cosine = cosine.reshape(rows, 1, HD)
    sine = sine.reshape(rows, 1, HD)
    query_raw = raw[:, : H * HD].reshape(rows, H, HD)
    key_raw = raw[:, H * HD :].reshape(rows, KVH, HD)
    query_inverse = lax.rsqrt(jnp.mean(query_raw * query_raw, axis=-1, keepdims=True) + EPSILON)
    query_unit = query_raw * query_inverse
    key_inverse = lax.rsqrt(jnp.mean(key_raw * key_raw, axis=-1, keepdims=True) + EPSILON)
    key_unit = key_raw * key_inverse
    upstream = cotangent.reshape(rows, width)
    (
        output,
        hidden,
        grad_gate,
        grad_upper,
        normed_two,
        grad_middle,
        branch_grad,
        grad_gain_two,
        grad_summed,
    ) = middle_part(
        attended_low, over_totals, full_output, full_gu, full_down, tokens.reshape(rows, width), upstream, gains
    )
    output = output.reshape(groups, rows, width)
    grad_gain_two = grad_gain_two.reshape(width)
    normed_other, upstream_other = swapped(normed_two), swapped(upstream)
    grad_down = chip_sums(hidden, swapped(hidden), upstream, upstream_other)
    grad_g = chip_sums(normed_two, normed_other, grad_gate, swapped(grad_gate))
    grad_u = chip_sums(normed_two, normed_other, grad_upper, swapped(grad_upper))
    grad_woutput = chip_sums(attended_low, swapped(attended_low), branch_grad, swapped(branch_grad))
    grad_query, grad_keys, grad_values = attention_back(
        blocks, pairs, query_low, key_all, value_all, grad_summed, attended
    )
    back_plan = (
        (("d", 0, width // 2, ABF), ("d", width // 2, width, BAF)),
        (
            (("g", 0, hidden_width // 2, FAB), ("g", hidden_width // 2, hidden_width, FBA)),
            (("u", 0, hidden_width // 2, FAB), ("u", hidden_width // 2, hidden_width, FBA)),
            (("o", 0, width // 2, FAB), ("o", width // 2, width, FBA)),
        ),
        (
            ("q", 0, 0, half_q, ABF),
            ("q", 0, half_q, 2 * half_q, BAF),
            ("k", H * HD, 0, 2 * half_k, FAB),
            ("v", (H + KVH) * HD, 0, 2 * half_k, FBA),
        ),
    )
    if back_fits(grid, back_plan, rows, width, hidden_width, total):
        out_g, out_u, out_down, out_output, out_q, out_k, out_v, grad_tokens, gain_sums, _ = back(
            grid,
            back_plan,
            (grad_g, grad_u, grad_down, grad_woutput),
            grad_keys,
            grad_values,
            full_qkv,
            grad_query,
            raw,
            cosine.reshape(rows, HD),
            turned,
            gains,
            normed,
            tokens.reshape(rows, width),
            inverse_rows,
            grad_middle,
            grad_gain_two.reshape(lanes, 128),
        )
        (
            out_g,
            out_u,
            out_down,
            out_output,
            out_q,
            out_k,
            out_v,
            grad_tokens,
            *own_gains,
        ) = handed(
            gain_pieces, gain_sums, out_g, out_u, out_down, out_output, out_q, out_k, out_v, grad_tokens
        )
        own_attn, own_mlp, own_query, own_key = [x.reshape(-1) for x in own_gains]
        return (
            output,
            grad_tokens.reshape(groups, rows, width),
            own_attn,
            out_q,
            out_k,
            out_v,
            own_query,
            own_key,
            out_output,
            own_mlp,
            out_g,
            out_u,
            out_down,
        )
    f32 = jnp.float32
    own_keys, own_values, out_g, out_u, out_down, out_output = scatter(
        grid,
        [SLOT_AXES] * 2 + [CHIP_AXES] * 4,
        [
            (0, 0, KVH * HD, AB),
            (1, 0, KVH * HD, BA),
            (2, 0, hidden_width, BFA),
            (3, 0, hidden_width, AFB),
            (4, 0, width // 2, BFA),
            (4, width // 2, width, AFB),
            (5, 0, width // 2, BFA),
            (5, width // 2, width, AFB),
        ],
        "scatter_mlp",
        (f32, low, f32, f32, f32, f32),
        grad_keys,
        grad_values,
        grad_g,
        grad_u,
        grad_down,
        grad_woutput,
    )
    grad_qrot = grad_query.reshape(rows, H, HD)
    grad_qnormed = grad_qrot * cosine + unrotate(grad_qrot) * sine
    grad_qscale = jnp.sum(grad_qnormed * query_unit, axis=(0, 1))
    grad_qraw = norm_back(grad_qnormed, query_unit, query_inverse, query_scale)
    grad_krot = own_keys.reshape(rows, KVH, HD)
    grad_knormed = grad_krot * cosine + unrotate(grad_krot) * sine
    grad_kscale = jnp.sum(grad_knormed * key_unit, axis=(0, 1))
    grad_kraw = norm_back(grad_knormed, key_unit, key_inverse, key_scale)
    grad_raw = jnp.concatenate(
        [
            grad_qraw.reshape(rows, H * HD).astype(low),
            grad_kraw.reshape(rows, KVH * HD).astype(low),
            own_values,
        ],
        axis=1,
    )
    grad_wqkv = chip_sums(normed, swapped(normed), grad_raw, swapped(grad_raw))
    grad_normed = right_dot(grad_raw, full_qkv)
    grad_gain_one = jnp.sum(grad_normed * normal_one, axis=0)
    grad_inputs = grad_middle + norm_back(grad_normed, normal_one, inverse_one, gain_one)
    out_qkv, out_gains = scatter(
        grid,
        [CHIP_AXES, ALL_AXES],
        [
            (0, 0, half // 2, FAB),
            (0, half // 2, half, FBA),
            (0, half, 3 * half // 2, BFA),
            (0, 3 * half // 2, 2 * half, AFB),
            (1, 0, 128, FAB + CORE),
        ],
        "scatter_attention",
        (f32, f32),
        grad_wqkv,
        gain_rows(total, grad_gain_one, grad_qscale, grad_kscale, grad_gain_two),
    )
    return (
        output,
        grad_inputs.astype(low).reshape(groups, rows, width),
        out_gains[0, : attn_gain.shape[0]],
        out_qkv[:, : H * HD],
        out_qkv[:, H * HD : (H + KVH) * HD],
        out_qkv[:, (H + KVH) * HD :],
        out_gains[1, : query_gain.shape[0]],
        out_gains[2, : key_gain.shape[0]],
        out_output,
        out_gains[3, : mlp_gain.shape[0]],
        out_g,
        out_u,
        out_down,
    )


def solution(mesh):
    return jax.shard_map(
        on_device,
        mesh=mesh,
        in_specs=(
            P("fsdp", "ctx", None),
            P("fsdp", "ctx", None),
            P("fsdp", None),
            P(("ctx", "fsdp")),
            P(("ctx", "fsdp"), None),
            P(("ctx", "fsdp"), None),
            P(("ctx", "fsdp"), None),
            P(("ctx", "fsdp")),
            P(("ctx", "fsdp")),
            P(("ctx", "fsdp"), None),
            P(("ctx", "fsdp")),
            P(("ctx", "fsdp"), None),
            P(("ctx", "fsdp"), None),
            P(("ctx", "fsdp"), None),
        ),
        out_specs=(
            P("fsdp", "ctx", None),
            P("fsdp", "ctx", None),
            P(("ctx", "fsdp")),
            P(("ctx", "fsdp"), None),
            P(("ctx", "fsdp"), None),
            P(("ctx", "fsdp"), None),
            P(("ctx", "fsdp")),
            P(("ctx", "fsdp")),
            P(("ctx", "fsdp"), None),
            P(("ctx", "fsdp")),
            P(("ctx", "fsdp"), None),
            P(("ctx", "fsdp"), None),
            P(("ctx", "fsdp"), None),
        ),
        check_vma=False,
    )
```

```python
import functools
import itertools
import math

import jax
import jax.numpy as jnp
from jax import lax
from jax.experimental import pallas as pl
from jax.experimental.pallas import tpu as pltpu
from jax.sharding import PartitionSpec as P

MESH = pl.DeviceIdType.MESH
ANY = pl.BlockSpec(memory_space=pl.ANY)


H = 16
KVH = 8
HD = 128
BLK = 128


EPSILON = 1e-06
ROPE_BASE = 1000000.0


def rope_tables(positions):
    half = HD // 2
    freqs = jnp.exp(jnp.arange(half, dtype=jnp.float32) * (-2.0 * math.log(ROPE_BASE) / HD))
    angles = positions.astype(jnp.float32)[..., None] * freqs
    cosine = jnp.cos(angles)
    sine = jnp.sin(angles)
    return (jnp.concatenate([cosine, cosine], axis=-1), jnp.concatenate([sine, sine], axis=-1))


def rotate(value_vectors):
    half = value_vectors.shape[-1] // 2
    return jnp.concatenate([-value_vectors[..., half:], value_vectors[..., :half]], axis=-1)


def unrotate(value_vectors):
    half = value_vectors.shape[-1] // 2
    return jnp.concatenate([value_vectors[..., half:], -value_vectors[..., :half]], axis=-1)


def left_dot(left, right):
    return lax.dot_general(
        left, right, (((0,), (0,)), ((), ())), preferred_element_type=jnp.float32
    )


def right_dot(left, right):
    return lax.dot_general(
        left, right, (((1,), (1,)), ((), ())), preferred_element_type=jnp.float32
    )


def plain_dot(left, right):
    return jnp.dot(left, right, preferred_element_type=jnp.float32)


def norm_back(grad_normed, unit, inverse, gain):
    scaled = grad_normed * gain
    return inverse * (scaled - unit * jnp.mean(scaled * unit, axis=-1, keepdims=True))


class Grid:
    def __init__(self, ctx, fsdp):
        self.sizes = {"a": ctx // 4, "b": 2, "core": 2, "f": fsdp}
        self.stride = {"a": 4, "b": 2, "core": 1}

    def enter(self):
        self.c = lax.axis_index("ctx")
        self.at = {
            "a": self.c // 4,
            "b": (self.c // 2) % 2,
            "core": self.c % 2,
            "f": lax.axis_index("fsdp"),
        }

    def barrier(self):
        sem = pltpu.get_barrier_semaphore()
        count = 0
        for axis in ("core", "b", "a", "f"):
            n, p = self.sizes[axis], self.at[axis]
            for step in range(1, n):
                pl.semaphore_signal(
                    sem, inc=1, device_id=self.peer(axis, lax.rem(p + step, n)), device_id_type=MESH
                )
                count += 1
        pl.semaphore_wait(sem, count)

    def peer(self, axis, place):
        if axis == "f":
            return {"fsdp": place}
        return {"ctx": self.c + (place - self.at[axis]) * self.stride[axis]}

    def others(self, axis):
        n, p = self.sizes[axis], self.at[axis]
        return [1 - p] if n == 2 else [lax.rem(p + step, n) for step in range(1, n)]

    def nearest(self, axis):
        return [self.at[axis]] + self.others(axis)


class Pairs:
    def __init__(self, ctx, fsdp):
        self.bits = {"b": ("b",), "core": ("core",)}
        self.stride = {"b": ("ctx", 2), "core": ("ctx", 1)}
        for axis, name, count, unit in (("a", "ctx", ctx // 4, 4), ("f", "fsdp", fsdp, 1)):
            bits = []
            for k in reversed(range(count.bit_length() - 1)):
                bits.append(f"{axis}{k}")
                self.stride[bits[-1]] = (name, unit << k)
            self.bits[axis] = tuple(bits)
        self.sizes = dict.fromkeys(self.stride, 2)

    def axes(self, order):
        return tuple(bit for axis in order for bit in self.bits[axis])

    def shape(self, order):
        return (2,) * len(self.axes(order))

    def enter(self):
        self.index = {"ctx": lax.axis_index("ctx"), "fsdp": lax.axis_index("fsdp")}
        self.at = {}
        for bit, (name, unit) in self.stride.items():
            self.at[bit] = lax.rem(self.index[name] // unit, 2)

    def barrier(self):
        sem = pltpu.get_barrier_semaphore()
        for bit in self.stride:
            pl.semaphore_signal(
                sem, inc=1, device_id=self.peer(bit, 1 - self.at[bit]), device_id_type=MESH
            )
        pl.semaphore_wait(sem, len(self.stride))

    def peer(self, axis, place):
        name, unit = self.stride[axis]
        return {name: self.index[name] + (place - self.at[axis]) * unit}

    def others(self, axis):
        return [1 - self.at[axis]]

    def nearest(self, axis):
        return [self.at[axis], 1 - self.at[axis]]


class Pool:
    def __init__(self, ref):
        self.ref, self.used = ref, 0

    def take(self, count):
        first = self.used
        self.used += count
        return self.ref.at[pl.ds(first, count)]


class Gather:
    def __init__(self, grid, order, src, dst, columns, send_sem, recv_sem, layout_axes):
        self.grid, self.order, self.src, self.dst = grid, order, src, dst
        self.columns, self.send_sem, self.recv_sem = columns, send_sem, recv_sem
        self.layout_axes = layout_axes
        self.pending = []

    @staticmethod
    def semaphores(grid, order):
        near = {x: grid.sizes[x] - 1 for x in order}
        sends, inner = sum(near.values()), 1
        for level in range(1, len(order)):
            axis = order[level]
            sends += inner * near[axis] * sum(near[x] for x in order[level + 1 :])
            inner *= grid.sizes[axis]
        return sends, grid.sizes[order[0]] + inner

    def view(self, places):
        idx = tuple(places.get(x, slice(None)) for x in self.layout_axes)
        return self.dst.at[idx + (slice(None), self.columns)]

    def unit_number(self, places):
        number = 0
        for x in self.order[1:]:
            number = number * self.grid.sizes[x] + places[x]
        return number

    def start(self, source, view, axis, place, sem):
        copy = pltpu.make_async_remote_copy(
            src_ref=source,
            dst_ref=view,
            send_sem=self.send_sem.at[len(self.pending)],
            recv_sem=self.recv_sem.at[sem],
            device_id=self.grid.peer(axis, place),
            device_id_type=MESH,
        )
        copy.start()
        self.pending.append(copy)

    def wait_recv(self, view, sem):
        pltpu.make_async_remote_copy(
            src_ref=view,
            dst_ref=view,
            send_sem=self.send_sem.at[0],
            recv_sem=self.recv_sem.at[sem],
            device_id={},
            device_id_type=MESH,
        ).wait_recv()

    def own_places(self):
        return {x: self.grid.at[x] for x in self.order}

    def open(self):
        axis = self.order[0]
        for place in self.grid.others(axis):
            self.start(self.src, self.view(self.own_places()), axis, place, self.grid.at[axis])

    def first(self):
        axis = self.order[0]
        for origin in self.grid.others(axis):
            self.wait_recv(self.view({**self.own_places(), axis: origin}), origin)
        self.pass_on(1, {x: self.grid.at[x] for x in self.order[1:]})

    def pass_on(self, level, places):
        sem = self.grid.sizes[self.order[0]] + self.unit_number(places)
        view = self.view(places)
        for axis in self.order[level:]:
            for place in self.grid.others(axis):
                self.start(view, view, axis, place, sem)

    def arrivals(self, level):
        n1 = self.grid.sizes[self.order[0]]
        axis = self.order[level]
        inner = [{}]
        for x in self.order[1:level]:
            inner = [{**places, x: j} for places in inner for j in self.grid.nearest(x)]
        fixed = {x: self.grid.at[x] for x in self.order[level + 1 :]}
        for places in inner:
            for origin in self.grid.others(axis):
                unit = {**places, **fixed, axis: origin}
                self.wait_recv(self.view(unit), n1 + self.unit_number(unit))
                self.pass_on(level + 1, unit)

    def close(self):
        for copy in self.pending:
            copy.wait_send()


def add_into(total, terms, out=None):
    shape = total.shape
    rows = min(16, shape[-2])
    steps = shape[-2] // rows
    lead = math.prod(shape[:-2])

    def body(i, carry):
        index = ()
        rest = i // steps
        for n in reversed(shape[:-2]):
            index = (lax.rem(rest, n),) + index
            rest = rest // n
        at = index + (pl.ds(pl.multiple_of(lax.rem(i, steps) * rows, rows), rows), slice(None))
        value = total[at].astype(jnp.float32)
        for term in terms:
            value = value + term[at].astype(jnp.float32)
        if out is None:
            total[at] = value.astype(total.dtype)
        else:
            out[at] = value.astype(out.dtype)
        return carry

    lax.fori_loop(0, lead * steps, body, 0)


class Scatter:
    def __init__(self, grid, order, src, columns, own, recvs, load_sem, send_sem, recv_sem, out, layout_axes):
        self.grid, self.order, self.src, self.columns = grid, order, src, columns
        self.own, self.recvs, self.out = own, recvs, out
        self.load_sem, self.send_sem, self.recv_sem = load_sem, send_sem, recv_sem
        self.layout_axes = layout_axes
        self.pending = []
        self.base = {}
        self.top = len(order) - 1
        number = 0
        for level in range(self.top, -1, -1):
            self.base[level] = number
            number += self.slots(grid, order, level)

    @staticmethod
    def inner(grid, order, level):
        return [grid.sizes[x] for x in order[1:level]]

    @staticmethod
    def slots(grid, order, level):
        return (grid.sizes[order[level]] - 1) * math.prod(Scatter.inner(grid, order, level))

    @staticmethod
    def scratch(grid, order, rows, columns, dtype):
        n1 = grid.sizes[order[0]]
        shapes = [tuple(grid.sizes[x] for x in order[1:-1]) + (n1, rows, columns)]
        for level, axis in enumerate(order):
            block = (rows, columns) if level == 0 else (n1, rows, columns)
            shapes.append((grid.sizes[axis] - 1,) + tuple(Scatter.inner(grid, order, level)) + block)
        return [pltpu.VMEM(x, dtype) for x in shapes]

    @staticmethod
    def semaphores(grid, order):
        loads = math.prod(grid.sizes[x] for x in order[1:-1])
        slots = sum(Scatter.slots(grid, order, level) for level in range(len(order)))
        return loads, slots, slots

    def hbm(self, places):
        idx = tuple(places.get(x, slice(None)) for x in self.layout_axes)
        return self.src.at[idx + (slice(None), self.columns)]

    def units(self, level):
        found = [{}]
        for x in self.order[1:level]:
            found = [{**places, x: j} for places in found for j in reversed(self.grid.nearest(x))]
        return found

    def mine(self, places):
        return self.own.at[tuple(places.get(x, self.grid.at[x]) for x in self.order[1:-1])]

    def number(self, places, axes):
        value = 0
        for x in axes:
            value = value * self.grid.sizes[x] + places[x]
        return value

    def slot(self, level, places, line):
        axes = self.order[1:level]
        number = line * math.prod(self.grid.sizes[x] for x in axes) + self.number(places, axes)
        ref = self.recvs[level].at[(line,) + tuple(places[x] for x in axes)]
        return ref, self.recv_sem.at[self.base[level] + number]

    def send(self, level, places, step, place, view):
        axis = self.order[level]
        ref, sem = self.slot(level, places, self.grid.sizes[axis] - 1 - step)
        copy = pltpu.make_async_remote_copy(
            src_ref=view,
            dst_ref=ref,
            send_sem=self.send_sem.at[len(self.pending)],
            recv_sem=sem,
            device_id=self.grid.peer(axis, place),
            device_id_type=MESH,
        )
        copy.start()
        self.pending.append(copy)

    def take(self, level, places, total, out=None):
        lines = self.grid.sizes[self.order[level]] - 1
        terms = []
        for line in range(lines):
            ref, sem = self.slot(level, places, line)
            pltpu.make_async_remote_copy(
                src_ref=ref,
                dst_ref=ref,
                send_sem=self.send_sem.at[0],
                recv_sem=sem,
                device_id={},
                device_id_type=MESH,
            ).wait_recv()
            terms.append(ref)
        add_into(total, terms, out)

    def load(self, places):
        here = {**places, self.order[-1]: self.grid.at[self.order[-1]]}
        number = self.number(places, self.order[1:-1])
        return pltpu.make_async_copy(self.hbm(here), self.mine(places), self.load_sem.at[number])

    def open(self):
        axis = self.order[self.top]
        for places in self.units(self.top):
            for step, place in enumerate(self.grid.others(axis), 1):
                self.send(self.top, places, step, place, self.hbm({**places, axis: place}))
            self.load(places).start()

    def settle(self, level, places):
        if level + 1 == self.top:
            self.load(places).wait()
        self.take(level + 1, places, self.mine(places))

    def step(self, level):
        axis = self.order[level]
        if level == 0:
            self.settle(0, {})
            for step, place in enumerate(self.grid.others(axis), 1):
                self.send(0, {}, step, place, self.mine({}).at[place])
            return
        for places in self.units(level):
            for step, place in enumerate(self.grid.others(axis), 1):
                unit = {**places, axis: place}
                self.settle(level, unit)
                self.send(level, places, step, place, self.mine(unit))
            self.settle(level, {**places, axis: self.grid.at[axis]})

    def finish(self):
        self.take(0, {}, self.mine({}).at[self.grid.at[self.order[0]]], self.out)

    def close(self):
        for copy in self.pending:
            copy.wait_send()


def half_pairs(ref, s):
    rows = pl.ds(s * BLK, BLK)
    return jnp.concatenate([ref[rows, :HD], ref[rows, HD:]], axis=0)


def read_map(blocks, table, pairs):
    @pl.when(pl.program_id(0) == 0)
    def _():
        for t in range(2 * pairs):
            table[blocks[t]] = t
        place = lax.axis_index("ctx")
        first, second = blocks[2 * place], blocks[2 * place + 1]
        table[2 * pairs] = jnp.where(second > first, 1, 0)
        table[2 * pairs + 1] = jnp.maximum(first, second)


def items(table, pairs):
    high_slot, high = table[pairs * 2], table[pairs * 2 + 1]
    low_block = 2 * pairs - 1 - high
    split = high // 2
    found = []
    for w in range(pairs - 1):
        upper = w < split
        found.append((jnp.where(upper, high_slot, 1 - high_slot), jnp.where(upper, w, w - split), None))
    found.append((high_slot, split, high))
    found.append((1 - high_slot, low_block // 2, low_block))
    return found


def chunk_of(ref, table, c):
    return jnp.concatenate(
        [ref[pl.ds(pl.multiple_of(table[2 * c + i] * BLK, BLK), BLK), :] for i in range(2)], axis=0
    )


def row_contract(left, right):
    return lax.dot_general(left, right, (((1,), (1,)), ((), ())), preferred_element_type=jnp.float32)


def attention_kernel(pairs, blocks, q_ref, k_ref, v_ref, o_ref, low_ref, over_ref, table, qs, acc, tot):
    read_map(blocks, table, pairs)
    for s in range(2):
        qs[s] = half_pairs(q_ref, s)
    acc[...] = jnp.zeros_like(acc)
    tot[...] = jnp.zeros_like(tot)
    for s, c, block in items(table, pairs):
        keys = chunk_of(k_ref, table, c)
        vals = chunk_of(v_ref, table, c)
        scores = row_contract(qs[s], keys) * (HD ** (-0.5) * math.log2(math.e))
        weights = jnp.exp2(scores)
        if block is not None:
            rows = lax.broadcasted_iota(jnp.int32, (2 * BLK, 2 * BLK), 0)
            cols = lax.broadcasted_iota(jnp.int32, (2 * BLK, 2 * BLK), 1)
            allowed = cols <= lax.rem(rows, BLK) + (block - 2 * c) * BLK
            weights = jnp.where(allowed, weights, 0.0)
        tot[s] += weights[:, :HD] + weights[:, HD:]
        acc[s] += jnp.dot(weights.astype(jnp.bfloat16), vals, preferred_element_type=jnp.float32)
    for s in range(2):
        over = 1.0 / jnp.sum(tot[s], axis=1, keepdims=True)
        value = acc[s] * over
        over = jnp.broadcast_to(over, value.shape)
        rows = pl.ds(s * BLK, BLK)
        for i in range(2):
            part = value[i * BLK : (i + 1) * BLK]
            o_ref[rows, i * HD : (i + 1) * HD] = part
            low_ref[rows, i * HD : (i + 1) * HD] = part.astype(jnp.bfloat16)
            over_ref[rows, i * HD : (i + 1) * HD] = over[i * BLK : (i + 1) * BLK]


def attention(blocks, pairs, queries, keys, values):
    rows, length = queries.shape[0], keys.shape[0]
    head = pl.BlockSpec((rows, 2 * HD), lambda h, t: (0, h))
    side = pl.BlockSpec((length, HD), lambda h, t: (0, h))
    return pl.pallas_call(
        functools.partial(attention_kernel, pairs),
        grid_spec=pltpu.PrefetchScalarGridSpec(
            num_scalar_prefetch=1,
            grid=(KVH,),
            in_specs=[head, side, side],
            out_specs=[head, head, head],
            scratch_shapes=[
                pltpu.SMEM((2 * pairs + 2,), jnp.int32),
                pltpu.VMEM((2, 2 * BLK, HD), jnp.bfloat16),
                pltpu.VMEM((2, 2 * BLK, HD), jnp.float32),
                pltpu.VMEM((2, 2 * BLK, HD), jnp.float32),
            ],
        ),
        out_shape=[
            jax.ShapeDtypeStruct((rows, H * HD), jnp.float32),
            jax.ShapeDtypeStruct((rows, H * HD), jnp.bfloat16),
            jax.ShapeDtypeStruct((rows, H * HD), jnp.float32),
        ],
        name="attention",
    )(blocks, queries, keys, values)


def attention_back_kernel(
    pairs, blocks, q_ref, k_ref, v_ref, g_ref, o_ref, dq_ref, dk_ref, dv_ref, table, qs, gs, drift, dq, dk, dv
):
    read_map(blocks, table, pairs)
    scale = HD ** (-0.5)
    for s in range(2):
        qs[s] = half_pairs(q_ref, s)
        gs[s] = half_pairs(g_ref, s)
        products = gs[s].astype(jnp.float32) * half_pairs(o_ref, s)
        drift[s : s + 1, :] = jnp.sum(products.T, axis=0, keepdims=True)
    for total in (dq, dk, dv):
        total[...] = jnp.zeros_like(total)
    for s, c, block in items(table, pairs):
        keys = chunk_of(k_ref, table, c)
        vals = chunk_of(v_ref, table, c)
        queries, grads = qs[s], gs[s]
        weights = jnp.exp2(row_contract(keys, queries) * (scale * math.log2(math.e)))
        if block is not None:
            rows = lax.broadcasted_iota(jnp.int32, (2 * BLK, 2 * BLK), 0)
            cols = lax.broadcasted_iota(jnp.int32, (2 * BLK, 2 * BLK), 1)
            allowed = rows <= lax.rem(cols, BLK) + (block - 2 * c) * BLK
            weights = jnp.where(allowed, weights, 0.0)
        through = row_contract(vals, grads)
        scores = (weights * (through - drift[pl.ds(s, 1), :])).astype(jnp.bfloat16)
        to_values = jnp.dot(weights.astype(jnp.bfloat16), grads, preferred_element_type=jnp.float32)
        to_keys = jnp.dot(scores, queries, preferred_element_type=jnp.float32)
        for i in range(2):
            at = pl.ds(pl.multiple_of(table[2 * c + i] * BLK, BLK), BLK)
            dv[at, :] += to_values[i * BLK : (i + 1) * BLK]
            dk[at, :] += to_keys[i * BLK : (i + 1) * BLK]
        dq[s] += left_dot(scores, keys)
    dk_ref[...] = (dk[...] * scale).astype(jnp.bfloat16)
    dv_ref[...] = dv[...].astype(jnp.bfloat16)
    for s in range(2):
        for i in range(2):
            dq_ref[pl.ds(s * BLK, BLK), i * HD : (i + 1) * HD] = dq[s, i * BLK : (i + 1) * BLK] * scale


def attention_back(blocks, pairs, queries, keys, values, grads, attended):
    rows, length = queries.shape[0], keys.shape[0]
    head = pl.BlockSpec((rows, 2 * HD), lambda h, t: (0, h))
    side = pl.BlockSpec((length, HD), lambda h, t: (0, h))
    return pl.pallas_call(
        functools.partial(attention_back_kernel, pairs),
        grid_spec=pltpu.PrefetchScalarGridSpec(
            num_scalar_prefetch=1,
            grid=(KVH,),
            in_specs=[head, side, side, head, head],
            out_specs=[head, side, side],
            scratch_shapes=[
                pltpu.SMEM((2 * pairs + 2,), jnp.int32),
                pltpu.VMEM((2, 2 * BLK, HD), jnp.bfloat16),
                pltpu.VMEM((2, 2 * BLK, HD), jnp.bfloat16),
                pltpu.VMEM((2, 2 * BLK), jnp.float32),
                pltpu.VMEM((2, 2 * BLK, HD), jnp.float32),
                pltpu.VMEM((length, HD), jnp.float32),
                pltpu.VMEM((length, HD), jnp.float32),
            ],
        ),
        out_shape=[
            jax.ShapeDtypeStruct((rows, H * HD), jnp.float32),
            jax.ShapeDtypeStruct((length, KVH * HD), jnp.bfloat16),
            jax.ShapeDtypeStruct((length, KVH * HD), jnp.bfloat16),
        ],
        cost_estimate=pl.CostEstimate(
            flops=20 * (pairs + 1) * KVH * (2 * BLK) ** 2 * HD,
            bytes_accessed=14 * rows * H * HD + 8 * length * KVH * HD,
            transcendentals=(pairs + 1) * KVH * (2 * BLK) ** 2,
        ),
        name="attention_back",
    )(blocks, queries, keys, values, grads, attended)


ALL_AXES = ("a", "b", "core", "f")
SLOT_AXES = ("a", "b", "core")
CHIP_AXES = ("a", "b", "f")
BFA, AFB, FAB, FBA = ("b", "f", "a"), ("a", "f", "b"), ("f", "a", "b"), ("f", "b", "a")
ABF, BAF = ("a", "b", "f"), ("b", "a", "f")
AB, BA = ("a", "b", "core"), ("b", "a", "core")
CORE = ("core",)


PUMP = (6, 1, 2, 2)
FRONT_SRC = ("q", "k", "v", "o", "g", "u", "d", "gains")


def front_kernel(grid, plan, pieces, *refs):
    n = len(FRONT_SRC)
    src = dict(zip(FRONT_SRC, refs[:n]))
    tokens_ref, cosine_ref, sine_ref = refs[n : n + 3]
    rows_of = refs[n - 1]
    outs = refs[n + 3 : n + 15]
    wqkv_ref, wo_ref, wgu_ref, wd_ref, allgains_ref, k_out, v_out = outs[:7]
    normed_ref, gains_ref, raw_ref, qlow_ref, inv_ref = outs[7:]
    scratch = refs[n + 15 :]
    held = dict(zip(FRONT_SRC, scratch[:n]))
    weights, klow, vlow, gbuf, gmine = scratch[n : n + 5]
    send, recv, local, load = scratch[n + 5 :]
    grid.enter()
    grid.barrier()
    send, recv = Pool(send), Pool(recv)
    device = grid.index["ctx"] * 2 ** len(grid.bits["f"]) + grid.index["fsdp"]
    block_rows = lax.broadcasted_iota(jnp.int32, gmine.shape, 0)
    block = jnp.zeros(gmine.shape, jnp.float32)
    for i, (at, size) in enumerate(pieces):
        spot = at + device * size
        line = jnp.broadcast_to(rows_of[i : i + 1, :], (8, 128))
        line = pltpu.roll(line, lax.rem(spot, 128), 1)[:1]
        block = jnp.where(block_rows == spot // 128, line, block)
    gmine[...] = block.astype(gmine.dtype)
    copy = pltpu.make_async_copy(gmine, held["gains"], local.at[n - 1])
    copy.start()
    copy.wait()
    src["gains"] = held["gains"]
    width = tokens_ref.shape[1]
    rows = tokens_ref.shape[0]
    spans = {"q": (wqkv_ref, 0), "k": (wqkv_ref, H * HD), "v": (wqkv_ref, (H + KVH) * HD)}
    hidden = src["g"].shape[1]
    spans.update({"o": (wo_ref, 0), "g": (wgu_ref, 0), "u": (wgu_ref, hidden), "d": (wd_ref, 0)})
    spans["gains"] = (allgains_ref, 0)
    mine = tuple(grid.at[x] for x in grid.axes(ALL_AXES))

    def own_copy(i, name):
        dst, at = spans[name]
        return pltpu.make_async_copy(
            held[name], dst.at[mine + (slice(None), pl.ds(at, src[name].shape[1]))], local.at[i]
        )

    for i, name in enumerate(FRONT_SRC[:-1]):
        pltpu.make_async_copy(src[name], held[name], local.at[i]).start()

    def part(name, low, high, order):
        dst, at = spans[name]
        order = grid.axes(order)
        sends, takes = Gather.semaphores(grid, order)
        columns = pl.ds(at + low, high - low)
        return Gather(
            grid, order, src[name].at[:, low:high], dst, columns, send.take(sends), recv.take(takes),
            grid.axes(ALL_AXES),
        )

    early = [part(*p) for p in plan[0]]
    late = [part(*p) for p in plan[1]]
    for p in early:
        p.open()
    for p in late:
        p.open()
    for i, name in enumerate(FRONT_SRC):
        if name != "gains":
            pltpu.make_async_copy(src[name], held[name], local.at[i]).wait()
        own_copy(i, name).start()
    inputs = tokens_ref[...].astype(jnp.float32)
    inverse = lax.rsqrt(jnp.mean(inputs * inputs, axis=-1, keepdims=True) + EPSILON)
    inv_ref[...] = jnp.broadcast_to(inverse, (rows, 128))
    for i, name in enumerate(FRONT_SRC):
        own_copy(i, name).wait()

    for p in early:
        p.first()
    levels = len(early[0].order)
    for level in range(1, levels - 1):
        for p in early:
            p.arrivals(level)
    pump = []
    for p in late:
        pump.append(p.first)
    for level in range(1, levels):
        for p in late:
            pump.append(functools.partial(p.arrivals, level))

    def step(count):
        for _ in range(count):
            if pump:
                pump.pop(0)()

    step(PUMP[0])
    for p in early:
        p.arrivals(levels - 1)

    places = math.prod(grid.shape(ALL_AXES))
    copy = pltpu.make_async_copy(allgains_ref, gbuf, load.at[0])
    copy.start()
    big = pltpu.make_async_copy(wqkv_ref, weights, load.at[1])
    big.start()
    copy.wait()
    blocks = gbuf[...].reshape((places,) + gbuf.shape[-2:]).astype(jnp.float32)
    gains = jnp.sum(blocks, axis=0)
    gains_ref[...] = gains
    lanes = width // 128
    for j in range(lanes):
        cols = slice(j * 128, (j + 1) * 128)
        part_of = tokens_ref[:, cols].astype(jnp.float32) * inv_ref[...] * gains_ref[j : j + 1, :]
        normed_ref[:, cols] = part_of.astype(jnp.bfloat16)
    big.wait()
    step(PUMP[1])
    flat = weights.reshape(width, weights.shape[-1])
    normed = normed_ref[...]
    chunk = 2 * HD

    def heads(low_out, gain_row, out_at, raw_at, c):
        at = pl.ds(pl.multiple_of(raw_at + c * chunk, chunk), chunk)
        raw = jnp.dot(normed, flat[:, at], preferred_element_type=jnp.float32)
        raw_ref[:, at] = raw
        done = []
        for i in range(2):
            one = raw[:, i * HD : (i + 1) * HD]
            unit = one * lax.rsqrt(jnp.mean(one * one, axis=-1, keepdims=True) + EPSILON)
            unit = unit * gains_ref[gain_row : gain_row + 1, :]
            done.append(unit * cosine_ref[...] + pltpu.roll(unit, HD // 2, 1) * sine_ref[...])
        to = pl.ds(pl.multiple_of(out_at + c * chunk, chunk), chunk)
        low_out[:, to] = jnp.concatenate(done, axis=1).astype(jnp.bfloat16)

    def loop(count, body):
        def once(c, carry):
            body(c)
            return carry

        lax.fori_loop(0, count, once, 0)

    def to_values(c):
        at = pl.ds(pl.multiple_of((H + KVH) * HD + c * chunk, chunk), chunk)
        to = pl.ds(pl.multiple_of(c * chunk, chunk), chunk)
        raw = jnp.dot(normed, flat[:, at], preferred_element_type=jnp.float32)
        vlow[:, to] = raw.astype(jnp.bfloat16)

    loop(KVH // 2, functools.partial(heads, klow, 2 * lanes + 1, 0, H * HD))
    loop(KVH // 2, to_values)

    def pair(source, dst, order):
        order = grid.axes(order)
        sends, takes = Gather.semaphores(grid, order)
        return Gather(
            grid, order, source, dst, pl.ds(0, KVH * HD), send.take(sends), recv.take(takes),
            grid.axes(SLOT_AXES),
        )

    slot = tuple(grid.at[x] for x in grid.axes(SLOT_AXES))
    slabs = [pair(klow, k_out, AB), pair(vlow, v_out, BA)]
    saves = [
        pltpu.make_async_copy(klow, k_out.at[slot], load.at[0]),
        pltpu.make_async_copy(vlow, v_out.at[slot], load.at[1]),
    ]
    for p, save in zip(slabs, saves):
        p.open()
        save.start()
    step(PUMP[2])
    loop(KVH // 2, functools.partial(heads, qlow_ref, 2 * lanes, 0, 0))
    for p, save in zip(slabs, saves):
        save.wait()
        p.first()
    step(PUMP[3])
    loop(KVH // 2, functools.partial(heads, qlow_ref, 2 * lanes, H * HD // 2, H * HD // 2))
    depth = len(slabs[0].order)
    for level in range(1, depth - 1):
        for p in slabs:
            p.arrivals(level)
    step(len(pump))
    for p in slabs:
        p.arrivals(depth - 1)
    for p in early + late + slabs:
        p.close()


def front(grid, plan, pieces, blocks, gain_rows, tokens, cosine, sine):
    n = len(FRONT_SRC)
    rows, width = tokens.shape
    places = grid.shape(ALL_AXES)
    slots = grid.shape(SLOT_AXES)
    gains = jax.ShapeDtypeStruct((width // 128 * 2 + 16, 128), jnp.bfloat16)
    blocks = tuple(blocks) + (gains,)
    by = dict(zip(FRONT_SRC, blocks))
    low, f32 = jnp.bfloat16, jnp.float32
    full = (H + 2 * KVH) * HD
    counts = [Gather.semaphores(grid, grid.axes(p[3])) for p in plan[0] + plan[1]]
    counts += [Gather.semaphores(grid, grid.axes(x)) for x in (AB, BA)]
    sends, takes = [sum(x) for x in zip(*counts)]
    shape = jax.ShapeDtypeStruct
    vmem = pl.BlockSpec(memory_space=pltpu.VMEM)
    outs = pl.pallas_call(
        functools.partial(front_kernel, grid, plan, pieces),
        out_shape=[
            shape(places + (by["q"].shape[0], full), low),
            shape(places + by["o"].shape, low),
            shape(places + (by["g"].shape[0], 2 * by["g"].shape[1]), low),
            shape(places + by["d"].shape, low),
            shape(places + by["gains"].shape, low),
            shape(slots + (rows, KVH * HD), low),
            shape(slots + (rows, KVH * HD), low),
            shape((rows, width), low),
            shape(by["gains"].shape, f32),
            shape((rows, (H + KVH) * HD), f32),
            shape((rows, H * HD), low),
            shape((rows, 128), f32),
        ],
        in_specs=[ANY] * (n - 1) + [vmem] * 4,
        out_specs=[ANY] * 7 + [vmem] * 5,
        scratch_shapes=[pltpu.VMEM(x.shape, x.dtype) for x in blocks]
        + [
            pltpu.VMEM(places + (by["q"].shape[0], full), low),
            pltpu.VMEM((rows, KVH * HD), low),
            pltpu.VMEM((rows, KVH * HD), low),
            pltpu.VMEM(places + by["gains"].shape, low),
            pltpu.VMEM(by["gains"].shape, low),
            pltpu.SemaphoreType.DMA((sends,)),
            pltpu.SemaphoreType.DMA((takes,)),
            pltpu.SemaphoreType.DMA((n,)),
            pltpu.SemaphoreType.DMA((2,)),
        ],
        compiler_params=pltpu.CompilerParams(
            has_side_effects=True, vmem_limit_bytes=60 * 2**20, collective_id=0
        ),
        name="front",
    )(*blocks[:-1], gain_rows, tokens, cosine, sine)
    wqkv, wo, wgu, wd, _, keys, vals, normed, gains, raw, qlow, inverse = outs
    flat = [x.reshape(-1, x.shape[-1]) for x in (wqkv, wo, wgu, wd, keys, vals)]
    return flat + [normed, gains, raw, qlow, inverse]


def sums_kernel(count, n, core, left, left_other, *refs):
    rights, outs, turned = refs[: 2 * n], refs[2 * n : 3 * n], refs[-1]
    rows, width = left.shape
    block = width // count

    @pl.when(pl.program_id(0) == 0)
    def _():
        for j in range(count // 2):
            at = pl.ds(pl.multiple_of((2 * j + core[0]) * block, block), block)
            for k, ref in enumerate((left, left_other)):
                turned[j * block : (j + 1) * block, k * rows : (k + 1) * rows] = ref[:, at].T

    for k, out in enumerate(outs):
        rhs = jnp.concatenate([rights[2 * k][...], rights[2 * k + 1][...]], axis=0)
        out[...] = jnp.dot(turned[...], rhs, preferred_element_type=jnp.float32).astype(out.dtype)


def chip_sums(left, left_other, *rights):
    rows, width = left.shape
    count = lax.axis_size("ctx")
    block = width // count
    tile = 512
    if block % 128:
        place = lax.axis_index("ctx") % 2
        halves = [
            lax.dynamic_index_in_dim(x.reshape(rows, count // 2, 2, block), place, 2, False)
            for x in (left, left_other)
        ]
        lhs = jnp.concatenate(halves, axis=0).reshape(2 * rows, width // 2)
        return [
            left_dot(lhs, jnp.concatenate(rights[k : k + 2], axis=0)).astype(jnp.bfloat16)
            for k in range(0, len(rights), 2)
        ]
    core = (lax.axis_index("ctx") % 2).astype(jnp.int32)[None]
    n, columns = len(rights) // 2, rights[0].shape[1]
    lhs = pl.BlockSpec((rows, width), lambda n, c: (0, 0))
    rhs = pl.BlockSpec((rows, tile), lambda n, c: (0, n))
    return pl.pallas_call(
        functools.partial(sums_kernel, count, n),
        grid_spec=pltpu.PrefetchScalarGridSpec(
            num_scalar_prefetch=1,
            grid=(columns // tile,),
            in_specs=[lhs, lhs] + [rhs] * (2 * n),
            out_specs=[pl.BlockSpec((width // 2, tile), lambda n, c: (0, n))] * n,
            scratch_shapes=[pltpu.VMEM((width // 2, 2 * rows), jnp.bfloat16)],
        ),
        out_shape=[jax.ShapeDtypeStruct((width // 2, columns), jnp.bfloat16)] * n,
        name="chip_sums",
    )(core, left, left_other, *rights)


def handed_kernel(pieces, count, sums_ref, *refs):
    results, outs = refs[: (len(refs) - len(pieces)) // 2], refs[(len(refs) - len(pieces)) // 2 :]
    for source, out in zip(results, outs):
        out[...] = source[...]
    device = lax.axis_index("ctx") * count + lax.axis_index("fsdp")
    for (at, size), out in zip(pieces, outs[len(results) :]):
        spot = at + device * size
        line = jnp.broadcast_to(sums_ref[pl.ds(spot // 128, 1), :], (8, 128))
        line = pltpu.roll(line, lax.rem(128 - lax.rem(spot, 128), 128), 1)
        out[...] = line[:1, :size]


def handed(pieces, sums, *results):
    vmem = pl.BlockSpec(memory_space=pltpu.VMEM)
    return pl.pallas_call(
        functools.partial(handed_kernel, pieces, lax.axis_size("fsdp")),
        out_shape=[jax.ShapeDtypeStruct(x.shape, x.dtype) for x in results]
        + [jax.ShapeDtypeStruct((1, size), jnp.float32) for _, size in pieces],
        in_specs=[vmem] * (1 + len(results)),
        out_specs=[vmem] * (len(results) + len(pieces)),
        name="handed",
    )(sums, *results)


BACK_SUMS = ("g", "u", "d", "o")


def back_kernel(grid, plan, *refs):
    refs = list(refs)

    def take(n):
        found = refs[:n]
        del refs[:n]
        return found

    src = dict(zip(BACK_SUMS, take(len(BACK_SUMS))))
    gk_ref, gv_ref, wqkv_ref = take(3)
    dq_ref, raw_ref, cos_ref, turn_ref, gains_ref, normed_ref, tokens_ref, inv_ref, mid_ref, gain2_ref = take(10)
    outs = dict(zip(BACK_SUMS + ("q", "k", "v"), take(len(BACK_SUMS) + 3)))
    din_ref, gsum_ref, sums_ref, gall_ref = take(4)
    weights, both_normed, both_raw, own_k, own_v, stage, acc, gbuf, gblock = take(9)
    load, send, recv, misc = [Pool(x) for x in refs[-4:]]
    del refs[-4:]
    scratch = refs
    grid.enter()
    grid.barrier()
    rows, width = tokens_ref.shape
    lanes = width // 128
    core = grid.at["core"]
    chunk = 2 * HD
    misc_sem = [misc.take(1).at[0] for _ in range(12)]

    def make(source, columns, order, out, layout):
        loads, sends, takes = Scatter.semaphores(grid, order)
        own, *recvs = scratch[: 1 + len(order)]
        del scratch[: 1 + len(order)]
        return Scatter(
            grid, order, source, columns, own, recvs,
            load.take(loads), send.take(sends), recv.take(takes), out, layout,
        )

    def portions(group):
        found = []
        for name, low, high, order in group:
            found.append(
                make(src[name], pl.ds(low, high - low), order, outs[name].at[:, low:high], CHIP_AXES)
            )
        return found

    slabs = [
        make(gk_ref, pl.ds(0, KVH * HD), AB, own_k, SLOT_AXES),
        make(gv_ref, pl.ds(0, KVH * HD), BA, own_v, SLOT_AXES),
    ]
    early, waves = portions(plan[0]), [portions(group) for group in plan[1]]
    late = [p for wave in waves for p in wave]
    last = []
    for name, at, low, high, order in plan[2]:
        last.append(
            make(sums_ref, pl.ds(at + low, high - low), order, outs[name].at[:, low:high], CHIP_AXES)
        )

    def sibling(source, dst, k):
        return pltpu.make_async_remote_copy(
            src_ref=source, dst_ref=dst, send_sem=misc_sem[2 * k], recv_sem=misc_sem[2 * k + 1],
            device_id=grid.peer("core", 1 - core), device_id_type=MESH,
        )

    for p in slabs + early:
        p.open()
    swap_normed = sibling(normed_ref, both_normed.at[1], 0)
    swap_normed.start()
    both_normed[0] = normed_ref[...]
    gblock[...] = jnp.zeros_like(gblock)
    gblock[lanes : 2 * lanes, :] = gain2_ref[...]

    def loop(count, body):
        def once(c, carry):
            body(c)
            return carry

        lax.fori_loop(0, count, once, 0)

    def heads(source, in_at, raw_at, gain_row, c):
        at = pl.ds(pl.multiple_of(raw_at + c * chunk, chunk), chunk)
        grads = source[:, pl.ds(pl.multiple_of(in_at + c * chunk, chunk), chunk)]
        raw = raw_ref[:, at]
        gain = gains_ref[gain_row : gain_row + 1, :]
        done = []
        for i in range(2):
            g = grads[:, i * HD : (i + 1) * HD]
            g = g * cos_ref[...] - pltpu.roll(g, HD // 2, 1) * turn_ref[...]
            one = raw[:, i * HD : (i + 1) * HD]
            inverse = lax.rsqrt(jnp.mean(one * one, axis=-1, keepdims=True) + EPSILON)
            unit = one * inverse
            gblock[gain_row : gain_row + 1, :] += jnp.sum(g * unit, axis=0, keepdims=True)
            done.append(norm_back(g, unit, inverse, gain))
        both_raw[0, :, at] = jnp.concatenate(done, axis=1).astype(jnp.bfloat16)

    half_q = H * HD // 2
    q_cols, kv_cols = pl.ds(0, H * HD), pl.ds(H * HD, 2 * KVH * HD)
    loop(H // 4, functools.partial(heads, dq_ref, 0, 0, 2 * lanes))
    for p in slabs:
        p.step(1)
    loop(H // 4, functools.partial(heads, dq_ref, half_q, half_q, 2 * lanes))
    swap_q = sibling(both_raw.at[0, :, q_cols], both_raw.at[1, :, q_cols], 1)
    swap_q.start()
    for p in slabs:
        p.step(0)
    def every(group, what, *args):
        for p in group:
            getattr(p, what)(*args)

    every(waves[0], "open")
    for p in slabs:
        p.finish()
    loop(KVH // 2, functools.partial(heads, own_k, 0, H * HD, 2 * lanes + 1))
    at = (H + KVH) * HD
    both_raw[0, :, at : at + KVH * HD] = own_v[...].astype(jnp.bfloat16)
    swap_kv = sibling(both_raw.at[0, :, kv_cols], both_raw.at[1, :, kv_cols], 2)
    swap_kv.start()
    every(waves[1], "open")
    swap_normed.wait()
    swap_q.wait()
    swap_kv.wait()
    flat_normed = both_normed.reshape(2 * rows, width)
    flat_raw = both_raw.reshape(2 * rows, both_raw.shape[-1])
    count = grid.sizes["a"] * grid.sizes["b"]
    block = width // (2 * count)
    piece = block // grid.sizes["f"]
    full = both_raw.shape[-1]
    tile = 512

    def stored(j):
        return pltpu.make_async_copy(stage.at[j % 2], sums_ref.at[j // 2, j % 2], misc_sem[9 + j % 2])

    for j in range(count):
        if j >= 2:
            stored(j - 2).wait()
        lhs = flat_normed[:, pl.ds(pl.multiple_of((2 * j + core) * block, block), block)]

        def sums(c):
            cols = pl.ds(pl.multiple_of(c * tile, tile), tile)
            value = left_dot(lhs, flat_raw[:, cols]).astype(jnp.bfloat16)
            stage[j % 2, :, :, cols] = value.reshape(grid.sizes["f"], piece, tile)

        loop(full // tile, sums)
        stored(j).start()
    for j in range(count - 2, count):
        stored(j).wait()
    every(waves[0], "step", 1)
    every(last, "open")
    every(waves[2], "open")
    every(early, "step", 1)
    every(waves[1], "step", 1)
    every(waves[0], "step", 0)
    tiles = [
        pltpu.make_async_copy(
            wqkv_ref.at[:, c * tile : (c + 1) * tile], weights.at[c % 2], misc_sem[6 + c % 2]
        )
        for c in range(full // tile)
    ]
    tiles[0].start()
    for c in range(full // tile):
        if c + 1 < full // tile:
            tiles[c + 1].start()
        tiles[c].wait()
        value = right_dot(both_raw[0, :, c * tile : (c + 1) * tile], weights[c % 2])
        acc[...] = value if c == 0 else acc[...] + value
    inverse = inv_ref[...]
    for j in range(lanes):
        cols = slice(j * 128, (j + 1) * 128)
        normal = tokens_ref[:, cols].astype(jnp.float32) * inverse
        gblock[j : j + 1, :] = jnp.sum(acc[:, cols] * normal, axis=0, keepdims=True)
    copy = pltpu.make_async_copy(gblock, gbuf, misc_sem[11])
    copy.start()
    copy.wait()
    order = FAB + CORE
    sends, takes = Gather.semaphores(grid, order)
    spread = Gather(
        grid, order, gbuf, gall_ref, slice(None), send.take(sends), recv.take(takes), ALL_AXES
    )
    spread.open()
    mine = tuple(grid.at[x] for x in ALL_AXES)
    gall_ref[mine] = gblock[...]
    every(early, "step", 0)
    every(last, "step", 1)
    every(waves[2], "step", 1)
    every(waves[1], "step", 0)
    spread.first()
    dots = jnp.zeros((rows, 1), jnp.float32)
    for j in range(lanes):
        cols = slice(j * 128, (j + 1) * 128)
        normal = tokens_ref[:, cols].astype(jnp.float32) * inverse
        dots += jnp.sum(acc[:, cols] * gains_ref[j : j + 1, :] * normal, axis=1, keepdims=True)
    dots = dots / width
    for j in range(lanes):
        cols = slice(j * 128, (j + 1) * 128)
        normal = tokens_ref[:, cols].astype(jnp.float32) * inverse
        grad = inverse * (acc[:, cols] * gains_ref[j : j + 1, :] - normal * dots)
        din_ref[:, cols] = (mid_ref[:, cols] + grad).astype(jnp.bfloat16)
    spread.arrivals(1)
    every(last, "step", 0)
    every(waves[2], "step", 0)
    spread.arrivals(2)
    every(waves[0] + early + waves[1], "finish")
    spread.arrivals(3)
    every(last + waves[2], "finish")
    places = math.prod(grid.sizes[x] for x in ALL_AXES)
    gsum_ref[...] = jnp.sum(gall_ref.reshape((places,) + gblock.shape)[...], axis=0)
    for p in slabs + early + late + last:
        p.close()
    spread.close()


def back_scratch(grid, plan, pieces, rows, width):
    low = jnp.bfloat16
    scratch, counts = [], []
    for order in (AB, BA):
        scratch += Scatter.scratch(grid, order, rows, KVH * HD, low)
        counts.append(Scatter.semaphores(grid, order))
    for name, begin, end, order in plan[0] + sum(plan[1], ()) + tuple((p[0],) + p[2:] for p in plan[2]):
        scratch += Scatter.scratch(grid, order, pieces[name], end - begin, low)
        counts.append(Scatter.semaphores(grid, order))
    return scratch, [sum(x) for x in zip(*counts)]


def back_fits(grid, plan, rows, width, hidden, total):
    pieces = {name: width // total for name in ("g", "u", "q", "k", "v")}
    pieces.update({"d": hidden // total, "o": H * HD // total})
    scratch = back_scratch(grid, plan, pieces, rows, width)[0]
    taken = sum(2 * math.prod(x.shape) for x in scratch)
    held = 2 * rows * (11 * width + 3 * (H + 2 * KVH) * HD + 4 * (H + KVH) * HD) + 6 * 2**20
    return taken + held < 62 * 2**20


def back(grid, plan, sums, gk, gv, wqkv, dq, raw, cosine, turned, gains, normed, tokens, inverse, middle, gain2):
    low, f32 = jnp.bfloat16, jnp.float32
    rows, width = tokens.shape
    chips = tuple(grid.sizes[x] for x in CHIP_AXES)
    places = tuple(grid.sizes[x] for x in ALL_AXES)
    slots = tuple(grid.sizes[x] for x in SLOT_AXES)
    blocks = [x.reshape(chips + (x.shape[0] // math.prod(chips), x.shape[1])) for x in sums]
    shape = jax.ShapeDtypeStruct
    vmem = pl.BlockSpec(memory_space=pltpu.VMEM)
    piece = width // math.prod(places)
    pieces = dict(zip(BACK_SUMS, [x.shape[-2] for x in blocks]))
    pieces.update({"q": piece, "k": piece, "v": piece})
    scratch, (loads, sends, takes) = back_scratch(grid, plan, pieces, rows, width)
    more = Gather.semaphores(grid, FAB + CORE)
    full = wqkv.shape[1]
    count = grid.sizes["a"] * grid.sizes["b"]
    outs = pl.pallas_call(
        functools.partial(back_kernel, grid, plan),
        out_shape=[shape(x.shape[-2:], f32) for x in blocks]
        + [shape((piece, n), f32) for n in (H * HD, KVH * HD, KVH * HD)]
        + [
            shape((rows, width), low),
            shape(gains.shape, f32),
            shape(chips + (piece, full), low),
        ],
        in_specs=[ANY] * (len(blocks) + 3) + [vmem] * 10,
        out_specs=[vmem] * (len(blocks) + 5) + [ANY],
        scratch_shapes=[
            pltpu.VMEM(places + gains.shape, f32),
            pltpu.VMEM((2, width, 512), low),
            pltpu.VMEM((2, rows, width), low),
            pltpu.VMEM((2, rows, full), low),
            pltpu.VMEM((rows, KVH * HD), f32),
            pltpu.VMEM((rows, KVH * HD), f32),
            pltpu.VMEM((2, grid.sizes["f"], piece, full), low),
            pltpu.VMEM((rows, width), f32),
            pltpu.VMEM(gains.shape, f32),
            pltpu.VMEM(gains.shape, f32),
        ]
        + scratch
        + [
            pltpu.SemaphoreType.DMA((loads,)),
            pltpu.SemaphoreType.DMA((sends + more[0],)),
            pltpu.SemaphoreType.DMA((takes + more[1],)),
            pltpu.SemaphoreType.DMA((12,)),
        ],
        compiler_params=pltpu.CompilerParams(
            has_side_effects=True, vmem_limit_bytes=63 * 2**20, collective_id=1
        ),
        name="back",
    )(
        *blocks,
        gk.reshape(slots + (rows, KVH * HD)),
        gv.reshape(slots + (rows, KVH * HD)),
        wqkv, dq, raw, cosine, turned, gains, normed, tokens, inverse, middle, gain2,
    )
    return outs


def middle_kernel(
    steps, alow_ref, over_ref, wo_ref, wg_ref, wu_ref, wd_ref, tokens_ref, cot_ref, gains_ref,
    out_ref, hidden_ref, gg_ref, gu_ref, normed_ref, mid_ref, branch_ref, gain_ref, gs_ref,
    middle, total, back, inv,
):
    c = pl.program_id(0)
    rows, width = tokens_ref.shape
    lanes = width // 128
    low = jnp.bfloat16

    @pl.when(c == 0)
    def _():
        value = tokens_ref[...].astype(jnp.float32) + plain_dot(alow_ref[...], wo_ref[...])
        inverse = lax.rsqrt(jnp.mean(value * value, axis=-1, keepdims=True) + EPSILON)
        inv[...] = jnp.broadcast_to(inverse, inv.shape)
        middle[...] = value
        total[...] = value
        for j in range(lanes):
            cols = slice(j * 128, (j + 1) * 128)
            gain = gains_ref[lanes + j : lanes + j + 1, :]
            normed_ref[:, cols] = (middle[:, cols] * inv[...] * gain).astype(low)
        back[...] = jnp.zeros_like(back)

    normed = normed_ref[...]
    gate = plain_dot(normed, wg_ref[...])
    upper = plain_dot(normed, wu_ref[...])
    grads = right_dot(cot_ref[...], wd_ref[...])
    sig = jax.nn.sigmoid(gate)
    activated = gate * sig
    hidden = (activated * upper).astype(low)
    grad_gate = (grads * upper * sig * (1.0 + gate * (1.0 - sig))).astype(low)
    grad_upper = (grads * activated).astype(low)
    hidden_ref[...] = hidden
    gg_ref[...] = grad_gate
    gu_ref[...] = grad_upper
    total[...] += plain_dot(hidden, wd_ref[...])
    back[...] += right_dot(grad_gate, wg_ref[...]) + right_dot(grad_upper, wu_ref[...])

    @pl.when(c == steps - 1)
    def _():
        out_ref[...] = total[...].astype(low)
        inverse = inv[...]
        dots = jnp.zeros((rows, 1), jnp.float32)
        for j in range(lanes):
            cols = slice(j * 128, (j + 1) * 128)
            normal = middle[:, cols] * inverse
            gain_ref[j : j + 1, :] = jnp.sum(back[:, cols] * normal, axis=0, keepdims=True)
            gain = gains_ref[lanes + j : lanes + j + 1, :]
            dots += jnp.sum(back[:, cols] * gain * normal, axis=1, keepdims=True)
        dots = dots / width
        for j in range(lanes):
            cols = slice(j * 128, (j + 1) * 128)
            gain = gains_ref[lanes + j : lanes + j + 1, :]
            normal = middle[:, cols] * inverse
            grad = cot_ref[:, cols].astype(jnp.float32) + inverse * (back[:, cols] * gain - normal * dots)
            mid_ref[:, cols] = grad
            branch_ref[:, cols] = grad.astype(low)
        tile = 512
        for j in range(gs_ref.shape[1] // tile):
            cols = slice(j * tile, (j + 1) * tile)
            attended = right_dot(branch_ref[...], wo_ref[cols, :])
            gs_ref[:, cols] = (attended * over_ref[:, cols]).astype(low)


def middle_part(alow, over, wo, wgu, wd, tokens, cotangent, gains):
    low, f32 = jnp.bfloat16, jnp.float32
    rows, width = tokens.shape
    hidden = wd.shape[0]
    tile = 512
    steps = hidden // tile
    shape = jax.ShapeDtypeStruct

    def whole(x):
        return pl.BlockSpec(x.shape, lambda c: (0,) * len(x.shape))

    def columns(at):
        return pl.BlockSpec((width, tile), lambda c: (0, at + c))

    chunk = pl.BlockSpec((rows, tile), lambda c: (0, c))
    outs = [
        shape((rows, width), low),
        shape((rows, hidden), low),
        shape((rows, hidden), low),
        shape((rows, hidden), low),
        shape((rows, width), low),
        shape((rows, width), f32),
        shape((rows, width), low),
        shape((width // 128, 128), f32),
        shape(alow.shape, low),
    ]
    return pl.pallas_call(
        functools.partial(middle_kernel, steps),
        grid=(steps,),
        in_specs=[
            whole(alow),
            whole(over),
            whole(wo),
            columns(0),
            columns(steps),
            pl.BlockSpec((tile, width), lambda c: (c, 0)),
            whole(tokens),
            whole(cotangent),
            whole(gains),
        ],
        out_specs=[whole(outs[0])] + [chunk] * 3 + [whole(x) for x in outs[4:]],
        out_shape=outs,
        scratch_shapes=[pltpu.VMEM((rows, width), f32)] * 3 + [pltpu.VMEM((rows, 128), f32)],
        compiler_params=pltpu.CompilerParams(vmem_limit_bytes=60 * 2**20),
        name="middle",
    )(alow, over, wo, wgu, wgu, wd, tokens, cotangent, gains)


def scatter_kernel(grid, portions, layouts, n, *refs):
    srcs, outs, scratch = refs[:n], refs[n : 2 * n], list(refs[2 * n : -3])
    load, send, recv = [Pool(x) for x in refs[-3:]]
    grid.enter()
    parts = []
    for i, low, high, order in portions:
        loads, sends, takes = Scatter.semaphores(grid, order)
        own, *recvs = scratch[: 1 + len(order)]
        del scratch[: 1 + len(order)]
        parts.append(
            Scatter(
                grid,
                order,
                srcs[i],
                pl.ds(low, high - low),
                own,
                recvs,
                load.take(loads),
                send.take(sends),
                recv.take(takes),
                outs[i].at[:, low:high],
                layouts[i],
            )
        )
        parts[-1].open()
    for level in (2, 1, 0):
        for part in parts:
            if level < part.top:
                part.step(level)
    for part in parts:
        part.finish()
    for part in parts:
        part.close()


def scatter(grid, layouts, portions, name, dtypes, *sums):
    n = len(sums)
    blocks = []
    for layout, x in zip(layouts, sums):
        places = tuple(grid.sizes[axis] for axis in layout)
        blocks.append(x.reshape(places + (x.shape[0] // math.prod(places), x.shape[1])))
    loads, sends, takes = [sum(x) for x in zip(*[Scatter.semaphores(grid, p[3]) for p in portions])]
    scratch = []
    for i, low, high, order in portions:
        scratch += Scatter.scratch(grid, order, blocks[i].shape[-2], high - low, blocks[i].dtype)
    return pl.pallas_call(
        functools.partial(scatter_kernel, grid, portions, layouts, n),
        out_shape=[jax.ShapeDtypeStruct(x.shape[-2:], t) for x, t in zip(blocks, dtypes)],
        in_specs=[ANY] * n,
        out_specs=[pl.BlockSpec(memory_space=pltpu.VMEM)] * n,
        scratch_shapes=scratch
        + [
            pltpu.SemaphoreType.DMA((loads,)),
            pltpu.SemaphoreType.DMA((sends,)),
            pltpu.SemaphoreType.DMA((takes,)),
        ],
        compiler_params=pltpu.CompilerParams(has_side_effects=True, vmem_limit_bytes=60 * 2**20),
        name=name,
    )(*blocks)


def gain_rows(total, *gains):
    pieces = [x.reshape(total, 1, -1) for x in gains]
    pieces = [jnp.pad(x, ((0, 0), (0, 0), (0, 128 - x.shape[2]))) for x in pieces]
    block = jnp.concatenate(pieces, axis=1)
    return jnp.pad(block, ((0, 0), (0, 8 - len(gains)), (0, 0))).reshape(total * 8, 128)


def swapped(x):
    count = lax.axis_size("ctx")
    return lax.ppermute(x, "ctx", [(i, i ^ 1) for i in range(count)])


def on_device(
    tokens,
    cotangent,
    block_map,
    attn_gain,
    query_weight,
    key_weight,
    value_weight,
    query_gain,
    key_gain,
    output_weight,
    mlp_gain,
    gate_weight,
    up_weight,
    down_weight,
):
    grid = Grid(lax.axis_size("ctx"), lax.axis_size("fsdp"))
    total = lax.axis_size("ctx") * lax.axis_size("fsdp")
    groups, rows, width = tokens.shape
    pairs = block_map.shape[1] // 2
    ratio = H // KVH
    low = jnp.bfloat16

    device = lax.axis_index("ctx") * lax.axis_size("fsdp") + lax.axis_index("fsdp")
    gain_pieces = [
        (at, x.shape[0])
        for at, x in ((0, attn_gain), (width, mlp_gain), (2 * width, query_gain), (2 * width + HD, key_gain))
    ]
    gain_lines = jnp.concatenate(
        [
            jnp.pad(x.astype(jnp.float32).reshape(1, -1), ((0, 0), (0, 128 - x.shape[0])))
            for x in (attn_gain, mlp_gain, query_gain, key_gain)
        ]
    )
    hidden_width = gate_weight.shape[1]

    place = lax.axis_index("ctx")
    blocks = block_map.reshape(-1)
    own_blocks = lax.dynamic_slice_in_dim(blocks, 2 * place, 2, 0)
    spots = (own_blocks[:, None] * BLK + jnp.arange(BLK, dtype=jnp.int32)).reshape(rows)
    cosine, sine = rope_tables(spots)
    turned = jnp.concatenate([-sine[:, : HD // 2], sine[:, HD // 2 :]], axis=1)
    half_q, half_k = H * HD // 2, KVH * HD // 2
    half = half_q + 2 * half_k
    plan = (
        (
            ("gains", 0, 128, FAB + CORE),
            ("q", 0, half_q, FAB + CORE),
            ("q", half_q, 2 * half_q, FBA + CORE),
            ("k", 0, 2 * half_k, BFA + CORE),
            ("v", 0, 2 * half_k, AFB + CORE),
        ),
        (
            ("o", 0, width // 2, FAB + CORE),
            ("o", width // 2, width, FBA + CORE),
            ("g", 0, hidden_width, BFA + CORE),
            ("u", 0, hidden_width, AFB + CORE),
            ("d", 0, width // 2, ABF + CORE),
            ("d", width // 2, width, BFA + CORE),
        ),
    )
    (
        full_qkv,
        full_output,
        full_gu,
        full_down,
        key_all,
        value_all,
        normed,
        gains,
        raw,
        query_low,
        inverse_one,
    ) = front(
        Pairs(lax.axis_size("ctx"), lax.axis_size("fsdp")),
        plan,
        gain_pieces,
        (query_weight, key_weight, value_weight, output_weight, gate_weight, up_weight, down_weight),
        gain_lines,
        tokens.reshape(rows, width),
        cosine,
        turned,
    )
    attended, attended_low, over_totals = attention(blocks, pairs, query_low, key_all, value_all)
    lanes = width // 128
    gain_one = gains[:lanes].reshape(-1)
    query_scale, key_scale = gains[2 * lanes], gains[2 * lanes + 1]
    inverse_rows = inverse_one
    inverse_one = inverse_one[:, :1]
    inputs = tokens.reshape(rows, width).astype(jnp.float32)
    normal_one = inputs * inverse_one
    cosine = cosine.reshape(rows, 1, HD)
    sine = sine.reshape(rows, 1, HD)
    query_raw = raw[:, : H * HD].reshape(rows, H, HD)
    key_raw = raw[:, H * HD :].reshape(rows, KVH, HD)
    query_inverse = lax.rsqrt(jnp.mean(query_raw * query_raw, axis=-1, keepdims=True) + EPSILON)
    query_unit = query_raw * query_inverse
    key_inverse = lax.rsqrt(jnp.mean(key_raw * key_raw, axis=-1, keepdims=True) + EPSILON)
    key_unit = key_raw * key_inverse
    upstream = cotangent.reshape(rows, width)
    (
        output,
        hidden,
        grad_gate,
        grad_upper,
        normed_two,
        grad_middle,
        branch_grad,
        grad_gain_two,
        grad_summed,
    ) = middle_part(
        attended_low, over_totals, full_output, full_gu, full_down, tokens.reshape(rows, width), upstream, gains
    )
    output = output.reshape(groups, rows, width)
    grad_gain_two = grad_gain_two.reshape(width)
    normed_other, upstream_other = swapped(normed_two), swapped(upstream)
    (grad_down,) = chip_sums(hidden, swapped(hidden), upstream, upstream_other)
    grad_g, grad_u = chip_sums(
        normed_two, normed_other, grad_gate, swapped(grad_gate), grad_upper, swapped(grad_upper)
    )
    (grad_woutput,) = chip_sums(attended_low, swapped(attended_low), branch_grad, swapped(branch_grad))
    grad_query, grad_keys, grad_values = attention_back(
        blocks, pairs, query_low, key_all, value_all, grad_summed, attended
    )
    back_plan = (
        (("d", 0, width // 2, ABF), ("d", width // 2, width, BAF)),
        (
            (("g", 0, hidden_width // 2, FAB), ("g", hidden_width // 2, hidden_width, FBA)),
            (("u", 0, hidden_width // 2, FAB), ("u", hidden_width // 2, hidden_width, FBA)),
            (("o", 0, width // 2, FAB), ("o", width // 2, width, FBA)),
        ),
        (
            ("q", 0, 0, half_q, ABF),
            ("q", 0, half_q, 2 * half_q, BAF),
            ("k", H * HD, 0, 2 * half_k, FAB),
            ("v", (H + KVH) * HD, 0, 2 * half_k, FBA),
        ),
    )
    if back_fits(grid, back_plan, rows, width, hidden_width, total):
        out_g, out_u, out_down, out_output, out_q, out_k, out_v, grad_tokens, gain_sums, _ = back(
            grid,
            back_plan,
            (grad_g, grad_u, grad_down, grad_woutput),
            grad_keys,
            grad_values,
            full_qkv,
            grad_query,
            raw,
            cosine.reshape(rows, HD),
            turned,
            gains,
            normed,
            tokens.reshape(rows, width),
            inverse_rows,
            grad_middle,
            grad_gain_two.reshape(lanes, 128),
        )
        (
            out_g,
            out_u,
            out_down,
            out_output,
            out_q,
            out_k,
            out_v,
            grad_tokens,
            *own_gains,
        ) = handed(
            gain_pieces, gain_sums, out_g, out_u, out_down, out_output, out_q, out_k, out_v, grad_tokens
        )
        own_attn, own_mlp, own_query, own_key = [x.reshape(-1) for x in own_gains]
        return (
            output,
            grad_tokens.reshape(groups, rows, width),
            own_attn,
            out_q,
            out_k,
            out_v,
            own_query,
            own_key,
            out_output,
            own_mlp,
            out_g,
            out_u,
            out_down,
        )
    f32 = jnp.float32
    own_keys, own_values, out_g, out_u, out_down, out_output = scatter(
        grid,
        [SLOT_AXES] * 2 + [CHIP_AXES] * 4,
        [
            (0, 0, KVH * HD, AB),
            (1, 0, KVH * HD, BA),
            (2, 0, hidden_width, BFA),
            (3, 0, hidden_width, AFB),
            (4, 0, width // 2, BFA),
            (4, width // 2, width, AFB),
            (5, 0, width // 2, BFA),
            (5, width // 2, width, AFB),
        ],
        "scatter_mlp",
        (f32, low, f32, f32, f32, f32),
        grad_keys,
        grad_values,
        grad_g,
        grad_u,
        grad_down,
        grad_woutput,
    )
    grad_qrot = grad_query.reshape(rows, H, HD)
    grad_qnormed = grad_qrot * cosine + unrotate(grad_qrot) * sine
    grad_qscale = jnp.sum(grad_qnormed * query_unit, axis=(0, 1))
    grad_qraw = norm_back(grad_qnormed, query_unit, query_inverse, query_scale)
    grad_krot = own_keys.reshape(rows, KVH, HD)
    grad_knormed = grad_krot * cosine + unrotate(grad_krot) * sine
    grad_kscale = jnp.sum(grad_knormed * key_unit, axis=(0, 1))
    grad_kraw = norm_back(grad_knormed, key_unit, key_inverse, key_scale)
    grad_raw = jnp.concatenate(
        [
            grad_qraw.reshape(rows, H * HD).astype(low),
            grad_kraw.reshape(rows, KVH * HD).astype(low),
            own_values,
        ],
        axis=1,
    )
    (grad_wqkv,) = chip_sums(normed, swapped(normed), grad_raw, swapped(grad_raw))
    grad_normed = right_dot(grad_raw, full_qkv)
    grad_gain_one = jnp.sum(grad_normed * normal_one, axis=0)
    grad_inputs = grad_middle + norm_back(grad_normed, normal_one, inverse_one, gain_one)
    out_qkv, out_gains = scatter(
        grid,
        [CHIP_AXES, ALL_AXES],
        [
            (0, 0, half // 2, FAB),
            (0, half // 2, half, FBA),
            (0, half, 3 * half // 2, BFA),
            (0, 3 * half // 2, 2 * half, AFB),
            (1, 0, 128, FAB + CORE),
        ],
        "scatter_attention",
        (f32, f32),
        grad_wqkv,
        gain_rows(total, grad_gain_one, grad_qscale, grad_kscale, grad_gain_two),
    )
    return (
        output,
        grad_inputs.astype(low).reshape(groups, rows, width),
        out_gains[0, : attn_gain.shape[0]],
        out_qkv[:, : H * HD],
        out_qkv[:, H * HD : (H + KVH) * HD],
        out_qkv[:, (H + KVH) * HD :],
        out_gains[1, : query_gain.shape[0]],
        out_gains[2, : key_gain.shape[0]],
        out_output,
        out_gains[3, : mlp_gain.shape[0]],
        out_g,
        out_u,
        out_down,
    )


def solution(mesh):
    return jax.shard_map(
        on_device,
        mesh=mesh,
        in_specs=(
            P("fsdp", "ctx", None),
            P("fsdp", "ctx", None),
            P("fsdp", None),
            P(("ctx", "fsdp")),
            P(("ctx", "fsdp"), None),
            P(("ctx", "fsdp"), None),
            P(("ctx", "fsdp"), None),
            P(("ctx", "fsdp")),
            P(("ctx", "fsdp")),
            P(("ctx", "fsdp"), None),
            P(("ctx", "fsdp")),
            P(("ctx", "fsdp"), None),
            P(("ctx", "fsdp"), None),
            P(("ctx", "fsdp"), None),
        ),
        out_specs=(
            P("fsdp", "ctx", None),
            P("fsdp", "ctx", None),
            P(("ctx", "fsdp")),
            P(("ctx", "fsdp"), None),
            P(("ctx", "fsdp"), None),
            P(("ctx", "fsdp"), None),
            P(("ctx", "fsdp")),
            P(("ctx", "fsdp")),
            P(("ctx", "fsdp"), None),
            P(("ctx", "fsdp")),
            P(("ctx", "fsdp"), None),
            P(("ctx", "fsdp"), None),
            P(("ctx", "fsdp"), None),
        ),
        check_vma=False,
    )
```
